32 devices in a mesh: seq: 4 (over y, x), fsdp: 8 (over z, core).
Axes of the slice: x: 2, y: 2, z: 4, core: 2. Of those that a mesh axis runs over, the one named last changes fastest.
Arguments:
- tokens: bfloat16 [8, 1024, 1536], P('fsdp', 'seq'), may hold values from -6 to 6
- input_projection_weight: bfloat16 [1536, 6448], P('fsdp'), may hold values from -0.15625 to 0.15625
- pre_gain: bfloat16 [1536], P('fsdp'), may hold values from 0.25 to 1.75
- conv_weight: bfloat16 [3328, 4], P('fsdp'), may hold values from -3 to 3
- conv_bias: bfloat16 [3328], P('fsdp'), may hold values from -0.5 to 0.5
- step_bias: bfloat16 [48], P('fsdp'), may hold values from -6 to -1
- decay_log: bfloat16 [48], P('fsdp'), may hold values from 0 to 2.765625
- skip_gain: bfloat16 [48], P('fsdp'), may hold values from 0.5 to 1.5
- post_gain: bfloat16 [3072], P('fsdp'), may hold values from 0.25 to 1.75
- output_projection_weight: bfloat16 [3072, 1536], P(None, 'fsdp'), may hold values from -0.109375 to 0.109375
- cotangent: bfloat16 [8, 1024, 1536], P('fsdp', 'seq'), may hold values from -6 to 6
Outputs:
- block_out: float32 [8, 1024, 1536], P('fsdp', 'seq')
- grad_tokens: float32 [8, 1024, 1536], P('fsdp', 'seq')
- grad_in_weight: float32 [1536, 6448], P('fsdp')
- grad_pre_gain: float32 [1536], P('fsdp')
- grad_conv_weight: float32 [3328, 4], P('fsdp')
- grad_conv_bias: float32 [3328], P('fsdp')
- grad_step_bias: float32 [48], P('fsdp')
- grad_decay_log: float32 [48], P('fsdp')
- grad_skip_gain: float32 [48], P('fsdp')
- grad_post_gain: float32 [3072], P('fsdp')
- grad_out_weight: float32 [3072, 1536], P(None, 'fsdp')
The draws below stay inside these ranges and needn't reach their ends.
All inputs are finite; a program needn't handle non-finite values.
Results may differ from the reference program's by a relative error of at most 0.012.
The reference program's roundings to bfloat16 on the way count: a program that leaves them out, or rounds other values in their place, can miss the bound.
Values may be sent and summed in bfloat16 or wider, within the bound.
A program may use at most 256 MiB of HBM per device.

```python
import jax
import jax.numpy as jnp
from jax import lax

D = 1536
INNER = 3072
STATE = 128
CONV = 4
BLOCK = 256
LEN = 1024
SEQ_GRP = 1
HEADS = 48
SEQS = 8
XBC = 3328
PROJ = 6448
N_FSDP = 8


def level_of(key, shape, cuts, smallest, top_value):
    level = 1.0
    for axis_at, shards_of in cuts:
        steps = jax.random.uniform(jax.random.fold_in(jax.random.fold_in(key, 6), axis_at), (shards_of,), jnp.float32, smallest / len(cuts), top_value / len(cuts))
        level = level * jnp.repeat(jnp.exp(steps), shape[axis_at] // shards_of).reshape((-1,) + (1,) * (len(shape) - 1 - axis_at))
    return level


def gaussian(rng, dims, deviation, limit, split=(), held_as=jnp.bfloat16):
    factor_of = level_of(rng, dims, split, -0.22, 0.18) if split else 1.0
    drawn = jax.random.normal(rng, dims, jnp.float32) * deviation * factor_of
    return jnp.minimum(jnp.maximum(drawn, -limit), limit).astype(held_as)


def setup_inputs(seed: int = 0) -> dict:
    seeds = jax.random.split(jax.random.key(seed), 12)
    return {
        "tokens": gaussian(seeds[0], (SEQS, LEN, D), 1.0, 6.0, ((0, 8), (1, 4))),
        "input_projection_weight": gaussian(seeds[1], (D, PROJ), D ** -0.5, 0.15625, ((0, 8),)),
        "pre_gain": jnp.clip(1.0 + 0.15 * jax.random.normal(seeds[2], (D,), jnp.float32), 0.25, 1.75).astype(jnp.bfloat16),
        "conv_weight": gaussian(seeds[3], (XBC, CONV), CONV ** -0.5, 3.0, ((0, 8),)),
        "conv_bias": jnp.clip(jax.random.uniform(seeds[4], (XBC,), jnp.float32, -0.5, 0.5) * level_of(seeds[4], (XBC,), ((0, 8),), -0.4, 0.0), -0.5, 0.5).astype(jnp.bfloat16),
        "step_bias": jnp.clip(-6.0 + 5.0 * jax.random.uniform(seeds[5], (HEADS,), jnp.float32) ** level_of(seeds[5], (HEADS,), ((0, 8),), -0.2, 0.2), -6.0, -1.0).astype(jnp.bfloat16),
        "decay_log": jnp.clip(2.765625 * jax.random.uniform(seeds[6], (HEADS,), jnp.float32) ** level_of(seeds[6], (HEADS,), ((0, 8),), -0.2, 0.2), 0.0, 2.765625).astype(jnp.bfloat16),
        "skip_gain": jnp.clip(0.5 + 1.0 * jax.random.uniform(seeds[7], (HEADS,), jnp.float32) ** level_of(seeds[7], (HEADS,), ((0, 8),), -0.2, 0.2), 0.5, 1.5).astype(jnp.bfloat16),
        "post_gain": jnp.clip(1.0 + 0.15 * jax.random.normal(seeds[8], (INNER,), jnp.float32), 0.25, 1.75).astype(jnp.bfloat16),
        "output_projection_weight": gaussian(seeds[9], (INNER, D), INNER ** -0.5, 0.109375, ((1, 8),)),
        "cotangent": gaussian(seeds[10], (SEQS, LEN, D), 1.0, 6.0, ((0, 8), (1, 4))),
    }


EPS = 1e-05
HIGH_PRECISION = lax.Precision.HIGHEST

@jax.custom_vjp
def low(v):
    return lax.optimization_barrier(v.astype(jnp.bfloat16)).astype(jnp.float32)

@jax.custom_vjp
def low_back(v):
    return v

def low_keep(v):
    return (low(v), None)

def low_pass(kept, grad):
    return (grad,)

def back_keep(v):
    return (v, None)

def back_low(kept, grad):
    return (low(grad),)
low.defvjp(low_keep, low_pass)
low_back.defvjp(back_keep, back_low)

def rms_scale(values, gain):
    return values * lax.rsqrt(lax.optimization_barrier(jnp.mean(values * values, axis=-1, keepdims=True)) + EPS) * gain

def conv_silu(signal, kernel, offset):
    tap_count = kernel.shape[1]
    length = signal.shape[1]
    padded = jnp.pad(signal, ((0, 0), (tap_count - 1, 0), (0, 0)))
    summed = offset + jnp.zeros_like(signal)
    for tap_index in range(tap_count):
        summed = summed + padded[:, tap_index:tap_index + length, :] * kernel[:, tap_index]
    return jax.nn.silu(summed)

def block_scan(values, rates, rate_scale, in_map, out_map, block_len):
    seq_count, length, head_count, head_width = values.shape
    block_count = length // block_len
    state_width = in_map.shape[-1]
    val_blocks = values.reshape(seq_count, block_count, block_len, head_count, head_width)
    rate_blocks = rates.reshape(seq_count, block_count, block_len, head_count)
    in_blocks = in_map.reshape(seq_count, block_count, block_len, state_width)
    out_blocks = out_map.reshape(seq_count, block_count, block_len, state_width)
    log_decay = jnp.cumsum(rate_blocks * rate_scale, axis=2)
    affinity = jnp.einsum('bcqn,bcsn->bcqs', out_blocks, in_blocks, precision=HIGH_PRECISION)
    positions = jnp.arange(block_len)
    causal = (positions[:, None] >= positions[None, :])[:, :, None]
    gap_log = log_decay[:, :, :, None, :] - log_decay[:, :, None, :, :]
    within = jnp.where(causal, jnp.exp(jnp.where(causal, gap_log, 0.0)), 0.0)
    mixing = affinity[..., None] * within * rate_blocks[:, :, None, :, :]
    local_out = jnp.einsum('bctsh,bcshp->bcthp', mixing, val_blocks, precision=HIGH_PRECISION)
    last_log = log_decay[:, :, -1, :]
    tail_weight = jnp.exp(last_log[:, :, None, :] - log_decay) * rate_blocks
    states = jnp.einsum('bcsh,bcsn,bcshp->bchpn', tail_weight, in_blocks, val_blocks, precision=HIGH_PRECISION)
    through = jnp.cumsum(last_log, axis=1)
    before = through - last_log
    block_ids = jnp.arange(block_count)
    earlier = (block_ids[:, None] > block_ids[None, :])[:, :, None]
    block_gap = before[:, :, None, :] - through[:, None, :, :]
    carry_weight = jnp.where(earlier, jnp.exp(jnp.where(earlier, block_gap, 0.0)), 0.0)
    entering = jnp.einsum('bcdh,bdhpn->bchpn', carry_weight, states, precision=HIGH_PRECISION)
    carried = jnp.einsum('bcqn,bchpn->bcqhp', out_blocks, entering, precision=HIGH_PRECISION) * jnp.exp(log_decay)[..., None]
    return (local_out + carried).reshape(seq_count, length, head_count, head_width)

def head_block(value_raw, state_raw, rate_raw, kernel_value, offset_value, kernel_state, offset_state, step_bias, decay_log, skip_gain, block_len):
    values = conv_silu(value_raw, kernel_value, offset_value)
    state_maps = conv_silu(state_raw, kernel_state, offset_state)
    state_width = state_raw.shape[-1] // 2
    rates = jax.nn.softplus(rate_raw + step_bias)
    head_count = rates.shape[-1]
    head_values = values.reshape(values.shape[0], values.shape[1], head_count, -1)
    mixed = block_scan(head_values, rates, -jnp.exp(decay_log), state_maps[..., :state_width], state_maps[..., state_width:], block_len)
    mixed = mixed + skip_gain[:, None] * head_values
    return mixed.reshape(values.shape)

def forward(tokens, input_projection_weight, pre_gain, conv_weight, conv_bias, step_bias, decay_log, skip_gain, post_gain, output_projection_weight):
    normalized_tokens = low(rms_scale(tokens, pre_gain))
    projected_rows = jnp.einsum('ner,ra->nea', normalized_tokens, input_projection_weight, precision=HIGH_PRECISION)
    projected_rows = low(low_back(projected_rows))
    gate_raw = projected_rows[..., :INNER]
    value_raw = projected_rows[..., INNER:2 * INNER]
    state_raw = projected_rows[..., 2 * INNER:2 * INNER + 2 * STATE]
    rate_raw = projected_rows[..., 2 * INNER + 2 * STATE:]

    def one_sequence(pieces):
        return head_block(pieces[0][None], pieces[1][None], pieces[2][None], conv_weight[:INNER], conv_bias[:INNER], conv_weight[INNER:], conv_bias[INNER:], step_bias, decay_log, skip_gain, BLOCK)[0]
    mixed = lax.map(jax.checkpoint(one_sequence), (value_raw, state_raw, rate_raw))
    mixed = low(low_back(mixed))
    reshaped_rows = low(rms_scale(mixed * jax.nn.silu(gate_raw), post_gain))
    return tokens + jnp.einsum('vip,pm->vim', reshaped_rows, output_projection_weight, precision=HIGH_PRECISION)

def reference(tokens, input_projection_weight, pre_gain, conv_weight, conv_bias, step_bias, decay_log, skip_gain, post_gain, output_projection_weight, cotangent):
    params = (input_projection_weight.astype(jnp.float32), pre_gain.astype(jnp.float32), conv_weight.astype(jnp.float32), conv_bias.astype(jnp.float32), step_bias.astype(jnp.float32), decay_log.astype(jnp.float32), skip_gain.astype(jnp.float32), post_gain.astype(jnp.float32), output_projection_weight.astype(jnp.float32))
    groups = tokens.astype(jnp.float32).reshape(N_FSDP, SEQ_GRP, LEN, D)
    cot_groups = cotangent.astype(jnp.float32).reshape(N_FSDP, SEQ_GRP, LEN, D)

    def group_step(summed, inputs):
        group_tokens, group_cot = inputs
        result, pullback = jax.vjp(forward, group_tokens, *params)
        grads = pullback(group_cot)
        summed = tuple((left + right for left, right in zip(summed, grads[1:])))
        return (summed, (result, grads[0]))
    zeros_init = tuple((jnp.zeros_like(item) for item in params))
    summed, (results, grad_groups) = lax.scan(group_step, zeros_init, (groups, cot_groups))
    return (results.reshape(SEQS, LEN, D), grad_groups.reshape(SEQS, LEN, D), summed[0], summed[1], summed[2], summed[3], summed[4], summed[5], summed[6], summed[7], summed[8])
```

```python
import functools

import jax
import jax.numpy as jnp
from jax import lax
from jax.experimental import pallas as pl
from jax.experimental.pallas import tpu as pltpu
from jax.sharding import PartitionSpec as P

D = 1536
INNER = 3072
STATE = 128
HEADS = 48
XBC = INNER + 2 * STATE
EPS = 1e-05

SEQ = 4
W = INNER // SEQ
HL = HEADS // SEQ
HW = INNER // HEADS
CH = W + 2 * STATE
VC = CH + 128
Q = 128

F32 = jnp.float32
BF16 = jnp.bfloat16
MESH = pl.DeviceIdType.MESH
HIGH = lax.Precision.HIGHEST
VMEM = pl.BlockSpec(memory_space=pltpu.VMEM)
ANY = pl.BlockSpec(memory_space=pl.ANY)
VMEM_LIMIT = 64000 * 1024


def rcopy(src, dst, send_sem, recv_sem, device):
    return pltpu.make_async_remote_copy(
        src_ref=src, dst_ref=dst, send_sem=send_sem, recv_sem=recv_sem, device_id=device, device_id_type=MESH
    )


def signal(sem, device):
    pl.semaphore_signal(sem, inc=1, device_id=device, device_id_type=MESH)


def nn(a, b, precision=None):
    return lax.dot_general(a, b, (((1,), (0,)), ((), ())), precision=precision, preferred_element_type=F32)


def nt(a, b, precision=None):
    return lax.dot_general(a, b, (((1,), (1,)), ((), ())), precision=precision, preferred_element_type=F32)


def seq_gather_start(refs, outs, send, recv, px, py, me):
    for g, (src, out) in enumerate(zip(refs, outs)):
        n = src.shape[0]
        own = out.at[pl.ds(me * n, n)]
        rcopy(src, own, send.at[g, 0], recv.at[g, 0], {"seq": px}).start()
        rcopy(src, own, send.at[g, 1], recv.at[g, 1], {"seq": py}).start()


def seq_gather_relay(g, src, out, send, recv, px, py, me):
    n = src.shape[0]
    h = n // 2
    own = out.at[pl.ds(me * n, n)]
    rcopy(src, own, send.at[g, 0], recv.at[g, 0], {"seq": px}).wait_recv()
    top = out.at[pl.ds(px * n, h)]
    rcopy(top, top, send.at[g, 2], recv.at[g, 2], {"seq": py}).start()
    rcopy(src, own, send.at[g, 1], recv.at[g, 1], {"seq": py}).wait_recv()
    low = out.at[pl.ds(py * n + h, h)]
    rcopy(low, low, send.at[g, 3], recv.at[g, 3], {"seq": px}).start()


def seq_gather_finish(g, src, out, send, recv, px, py, me):
    n = src.shape[0]
    h = n // 2
    own = out.at[pl.ds(me * n, n)]
    half = out.at[pl.ds(me * n, h)]
    rcopy(half, half, send.at[g, 2], recv.at[g, 2], {"seq": py}).wait()
    rcopy(half, half, send.at[g, 3], recv.at[g, 3], {"seq": px}).wait()
    rcopy(src, own, send.at[g, 0], recv.at[g, 0], {"seq": px}).wait_send()
    rcopy(src, own, send.at[g, 1], recv.at[g, 1], {"seq": py}).wait_send()


def gather_kernel(nf, tok, cot, w0, w1, w2, small, tok_all, cot_all, g0, g1, g2, small_all, xs, xr, zs, zr, ms, mr, ls):
    s = lax.axis_index("seq")
    f = lax.axis_index("fsdp")
    px, py = s ^ 1, s ^ 2
    nl = nf // 2
    p, c = f // 2, f % 2
    partner = p * 2 + 1 - c
    bar = pltpu.get_barrier_semaphore()
    signal(bar, {"seq": px})
    signal(bar, {"seq": py})
    for k in range(1, nf):
        signal(bar, {"fsdp": lax.rem(f + k, nf)})
    pl.semaphore_wait(bar, nf + 1)

    ns = small.shape[0]
    own_small = small_all.at[pl.ds(f * ns, ns)]
    for k in range(1, nf):
        rcopy(small, own_small, ms.at[k], mr.at[k], {"fsdp": lax.rem(f + k, nf)}).start()
    seq_gather_start((tok, cot), (tok_all, cot_all), xs, xr, px, py, s)

    ins, outs = (w0, w1, w2), (g0, g1, g2)
    n = w0.shape[0]

    def row(g, i):
        return outs[g].at[pl.ds(i * n, n)]

    def hop(g, src, i, way, k, device):
        return rcopy(src, row(g, i), zs.at[g, way, k], zr.at[g, i], {"fsdp": device})

    locals_ = [
        pltpu.make_async_copy(small, own_small, ls.at[0]),
        pltpu.make_async_copy(tok, tok_all.at[pl.ds(s * tok.shape[0], tok.shape[0])], ls.at[1]),
        pltpu.make_async_copy(cot, cot_all.at[pl.ds(s * cot.shape[0], cot.shape[0])], ls.at[2]),
    ]
    for g in range(3):
        @pl.when(p < nl - 1)
        def _():
            hop(g, ins[g], f, 0, 0, f + 2).start()

        @pl.when(p > 0)
        def _():
            hop(g, ins[g], f, 1, 0, f - 2).start()

        hop(g, ins[g], f, 2, 0, partner).start()
        locals_.append(pltpu.make_async_copy(ins[g], row(g, f), ls.at[3 + g]))
    for copy in locals_:
        copy.start()
    seq_gather_relay(0, tok, tok_all, xs, xr, px, py, s)

    for g in range(3):
        for k in range(1, nl):
            @pl.when(p - k >= 0)
            def _():
                o = f - 2 * k
                hop(g, row(g, o), o, 0, k, f).wait_recv()

                @pl.when(p < nl - 1)
                def _():
                    hop(g, row(g, o), o, 0, k, f + 2).start()

                hop(g, row(g, o), o, 2, k, partner).start()

            @pl.when(p + k < nl)
            def _():
                o = f + 2 * k
                hop(g, row(g, o), o, 1, k, f).wait_recv()

                @pl.when(p > 0)
                def _():
                    hop(g, row(g, o), o, 1, k, f - 2).start()

                hop(g, row(g, o), o, 3, k, partner).start()

        if g == 1:
            seq_gather_relay(1, cot, cot_all, xs, xr, px, py, s)

    for copy in locals_:
        copy.wait()
    for k in range(1, nf):
        rcopy(small, own_small, ms.at[k], mr.at[k], {"fsdp": lax.rem(f + k, nf)}).wait()
    seq_gather_finish(0, tok, tok_all, xs, xr, px, py, s)
    seq_gather_finish(1, cot, cot_all, xs, xr, px, py, s)
    for g in range(3):
        for q in range(nl):
            o = q * 2 + 1 - c
            hop(g, row(g, o), o, 2, 0, partner).wait_recv()
        hop(g, ins[g], f, 2, 0, partner).wait_send()

        @pl.when(p < nl - 1)
        def _():
            hop(g, ins[g], f, 0, 0, f + 2).wait_send()

        @pl.when(p > 0)
        def _():
            hop(g, ins[g], f, 1, 0, f - 2).wait_send()

        for k in range(1, nl):
            @pl.when(p - k >= 0)
            def _():
                o = f - 2 * k

                @pl.when(p < nl - 1)
                def _():
                    hop(g, row(g, o), o, 0, k, f + 2).wait_send()

                hop(g, row(g, o), o, 2, k, partner).wait_send()

            @pl.when(p + k < nl)
            def _():
                o = f + 2 * k

                @pl.when(p > 0)
                def _():
                    hop(g, row(g, o), o, 1, k, f - 2).wait_send()

                hop(g, row(g, o), o, 3, k, partner).wait_send()


def gather_all(nf, tok, cot, w0, w1, w2, small):
    shape = jax.ShapeDtypeStruct
    dma = pltpu.SemaphoreType.DMA
    return pl.pallas_call(
        functools.partial(gather_kernel, nf),
        out_shape=[
            shape((SEQ * tok.shape[0], D), BF16),
            shape((SEQ * tok.shape[0], D), BF16),
            shape((nf * w0.shape[0], w0.shape[1]), BF16),
            shape((nf * w1.shape[0], w1.shape[1]), BF16),
            shape((nf * w2.shape[0], w2.shape[1]), BF16),
            shape((nf * small.shape[0], 128), F32),
        ],
        in_specs=[ANY] * 6,
        out_specs=[ANY] * 6,
        scratch_shapes=[
            dma((2, 4)),
            dma((2, 4)),
            dma((3, 4, nf // 2)),
            dma((3, nf)),
            dma((nf,)),
            dma((nf,)),
            dma((6,)),
        ],
        name="gather_all",
        compiler_params=pltpu.CompilerParams(collective_id=1, has_side_effects=True),
    )(tok, cot, w0, w1, w2, small)


def stats_kernel(a, out, got, send, recv):
    s = lax.axis_index("seq")
    bar = pltpu.get_barrier_semaphore()
    for k in range(1, SEQ):
        signal(bar, {"seq": s ^ k})
    pl.semaphore_wait(bar, SEQ - 1)
    copies = [rcopy(a, got.at[k], send.at[k], recv.at[k], {"seq": s ^ k}) for k in range(1, SEQ)]
    for copy in copies:
        copy.start()
    for copy in copies:
        copy.wait()
    out[...] = a[...] + got[1] + (got[2] + got[3])


def stats_sum(a):
    dma = pltpu.SemaphoreType.DMA
    return pl.pallas_call(
        stats_kernel,
        out_shape=jax.ShapeDtypeStruct(a.shape, F32),
        in_specs=[VMEM],
        out_specs=VMEM,
        scratch_shapes=[pltpu.VMEM((SEQ,) + a.shape, F32), dma((SEQ,)), dma((SEQ,))],
        name="stats_sum",
        compiler_params=pltpu.CompilerParams(collective_id=2, has_side_effects=True),
    )(a)


def softplus(x):
    return jnp.maximum(x, 0.0) + jnp.log1p(jnp.exp(-jnp.abs(x)))


def sigmoid(x):
    return 1.0 / (1.0 + jnp.exp(-x))


def rates_of(r_ref, rows, hp_ref, tri):
    raw = r_ref[rows, :].astype(F32) + hp_ref[0:1, :]
    dt = softplus(raw)
    lam = nn(tri, dt * hp_ref[1:2, :], HIGH)
    return raw, dt, lam


def spread(mat, h):
    return jnp.broadcast_to(mat[:, h : h + 1], (mat.shape[0], 128))


def scan_fwd_kernel(v_ref, s_ref, r_ref, kw_ref, hp_ref, ex_ref, mixed_ref, k_ref, st_ref, buf, hst, xw_s, er_s):
    blocks = v_ref.shape[0] // Q
    row = lax.broadcasted_iota(jnp.int32, (Q, Q), 0)
    col = lax.broadcasted_iota(jnp.int32, (Q, Q), 1)
    causal = row >= col
    tri = causal.astype(F32)
    low = lax.broadcasted_iota(jnp.int32, (Q, 128), 1) < HW
    low1 = lax.broadcasted_iota(jnp.int32, (1, 128), 1) < HW
    buf[0:8, :] = jnp.zeros((8, CH), F32)
    hst[...] = jnp.zeros_like(hst)

    def block(b, carry):
        rows = pl.ds(pl.multiple_of(b * Q, Q), Q)
        buf[8 : 8 + Q, 0:W] = v_ref[rows, :].astype(F32)
        buf[8 : 8 + Q, W:CH] = s_ref[rows, :].astype(F32)
        k = kw_ref[4:5, :] + buf[5 : 5 + Q, :] * kw_ref[0:1, :]
        for j in range(1, 4):
            k = k + buf[5 + j : 5 + j + Q, :] * kw_ref[j : j + 1, :]
        k_ref[rows, :] = k
        buf[0:8, :] = buf[Q : Q + 8, :]
        x = k * sigmoid(k)
        bs, cs = x[:, W : W + STATE], x[:, W + STATE :]
        _, dt, lam = rates_of(r_ref, rows, hp_ref, tri)
        lam_t, dt_t = lam.T, dt.T
        last = lam[Q - 1 : Q, :]
        tail = dt * jnp.exp(last - lam)
        aff = nt(cs, bs, HIGH)
        st_ref[b] = hst[...].astype(BF16)
        ch = nn(cs.astype(BF16), st_ref[b])
        for i in range(HL // 2):
            at = slice(128 * i, 128 * i + 128)
            xp = x[:, at]
            xb = xp.astype(BF16)
            y, lc = [], []
            for h in (2 * i, 2 * i + 1):
                lcol = spread(lam, h)
                within = jnp.exp(jnp.where(causal, lcol - lam_t[h : h + 1, :], -1e30))
                y.append(nn((aff * within * dt_t[h : h + 1, :]).astype(BF16), xb))
                lc.append(lcol)
            out = jnp.where(low, y[0], y[1])
            out = out + jnp.exp(jnp.where(low, lc[0], lc[1])) * ch[:, at] + ex_ref[0:1, at] * xp
            mixed_ref[rows, at] = out.astype(BF16)
            xw_s[:, at] = (xp * jnp.where(low, spread(tail, 2 * i), spread(tail, 2 * i + 1))).astype(BF16)
            er_s[0:1, at] = jnp.exp(jnp.where(low1, spread(last, 2 * i), spread(last, 2 * i + 1)))
        hst[...] = hst[...] * er_s[0:1, :] + nn(bs.T.astype(BF16), xw_s[...])
        return carry

    lax.fori_loop(0, blocks, block, 0)


def scan_fwd(v, s, r, kw, hp, ex):
    length = v.shape[0]
    shape = jax.ShapeDtypeStruct
    return pl.pallas_call(
        scan_fwd_kernel,
        out_shape=[shape((length, W), BF16), shape((length, CH), F32), shape((length // Q, STATE, W), BF16)],
        in_specs=[VMEM] * 6,
        out_specs=[VMEM] * 3,
        scratch_shapes=[
            pltpu.VMEM((Q + 8, CH), F32),
            pltpu.VMEM((STATE, W), F32),
            pltpu.VMEM((Q, W), BF16),
            pltpu.VMEM((8, W), F32),
        ],
        name="scan_fwd",
        compiler_params=pltpu.CompilerParams(vmem_limit_bytes=VMEM_LIMIT),
    )(v, s, r, kw, hp, ex)


def scan_bwd_kernel(
    v_ref, s_ref, r_ref, k_ref, dy_ref, st_ref, kw_ref, hp_ref, ex_ref,
    dv_ref, gcw_ref, gch_ref, ghd_ref,
    buf, dhst, rowp, xw_s, e_s, er_s,
):
    blocks = v_ref.shape[0] // Q
    row = lax.broadcasted_iota(jnp.int32, (Q, Q), 0)
    col = lax.broadcasted_iota(jnp.int32, (Q, Q), 1)
    tri = (row >= col).astype(F32)
    later = col >= row
    suffix = later.astype(F32)
    strict = (col < row).astype(F32)
    lane = lax.broadcasted_iota(jnp.int32, (Q, 128), 1)
    lane1 = lax.broadcasted_iota(jnp.int32, (1, 128), 1)
    low = lane < HW
    low1 = lane1 < HW
    buf[Q : Q + 8, :] = jnp.zeros((8, CH), F32)
    dhst[...] = jnp.zeros_like(dhst)
    rowp[...] = jnp.zeros_like(rowp)
    gcw_ref[...] = jnp.zeros_like(gcw_ref)
    gch_ref[...] = jnp.zeros_like(gch_ref)
    ghd_ref[...] = jnp.zeros_like(ghd_ref)

    def block(i0, carry):
        b = blocks - 1 - i0
        rows = pl.ds(pl.multiple_of(b * Q, Q), Q)
        k = k_ref[rows, :]
        sg = sigmoid(k)
        x = k * sg
        ds = sg * (1.0 + k * (1.0 - sg))
        bs, cs = x[:, W : W + STATE], x[:, W + STATE :]
        bb, cb = bs.astype(BF16), cs.astype(BF16)
        raw, dt, lam = rates_of(r_ref, rows, hp_ref, tri)
        lam_t = lam.T
        last = lam[Q - 1 : Q, :]
        aff_t = nt(bs, cs, HIGH)
        hb = st_ref[b]
        dhb = dhst[...].astype(BF16)
        ch = nn(cb, hb)
        bd = nn(bb, dhb)
        daff_t = jnp.zeros((Q, Q), F32)
        col_n = jnp.zeros((Q, 128), F32)
        col_i = jnp.zeros((Q, 128), F32)
        row_i = jnp.zeros((Q, 128), F32)
        through = jnp.zeros((1, 128), F32)
        for i in range(HL // 2):
            at = slice(128 * i, 128 * i + 128)
            xp = x[:, at]
            xb = xp.astype(BF16)
            dyb = dy_ref[rows, at]
            dyf = dyb.astype(F32)
            z, lc, dc = [], [], []
            for h in (2 * i, 2 * i + 1):
                mine = low if h % 2 == 0 else jnp.logical_not(low)
                lcol, dcol = spread(lam, h), spread(dt, h)
                within = jnp.exp(jnp.where(later, lam_t[h : h + 1, :] - lcol, -1e30))
                g = nt(jnp.where(mine, xp, 0.0).astype(BF16), dyb)
                lg = within * g
                lgd = lg * dcol
                daff_t = daff_t + lgd
                col_n = jnp.where(lane == h, jnp.sum(aff_t * lg, axis=1, keepdims=True), col_n)
                rowp[h : h + 1, :] = jnp.sum(aff_t * lgd, axis=0, keepdims=True)
                z.append(nn((aff_t * within).astype(BF16), dyb))
                lc.append(lcol)
                dc.append(dcol)
            lamp = jnp.where(low, lc[0], lc[1])
            dtp = jnp.where(low, dc[0], dc[1])
            lastp = jnp.where(low1, spread(last, 2 * i), spread(last, 2 * i + 1))
            e = dyf * jnp.exp(lamp)
            e_s[:, at] = e.astype(BF16)
            ew = jnp.exp(lastp - lamp)
            bdp = bd[:, at]
            xw_s[:, at] = (xp * (dtp * ew)).astype(BF16)
            er_s[0:1, at] = jnp.exp(lastp)
            re = e * ch[:, at]
            ci = xp * bdp * ew
            th = jnp.sum(dhst[:, at] * hb[:, at].astype(F32), axis=0, keepdims=True) * er_s[0:1, at]
            for h in (2 * i, 2 * i + 1):
                mine = low if h % 2 == 0 else jnp.logical_not(low)
                mine1 = low1 if h % 2 == 0 else jnp.logical_not(low1)
                row_i = jnp.where(lane == h, jnp.sum(jnp.where(mine, re, 0.0), axis=1, keepdims=True), row_i)
                col_i = jnp.where(lane == h, jnp.sum(jnp.where(mine, ci, 0.0), axis=1, keepdims=True), col_i)
                through = jnp.where(
                    lane1 == h, jnp.sum(jnp.where(mine1, th, 0.0), axis=1, keepdims=True), through
                )
            dx = dtp * jnp.where(low, z[0], z[1]) + bdp * (dtp * ew) + ex_ref[0:1, at] * dyf
            gch_ref[0:1, at] += jnp.sum(dyf * xp, axis=0, keepdims=True)
            buf[0:Q, at] = dx * ds[:, at]
        daff_b = daff_t.astype(BF16)
        d_bs = nt(xw_s[...], dhb) + nn(daff_b, cb)
        d_cs = nt(e_s[...], hb) + nn(daff_t.T.astype(BF16), bb)
        buf[0:Q, W : W + STATE] = d_bs * ds[:, W : W + STATE]
        buf[0:Q, W + STATE : CH] = d_cs * ds[:, W + STATE :]
        dhst[...] = dhst[...] * er_s[0:1, :] + nn(cs.T.astype(BF16), e_s[...])
        after = nn(suffix, rowp[...].T - dt * col_n + row_i, HIGH) + nn(strict, dt * col_i, HIGH) + through
        d_rate = (col_n + col_i + hp_ref[1:2, :] * after) * sigmoid(raw)
        ghd_ref[0:1, :] += jnp.sum(d_rate, axis=0, keepdims=True)
        ghd_ref[1:2, :] += jnp.sum(dt * after, axis=0, keepdims=True) * hp_ref[1:2, :]
        dv_ref[rows, CH:VC] = d_rate.astype(BF16)
        for at, ref in ((slice(0, W), v_ref), (slice(W, CH), s_ref)):
            raw_v = ref[rows, :].astype(F32)
            dk = buf[0:Q, at]
            dv = dk * kw_ref[3:4, at]
            gcw_ref[4:5, at] += jnp.sum(dk, axis=0, keepdims=True)
            gcw_ref[3:4, at] += jnp.sum(dk * raw_v, axis=0, keepdims=True)
            for j in range(3):
                dk = buf[3 - j : 3 - j + Q, at]
                dv = dv + dk * kw_ref[j : j + 1, at]
                gcw_ref[j : j + 1, at] += jnp.sum(dk * raw_v, axis=0, keepdims=True)
            dv_ref[rows, at] = dv.astype(BF16)
        buf[Q : Q + 8, :] = buf[0:8, :]
        return carry

    lax.fori_loop(0, blocks, block, 0)


def scan_bwd(v, s, r, k, dy, st, kw, hp, ex):
    length = v.shape[0]
    shape = jax.ShapeDtypeStruct
    return pl.pallas_call(
        scan_bwd_kernel,
        out_shape=[shape((length, VC), BF16), shape((8, CH), F32), shape((8, W), F32), shape((8, 128), F32)],
        in_specs=[VMEM] * 9,
        out_specs=[VMEM] * 4,
        scratch_shapes=[
            pltpu.VMEM((Q + 8, CH), F32),
            pltpu.VMEM((STATE, W), F32),
            pltpu.VMEM((128, Q), F32),
            pltpu.VMEM((Q, W), BF16),
            pltpu.VMEM((Q, W), BF16),
            pltpu.VMEM((8, W), F32),
        ],
        name="scan_bwd",
        compiler_params=pltpu.CompilerParams(vmem_limit_bytes=VMEM_LIMIT),
    )(v, s, r, k, dy, st, kw, hp, ex)


def reduce_kernel(nf, *refs):
    ins, outs = refs[:6], refs[6:12]
    pb, ub, db, cs, own = refs[12:16], refs[16:20], refs[20:24], refs[24:28], refs[28:32]
    ab, az = refs[32:34], refs[34:36]
    zs, zr, xs, xr, as_, ar, ls = refs[36:]
    s = lax.axis_index("seq")
    f = lax.axis_index("fsdp")
    px, py = s ^ 1, s ^ 2
    nl = nf // 2
    p, c = f // 2, f % 2
    partner = p * 2 + 1 - c
    bar = pltpu.get_barrier_semaphore()
    signal(bar, {"seq": px})
    signal(bar, {"seq": py})
    signal(bar, {"fsdp": partner})

    @pl.when(p < nl - 1)
    def _():
        signal(bar, {"fsdp": f + 2})

    @pl.when(p > 0)
    def _():
        signal(bar, {"fsdp": f - 2})

    pl.semaphore_wait(bar, 3 + jnp.where(p < nl - 1, 1, 0) + jnp.where(p > 0, 1, 0))

    rows = ins[4].shape[0] // SEQ
    half = D // 2
    cols = (slice(0, half), slice(half, D))
    first, second = (px, py), (py, px)

    def chunk(ref, i, a):
        return ref.at[pl.ds(i * rows, rows), cols[a]]

    def seq_one(t, a, m):
        i = (first[a] ^ second[a] ^ s) if m == 0 else first[a]
        return rcopy(
            chunk(ins[4 + t], i, a), ab[t].at[a, m], xs.at[t, a, m], xr.at[t, a, m], {"seq": first[a]}
        )

    def seq_two(t, a):
        return rcopy(az[t].at[a, 0], az[t].at[a, 1], xs.at[t, a, 2], xr.at[t, a, 2], {"seq": second[a]})

    shard = [ins[g].shape[0] // nf for g in range(4)]

    def piece(g, i):
        return ins[g].at[pl.ds(i * shard[g], shard[g])]

    def swap(g, q):
        return rcopy(piece(g, q * 2 + 1 - c), pb[g].at[q], zs.at[g, 0, q], zr.at[g, 0, q], {"fsdp": partner})

    def up(g, q):
        return rcopy(cs[g].at[q], ub[g].at[q], zs.at[g, 1, q], zr.at[g, 1, q], {"fsdp": f + 2})

    def down(g, q):
        return rcopy(cs[g].at[q], db[g].at[q], zs.at[g, 2, q], zr.at[g, 2, q], {"fsdp": f - 2})

    order = []
    for k in range(nl // 2):
        order += [nl - 1 - k, k]
    for g in range(4):
        for q in order:
            swap(g, q).start()
    for t in range(2):
        for m in range(2):
            for a in range(2):
                seq_one(t, a, m).start()

    def add(*terms):
        total = terms[0].astype(F32)
        for term in terms[1:]:
            total = total + term.astype(F32)
        return total

    def line(g):
        for q in order:
            swap(g, q).wait_recv()
            mine = piece(g, q * 2 + c)

            @pl.when(q > p)
            def _():
                @pl.when(p > 0)
                def _():
                    up(g, q).wait_recv()
                    cs[g][q] = add(mine[...], pb[g][q], ub[g][q]).astype(cs[g].dtype)

                @pl.when(p == 0)
                def _():
                    cs[g][q] = add(mine[...], pb[g][q]).astype(cs[g].dtype)

                up(g, q).start()

            @pl.when(q < p)
            def _():
                @pl.when(p < nl - 1)
                def _():
                    down(g, q).wait_recv()
                    cs[g][q] = add(mine[...], pb[g][q], db[g][q]).astype(cs[g].dtype)

                @pl.when(p == nl - 1)
                def _():
                    cs[g][q] = add(mine[...], pb[g][q]).astype(cs[g].dtype)

                down(g, q).start()

    def close(g):
        mine = piece(g, f)

        @pl.when(p > 0)
        def _():
            up(g, p).wait_recv()

        @pl.when(p < nl - 1)
        def _():
            down(g, p).wait_recv()

        @pl.when(p == 0)
        def _():
            own[g][...] = add(mine[...], pb[g][p], db[g][p]).astype(own[g].dtype)

        @pl.when(p == nl - 1)
        def _():
            own[g][...] = add(mine[...], pb[g][p], ub[g][p]).astype(own[g].dtype)

        @pl.when(jnp.logical_and(p > 0, p < nl - 1))
        def _():
            own[g][...] = add(mine[...], pb[g][p], ub[g][p], db[g][p]).astype(own[g].dtype)

    for g in range(4):
        line(g)
        if g == 1:
            for t in range(2):
                for a in range(2):
                    seq_one(t, a, 0).wait_recv()
                    az[t][a, 0] = add(chunk(ins[4 + t], second[a], a)[...], ab[t][a, 0]).astype(BF16)
                    seq_two(t, a).start()

    for g in range(4):
        close(g)
        n = shard[g]
        place = outs[g].at[pl.ds(s * n, n)]
        rcopy(own[g], place, as_.at[g, 0], ar.at[g, 0], {"seq": px}).start()
        rcopy(own[g], place, as_.at[g, 1], ar.at[g, 1], {"seq": py}).start()
        pltpu.make_async_copy(own[g], place, ls.at[g]).start()

    for t in range(2):
        for a in range(2):
            seq_one(t, a, 1).wait_recv()
            seq_two(t, a).wait_recv()
            outs[4 + t][:, cols[a]] = add(chunk(ins[4 + t], s, a)[...], ab[t][a, 1], az[t][a, 1])

    for g in range(4):
        seq_gather_relay(g, own[g], outs[g], as_, ar, px, py, s)
    for g in range(4):
        seq_gather_finish(g, own[g], outs[g], as_, ar, px, py, s)
        place = outs[g].at[pl.ds(s * shard[g], shard[g])]
        pltpu.make_async_copy(own[g], place, ls.at[g]).wait()
        for q in range(nl):
            swap(g, q).wait_send()

            @pl.when(q > p)
            def _():
                up(g, q).wait_send()

            @pl.when(q < p)
            def _():
                down(g, q).wait_send()

    for t in range(2):
        for a in range(2):
            seq_one(t, a, 0).wait_send()
            seq_one(t, a, 1).wait_send()
            seq_two(t, a).wait_send()


def reduce_all(nf, gv, gg, go, small, out_part, dn_part):
    shape = jax.ShapeDtypeStruct
    dma = pltpu.SemaphoreType.DMA
    nl = nf // 2
    groups = (small, gv, gg, go)
    rows = out_part.shape[0] // SEQ
    boxes = [((g.shape[0] // nf, g.shape[1]), g.dtype) for g in groups]
    lines = [pltpu.VMEM((nl,) + box, dtype) for box, dtype in boxes]
    return pl.pallas_call(
        functools.partial(reduce_kernel, nf),
        out_shape=[shape((SEQ * box[0], box[1]), dtype) for box, dtype in boxes] + [shape((rows, D), F32)] * 2,
        in_specs=[VMEM] * 6,
        out_specs=[VMEM] * 6,
        scratch_shapes=lines * 4
        + [pltpu.VMEM(box, dtype) for box, dtype in boxes]
        + [pltpu.VMEM((2, 2, rows, D // 2), BF16)] * 4
        + [
            dma((4, 3, nl)),
            dma((4, 3, nl)),
            dma((2, 2, 3)),
            dma((2, 2, 3)),
            dma((4, 4)),
            dma((4, 4)),
            dma((4,)),
        ],
        name="reduce_all",
        compiler_params=pltpu.CompilerParams(
            collective_id=3, has_side_effects=True, vmem_limit_bytes=VMEM_LIMIT
        ),
    )(small, gv, gg, go, out_part, dn_part)


def own_rows(array, index, row_count):
    return lax.dynamic_slice_in_dim(array, index * row_count, row_count, 0)


def pack(parts, nf):
    flat = jnp.concatenate([part.reshape(nf, -1) for part in parts], axis=1)
    rows = -(-flat.shape[1] // 1024) * 8
    flat = jnp.pad(flat, ((0, 0), (0, rows * 128 - flat.shape[1])))
    return flat.reshape(nf * rows, 128)


def unpack(packed, shapes, count):
    flat = packed.reshape(count, -1)
    out, at = [], 0
    for shape in shapes:
        size = 1
        for extent in shape:
            size *= extent
        size //= count
        out.append(flat[:, at : at + size].reshape(shape))
        at += size
    return out


def body(
    tokens,
    input_projection_weight,
    pre_gain,
    conv_weight,
    conv_bias,
    step_bias,
    decay_log,
    skip_gain,
    post_gain,
    output_projection_weight,
    cotangent,
):
    nf = lax.axis_size("fsdp")
    s = lax.axis_index("seq")
    tok = tokens.reshape(tokens.shape[1:])
    cot = cotangent.reshape(cotangent.shape[1:])
    win = input_projection_weight
    n = win.shape[0]

    w_gate = lax.dynamic_slice(win, (0, s * W), (n, W))
    w_mix = jnp.concatenate(
        [
            lax.dynamic_slice(win, (0, INNER + s * W), (n, W)),
            win[:, 2 * INNER : 2 * INNER + 2 * STATE],
            lax.dynamic_slice(win, (0, 2 * INNER + 2 * STATE + s * HL), (n, HL)),
            jnp.zeros((n, 128 - HL), BF16),
        ],
        axis=1,
    )
    w_out = own_rows(output_projection_weight, s, W).T
    small = pack(
        [
            v.astype(F32)
            for v in (pre_gain, conv_weight, conv_bias, step_bias, decay_log, skip_gain, post_gain)
        ],
        1,
    )
    tok_all, cot_all, w_mix, w_gate, w_out, small = gather_all(nf, tok, cot, w_mix, w_gate, w_out, small)
    shapes = ((D,), (XBC, 4), (XBC,), (HEADS,), (HEADS,), (HEADS,), (INNER,))
    pre, conv_w, conv_b, step_b, decay, skip, post = unpack(small, shapes, nf)
    kw = jnp.concatenate([conv_w.T, conv_b[None], jnp.zeros((3, XBC), F32)], axis=0)
    kw = jnp.concatenate([lax.dynamic_slice(kw, (0, s * W), (8, W)), kw[:, INNER:]], axis=1)
    per_head = jnp.stack([step_b, -jnp.exp(decay), skip])
    per_head = lax.dynamic_slice(per_head, (0, s * HL), (3, HL))
    hp = jnp.pad(per_head, ((0, 5), (0, 128 - HL)))
    ex = jnp.broadcast_to(jnp.repeat(per_head[2], HW)[None], (8, W))
    post = own_rows(post, s, W)

    residual = tok_all.astype(F32)
    rho0 = lax.rsqrt(jnp.mean(residual * residual, axis=-1, keepdims=True) + EPS)
    n0 = residual * rho0
    normed = (n0 * pre).astype(BF16)
    mix_raw = nn(normed, w_mix).astype(BF16)
    gate_raw = nn(normed, w_gate).astype(BF16)
    v_raw, s_raw, r_raw = mix_raw[:, :W], mix_raw[:, W:CH], mix_raw[:, CH:]
    mixed, k, st = scan_fwd(v_raw, s_raw, r_raw, kw, hp, ex)

    d_shaped = nn(cot_all, w_out)
    gate = gate_raw.astype(F32)
    mixed = mixed.astype(F32)
    sg = jax.nn.sigmoid(gate)
    sl = gate * sg
    gated = mixed * sl
    e1 = d_shaped * post
    sums = jnp.concatenate(
        [jnp.sum(gated * gated, axis=-1).reshape(-1, 128), jnp.sum(e1 * gated, axis=-1).reshape(-1, 128)]
    )
    sums = stats_sum(sums)
    half = sums.shape[0] // 2
    rho1 = lax.rsqrt(sums[:half].reshape(-1, 1) / INNER + EPS)
    mean1 = rho1 * sums[half:].reshape(-1, 1) / INNER
    n1 = gated * rho1
    shaped = (n1 * post).astype(BF16)
    g_post = jnp.sum(d_shaped * n1, axis=0)
    d_gated = rho1 * (e1 - n1 * mean1)
    d_mixed = (d_gated * sl).astype(BF16)
    d_gate = (d_gated * mixed * (sg * (1.0 + gate * (1.0 - sg)))).astype(BF16)

    out_part = nt(shaped, w_out).astype(BF16)
    tn = (((0,), (0,)), ((), ()))
    g_out = lax.dot_general(cot_all, shaped, tn, preferred_element_type=F32).astype(BF16)
    g_gate = lax.dot_general(normed, d_gate, tn, preferred_element_type=F32).astype(BF16)

    dv, g_conv, g_chan, g_head = scan_bwd(v_raw, s_raw, r_raw, k, d_mixed, st, kw, hp, ex)
    g_mix = lax.dot_general(normed, dv, tn, preferred_element_type=F32).astype(BF16)
    dn_part = nt(d_gate, w_gate) + nt(dv, w_mix)
    g_pre = jnp.sum(dn_part * n0, axis=0)

    def placed(full, piece, at):
        return lax.dynamic_update_slice_in_dim(jnp.zeros((full,) + piece.shape[1:], F32), piece, at, 0)

    g_cw = jnp.concatenate([placed(INNER, g_conv[:4, :W].T, s * W), g_conv[:4, W:].T])
    g_cb = jnp.concatenate([placed(INNER, g_conv[4, :W], s * W), g_conv[4, W:]])
    small = pack(
        [
            g_pre,
            g_cw,
            g_cb,
            placed(HEADS, g_head[0, :HL], s * HL),
            placed(HEADS, g_head[1, :HL], s * HL),
            placed(HEADS, jnp.sum(g_chan[0].reshape(HL, HW), axis=1), s * HL),
            placed(INNER, g_post, s * W),
        ],
        nf,
    )
    small, g_mix, g_gate, g_out, out_sum, dn = reduce_all(
        nf, g_mix, g_gate, g_out, small, out_part, dn_part.astype(BF16)
    )

    block_out = tok.astype(F32) + out_sum
    res = tok.astype(F32)
    r0 = lax.rsqrt(jnp.mean(res * res, axis=-1, keepdims=True) + EPS)
    m0 = res * r0
    e0 = dn * pre
    grad_tokens = cot.astype(F32) + r0 * (e0 - m0 * jnp.mean(e0 * m0, axis=-1, keepdims=True))

    g_mix = g_mix.reshape(SEQ, n, VC).astype(F32)
    g_gate = g_gate.reshape(SEQ, n, W).astype(F32)
    grad_in = jnp.concatenate(
        [g_gate[i] for i in range(SEQ)]
        + [g_mix[i, :, :W] for i in range(SEQ)]
        + [jnp.sum(g_mix[:, :, W:CH], axis=0)]
        + [g_mix[i, :, CH : CH + HL] for i in range(SEQ)],
        axis=1,
    )
    grad_out = jnp.swapaxes(g_out.reshape(SEQ, n, W), 1, 2).reshape(INNER, n).astype(F32)
    small = jnp.sum(small.reshape(SEQ, -1, 128), axis=0)
    shards = [(shape[0] // nf,) + shape[1:] for shape in shapes]
    grad_pre, grad_cw, grad_cb, grad_step, grad_decay, grad_skip, grad_post = unpack(small, shards, 1)
    return (
        block_out[None],
        grad_tokens[None],
        grad_in,
        grad_pre,
        grad_cw,
        grad_cb,
        grad_step,
        grad_decay,
        grad_skip,
        grad_post,
        grad_out,
    )


def solution(mesh):
    in_specs = (
        P("fsdp", "seq", None),
        P("fsdp", None),
        P("fsdp"),
        P("fsdp", None),
        P("fsdp"),
        P("fsdp"),
        P("fsdp"),
        P("fsdp"),
        P("fsdp"),
        P(None, "fsdp"),
        P("fsdp", "seq", None),
    )
    out_specs = (
        P("fsdp", "seq", None),
        P("fsdp", "seq", None),
        P("fsdp", None),
        P("fsdp"),
        P("fsdp", None),
        P("fsdp"),
        P("fsdp"),
        P("fsdp"),
        P("fsdp"),
        P("fsdp"),
        P(None, "fsdp"),
    )
    return jax.shard_map(body, mesh=mesh, in_specs=in_specs, out_specs=out_specs, check_vma=False)
```

```python
import functools

import jax
import jax.numpy as jnp
from jax import lax
from jax.experimental import pallas as pl
from jax.experimental.pallas import tpu as pltpu
from jax.sharding import PartitionSpec as P

D = 1536
INNER = 3072
STATE = 128
HEADS = 48
XBC = INNER + 2 * STATE
EPS = 1e-05

SEQ = 4
W = INNER // SEQ
HL = HEADS // SEQ
HW = INNER // HEADS
CH = W + 2 * STATE
VC = CH + 128
Q = 128

F32 = jnp.float32
BF16 = jnp.bfloat16
MESH = pl.DeviceIdType.MESH
HIGH = lax.Precision.HIGHEST
VMEM = pl.BlockSpec(memory_space=pltpu.VMEM)
ANY = pl.BlockSpec(memory_space=pl.ANY)
VMEM_LIMIT = 64000 * 1024


def rcopy(src, dst, send_sem, recv_sem, device):
    return pltpu.make_async_remote_copy(
        src_ref=src, dst_ref=dst, send_sem=send_sem, recv_sem=recv_sem, device_id=device, device_id_type=MESH
    )


def signal(sem, device):
    pl.semaphore_signal(sem, inc=1, device_id=device, device_id_type=MESH)


def nn(a, b, precision=None):
    return lax.dot_general(a, b, (((1,), (0,)), ((), ())), precision=precision, preferred_element_type=F32)


def nt(a, b, precision=None):
    return lax.dot_general(a, b, (((1,), (1,)), ((), ())), precision=precision, preferred_element_type=F32)


def seq_gather_start(refs, outs, send, recv, px, py, me):
    for g, (src, out) in enumerate(zip(refs, outs)):
        n = src.shape[0]
        own = out.at[pl.ds(me * n, n)]
        rcopy(src, own, send.at[g, 0], recv.at[g, 0], {"seq": px}).start()
        rcopy(src, own, send.at[g, 1], recv.at[g, 1], {"seq": py}).start()


def seq_gather_relay(g, src, out, send, recv, px, py, me):
    n = src.shape[0]
    h = n // 2
    own = out.at[pl.ds(me * n, n)]
    rcopy(src, own, send.at[g, 0], recv.at[g, 0], {"seq": px}).wait_recv()
    top = out.at[pl.ds(px * n, h)]
    rcopy(top, top, send.at[g, 2], recv.at[g, 2], {"seq": py}).start()
    rcopy(src, own, send.at[g, 1], recv.at[g, 1], {"seq": py}).wait_recv()
    low = out.at[pl.ds(py * n + h, h)]
    rcopy(low, low, send.at[g, 3], recv.at[g, 3], {"seq": px}).start()


def seq_gather_finish(g, src, out, send, recv, px, py, me):
    n = src.shape[0]
    h = n // 2
    own = out.at[pl.ds(me * n, n)]
    half = out.at[pl.ds(me * n, h)]
    rcopy(half, half, send.at[g, 2], recv.at[g, 2], {"seq": py}).wait()
    rcopy(half, half, send.at[g, 3], recv.at[g, 3], {"seq": px}).wait()
    rcopy(src, own, send.at[g, 0], recv.at[g, 0], {"seq": px}).wait_send()
    rcopy(src, own, send.at[g, 1], recv.at[g, 1], {"seq": py}).wait_send()


def softplus(x):
    return jnp.maximum(x, 0.0) + jnp.log1p(jnp.exp(-jnp.abs(x)))


def sigmoid(x):
    return 1.0 / (1.0 + jnp.exp(-x))


def rates_of(r_ref, rows, hp_ref, tri):
    raw = r_ref[rows, :].astype(F32) + hp_ref[0:1, :]
    dt = softplus(raw)
    lam = nn(tri, dt * hp_ref[1:2, :], HIGH)
    return raw, dt, lam


def spread(mat, h):
    return jnp.broadcast_to(mat[:, h : h + 1], (mat.shape[0], 128))


def scan_fwd_blocks(
    v_ref, s_ref, r_ref, kw_ref, hp_ref, ex_ref, mixed_ref, k_ref, st_ref, buf, hst, xw_s, er_s, between
):
    blocks = v_ref.shape[0] // Q
    row = lax.broadcasted_iota(jnp.int32, (Q, Q), 0)
    col = lax.broadcasted_iota(jnp.int32, (Q, Q), 1)
    causal = row >= col
    tri = causal.astype(F32)
    low = lax.broadcasted_iota(jnp.int32, (Q, 128), 1) < HW
    low1 = lax.broadcasted_iota(jnp.int32, (1, 128), 1) < HW
    buf[0:8, :] = jnp.zeros((8, CH), F32)
    hst[...] = jnp.zeros_like(hst)

    def block(b, carry):
        rows = pl.ds(pl.multiple_of(b * Q, Q), Q)
        buf[8 : 8 + Q, 0:W] = v_ref[rows, :].astype(F32)
        buf[8 : 8 + Q, W:CH] = s_ref[rows, :].astype(F32)
        k = kw_ref[4:5, :] + buf[5 : 5 + Q, :] * kw_ref[0:1, :]
        for j in range(1, 4):
            k = k + buf[5 + j : 5 + j + Q, :] * kw_ref[j : j + 1, :]
        k_ref[rows, :] = k
        buf[0:8, :] = buf[Q : Q + 8, :]
        x = k * sigmoid(k)
        bs, cs = x[:, W : W + STATE], x[:, W + STATE :]
        _, dt, lam = rates_of(r_ref, rows, hp_ref, tri)
        lam_t, dt_t = lam.T, dt.T
        last = lam[Q - 1 : Q, :]
        tail = dt * jnp.exp(last - lam)
        aff = nt(cs, bs, HIGH)
        st_ref[b] = hst[...].astype(BF16)
        ch = nn(cs.astype(BF16), st_ref[b])
        for i in range(HL // 2):
            at = slice(128 * i, 128 * i + 128)
            xp = x[:, at]
            xb = xp.astype(BF16)
            y, lc = [], []
            for h in (2 * i, 2 * i + 1):
                lcol = spread(lam, h)
                within = jnp.exp(jnp.where(causal, lcol - lam_t[h : h + 1, :], -1e30))
                y.append(nn((aff * within * dt_t[h : h + 1, :]).astype(BF16), xb))
                lc.append(lcol)
            out = jnp.where(low, y[0], y[1])
            out = out + jnp.exp(jnp.where(low, lc[0], lc[1])) * ch[:, at] + ex_ref[0:1, at] * xp
            mixed_ref[rows, at] = out.astype(BF16)
            xw_s[:, at] = (xp * jnp.where(low, spread(tail, 2 * i), spread(tail, 2 * i + 1))).astype(BF16)
            er_s[0:1, at] = jnp.exp(jnp.where(low1, spread(last, 2 * i), spread(last, 2 * i + 1)))
        hst[...] = hst[...] * er_s[0:1, :] + nn(bs.T.astype(BF16), xw_s[...])
        between(b)
        return carry

    lax.fori_loop(0, blocks, block, 0)


def scan_bwd_kernel(
    v_ref, s_ref, r_ref, k_ref, dy_ref, st_ref, kw_ref, hp_ref, ex_ref,
    dv_ref, gcw_ref, gch_ref, ghd_ref,
    buf, dhst, rowp, xw_s, e_s, er_s,
):
    blocks = v_ref.shape[0] // Q
    row = lax.broadcasted_iota(jnp.int32, (Q, Q), 0)
    col = lax.broadcasted_iota(jnp.int32, (Q, Q), 1)
    tri = (row >= col).astype(F32)
    later = col >= row
    suffix = later.astype(F32)
    strict = (col < row).astype(F32)
    lane = lax.broadcasted_iota(jnp.int32, (Q, 128), 1)
    lane1 = lax.broadcasted_iota(jnp.int32, (1, 128), 1)
    low = lane < HW
    low1 = lane1 < HW
    buf[Q : Q + 8, :] = jnp.zeros((8, CH), F32)
    dhst[...] = jnp.zeros_like(dhst)
    rowp[...] = jnp.zeros_like(rowp)
    gcw_ref[...] = jnp.zeros_like(gcw_ref)
    gch_ref[...] = jnp.zeros_like(gch_ref)
    ghd_ref[...] = jnp.zeros_like(ghd_ref)

    def block(i0, carry):
        b = blocks - 1 - i0
        rows = pl.ds(pl.multiple_of(b * Q, Q), Q)
        k = k_ref[rows, :]
        sg = sigmoid(k)
        x = k * sg
        ds = sg * (1.0 + k * (1.0 - sg))
        bs, cs = x[:, W : W + STATE], x[:, W + STATE :]
        bb, cb = bs.astype(BF16), cs.astype(BF16)
        raw, dt, lam = rates_of(r_ref, rows, hp_ref, tri)
        lam_t = lam.T
        last = lam[Q - 1 : Q, :]
        aff_t = nt(bs, cs, HIGH)
        hb = st_ref[b]
        dhb = dhst[...].astype(BF16)
        ch = nn(cb, hb)
        bd = nn(bb, dhb)
        daff_t = jnp.zeros((Q, Q), F32)
        col_n = jnp.zeros((Q, 128), F32)
        col_i = jnp.zeros((Q, 128), F32)
        row_i = jnp.zeros((Q, 128), F32)
        through = jnp.zeros((1, 128), F32)
        for i in range(HL // 2):
            at = slice(128 * i, 128 * i + 128)
            xp = x[:, at]
            xb = xp.astype(BF16)
            dyb = dy_ref[rows, at]
            dyf = dyb.astype(F32)
            z, lc, dc = [], [], []
            for h in (2 * i, 2 * i + 1):
                mine = low if h % 2 == 0 else jnp.logical_not(low)
                lcol, dcol = spread(lam, h), spread(dt, h)
                within = jnp.exp(jnp.where(later, lam_t[h : h + 1, :] - lcol, -1e30))
                g = nt(jnp.where(mine, xp, 0.0).astype(BF16), dyb)
                lg = within * g
                lgd = lg * dcol
                daff_t = daff_t + lgd
                col_n = jnp.where(lane == h, jnp.sum(aff_t * lg, axis=1, keepdims=True), col_n)
                rowp[h : h + 1, :] = jnp.sum(aff_t * lgd, axis=0, keepdims=True)
                z.append(nn((aff_t * within).astype(BF16), dyb))
                lc.append(lcol)
                dc.append(dcol)
            lamp = jnp.where(low, lc[0], lc[1])
            dtp = jnp.where(low, dc[0], dc[1])
            lastp = jnp.where(low1, spread(last, 2 * i), spread(last, 2 * i + 1))
            e = dyf * jnp.exp(lamp)
            e_s[:, at] = e.astype(BF16)
            ew = jnp.exp(lastp - lamp)
            bdp = bd[:, at]
            xw_s[:, at] = (xp * (dtp * ew)).astype(BF16)
            er_s[0:1, at] = jnp.exp(lastp)
            re = e * ch[:, at]
            ci = xp * bdp * ew
            th = jnp.sum(dhst[:, at] * hb[:, at].astype(F32), axis=0, keepdims=True) * er_s[0:1, at]
            for h in (2 * i, 2 * i + 1):
                mine = low if h % 2 == 0 else jnp.logical_not(low)
                mine1 = low1 if h % 2 == 0 else jnp.logical_not(low1)
                row_i = jnp.where(lane == h, jnp.sum(jnp.where(mine, re, 0.0), axis=1, keepdims=True), row_i)
                col_i = jnp.where(lane == h, jnp.sum(jnp.where(mine, ci, 0.0), axis=1, keepdims=True), col_i)
                through = jnp.where(
                    lane1 == h, jnp.sum(jnp.where(mine1, th, 0.0), axis=1, keepdims=True), through
                )
            dx = dtp * jnp.where(low, z[0], z[1]) + bdp * (dtp * ew) + ex_ref[0:1, at] * dyf
            gch_ref[0:1, at] += jnp.sum(dyf * xp, axis=0, keepdims=True)
            buf[0:Q, at] = dx * ds[:, at]
        daff_b = daff_t.astype(BF16)
        d_bs = nt(xw_s[...], dhb) + nn(daff_b, cb)
        d_cs = nt(e_s[...], hb) + nn(daff_t.T.astype(BF16), bb)
        buf[0:Q, W : W + STATE] = d_bs * ds[:, W : W + STATE]
        buf[0:Q, W + STATE : CH] = d_cs * ds[:, W + STATE :]
        dhst[...] = dhst[...] * er_s[0:1, :] + nn(cs.T.astype(BF16), e_s[...])
        after = nn(suffix, rowp[...].T - dt * col_n + row_i, HIGH) + nn(strict, dt * col_i, HIGH) + through
        d_rate = (col_n + col_i + hp_ref[1:2, :] * after) * sigmoid(raw)
        ghd_ref[0:1, :] += jnp.sum(d_rate, axis=0, keepdims=True)
        ghd_ref[1:2, :] += jnp.sum(dt * after, axis=0, keepdims=True) * hp_ref[1:2, :]
        dv_ref[rows, CH:VC] = d_rate.astype(BF16)
        for at, ref in ((slice(0, W), v_ref), (slice(W, CH), s_ref)):
            raw_v = ref[rows, :].astype(F32)
            dk = buf[0:Q, at]
            dv = dk * kw_ref[3:4, at]
            gcw_ref[4:5, at] += jnp.sum(dk, axis=0, keepdims=True)
            gcw_ref[3:4, at] += jnp.sum(dk * raw_v, axis=0, keepdims=True)
            for j in range(3):
                dk = buf[3 - j : 3 - j + Q, at]
                dv = dv + dk * kw_ref[j : j + 1, at]
                gcw_ref[j : j + 1, at] += jnp.sum(dk * raw_v, axis=0, keepdims=True)
            dv_ref[rows, at] = dv.astype(BF16)
        buf[Q : Q + 8, :] = buf[0:8, :]
        return carry

    lax.fori_loop(0, blocks, block, 0)


def scan_bwd(v, s, r, k, dy, st, kw, hp, ex):
    length = v.shape[0]
    shape = jax.ShapeDtypeStruct
    return pl.pallas_call(
        scan_bwd_kernel,
        out_shape=[shape((length, VC), BF16), shape((8, CH), F32), shape((8, W), F32), shape((8, 128), F32)],
        in_specs=[VMEM] * 9,
        out_specs=[VMEM] * 4,
        scratch_shapes=[
            pltpu.VMEM((Q + 8, CH), F32),
            pltpu.VMEM((STATE, W), F32),
            pltpu.VMEM((128, Q), F32),
            pltpu.VMEM((Q, W), BF16),
            pltpu.VMEM((Q, W), BF16),
            pltpu.VMEM((8, W), F32),
        ],
        name="scan_bwd",
        compiler_params=pltpu.CompilerParams(vmem_limit_bytes=VMEM_LIMIT),
    )(v, s, r, k, dy, st, kw, hp, ex)


GROUPS = 4


def place(block, at, width):
    start, shift = at // 128 * 128, at % 128
    lanes = -(-(width + shift) // 128) * 128
    have = block.shape[1]
    if lanes > have:
        block = jnp.concatenate([block, jnp.zeros((block.shape[0], lanes - have), block.dtype)], axis=1)
    else:
        block = block[:, :lanes]
    if shift:
        block = pltpu.roll(block, shift, 1)
    return start, lanes, block


def front_kernel(
    nf, tok, cot, win, wst, wout, small,
    x_out, cot_out, nrm_out, wv_out, ws_out, wg_out, wo_out, mix_out, gate_out, mixed_out, k_out, st_out, dsh_out,
    kw_s, hp_s, ex_s, pre_s, stat_s,
    x_s, cot_s, nrm_s, wv_s, ws_s, wg_s, wo_s, mix_s, gate_s, mixed_s, k_s, st_s, dsh_s,
    small_s, conv_s, post_s, stat_own, stat_got,
    buf, hst, xw_s, er_s,
    xs, xr, zs, zr, ms, mr, es, er, ls, os_,
):
    s = lax.axis_index("seq")
    f = lax.axis_index("fsdp")
    px, py = s ^ 1, s ^ 2
    nl = nf // 2
    p, c = f // 2, f % 2
    partner = p * 2 + 1 - c
    bar = pltpu.get_barrier_semaphore()
    for k in range(1, SEQ):
        signal(bar, {"seq": s ^ k})
    for k in range(1, nf):
        signal(bar, {"fsdp": lax.rem(f + k, nf)})
    pl.semaphore_wait(bar, nf - 1 + SEQ - 1)

    n = win.shape[0]
    rows = tok.shape[0]
    length = rows * SEQ
    ins = (
        win.at[:, pl.ds(pl.multiple_of(INNER + s * W, 128), W)],
        wst,
        win.at[:, pl.ds(pl.multiple_of(s * W, 128), W)],
        wout,
    )
    outs = (wv_s, ws_s, wg_s, wo_s)

    def row(g, i):
        return outs[g].at[pl.ds(i * n, n)]

    def hop(g, src, i, way, k, device):
        return rcopy(src, row(g, i), zs.at[g, way, k], zr.at[g, i], {"fsdp": device})

    def own_send(g):
        @pl.when(p < nl - 1)
        def _():
            hop(g, ins[g], f, 0, 0, f + 2).start()

        @pl.when(p > 0)
        def _():
            hop(g, ins[g], f, 1, 0, f - 2).start()

        hop(g, ins[g], f, 2, 0, partner).start()
        pltpu.make_async_copy(ins[g], row(g, f), ls.at[g]).start()

    def step(g, k):
        @pl.when(p - k >= 0)
        def _():
            o = f - 2 * k
            hop(g, row(g, o), o, 0, k, f).wait_recv()

            @pl.when(p < nl - 1)
            def _():
                hop(g, row(g, o), o, 0, k, f + 2).start()

            hop(g, row(g, o), o, 2, k, partner).start()

        @pl.when(p + k < nl)
        def _():
            o = f + 2 * k
            hop(g, row(g, o), o, 1, k, f).wait_recv()

            @pl.when(p > 0)
            def _():
                hop(g, row(g, o), o, 1, k, f - 2).start()

            hop(g, row(g, o), o, 3, k, partner).start()

    def arrive(g):
        pltpu.make_async_copy(ins[g], row(g, f), ls.at[g]).wait()
        for q in range(nl):
            o = q * 2 + 1 - c
            hop(g, row(g, o), o, 2, 0, partner).wait_recv()

    def sent(g):
        hop(g, ins[g], f, 2, 0, partner).wait_send()

        @pl.when(p < nl - 1)
        def _():
            hop(g, ins[g], f, 0, 0, f + 2).wait_send()

        @pl.when(p > 0)
        def _():
            hop(g, ins[g], f, 1, 0, f - 2).wait_send()

        for k in range(1, nl):
            @pl.when(p - k >= 0)
            def _():
                o = f - 2 * k

                @pl.when(p < nl - 1)
                def _():
                    hop(g, row(g, o), o, 0, k, f + 2).wait_send()

                hop(g, row(g, o), o, 2, k, partner).wait_send()

            @pl.when(p + k < nl)
            def _():
                o = f + 2 * k

                @pl.when(p > 0)
                def _():
                    hop(g, row(g, o), o, 1, k, f - 2).wait_send()

                hop(g, row(g, o), o, 3, k, partner).wait_send()

    def small_copy(k):
        return rcopy(small, small_s.at[f], ms.at[k], mr.at[k], {"fsdp": lax.rem(f + k, nf)})

    mine = pl.ds(s * rows, rows)
    own_small = pltpu.make_async_copy(small, small_s.at[f], ls.at[4])
    own_tok = pltpu.make_async_copy(tok, x_s.at[mine], ls.at[5])
    own_cot = pltpu.make_async_copy(cot, cot_s.at[mine], ls.at[6])

    for k in range(1, nf):
        small_copy(k).start()
    own_small.start()
    own_tok.start()
    seq_gather_start((tok,), (x_s,), xs, xr, px, py, s)
    own_send(0)
    own_send(1)
    own_cot.start()
    seq_gather_relay(0, tok, x_s, xs, xr, px, py, s)

    def cot_first():
        own = cot_s.at[mine]
        rcopy(cot, own, xs.at[1, 0], xr.at[1, 0], {"seq": px}).start()
        rcopy(cot, own, xs.at[1, 1], xr.at[1, 1], {"seq": py}).start()

    cot_first()
    step(0, 1)
    step(1, 1)
    own_send(2)

    own_small.wait()
    for k in range(1, nf):
        small_copy(k).wait()
    conv_s[...] = jnp.zeros_like(conv_s)
    pre_s[...] = jnp.zeros_like(pre_s)
    post_s[...] = jnp.zeros_like(post_s)
    heads = [jnp.zeros((8, 128), F32) for _ in range(3)]
    for i in range(nf):
        block = small_s[i]
        at, lanes, moved = place(block, i * (XBC // nf), XBC // nf)
        conv_s[:, at : at + lanes] += moved
        at, lanes, moved = place(block, i * (D // nf), D // nf)
        pre_s[:, at : at + lanes] += jnp.where(lax.broadcasted_iota(jnp.int32, moved.shape, 0) == 5, moved, 0.0)
        at, lanes, moved = place(block, i * (INNER // nf), INNER // nf)
        post_s[:, at : at + lanes] += jnp.where(lax.broadcasted_iota(jnp.int32, moved.shape, 0) == 6, moved, 0.0)
        for j in range(3):
            piece = block[:, 128 * j : 128 * j + 128]
            at = i * (HEADS // nf)
            heads[j] = heads[j] + (pltpu.roll(piece, at, 1) if at else piece)
    kw_s[:, 0:W] = conv_s[:, pl.ds(pl.multiple_of(s * W, 128), W)]
    kw_s[:, W:CH] = conv_s[:, INNER:XBC]
    lane1 = lax.broadcasted_iota(jnp.int32, (1, 128), 1)
    low1 = lane1 < HW
    back = lax.rem(128 - s * HL, 128)
    step_b, decay, skip = [pltpu.roll(h, back, 1)[7:8, :] for h in heads]
    hp_s[...] = jnp.zeros_like(hp_s)
    hp_s[0:1, :] = jnp.where(lane1 < HL, step_b, 0.0)
    hp_s[1:2, :] = jnp.where(lane1 < HL, -jnp.exp(decay), 0.0)
    ex_s[...] = jnp.zeros_like(ex_s)
    for i in range(HL // 2):
        ex_s[0:1, 128 * i : 128 * i + 128] = jnp.where(low1, spread(skip, 2 * i), spread(skip, 2 * i + 1))
    ex_s[1:2, :] = post_s[6:7, pl.ds(pl.multiple_of(s * W, 128), W)]

    for k in range(2, nl):
        step(0, k)
        step(1, k)
    own_tok.wait()
    seq_gather_finish(0, tok, x_s, xs, xr, px, py, s)
    seq_gather_relay(1, cot, cot_s, xs, xr, px, py, s)

    def norm(i, carry):
        r = pl.ds(pl.multiple_of(i * 128, 128), 128)
        x = x_s[r, :].astype(F32)
        rho = lax.rsqrt(jnp.sum(x * x, axis=1, keepdims=True) * (1.0 / D) + EPS)
        nrm_s[r, :] = (x * rho * pre_s[5:6, :]).astype(BF16)
        return carry

    lax.fori_loop(0, length // 128, norm, 0)
    step(2, 1)
    own_send(3)
    arrive(0)
    arrive(1)

    saves = [
        pltpu.make_async_copy(a, b, os_.at[i])
        for i, (a, b) in enumerate(
            (
                (x_s, x_out), (cot_s, cot_out), (nrm_s, nrm_out), (wv_s, wv_out), (ws_s, ws_out), (wg_s, wg_out),
                (wo_s, wo_out), (mix_s, mix_out), (gate_s, gate_out), (mixed_s, mixed_out), (k_s, k_out),
                (st_s, st_out), (dsh_s, dsh_out),
            )
        )
    ]
    for i in (0, 2, 3, 4):
        saves[i].start()

    def project(i, carry):
        r = pl.ds(pl.multiple_of(i * 256, 256), 256)
        a = nrm_s[r, :]
        mix_s[r, 0:W] = nn(a, wv_s[...]).astype(BF16)
        mix_s[r, W:VC] = nn(a, ws_s[...]).astype(BF16)
        return carry

    lax.fori_loop(0, length // 256, project, 0)
    saves[7].start()

    def between(b):
        @pl.when(b == 0)
        def _():
            step(2, 2)

        @pl.when(b == 3)
        def _():
            for k in range(3, nl):
                step(2, k)

        @pl.when(b == 6)
        def _():
            step(3, 1)

    scan_fwd_blocks(
        mix_s.at[:, 0:W], mix_s.at[:, W:CH], mix_s.at[:, CH:VC], kw_s, hp_s, ex_s, mixed_s, k_s, st_s,
        buf, hst, xw_s, er_s, between,
    )
    for i in (9, 10, 11):
        saves[i].start()
    arrive(2)
    saves[5].start()

    def project_gate(i, carry):
        r = pl.ds(pl.multiple_of(i * 256, 256), 256)
        gate_s[r, :] = nn(nrm_s[r, :], wg_s[...]).astype(BF16)
        return carry

    step(3, 2)
    lax.fori_loop(0, length // 256, project_gate, 0)
    saves[8].start()
    for k in range(3, nl):
        step(3, k)
    own_cot.wait()
    seq_gather_finish(1, cot, cot_s, xs, xr, px, py, s)
    saves[1].start()
    arrive(3)
    saves[6].start()
    eye = lax.broadcasted_iota(jnp.int32, (128, 128), 0) == lax.broadcasted_iota(jnp.int32, (128, 128), 1)

    def stats(i, carry):
        r = pl.ds(pl.multiple_of(i * 128, 128), 128)
        dsh = nn(cot_s[r, :], wo_s[...])
        dsh_s[r, :] = dsh
        gate = gate_s[r, :].astype(F32)
        gated = mixed_s[r, :].astype(F32) * (gate * sigmoid(gate))
        one = jnp.sum(gated * gated, axis=1, keepdims=True)
        two = jnp.sum(dsh * ex_s[1:2, :] * gated, axis=1, keepdims=True)
        stat_own[pl.ds(i, 1), :] = jnp.sum(jnp.where(eye, one, 0.0), axis=0, keepdims=True)
        stat_own[pl.ds(length // 128 + i, 1), :] = jnp.sum(jnp.where(eye, two, 0.0), axis=0, keepdims=True)
        return carry

    lax.fori_loop(0, length // 128, stats, 0)
    saves[12].start()
    copies = [rcopy(stat_own, stat_got.at[k], es.at[k], er.at[k], {"seq": s ^ k}) for k in range(1, SEQ)]
    for copy in copies:
        copy.start()
    for copy in copies:
        copy.wait()
    stat_s[...] = stat_own[...] + stat_got[1] + (stat_got[2] + stat_got[3])
    for g in range(GROUPS):
        sent(g)
    for save in saves:
        save.wait()


def front(nf, tok, cot, win, wst, wout, small):
    shape = jax.ShapeDtypeStruct
    dma = pltpu.SemaphoreType.DMA
    length = SEQ * tok.shape[0]
    big = [
        shape((length, D), BF16),
        shape((length, D), BF16),
        shape((length, D), BF16),
        shape((D, W), BF16),
        shape((D, VC - W), BF16),
        shape((D, W), BF16),
        shape((D, W), BF16),
        shape((length, VC), BF16),
        shape((length, W), BF16),
        shape((length, W), BF16),
        shape((length, CH), F32),
        shape((length // Q, STATE, W), BF16),
        shape((length, W), F32),
    ]
    par = [
        shape((8, CH), F32),
        shape((8, 128), F32),
        shape((8, W), F32),
        shape((8, D), F32),
        shape((2 * length // 128, 128), F32),
    ]
    return pl.pallas_call(
        functools.partial(front_kernel, nf),
        out_shape=big + par,
        in_specs=[ANY] * 5 + [VMEM],
        out_specs=[ANY] * len(big) + [VMEM] * len(par),
        scratch_shapes=[pltpu.VMEM(b.shape, b.dtype) for b in big]
        + [
            pltpu.VMEM((nf, 8, 512), F32),
            pltpu.VMEM((8, XBC), F32),
            pltpu.VMEM((8, INNER), F32),
            pltpu.VMEM((2 * length // 128, 128), F32),
            pltpu.VMEM((SEQ, 2 * length // 128, 128), F32),
            pltpu.VMEM((Q + 8, CH), F32),
            pltpu.VMEM((STATE, W), F32),
            pltpu.VMEM((Q, W), BF16),
            pltpu.VMEM((8, W), F32),
            dma((2, 4)),
            dma((2, 4)),
            dma((GROUPS, 4, nf // 2)),
            dma((GROUPS, nf)),
            dma((nf,)),
            dma((nf,)),
            dma((SEQ,)),
            dma((SEQ,)),
            dma((7,)),
            dma((len(big),)),
        ],
        name="front",
        compiler_params=pltpu.CompilerParams(
            collective_id=1, has_side_effects=True, vmem_limit_bytes=VMEM_LIMIT
        ),
    )(tok, cot, win, wst, wout, small)


def reduce_kernel(nf, *refs):
    ins, outs = refs[:6], refs[6:12]
    pb, ub, db, cs, own = refs[12:16], refs[16:20], refs[20:24], refs[24:28], refs[28:32]
    ab, az = refs[32:34], refs[34:36]
    zs, zr, xs, xr, as_, ar, ls = refs[36:]
    s = lax.axis_index("seq")
    f = lax.axis_index("fsdp")
    px, py = s ^ 1, s ^ 2
    nl = nf // 2
    p, c = f // 2, f % 2
    partner = p * 2 + 1 - c
    bar = pltpu.get_barrier_semaphore()
    signal(bar, {"seq": px})
    signal(bar, {"seq": py})
    signal(bar, {"fsdp": partner})

    @pl.when(p < nl - 1)
    def _():
        signal(bar, {"fsdp": f + 2})

    @pl.when(p > 0)
    def _():
        signal(bar, {"fsdp": f - 2})

    pl.semaphore_wait(bar, 3 + jnp.where(p < nl - 1, 1, 0) + jnp.where(p > 0, 1, 0))

    rows = ins[4].shape[0] // SEQ
    half = D // 2
    cols = (slice(0, half), slice(half, D))
    first, second = (px, py), (py, px)

    def chunk(ref, i, a):
        return ref.at[pl.ds(i * rows, rows), cols[a]]

    def seq_one(t, a, m):
        i = (first[a] ^ second[a] ^ s) if m == 0 else first[a]
        return rcopy(
            chunk(ins[4 + t], i, a), ab[t].at[a, m], xs.at[t, a, m], xr.at[t, a, m], {"seq": first[a]}
        )

    def seq_two(t, a):
        return rcopy(az[t].at[a, 0], az[t].at[a, 1], xs.at[t, a, 2], xr.at[t, a, 2], {"seq": second[a]})

    shard = [ins[g].shape[0] // nf for g in range(4)]

    def piece(g, i):
        return ins[g].at[pl.ds(i * shard[g], shard[g])]

    def swap(g, q):
        return rcopy(piece(g, q * 2 + 1 - c), pb[g].at[q], zs.at[g, 0, q], zr.at[g, 0, q], {"fsdp": partner})

    def up(g, q):
        return rcopy(cs[g].at[q], ub[g].at[q], zs.at[g, 1, q], zr.at[g, 1, q], {"fsdp": f + 2})

    def down(g, q):
        return rcopy(cs[g].at[q], db[g].at[q], zs.at[g, 2, q], zr.at[g, 2, q], {"fsdp": f - 2})

    order = []
    for k in range(nl // 2):
        order += [nl - 1 - k, k]
    for g in range(4):
        for q in order:
            swap(g, q).start()
    for t in range(2):
        for m in range(2):
            for a in range(2):
                seq_one(t, a, m).start()

    def add(*terms):
        total = terms[0].astype(F32)
        for term in terms[1:]:
            total = total + term.astype(F32)
        return total

    def line(g):
        for q in order:
            swap(g, q).wait_recv()
            mine = piece(g, q * 2 + c)

            @pl.when(q > p)
            def _():
                @pl.when(p > 0)
                def _():
                    up(g, q).wait_recv()
                    cs[g][q] = add(mine[...], pb[g][q], ub[g][q]).astype(cs[g].dtype)

                @pl.when(p == 0)
                def _():
                    cs[g][q] = add(mine[...], pb[g][q]).astype(cs[g].dtype)

                up(g, q).start()

            @pl.when(q < p)
            def _():
                @pl.when(p < nl - 1)
                def _():
                    down(g, q).wait_recv()
                    cs[g][q] = add(mine[...], pb[g][q], db[g][q]).astype(cs[g].dtype)

                @pl.when(p == nl - 1)
                def _():
                    cs[g][q] = add(mine[...], pb[g][q]).astype(cs[g].dtype)

                down(g, q).start()

    def close(g):
        mine = piece(g, f)

        @pl.when(p > 0)
        def _():
            up(g, p).wait_recv()

        @pl.when(p < nl - 1)
        def _():
            down(g, p).wait_recv()

        @pl.when(p == 0)
        def _():
            own[g][...] = add(mine[...], pb[g][p], db[g][p]).astype(own[g].dtype)

        @pl.when(p == nl - 1)
        def _():
            own[g][...] = add(mine[...], pb[g][p], ub[g][p]).astype(own[g].dtype)

        @pl.when(jnp.logical_and(p > 0, p < nl - 1))
        def _():
            own[g][...] = add(mine[...], pb[g][p], ub[g][p], db[g][p]).astype(own[g].dtype)

    for g in range(4):
        line(g)
        if g == 1:
            for t in range(2):
                for a in range(2):
                    seq_one(t, a, 0).wait_recv()
                    az[t][a, 0] = add(chunk(ins[4 + t], second[a], a)[...], ab[t][a, 0]).astype(BF16)
                    seq_two(t, a).start()

    for g in range(4):
        close(g)
        n = shard[g]
        place = outs[g].at[pl.ds(s * n, n)]
        rcopy(own[g], place, as_.at[g, 0], ar.at[g, 0], {"seq": px}).start()
        rcopy(own[g], place, as_.at[g, 1], ar.at[g, 1], {"seq": py}).start()
        pltpu.make_async_copy(own[g], place, ls.at[g]).start()

    for t in range(2):
        for a in range(2):
            seq_one(t, a, 1).wait_recv()
            seq_two(t, a).wait_recv()
            outs[4 + t][:, cols[a]] = add(chunk(ins[4 + t], s, a)[...], ab[t][a, 1], az[t][a, 1])

    for g in range(4):
        seq_gather_relay(g, own[g], outs[g], as_, ar, px, py, s)
    for g in range(4):
        seq_gather_finish(g, own[g], outs[g], as_, ar, px, py, s)
        place = outs[g].at[pl.ds(s * shard[g], shard[g])]
        pltpu.make_async_copy(own[g], place, ls.at[g]).wait()
        for q in range(nl):
            swap(g, q).wait_send()

            @pl.when(q > p)
            def _():
                up(g, q).wait_send()

            @pl.when(q < p)
            def _():
                down(g, q).wait_send()

    for t in range(2):
        for a in range(2):
            seq_one(t, a, 0).wait_send()
            seq_one(t, a, 1).wait_send()
            seq_two(t, a).wait_send()


def reduce_all(nf, gv, gg, go, small, out_part, dn_part):
    shape = jax.ShapeDtypeStruct
    dma = pltpu.SemaphoreType.DMA
    nl = nf // 2
    groups = (small, gv, gg, go)
    rows = out_part.shape[0] // SEQ
    boxes = [((g.shape[0] // nf, g.shape[1]), g.dtype) for g in groups]
    lines = [pltpu.VMEM((nl,) + box, dtype) for box, dtype in boxes]
    return pl.pallas_call(
        functools.partial(reduce_kernel, nf),
        out_shape=[shape((SEQ * box[0], box[1]), dtype) for box, dtype in boxes] + [shape((rows, D), F32)] * 2,
        in_specs=[VMEM] * 6,
        out_specs=[VMEM] * 6,
        scratch_shapes=lines * 4
        + [pltpu.VMEM(box, dtype) for box, dtype in boxes]
        + [pltpu.VMEM((2, 2, rows, D // 2), BF16)] * 4
        + [
            dma((4, 3, nl)),
            dma((4, 3, nl)),
            dma((2, 2, 3)),
            dma((2, 2, 3)),
            dma((4, 4)),
            dma((4, 4)),
            dma((4,)),
        ],
        name="reduce_all",
        compiler_params=pltpu.CompilerParams(
            collective_id=3, has_side_effects=True, vmem_limit_bytes=VMEM_LIMIT
        ),
    )(small, gv, gg, go, out_part, dn_part)


def own_rows(array, index, row_count):
    return lax.dynamic_slice_in_dim(array, index * row_count, row_count, 0)


def pack(parts, nf):
    flat = jnp.concatenate([part.reshape(nf, -1) for part in parts], axis=1)
    rows = -(-flat.shape[1] // 1024) * 8
    flat = jnp.pad(flat, ((0, 0), (0, rows * 128 - flat.shape[1])))
    return flat.reshape(nf * rows, 128)


def unpack(packed, shapes, count):
    flat = packed.reshape(count, -1)
    out, at = [], 0
    for shape in shapes:
        size = 1
        for extent in shape:
            size *= extent
        size //= count
        out.append(flat[:, at : at + size].reshape(shape))
        at += size
    return out


def body(
    tokens,
    input_projection_weight,
    pre_gain,
    conv_weight,
    conv_bias,
    step_bias,
    decay_log,
    skip_gain,
    post_gain,
    output_projection_weight,
    cotangent,
):
    nf = lax.axis_size("fsdp")
    s = lax.axis_index("seq")
    tok = tokens.reshape(tokens.shape[1:])
    cot = cotangent.reshape(cotangent.shape[1:])
    win = input_projection_weight
    n = win.shape[0]

    w_state = jnp.concatenate(
        [
            win[:, 2 * INNER : 2 * INNER + 2 * STATE],
            lax.dynamic_slice(win, (0, 2 * INNER + 2 * STATE + s * HL), (n, HL)),
            jnp.zeros((n, 128 - HL), BF16),
        ],
        axis=1,
    )
    w_out = own_rows(output_projection_weight, s, W).T

    def line(*pieces):
        return jnp.concatenate([jnp.pad(v[None], ((0, 0), (0, 128 * t - v.shape[0]))) for v, t in pieces], axis=1)

    small = jnp.concatenate(
        [
            jnp.pad(conv_weight.T, ((0, 0), (0, 512 - conv_weight.shape[0]))),
            line((conv_bias, 4)),
            line((pre_gain, 4)),
            line((post_gain, 4)),
            line((step_bias, 1), (decay_log, 1), (skip_gain, 2)),
        ]
    ).astype(F32)
    (
        x_all, cot_all, normed, w_val, w_state, w_gate, w_out, mix_raw, gate_raw, mixed, k, st, d_shaped,
        kw, hp, ex, pre, sums,
    ) = front(nf, tok, cot, win, w_state, w_out, small)
    shapes = ((D,), (XBC, 4), (XBC,), (HEADS,), (HEADS,), (HEADS,), (INNER,))
    v_raw, s_raw, r_raw = mix_raw[:, :W], mix_raw[:, W:CH], mix_raw[:, CH:]
    post, pre = ex[1], pre[5]

    residual = x_all.astype(F32)
    rho0 = lax.rsqrt(jnp.mean(residual * residual, axis=-1, keepdims=True) + EPS)
    n0 = residual * rho0
    gate = gate_raw.astype(F32)
    mixed = mixed.astype(F32)
    sg = jax.nn.sigmoid(gate)
    sl = gate * sg
    gated = mixed * sl
    e1 = d_shaped * post
    half = sums.shape[0] // 2
    rho1 = lax.rsqrt(sums[:half].reshape(-1, 1) / INNER + EPS)
    mean1 = rho1 * sums[half:].reshape(-1, 1) / INNER
    n1 = gated * rho1
    shaped = (n1 * post).astype(BF16)
    g_post = jnp.sum(d_shaped * n1, axis=0)
    d_gated = rho1 * (e1 - n1 * mean1)
    d_mixed = (d_gated * sl).astype(BF16)
    d_gate = (d_gated * mixed * (sg * (1.0 + gate * (1.0 - sg)))).astype(BF16)

    out_part = nt(shaped, w_out).astype(BF16)
    tn = (((0,), (0,)), ((), ()))
    g_out = lax.dot_general(cot_all, shaped, tn, preferred_element_type=F32).astype(BF16)
    g_gate = lax.dot_general(normed, d_gate, tn, preferred_element_type=F32).astype(BF16)

    dv, g_conv, g_chan, g_head = scan_bwd(v_raw, s_raw, r_raw, k, d_mixed, st, kw, hp, ex)
    g_mix = lax.dot_general(normed, dv, tn, preferred_element_type=F32).astype(BF16)
    dn_part = nt(d_gate, w_gate) + nt(dv[:, :W], w_val) + nt(dv[:, W:], w_state)
    g_pre = jnp.sum(dn_part * n0, axis=0)

    def placed(full, piece, at):
        return lax.dynamic_update_slice_in_dim(jnp.zeros((full,) + piece.shape[1:], F32), piece, at, 0)

    g_cw = jnp.concatenate([placed(INNER, g_conv[:4, :W].T, s * W), g_conv[:4, W:].T])
    g_cb = jnp.concatenate([placed(INNER, g_conv[4, :W], s * W), g_conv[4, W:]])
    small = pack(
        [
            g_pre,
            g_cw,
            g_cb,
            placed(HEADS, g_head[0, :HL], s * HL),
            placed(HEADS, g_head[1, :HL], s * HL),
            placed(HEADS, jnp.sum(g_chan[0].reshape(HL, HW), axis=1), s * HL),
            placed(INNER, g_post, s * W),
        ],
        nf,
    )
    small, g_mix, g_gate, g_out, out_sum, dn = reduce_all(
        nf, g_mix, g_gate, g_out, small, out_part, dn_part.astype(BF16)
    )

    block_out = tok.astype(F32) + out_sum
    res = tok.astype(F32)
    r0 = lax.rsqrt(jnp.mean(res * res, axis=-1, keepdims=True) + EPS)
    m0 = res * r0
    e0 = dn * pre
    grad_tokens = cot.astype(F32) + r0 * (e0 - m0 * jnp.mean(e0 * m0, axis=-1, keepdims=True))

    g_mix = g_mix.reshape(SEQ, n, VC).astype(F32)
    g_gate = g_gate.reshape(SEQ, n, W).astype(F32)
    grad_in = jnp.concatenate(
        [g_gate[i] for i in range(SEQ)]
        + [g_mix[i, :, :W] for i in range(SEQ)]
        + [jnp.sum(g_mix[:, :, W:CH], axis=0)]
        + [g_mix[i, :, CH : CH + HL] for i in range(SEQ)],
        axis=1,
    )
    grad_out = jnp.swapaxes(g_out.reshape(SEQ, n, W), 1, 2).reshape(INNER, n).astype(F32)
    small = jnp.sum(small.reshape(SEQ, -1, 128), axis=0)
    shards = [(shape[0] // nf,) + shape[1:] for shape in shapes]
    grad_pre, grad_cw, grad_cb, grad_step, grad_decay, grad_skip, grad_post = unpack(small, shards, 1)
    return (
        block_out[None],
        grad_tokens[None],
        grad_in,
        grad_pre,
        grad_cw,
        grad_cb,
        grad_step,
        grad_decay,
        grad_skip,
        grad_post,
        grad_out,
    )


def solution(mesh):
    in_specs = (
        P("fsdp", "seq", None),
        P("fsdp", None),
        P("fsdp"),
        P("fsdp", None),
        P("fsdp"),
        P("fsdp"),
        P("fsdp"),
        P("fsdp"),
        P("fsdp"),
        P(None, "fsdp"),
        P("fsdp", "seq", None),
    )
    out_specs = (
        P("fsdp", "seq", None),
        P("fsdp", "seq", None),
        P("fsdp", None),
        P("fsdp"),
        P("fsdp", None),
        P("fsdp"),
        P("fsdp"),
        P("fsdp"),
        P("fsdp"),
        P("fsdp"),
        P(None, "fsdp"),
    )
    return jax.shard_map(body, mesh=mesh, in_specs=in_specs, out_specs=out_specs, check_vma=False)
```

```python
import functools

import jax
import jax.numpy as jnp
from jax import lax
from jax.experimental import pallas as pl
from jax.experimental.pallas import tpu as pltpu
from jax.sharding import PartitionSpec as P

D = 1536
INNER = 3072
STATE = 128
HEADS = 48
XBC = INNER + 2 * STATE
EPS = 1e-05

SEQ = 4
W = INNER // SEQ
HL = HEADS // SEQ
HW = INNER // HEADS
CH = W + 2 * STATE
VC = CH + 128
Q = 128

F32 = jnp.float32
BF16 = jnp.bfloat16
MESH = pl.DeviceIdType.MESH
HIGH = lax.Precision.HIGHEST
VMEM = pl.BlockSpec(memory_space=pltpu.VMEM)
ANY = pl.BlockSpec(memory_space=pl.ANY)
VMEM_LIMIT = 64000 * 1024


def rcopy(src, dst, send_sem, recv_sem, device):
    return pltpu.make_async_remote_copy(
        src_ref=src, dst_ref=dst, send_sem=send_sem, recv_sem=recv_sem, device_id=device, device_id_type=MESH
    )


def signal(sem, device):
    pl.semaphore_signal(sem, inc=1, device_id=device, device_id_type=MESH)


def nn(a, b, precision=None):
    return lax.dot_general(a, b, (((1,), (0,)), ((), ())), precision=precision, preferred_element_type=F32)


def nt(a, b, precision=None):
    return lax.dot_general(a, b, (((1,), (1,)), ((), ())), precision=precision, preferred_element_type=F32)


def seq_gather_start(refs, outs, send, recv, px, py, me):
    for g, (src, out) in enumerate(zip(refs, outs)):
        n = src.shape[0]
        own = out.at[pl.ds(me * n, n)]
        rcopy(src, own, send.at[g, 0], recv.at[g, 0], {"seq": px}).start()
        rcopy(src, own, send.at[g, 1], recv.at[g, 1], {"seq": py}).start()


def seq_gather_relay(g, src, out, send, recv, px, py, me):
    n = src.shape[0]
    h = n // 2
    own = out.at[pl.ds(me * n, n)]
    rcopy(src, own, send.at[g, 0], recv.at[g, 0], {"seq": px}).wait_recv()
    top = out.at[pl.ds(px * n, h)]
    rcopy(top, top, send.at[g, 2], recv.at[g, 2], {"seq": py}).start()
    rcopy(src, own, send.at[g, 1], recv.at[g, 1], {"seq": py}).wait_recv()
    low = out.at[pl.ds(py * n + h, h)]
    rcopy(low, low, send.at[g, 3], recv.at[g, 3], {"seq": px}).start()


def seq_gather_finish(g, src, out, send, recv, px, py, me):
    n = src.shape[0]
    h = n // 2
    own = out.at[pl.ds(me * n, n)]
    half = out.at[pl.ds(me * n, h)]
    rcopy(half, half, send.at[g, 2], recv.at[g, 2], {"seq": py}).wait()
    rcopy(half, half, send.at[g, 3], recv.at[g, 3], {"seq": px}).wait()
    rcopy(src, own, send.at[g, 0], recv.at[g, 0], {"seq": px}).wait_send()
    rcopy(src, own, send.at[g, 1], recv.at[g, 1], {"seq": py}).wait_send()


def softplus(x):
    return jnp.maximum(x, 0.0) + jnp.log1p(jnp.exp(-jnp.abs(x)))


def sigmoid(x):
    return 1.0 / (1.0 + jnp.exp(-x))


def rates_of(r_ref, rows, hp_ref, tri):
    raw = r_ref[rows, :].astype(F32) + hp_ref[0:1, :]
    dt = softplus(raw)
    lam = nn(tri, dt * hp_ref[1:2, :], HIGH)
    return raw, dt, lam


def spread(mat, h):
    return jnp.broadcast_to(mat[:, h : h + 1], (mat.shape[0], 128))


def scan_fwd_blocks(
    v_ref, s_ref, r_ref, kw_ref, hp_ref, ex_ref, mixed_ref, st_ref, buf, hst, xw_s, er_s, between
):
    blocks = v_ref.shape[0] // Q
    row = lax.broadcasted_iota(jnp.int32, (Q, Q), 0)
    col = lax.broadcasted_iota(jnp.int32, (Q, Q), 1)
    causal = row >= col
    tri = causal.astype(F32)
    low = lax.broadcasted_iota(jnp.int32, (Q, 128), 1) < HW
    low1 = lax.broadcasted_iota(jnp.int32, (1, 128), 1) < HW
    buf[0:8, :] = jnp.zeros((8, CH), F32)
    hst[...] = jnp.zeros_like(hst)

    def block(b, carry):
        rows = pl.ds(pl.multiple_of(b * Q, Q), Q)
        buf[8 : 8 + Q, 0:W] = v_ref[rows, :].astype(F32)
        buf[8 : 8 + Q, W:CH] = s_ref[rows, :].astype(F32)
        k = kw_ref[4:5, :] + buf[5 : 5 + Q, :] * kw_ref[0:1, :]
        for j in range(1, 4):
            k = k + buf[5 + j : 5 + j + Q, :] * kw_ref[j : j + 1, :]
        buf[0:8, :] = buf[Q : Q + 8, :]
        x = k * sigmoid(k)
        bs, cs = x[:, W : W + STATE], x[:, W + STATE :]
        _, dt, lam = rates_of(r_ref, rows, hp_ref, tri)
        lam_t, dt_t = lam.T, dt.T
        last = lam[Q - 1 : Q, :]
        tail = dt * jnp.exp(last - lam)
        aff = nt(cs, bs, HIGH)
        st_ref[b] = hst[...].astype(BF16)
        ch = nn(cs.astype(BF16), st_ref[b])
        for i in range(HL // 2):
            at = slice(128 * i, 128 * i + 128)
            xp = x[:, at]
            xb = xp.astype(BF16)
            y, lc = [], []
            for h in (2 * i, 2 * i + 1):
                lcol = spread(lam, h)
                within = jnp.exp(jnp.where(causal, lcol - lam_t[h : h + 1, :], -1e30))
                y.append(nn((aff * within * dt_t[h : h + 1, :]).astype(BF16), xb))
                lc.append(lcol)
            out = jnp.where(low, y[0], y[1])
            out = out + jnp.exp(jnp.where(low, lc[0], lc[1])) * ch[:, at] + ex_ref[0:1, at] * xp
            mixed_ref[rows, at] = out.astype(BF16)
            xw_s[:, at] = (xp * jnp.where(low, spread(tail, 2 * i), spread(tail, 2 * i + 1))).astype(BF16)
            er_s[0:1, at] = jnp.exp(jnp.where(low1, spread(last, 2 * i), spread(last, 2 * i + 1)))
        hst[...] = hst[...] * er_s[0:1, :] + nn(bs.T.astype(BF16), xw_s[...])
        between(b)
        return carry

    lax.fori_loop(0, blocks, block, 0)


def scan_bwd_blocks(
    v_ref, s_ref, r_ref, dy_ref, st_ref, kw_ref, hp_ref, ex_ref,
    dv_ref, gcw_ref, gch_ref, ghd_ref,
    buf, cbuf, dhst, rowp, xw_s, e_s, er_s, between,
):
    blocks = v_ref.shape[0] // Q
    row = lax.broadcasted_iota(jnp.int32, (Q, Q), 0)
    col = lax.broadcasted_iota(jnp.int32, (Q, Q), 1)
    tri = (row >= col).astype(F32)
    later = col >= row
    suffix = later.astype(F32)
    strict = (col < row).astype(F32)
    lane = lax.broadcasted_iota(jnp.int32, (Q, 128), 1)
    lane1 = lax.broadcasted_iota(jnp.int32, (1, 128), 1)
    low = lane < HW
    low1 = lane1 < HW
    buf[Q : Q + 8, :] = jnp.zeros((8, CH), F32)
    dhst[...] = jnp.zeros_like(dhst)
    rowp[...] = jnp.zeros_like(rowp)
    gcw_ref[...] = jnp.zeros_like(gcw_ref)
    gch_ref[...] = jnp.zeros_like(gch_ref)
    ghd_ref[...] = jnp.zeros_like(ghd_ref)

    def block(i0, carry):
        b = blocks - 1 - i0
        rows = pl.ds(pl.multiple_of(b * Q, Q), Q)
        before = pl.ds(pl.multiple_of(jnp.maximum(b * Q - 16, 0), 16), 16)
        keep = (b > 0).astype(F32)
        cbuf[0:8, 0:W] = v_ref[before, :].astype(F32)[8:16, :] * keep
        cbuf[0:8, W:CH] = s_ref[before, :].astype(F32)[8:16, :] * keep
        cbuf[8 : 8 + Q, 0:W] = v_ref[rows, :].astype(F32)
        cbuf[8 : 8 + Q, W:CH] = s_ref[rows, :].astype(F32)
        k = kw_ref[4:5, :] + cbuf[5 : 5 + Q, :] * kw_ref[0:1, :]
        for j in range(1, 4):
            k = k + cbuf[5 + j : 5 + j + Q, :] * kw_ref[j : j + 1, :]
        sg = sigmoid(k)
        x = k * sg
        ds = sg * (1.0 + k * (1.0 - sg))
        bs, cs = x[:, W : W + STATE], x[:, W + STATE :]
        bb, cb = bs.astype(BF16), cs.astype(BF16)
        raw, dt, lam = rates_of(r_ref, rows, hp_ref, tri)
        lam_t = lam.T
        last = lam[Q - 1 : Q, :]
        aff_t = nt(bs, cs, HIGH)
        hb = st_ref[b]
        dhb = dhst[...].astype(BF16)
        ch = nn(cb, hb)
        bd = nn(bb, dhb)
        daff_t = jnp.zeros((Q, Q), F32)
        col_n = jnp.zeros((Q, 128), F32)
        col_i = jnp.zeros((Q, 128), F32)
        row_i = jnp.zeros((Q, 128), F32)
        through = jnp.zeros((1, 128), F32)
        for i in range(HL // 2):
            at = slice(128 * i, 128 * i + 128)
            xp = x[:, at]
            xb = xp.astype(BF16)
            dyb = dy_ref[rows, at]
            dyf = dyb.astype(F32)
            z, lc, dc = [], [], []
            for h in (2 * i, 2 * i + 1):
                mine = low if h % 2 == 0 else jnp.logical_not(low)
                lcol, dcol = spread(lam, h), spread(dt, h)
                within = jnp.exp(jnp.where(later, lam_t[h : h + 1, :] - lcol, -1e30))
                g = nt(jnp.where(mine, xp, 0.0).astype(BF16), dyb)
                lg = within * g
                lgd = lg * dcol
                daff_t = daff_t + lgd
                col_n = jnp.where(lane == h, jnp.sum(aff_t * lg, axis=1, keepdims=True), col_n)
                rowp[h : h + 1, :] = jnp.sum(aff_t * lgd, axis=0, keepdims=True)
                z.append(nn((aff_t * within).astype(BF16), dyb))
                lc.append(lcol)
                dc.append(dcol)
            lamp = jnp.where(low, lc[0], lc[1])
            dtp = jnp.where(low, dc[0], dc[1])
            lastp = jnp.where(low1, spread(last, 2 * i), spread(last, 2 * i + 1))
            e = dyf * jnp.exp(lamp)
            e_s[:, at] = e.astype(BF16)
            ew = jnp.exp(lastp - lamp)
            bdp = bd[:, at]
            xw_s[:, at] = (xp * (dtp * ew)).astype(BF16)
            er_s[0:1, at] = jnp.exp(lastp)
            re = e * ch[:, at]
            ci = xp * bdp * ew
            th = jnp.sum(dhst[:, at] * hb[:, at].astype(F32), axis=0, keepdims=True) * er_s[0:1, at]
            for h in (2 * i, 2 * i + 1):
                mine = low if h % 2 == 0 else jnp.logical_not(low)
                mine1 = low1 if h % 2 == 0 else jnp.logical_not(low1)
                row_i = jnp.where(lane == h, jnp.sum(jnp.where(mine, re, 0.0), axis=1, keepdims=True), row_i)
                col_i = jnp.where(lane == h, jnp.sum(jnp.where(mine, ci, 0.0), axis=1, keepdims=True), col_i)
                through = jnp.where(
                    lane1 == h, jnp.sum(jnp.where(mine1, th, 0.0), axis=1, keepdims=True), through
                )
            dx = dtp * jnp.where(low, z[0], z[1]) + bdp * (dtp * ew) + ex_ref[0:1, at] * dyf
            gch_ref[0:1, at] += jnp.sum(dyf * xp, axis=0, keepdims=True)
            buf[0:Q, at] = dx * ds[:, at]
        daff_b = daff_t.astype(BF16)
        d_bs = nt(xw_s[...], dhb) + nn(daff_b, cb)
        d_cs = nt(e_s[...], hb) + nn(daff_t.T.astype(BF16), bb)
        buf[0:Q, W : W + STATE] = d_bs * ds[:, W : W + STATE]
        buf[0:Q, W + STATE : CH] = d_cs * ds[:, W + STATE :]
        dhst[...] = dhst[...] * er_s[0:1, :] + nn(cs.T.astype(BF16), e_s[...])
        after = nn(suffix, rowp[...].T - dt * col_n + row_i, HIGH) + nn(strict, dt * col_i, HIGH) + through
        d_rate = (col_n + col_i + hp_ref[1:2, :] * after) * sigmoid(raw)
        ghd_ref[0:1, :] += jnp.sum(d_rate, axis=0, keepdims=True)
        ghd_ref[1:2, :] += jnp.sum(dt * after, axis=0, keepdims=True) * hp_ref[1:2, :]
        dv_ref[rows, CH:VC] = d_rate.astype(BF16)
        for at in (slice(0, W), slice(W, CH)):
            raw_v = cbuf[8 : 8 + Q, at]
            dk = buf[0:Q, at]
            dv = dk * kw_ref[3:4, at]
            gcw_ref[4:5, at] += jnp.sum(dk, axis=0, keepdims=True)
            gcw_ref[3:4, at] += jnp.sum(dk * raw_v, axis=0, keepdims=True)
            for j in range(3):
                dk = buf[3 - j : 3 - j + Q, at]
                dv = dv + dk * kw_ref[j : j + 1, at]
                gcw_ref[j : j + 1, at] += jnp.sum(dk * raw_v, axis=0, keepdims=True)
            dv_ref[rows, at] = dv.astype(BF16)
        buf[Q : Q + 8, :] = buf[0:8, :]
        between(i0)
        return carry

    lax.fori_loop(0, blocks, block, 0)


GROUPS = 4


def place(block, at, width):
    start, shift = at // 128 * 128, at % 128
    lanes = -(-(width + shift) // 128) * 128
    have = block.shape[1]
    if lanes > have:
        block = jnp.concatenate([block, jnp.zeros((block.shape[0], lanes - have), block.dtype)], axis=1)
    else:
        block = block[:, :lanes]
    if shift:
        block = pltpu.roll(block, shift, 1)
    return start, lanes, block


def front_kernel(
    nf, tok, cot, win, wst, wout, small,
    x_out, cot_out, nrm_out, wv_out, ws_out, wg_out, wo_out, mix_out, gate_out, mixed_out, st_out, dsh_out,
    kw_s, hp_s, ex_s, pre_s, stat_s,
    x_s, cot_s, nrm_s, wv_s, ws_s, wg_s, wo_s, mix_s, gate_s, mixed_s, st_s, dsh_s,
    small_s, conv_s, post_s, stat_own, stat_got,
    buf, hst, xw_s, er_s,
    xs, xr, zs, zr, ms, mr, es, er, ls, os_,
):
    s = lax.axis_index("seq")
    f = lax.axis_index("fsdp")
    px, py = s ^ 1, s ^ 2
    nl = nf // 2
    p, c = f // 2, f % 2
    partner = p * 2 + 1 - c
    bar = pltpu.get_barrier_semaphore()
    for k in range(1, SEQ):
        signal(bar, {"seq": s ^ k})
    for k in range(1, nf):
        signal(bar, {"fsdp": lax.rem(f + k, nf)})
    pl.semaphore_wait(bar, nf - 1 + SEQ - 1)

    n = win.shape[0]
    rows = tok.shape[0]
    length = rows * SEQ
    ins = (
        win.at[:, pl.ds(pl.multiple_of(INNER + s * W, 128), W)],
        wst,
        win.at[:, pl.ds(pl.multiple_of(s * W, 128), W)],
        wout,
    )
    outs = (wv_s, ws_s, wg_s, wo_s)

    def row(g, i):
        return outs[g].at[pl.ds(i * n, n)]

    def hop(g, src, i, way, k, device):
        return rcopy(src, row(g, i), zs.at[g, way, k], zr.at[g, i], {"fsdp": device})

    def own_send(g):
        @pl.when(p < nl - 1)
        def _():
            hop(g, ins[g], f, 0, 0, f + 2).start()

        @pl.when(p > 0)
        def _():
            hop(g, ins[g], f, 1, 0, f - 2).start()

        hop(g, ins[g], f, 2, 0, partner).start()
        pltpu.make_async_copy(ins[g], row(g, f), ls.at[g]).start()

    def step(g, k):
        @pl.when(p - k >= 0)
        def _():
            o = f - 2 * k
            hop(g, row(g, o), o, 0, k, f).wait_recv()

            @pl.when(p < nl - 1)
            def _():
                hop(g, row(g, o), o, 0, k, f + 2).start()

            hop(g, row(g, o), o, 2, k, partner).start()

        @pl.when(p + k < nl)
        def _():
            o = f + 2 * k
            hop(g, row(g, o), o, 1, k, f).wait_recv()

            @pl.when(p > 0)
            def _():
                hop(g, row(g, o), o, 1, k, f - 2).start()

            hop(g, row(g, o), o, 3, k, partner).start()

    def arrive(g):
        pltpu.make_async_copy(ins[g], row(g, f), ls.at[g]).wait()
        for q in range(nl):
            o = q * 2 + 1 - c
            hop(g, row(g, o), o, 2, 0, partner).wait_recv()

    def sent(g):
        hop(g, ins[g], f, 2, 0, partner).wait_send()

        @pl.when(p < nl - 1)
        def _():
            hop(g, ins[g], f, 0, 0, f + 2).wait_send()

        @pl.when(p > 0)
        def _():
            hop(g, ins[g], f, 1, 0, f - 2).wait_send()

        for k in range(1, nl):
            @pl.when(p - k >= 0)
            def _():
                o = f - 2 * k

                @pl.when(p < nl - 1)
                def _():
                    hop(g, row(g, o), o, 0, k, f + 2).wait_send()

                hop(g, row(g, o), o, 2, k, partner).wait_send()

            @pl.when(p + k < nl)
            def _():
                o = f + 2 * k

                @pl.when(p > 0)
                def _():
                    hop(g, row(g, o), o, 1, k, f - 2).wait_send()

                hop(g, row(g, o), o, 3, k, partner).wait_send()

    def small_copy(k):
        return rcopy(small, small_s.at[f], ms.at[k], mr.at[k], {"fsdp": lax.rem(f + k, nf)})

    mine = pl.ds(s * rows, rows)
    own_small = pltpu.make_async_copy(small, small_s.at[f], ls.at[4])
    own_tok = pltpu.make_async_copy(tok, x_s.at[mine], ls.at[5])
    own_cot = pltpu.make_async_copy(cot, cot_s.at[mine], ls.at[6])

    for k in range(1, nf):
        small_copy(k).start()
    own_small.start()
    own_tok.start()
    seq_gather_start((tok,), (x_s,), xs, xr, px, py, s)
    own_send(0)
    own_send(1)
    own_cot.start()
    seq_gather_relay(0, tok, x_s, xs, xr, px, py, s)

    def cot_first():
        own = cot_s.at[mine]
        rcopy(cot, own, xs.at[1, 0], xr.at[1, 0], {"seq": px}).start()
        rcopy(cot, own, xs.at[1, 1], xr.at[1, 1], {"seq": py}).start()

    cot_first()
    step(0, 1)
    step(1, 1)
    own_send(2)

    own_small.wait()
    for k in range(1, nf):
        small_copy(k).wait()
    conv_s[...] = jnp.zeros_like(conv_s)
    pre_s[...] = jnp.zeros_like(pre_s)
    post_s[...] = jnp.zeros_like(post_s)
    heads = [jnp.zeros((8, 128), F32) for _ in range(3)]
    for i in range(nf):
        block = small_s[i]
        at, lanes, moved = place(block, i * (XBC // nf), XBC // nf)
        conv_s[:, at : at + lanes] += moved
        at, lanes, moved = place(block, i * (D // nf), D // nf)
        pre_s[:, at : at + lanes] += jnp.where(lax.broadcasted_iota(jnp.int32, moved.shape, 0) == 5, moved, 0.0)
        at, lanes, moved = place(block, i * (INNER // nf), INNER // nf)
        post_s[:, at : at + lanes] += jnp.where(lax.broadcasted_iota(jnp.int32, moved.shape, 0) == 6, moved, 0.0)
        for j in range(3):
            piece = block[:, 128 * j : 128 * j + 128]
            at = i * (HEADS // nf)
            heads[j] = heads[j] + (pltpu.roll(piece, at, 1) if at else piece)
    kw_s[:, 0:W] = conv_s[:, pl.ds(pl.multiple_of(s * W, 128), W)]
    kw_s[:, W:CH] = conv_s[:, INNER:XBC]
    lane1 = lax.broadcasted_iota(jnp.int32, (1, 128), 1)
    low1 = lane1 < HW
    back = lax.rem(128 - s * HL, 128)
    step_b, decay, skip = [pltpu.roll(h, back, 1)[7:8, :] for h in heads]
    hp_s[...] = jnp.zeros_like(hp_s)
    hp_s[0:1, :] = jnp.where(lane1 < HL, step_b, 0.0)
    hp_s[1:2, :] = jnp.where(lane1 < HL, -jnp.exp(decay), 0.0)
    ex_s[...] = jnp.zeros_like(ex_s)
    for i in range(HL // 2):
        ex_s[0:1, 128 * i : 128 * i + 128] = jnp.where(low1, spread(skip, 2 * i), spread(skip, 2 * i + 1))
    ex_s[1:2, :] = post_s[6:7, pl.ds(pl.multiple_of(s * W, 128), W)]

    for k in range(2, nl):
        step(0, k)
        step(1, k)
    own_tok.wait()
    seq_gather_finish(0, tok, x_s, xs, xr, px, py, s)
    seq_gather_relay(1, cot, cot_s, xs, xr, px, py, s)

    def norm(i, carry):
        r = pl.ds(pl.multiple_of(i * 128, 128), 128)
        x = x_s[r, :].astype(F32)
        rho = lax.rsqrt(jnp.sum(x * x, axis=1, keepdims=True) * (1.0 / D) + EPS)
        nrm_s[r, :] = (x * rho * pre_s[5:6, :]).astype(BF16)
        return carry

    lax.fori_loop(0, length // 128, norm, 0)
    step(2, 1)
    own_send(3)
    arrive(0)
    arrive(1)

    saves = [
        pltpu.make_async_copy(a, b, os_.at[i])
        for i, (a, b) in enumerate(
            (
                (x_s, x_out), (cot_s, cot_out), (nrm_s, nrm_out), (wv_s, wv_out), (ws_s, ws_out), (wg_s, wg_out),
                (wo_s, wo_out), (mix_s, mix_out), (gate_s, gate_out), (mixed_s, mixed_out), (st_s, st_out),
                (dsh_s, dsh_out),
            )
        )
    ]
    for i in (0, 2, 3, 4):
        saves[i].start()

    def project(i, carry):
        r = pl.ds(pl.multiple_of(i * 256, 256), 256)
        a = nrm_s[r, :]
        mix_s[r, 0:W] = nn(a, wv_s[...]).astype(BF16)
        mix_s[r, W:VC] = nn(a, ws_s[...]).astype(BF16)
        return carry

    lax.fori_loop(0, length // 256, project, 0)
    saves[7].start()

    def between(b):
        @pl.when(b == 0)
        def _():
            step(2, 2)

        @pl.when(b == 3)
        def _():
            for k in range(3, nl):
                step(2, k)

        @pl.when(b == 6)
        def _():
            step(3, 1)

    scan_fwd_blocks(
        mix_s.at[:, 0:W], mix_s.at[:, W:CH], mix_s.at[:, CH:VC], kw_s, hp_s, ex_s, mixed_s, st_s,
        buf, hst, xw_s, er_s, between,
    )
    for i in (9, 10):
        saves[i].start()
    arrive(2)
    saves[5].start()

    def project_gate(i, carry):
        r = pl.ds(pl.multiple_of(i * 256, 256), 256)
        gate_s[r, :] = nn(nrm_s[r, :], wg_s[...]).astype(BF16)
        return carry

    step(3, 2)
    lax.fori_loop(0, length // 256, project_gate, 0)
    saves[8].start()
    for k in range(3, nl):
        step(3, k)
    own_cot.wait()
    seq_gather_finish(1, cot, cot_s, xs, xr, px, py, s)
    saves[1].start()
    arrive(3)
    saves[6].start()
    eye = lax.broadcasted_iota(jnp.int32, (128, 128), 0) == lax.broadcasted_iota(jnp.int32, (128, 128), 1)

    def stats(i, carry):
        r = pl.ds(pl.multiple_of(i * 128, 128), 128)
        dsh = nn(cot_s[r, :], wo_s[...])
        dsh_s[r, :] = dsh
        gate = gate_s[r, :].astype(F32)
        gated = mixed_s[r, :].astype(F32) * (gate * sigmoid(gate))
        one = jnp.sum(gated * gated, axis=1, keepdims=True)
        two = jnp.sum(dsh * ex_s[1:2, :] * gated, axis=1, keepdims=True)
        stat_own[pl.ds(i, 1), :] = jnp.sum(jnp.where(eye, one, 0.0), axis=0, keepdims=True)
        stat_own[pl.ds(length // 128 + i, 1), :] = jnp.sum(jnp.where(eye, two, 0.0), axis=0, keepdims=True)
        return carry

    lax.fori_loop(0, length // 128, stats, 0)
    saves[11].start()
    copies = [rcopy(stat_own, stat_got.at[k], es.at[k], er.at[k], {"seq": s ^ k}) for k in range(1, SEQ)]
    for copy in copies:
        copy.start()
    for copy in copies:
        copy.wait()
    stat_s[...] = stat_own[...] + stat_got[1] + (stat_got[2] + stat_got[3])
    for g in range(GROUPS):
        sent(g)
    for save in saves:
        save.wait()


def front(nf, tok, cot, win, wst, wout, small):
    shape = jax.ShapeDtypeStruct
    dma = pltpu.SemaphoreType.DMA
    length = SEQ * tok.shape[0]
    big = [
        shape((length, D), BF16),
        shape((length, D), BF16),
        shape((length, D), BF16),
        shape((D, W), BF16),
        shape((D, VC - W), BF16),
        shape((D, W), BF16),
        shape((D, W), BF16),
        shape((length, VC), BF16),
        shape((length, W), BF16),
        shape((length, W), BF16),
        shape((length // Q, STATE, W), BF16),
        shape((length, W), F32),
    ]
    par = [
        shape((8, CH), F32),
        shape((8, 128), F32),
        shape((8, W), F32),
        shape((8, D), F32),
        shape((2 * length // 128, 128), F32),
    ]
    return pl.pallas_call(
        functools.partial(front_kernel, nf),
        out_shape=big + par,
        in_specs=[ANY] * 5 + [VMEM],
        out_specs=[ANY] * len(big) + [VMEM] * len(par),
        scratch_shapes=[pltpu.VMEM(b.shape, b.dtype) for b in big]
        + [
            pltpu.VMEM((nf, 8, 512), F32),
            pltpu.VMEM((8, XBC), F32),
            pltpu.VMEM((8, INNER), F32),
            pltpu.VMEM((2 * length // 128, 128), F32),
            pltpu.VMEM((SEQ, 2 * length // 128, 128), F32),
            pltpu.VMEM((Q + 8, CH), F32),
            pltpu.VMEM((STATE, W), F32),
            pltpu.VMEM((Q, W), BF16),
            pltpu.VMEM((8, W), F32),
            dma((2, 4)),
            dma((2, 4)),
            dma((GROUPS, 4, nf // 2)),
            dma((GROUPS, nf)),
            dma((nf,)),
            dma((nf,)),
            dma((SEQ,)),
            dma((SEQ,)),
            dma((7,)),
            dma((len(big),)),
        ],
        name="front",
        compiler_params=pltpu.CompilerParams(
            collective_id=1, has_side_effects=True, vmem_limit_bytes=VMEM_LIMIT
        ),
    )(tok, cot, win, wst, wout, small)


TN = (((0,), (0,)), ((), ()))
STRIP = 384


def unplace(block, at, width):
    start, shift = at // 128 * 128, at % 128
    lanes = -(-(width + shift) // 128) * 128
    piece = block[:, start : start + lanes]
    if shift:
        piece = pltpu.roll(piece, lanes - shift, 1)
    if lanes < 512:
        piece = jnp.concatenate([piece, jnp.zeros((piece.shape[0], 512 - lanes), piece.dtype)], axis=1)
    else:
        piece = piece[:, :512]
    return jnp.where(lax.broadcasted_iota(jnp.int32, piece.shape, 1) < width, piece, 0.0)


def back_kernel(
    nf, x_in, cot_in, nrm_in, wv_in, ws_in, wg_in, wo_in, mix_in, gate_in, mixed_in, st_in, dsh_in,
    kw_s, hp_s, ex_s, pre_s, stat_s,
    out_ref, gt_ref, go_ref, gg_ref, gv_ref, gs_ref, small_ref,
    xc_s, nrm_s, wv_s, ws_s, wg_s, wo_s, mix_s, gate_s, mixed_s, st_s, dsh_s,
    dy_s, dv_s, cotrow_s, part_s, ga_s, gb_s, gc_s,
    pb0, pb1, pb2, pb3, lb0, lb1, lb2, lb3, own0, own1, own2, own3,
    ab0, ab1, az0, az1,
    gcw_s, gch_s, ghd_s, gpost_s, gpre_s, conv_s, post_s, snd_s, got_s, sown_s, sgot_s,
    buf, cbuf, dhst, rowp, xw_s, e_s, er_s,
    ls, zs, zr, xs, xr, as_, ar, ms, mr, es, er, os_,
):
    s = lax.axis_index("seq")
    f = lax.axis_index("fsdp")
    px, py = s ^ 1, s ^ 2
    nl = nf // 2
    p, c = f // 2, f % 2
    partner = p * 2 + 1 - c
    bar = pltpu.get_barrier_semaphore()
    for k in range(1, SEQ):
        signal(bar, {"seq": s ^ k})
    for k in range(1, nf):
        signal(bar, {"fsdp": lax.rem(f + k, nf)})

    length = nrm_s.shape[0]
    rows = length // SEQ
    n = D // nf
    mine = pl.ds(s * rows, rows)
    loads = [
        pltpu.make_async_copy(a, b, ls.at[i])
        for i, (a, b) in enumerate(
            (
                (gate_in, gate_s), (mixed_in, mixed_s), (dsh_in, dsh_s), (cot_in, xc_s), (wo_in, wo_s),
                (nrm_in, nrm_s), (mix_in, mix_s), (st_in, st_s), (wg_in, wg_s), (wv_in, wv_s), (ws_in, ws_s),
                (cot_in.at[mine], cotrow_s), (x_in, xc_s),
            )
        )
    ]
    for load in loads[:-1]:
        load.start()
    pl.semaphore_wait(bar, nf - 1 + SEQ - 1)

    half = D // 2
    cols = (slice(0, half), slice(half, D))
    first, second = (px, py), (py, px)
    ab, az = (ab0, ab1), (az0, az1)

    def chunk(i, a):
        return part_s.at[pl.ds(i * rows, rows), cols[a]]

    def seq_one(t, a, m):
        i = (first[a] ^ second[a] ^ s) if m == 0 else first[a]
        return rcopy(chunk(i, a), ab[t].at[a, m], xs.at[t, a, m], xr.at[t, a, m], {"seq": first[a]})

    def seq_two(t, a):
        return rcopy(az[t].at[a, 0], az[t].at[a, 1], xs.at[t, a, 2], xr.at[t, a, 2], {"seq": second[a]})

    def add(*terms):
        total = terms[0].astype(F32)
        for term in terms[1:]:
            total = total + term.astype(F32)
        return total

    def seq_pass(t):
        for a in range(2):
            seq_one(t, a, 0).wait_recv()
            az[t][a, 0] = add(chunk(second[a], a)[...], ab[t][a, 0]).astype(BF16)
            seq_two(t, a).start()

    def seq_last(t, out):
        for a in range(2):
            seq_one(t, a, 1).wait_recv()
            seq_two(t, a).wait_recv()
            out[:, cols[a]] = add(chunk(s, a)[...], ab[t][a, 1], az[t][a, 1])

    def seq_sent(t):
        for a in range(2):
            seq_one(t, a, 0).wait_send()
            seq_one(t, a, 1).wait_send()
            seq_two(t, a).wait_send()

    parts = (ga_s, gb_s, ga_s, gc_s)
    pbs, lbs, owns = (pb0, pb1, pb2, pb3), (lb0, lb1, lb2, lb3), (own0, own1, own2, own3)
    gouts = (go_ref, gg_ref, gv_ref, gs_ref)

    def piece(g, i):
        return parts[g].at[pl.ds(pl.multiple_of(i * n, 16), n)]

    def swap(g, q):
        return rcopy(piece(g, q * 2 + 1 - c), pbs[g].at[q], zs.at[g, 0, q], zr.at[g, 0, q], {"fsdp": partner})

    def up(g, q):
        return rcopy(pbs[g].at[q], lbs[g].at[q], zs.at[g, 1, q], zr.at[g, 1, q], {"fsdp": f + 2})

    def down(g, q):
        to = jnp.where(q == p - 1, nl, q)
        return rcopy(pbs[g].at[q], lbs[g].at[to], zs.at[g, 2, q], zr.at[g, 2, q], {"fsdp": f - 2})

    def slot(g, t):
        @pl.when(p <= t)
        def _():
            q = nl - 1 - t + p
            swap(g, q).wait_recv()

            @pl.when(p > 0)
            def _():
                up(g, q).wait_recv()
                pbs[g][q] = add(piece(g, q * 2 + c)[...], pbs[g][q], lbs[g][q]).astype(BF16)

            @pl.when(p == 0)
            def _():
                pbs[g][q] = add(piece(g, q * 2 + c)[...], pbs[g][q]).astype(BF16)

            up(g, q).start()

        @pl.when(nl - 1 - p <= t)
        def _():
            q = t - (nl - 1 - p)
            swap(g, q).wait_recv()

            @pl.when(p < nl - 1)
            def _():
                down(g, q).wait_recv()
                pbs[g][q] = add(piece(g, q * 2 + c)[...], pbs[g][q], lbs[g][q]).astype(BF16)

            @pl.when(p == nl - 1)
            def _():
                pbs[g][q] = add(piece(g, q * 2 + c)[...], pbs[g][q]).astype(BF16)

            down(g, q).start()

    def close(g):
        swap(g, p).wait_recv()

        @pl.when(p > 0)
        def _():
            up(g, p).wait_recv()

        @pl.when(p < nl - 1)
        def _():
            down(g, p).wait_recv()

        @pl.when(p == 0)
        def _():
            owns[g][...] = add(piece(g, f)[...], pbs[g][p], lbs[g][nl]).astype(BF16)

        @pl.when(p == nl - 1)
        def _():
            owns[g][...] = add(piece(g, f)[...], pbs[g][p], lbs[g][p]).astype(BF16)

        @pl.when(jnp.logical_and(p > 0, p < nl - 1))
        def _():
            owns[g][...] = add(piece(g, f)[...], pbs[g][p], lbs[g][p], lbs[g][nl]).astype(BF16)

        place_ = gouts[g].at[pl.ds(s * n, n)]
        rcopy(owns[g], place_, as_.at[g, 0], ar.at[g, 0], {"seq": px}).start()
        rcopy(owns[g], place_, as_.at[g, 1], ar.at[g, 1], {"seq": py}).start()
        pltpu.make_async_copy(owns[g], place_, os_.at[g]).start()

    def relay(g):
        seq_gather_relay(g, owns[g], gouts[g], as_, ar, px, py, s)

    def swaps_sent(g):
        for q in range(nl):
            swap(g, q).wait_send()

    def line_sent(g):
        for q in range(nl):
            @pl.when(q > p)
            def _():
                up(g, q).wait_send()

            @pl.when(q < p)
            def _():
                down(g, q).wait_send()

    order = []
    for k in range(D // STRIP // 2):
        order += [D // STRIP - 1 - k, k]

    def strip(j, a_ref, b_ref, bcols, g):
        at = slice(j * STRIP, (j + 1) * STRIP)
        parts[g][at, :] = lax.dot_general(a_ref[:, at], b_ref[:, bcols], TN, preferred_element_type=F32).astype(BF16)
        for q in range(nl):
            if j * STRIP <= q * 2 * n < (j + 1) * STRIP:
                swap(g, q).start()

    for i in range(3):
        loads[i].wait()
    eye = lax.broadcasted_iota(jnp.int32, (128, 128), 0) == lax.broadcasted_iota(jnp.int32, (128, 128), 1)
    gpost_s[...] = jnp.zeros_like(gpost_s)

    def gated_norm(i, carry):
        r = pl.ds(pl.multiple_of(i * 128, 128), 128)
        one = jnp.sum(jnp.where(eye, stat_s[pl.ds(i, 1), :], 0.0), axis=1, keepdims=True)
        two = jnp.sum(jnp.where(eye, stat_s[pl.ds(length // 128 + i, 1), :], 0.0), axis=1, keepdims=True)
        rho = lax.rsqrt(one * (1.0 / INNER) + EPS)
        mean = rho * two * (1.0 / INNER)
        gate = gate_s[r, :].astype(F32)
        mixed = mixed_s[r, :].astype(F32)
        dsh = dsh_s[r, :]
        post = ex_s[1:2, :]
        sg = sigmoid(gate)
        sl = gate * sg
        n1 = mixed * sl * rho
        gpost_s[0:1, :] += jnp.sum(dsh * n1, axis=0, keepdims=True)
        d_gated = rho * (dsh * post - n1 * mean)
        mixed_s[r, :] = (n1 * post).astype(BF16)
        dy_s[r, :] = (d_gated * sl).astype(BF16)
        gate_s[r, :] = (d_gated * mixed * (sg * (1.0 + gate * (1.0 - sg)))).astype(BF16)
        return carry

    lax.fori_loop(0, length // 128, gated_norm, 0)

    every = slice(0, W)
    loads[3].wait()
    for j in order:
        strip(j, xc_s, mixed_s, every, 0)
    loads[-1].start()
    slot(0, 0)

    loads[4].wait()

    def out_part(i, carry):
        r = pl.ds(pl.multiple_of(i * rows, rows), rows)
        part_s[r, :] = nt(mixed_s[r, :], wo_s[...]).astype(BF16)
        return carry

    lax.fori_loop(0, SEQ, out_part, 0)
    for m in range(2):
        for a in range(2):
            seq_one(0, a, m).start()

    loads[5].wait()
    for j in order:
        strip(j, nrm_s, gate_s, every, 1)
    slot(0, 1)
    slot(1, 0)
    loads[6].wait()
    loads[7].wait()

    def between(i):
        @pl.when(i == 1)
        def _():
            for t in range(2, nl - 1):
                slot(0, t)

        @pl.when(i == 2)
        def _():
            seq_pass(0)

        @pl.when(i == 3)
        def _():
            close(0)
            slot(1, 1)

        @pl.when(i == 5)
        def _():
            for t in range(2, nl - 1):
                slot(1, t)
            relay(0)

    scan_bwd_blocks(
        mix_s.at[:, 0:W], mix_s.at[:, W:CH], mix_s.at[:, CH:VC], dy_s, st_s, kw_s, hp_s, ex_s,
        dv_s, gcw_s, gch_s, ghd_s, buf, cbuf, dhst, rowp, xw_s, e_s, er_s, between,
    )

    loads[-1].wait()
    out_ref[...] = xc_s[mine, :].astype(F32)
    for a in range(2):
        seq_one(0, a, 1).wait_recv()
        seq_two(0, a).wait_recv()
        out_ref[:, cols[a]] += add(chunk(s, a)[...], ab0[a, 1], az0[a, 1])
    seq_sent(0)
    close(1)
    swaps_sent(0)
    for i, j in enumerate(order):
        strip(j, nrm_s, dv_s, every, 2)
        strip(j, nrm_s, dv_s, slice(W, VC), 3)
        if i == 1:
            slot(2, 0)
            slot(3, 0)
    relay(1)

    for i in range(8, 12):
        loads[i].wait()
    gpre_s[...] = jnp.zeros_like(gpre_s)

    def dn_part(i, carry):
        r = pl.ds(pl.multiple_of((s ^ (SEQ - 1 - i)) * rows, rows), rows)
        dn = nt(gate_s[r, :], wg_s[...]) + nt(dv_s[r, 0:W], wv_s[...]) + nt(dv_s[r, W:VC], ws_s[...])
        part_s[r, :] = dn.astype(BF16)
        x = xc_s[r, :].astype(F32)
        rho = lax.rsqrt(jnp.sum(x * x, axis=1, keepdims=True) * (1.0 / D) + EPS)
        gpre_s[5:6, :] += jnp.sum(dn * (x * rho), axis=0, keepdims=True)

        @pl.when(i == 0)
        def _():
            for a in range(2):
                seq_one(1, a, 0).start()

        @pl.when(i == 2)
        def _():
            for a in range(2):
                seq_one(1, a, 1).start()
            for g in (2, 3):
                for t in range(1, min(2, nl - 1)):
                    slot(g, t)

        return carry

    lax.fori_loop(0, SEQ, dn_part, 0)

    conv_s[...] = jnp.zeros_like(conv_s)
    conv_s[:, pl.ds(pl.multiple_of(s * W, 128), W)] = gcw_s[:, 0:W]
    conv_s[:, INNER:XBC] = gcw_s[:, W:CH]
    post_s[...] = jnp.zeros_like(post_s)
    post_s[6:7, pl.ds(pl.multiple_of(s * W, 128), W)] = gpost_s[0:1, :]
    lane8 = lax.broadcasted_iota(jnp.int32, (8, 128), 1)
    row8 = lax.broadcasted_iota(jnp.int32, (8, 128), 0)
    skip = jnp.zeros((1, 128), F32)
    lane1 = lax.broadcasted_iota(jnp.int32, (1, 128), 1)
    for h in range(HL):
        at = slice(128 * (h // 2), 128 * (h // 2) + 128)
        half_of = (lane1 < HW) if h % 2 == 0 else (lane1 >= HW)
        skip = jnp.where(lane1 == h, jnp.sum(jnp.where(half_of, gch_s[0:1, at], 0.0), axis=1, keepdims=True), skip)
    heads = [
        pltpu.roll(jnp.where(row8 == 7, jnp.broadcast_to(v, (8, 128)), 0.0), s * HL, 1)
        for v in (ghd_s[0:1, :], ghd_s[1:2, :], skip)
    ]
    row512 = lax.broadcasted_iota(jnp.int32, (8, 512), 0)
    hn = HEADS // nf
    for i in range(nf):
        conv = unplace(conv_s, i * (XBC // nf), XBC // nf)
        block = jnp.where(row512 < 5, conv, 0.0)
        block = block + unplace(gpre_s, i * (D // nf), D // nf)
        block = block + unplace(post_s, i * (INNER // nf), INNER // nf)
        tiles = []
        for v in heads:
            moved = pltpu.roll(v, (128 - i * hn) % 128, 1) if i else v
            tiles.append(jnp.where(lane8 < hn, moved, 0.0))
        block = block + jnp.concatenate(tiles + [jnp.zeros((8, 128), F32)], axis=1)
        snd_s[i] = block

    def small_send(k):
        to = lax.rem(f + k, nf)
        return rcopy(snd_s.at[to], got_s.at[k], ms.at[k], mr.at[k], {"fsdp": to})

    for k in range(1, nf):
        small_send(k).start()
    seq_pass(1)
    for g in (2, 3):
        for t in range(2, nl - 1):
            slot(g, t)
    total = snd_s[f]
    for k in range(1, nf):
        small_send(k).wait_recv()
        total = total + got_s[k]
    sown_s[...] = total

    def small_share(k):
        return rcopy(sown_s, sgot_s.at[s], es.at[k], er.at[k], {"seq": s ^ k})

    for k in range(1, SEQ):
        small_share(k).start()
    close(2)
    close(3)
    relay(2)
    relay(3)

    for a in range(2):
        seq_one(1, a, 1).wait_recv()
        seq_two(1, a).wait_recv()
        gt_ref[:, cols[a]] = add(chunk(s, a)[...], ab1[a, 1], az1[a, 1])

    def grad_tokens(i, carry):
        r = pl.ds(pl.multiple_of(i * 64, 64), 64)
        x = xc_s[pl.ds(pl.multiple_of(s * rows + i * 64, 64), 64), :].astype(F32)
        rho = lax.rsqrt(jnp.sum(x * x, axis=1, keepdims=True) * (1.0 / D) + EPS)
        n0 = x * rho
        e0 = gt_ref[r, :] * pre_s[5:6, :]
        mean = jnp.sum(e0 * n0, axis=1, keepdims=True) * (1.0 / D)
        gt_ref[r, :] = cotrow_s[r, :].astype(F32) + rho * (e0 - n0 * mean)
        return carry

    lax.fori_loop(0, rows // 64, grad_tokens, 0)

    for k in range(1, SEQ):
        small_share(k).wait()
    total = jnp.zeros_like(sown_s)
    for k in range(SEQ):
        total = total + jnp.where(s == k, sown_s[...], sgot_s[k])
    small_ref[...] = total
    for k in range(1, nf):
        small_send(k).wait_send()
    seq_sent(1)
    for g in range(4):
        seq_gather_finish(g, owns[g], gouts[g], as_, ar, px, py, s)
        pltpu.make_async_copy(owns[g], gouts[g].at[pl.ds(s * n, n)], os_.at[g]).wait()
        line_sent(g)
    for g in range(1, 4):
        swaps_sent(g)


def back(nf, big, par):
    shape = jax.ShapeDtypeStruct
    vm = pltpu.VMEM
    dma = pltpu.SemaphoreType.DMA
    length = big[0].shape[0]
    rows = length // SEQ
    nl = nf // 2
    n = D // nf
    widths = (W, W, W, VC - W)
    boxes = [vm((nl, n, w), BF16) for w in widths] + [vm((nl + 1, n, w), BF16) for w in widths]
    boxes += [vm((n, w), BF16) for w in widths]
    return pl.pallas_call(
        functools.partial(back_kernel, nf),
        out_shape=[shape((rows, D), F32)] * 2 + [shape((SEQ * n, w), BF16) for w in widths] + [shape((8, 512), F32)],
        in_specs=[ANY] * len(big) + [VMEM] * len(par),
        out_specs=[VMEM] * 2 + [ANY] * 4 + [VMEM],
        scratch_shapes=[
            vm((length, D), BF16),
            vm((length, D), BF16),
            vm((D, W), BF16),
            vm((D, VC - W), BF16),
            vm((D, W), BF16),
            vm((D, W), BF16),
            vm((length, VC), BF16),
            vm((length, W), BF16),
            vm((length, W), BF16),
            vm((length // Q, STATE, W), BF16),
            vm((length, W), F32),
            vm((length, W), BF16),
            vm((length, VC), BF16),
            vm((rows, D), BF16),
            vm((length, D), BF16),
            vm((D, W), BF16),
            vm((D, W), BF16),
            vm((D, VC - W), BF16),
        ]
        + boxes
        + [vm((2, 2, rows, D // 2), BF16)] * 4
        + [
            vm((8, CH), F32),
            vm((8, W), F32),
            vm((8, 128), F32),
            vm((8, W), F32),
            vm((8, D), F32),
            vm((8, XBC), F32),
            vm((8, INNER), F32),
            vm((nf, 8, 512), F32),
            vm((nf, 8, 512), F32),
            vm((8, 512), F32),
            vm((SEQ, 8, 512), F32),
            vm((Q + 8, CH), F32),
            vm((Q + 8, CH), F32),
            vm((STATE, W), F32),
            vm((128, Q), F32),
            vm((Q, W), BF16),
            vm((Q, W), BF16),
            vm((8, W), F32),
            dma((13,)),
            dma((4, 3, nl)),
            dma((4, 3, nl)),
            dma((2, 2, 3)),
            dma((2, 2, 3)),
            dma((4, 4)),
            dma((4, 4)),
            dma((nf,)),
            dma((nf,)),
            dma((SEQ,)),
            dma((SEQ,)),
            dma((4,)),
        ],
        name="back",
        compiler_params=pltpu.CompilerParams(
            collective_id=2, has_side_effects=True, vmem_limit_bytes=67043328
        ),
    )(*big, *par)


def own_rows(array, index, row_count):
    return lax.dynamic_slice_in_dim(array, index * row_count, row_count, 0)


def body(
    tokens,
    input_projection_weight,
    pre_gain,
    conv_weight,
    conv_bias,
    step_bias,
    decay_log,
    skip_gain,
    post_gain,
    output_projection_weight,
    cotangent,
):
    nf = lax.axis_size("fsdp")
    s = lax.axis_index("seq")
    tok = tokens.reshape(tokens.shape[1:])
    cot = cotangent.reshape(cotangent.shape[1:])
    win = input_projection_weight
    n = win.shape[0]

    w_state = jnp.concatenate(
        [
            win[:, 2 * INNER : 2 * INNER + 2 * STATE],
            lax.dynamic_slice(win, (0, 2 * INNER + 2 * STATE + s * HL), (n, HL)),
            jnp.zeros((n, 128 - HL), BF16),
        ],
        axis=1,
    )
    w_out = own_rows(output_projection_weight, s, W).T

    def line(*pieces):
        return jnp.concatenate([jnp.pad(v[None], ((0, 0), (0, 128 * t - v.shape[0]))) for v, t in pieces], axis=1)

    small = jnp.concatenate(
        [
            jnp.pad(conv_weight.T, ((0, 0), (0, 512 - conv_weight.shape[0]))),
            line((conv_bias, 4)),
            line((pre_gain, 4)),
            line((post_gain, 4)),
            line((step_bias, 1), (decay_log, 1), (skip_gain, 2)),
        ]
    ).astype(F32)
    outs = front(nf, tok, cot, win, w_state, w_out, small)
    block_out, grad_tokens, g_out, g_gate, g_val, g_state, small = back(nf, outs[:12], outs[12:])

    g_gate = g_gate.reshape(SEQ, n, W).astype(F32)
    g_val = g_val.reshape(SEQ, n, W).astype(F32)
    g_state = g_state.reshape(SEQ, n, VC - W).astype(F32)
    grad_in = jnp.concatenate(
        [g_gate[i] for i in range(SEQ)]
        + [g_val[i] for i in range(SEQ)]
        + [jnp.sum(g_state[:, :, : 2 * STATE], axis=0)]
        + [g_state[i, :, 2 * STATE : 2 * STATE + HL] for i in range(SEQ)],
        axis=1,
    )
    grad_out = jnp.swapaxes(g_out.reshape(SEQ, n, W), 1, 2).reshape(INNER, n).astype(F32)
    nc = XBC // nf
    nh = HEADS // nf
    grad_cw, grad_cb = small[:4, :nc].T, small[4, :nc]
    grad_pre, grad_post = small[5, :n], small[6, : INNER // nf]
    grad_step, grad_decay, grad_skip = [small[7, 128 * i : 128 * i + nh] for i in range(3)]
    return (
        block_out[None],
        grad_tokens[None],
        grad_in,
        grad_pre,
        grad_cw,
        grad_cb,
        grad_step,
        grad_decay,
        grad_skip,
        grad_post,
        grad_out,
    )


def solution(mesh):
    in_specs = (
        P("fsdp", "seq", None),
        P("fsdp", None),
        P("fsdp"),
        P("fsdp", None),
        P("fsdp"),
        P("fsdp"),
        P("fsdp"),
        P("fsdp"),
        P("fsdp"),
        P(None, "fsdp"),
        P("fsdp", "seq", None),
    )
    out_specs = (
        P("fsdp", "seq", None),
        P("fsdp", "seq", None),
        P("fsdp", None),
        P("fsdp"),
        P("fsdp", None),
        P("fsdp"),
        P("fsdp"),
        P("fsdp"),
        P("fsdp"),
        P("fsdp"),
        P(None, "fsdp"),
    )
    return jax.shard_map(body, mesh=mesh, in_specs=in_specs, out_specs=out_specs, check_vma=False)
```

```python
import functools

import jax
import jax.numpy as jnp
from jax import lax
from jax.experimental import pallas as pl
from jax.experimental.pallas import tpu as pltpu
from jax.sharding import PartitionSpec as P

D = 1536
INNER = 3072
STATE = 128
HEADS = 48
XBC = INNER + 2 * STATE
EPS = 1e-05

SEQ = 4
W = INNER // SEQ
HL = HEADS // SEQ
HW = INNER // HEADS
CH = W + 2 * STATE
VC = CH + 128
Q = 128

F32 = jnp.float32
BF16 = jnp.bfloat16
MESH = pl.DeviceIdType.MESH
HIGH = lax.Precision.HIGHEST
VMEM = pl.BlockSpec(memory_space=pltpu.VMEM)
ANY = pl.BlockSpec(memory_space=pl.ANY)
VMEM_LIMIT = 64000 * 1024


def rcopy(src, dst, send_sem, recv_sem, device):
    return pltpu.make_async_remote_copy(
        src_ref=src, dst_ref=dst, send_sem=send_sem, recv_sem=recv_sem, device_id=device, device_id_type=MESH
    )


def signal(sem, device):
    pl.semaphore_signal(sem, inc=1, device_id=device, device_id_type=MESH)


def nn(a, b, precision=None):
    return lax.dot_general(a, b, (((1,), (0,)), ((), ())), precision=precision, preferred_element_type=F32)


def nt(a, b, precision=None):
    return lax.dot_general(a, b, (((1,), (1,)), ((), ())), precision=precision, preferred_element_type=F32)


def seq_gather_start(refs, outs, send, recv, px, py, me):
    for g, (src, out) in enumerate(zip(refs, outs)):
        n = src.shape[0]
        own = out.at[pl.ds(me * n, n)]
        rcopy(src, own, send.at[g, 0], recv.at[g, 0], {"seq": px}).start()
        rcopy(src, own, send.at[g, 1], recv.at[g, 1], {"seq": py}).start()


def seq_gather_relay(g, src, out, send, recv, px, py, me):
    n = src.shape[0]
    h = n // 2
    own = out.at[pl.ds(me * n, n)]
    rcopy(src, own, send.at[g, 0], recv.at[g, 0], {"seq": px}).wait_recv()
    top = out.at[pl.ds(px * n, h)]
    rcopy(top, top, send.at[g, 2], recv.at[g, 2], {"seq": py}).start()
    rcopy(src, own, send.at[g, 1], recv.at[g, 1], {"seq": py}).wait_recv()
    low = out.at[pl.ds(py * n + h, h)]
    rcopy(low, low, send.at[g, 3], recv.at[g, 3], {"seq": px}).start()


def seq_gather_finish(g, src, out, send, recv, px, py, me):
    n = src.shape[0]
    h = n // 2
    own = out.at[pl.ds(me * n, n)]
    half = out.at[pl.ds(me * n, h)]
    rcopy(half, half, send.at[g, 2], recv.at[g, 2], {"seq": py}).wait()
    rcopy(half, half, send.at[g, 3], recv.at[g, 3], {"seq": px}).wait()
    rcopy(src, own, send.at[g, 0], recv.at[g, 0], {"seq": px}).wait_send()
    rcopy(src, own, send.at[g, 1], recv.at[g, 1], {"seq": py}).wait_send()


def softplus(x):
    return jnp.maximum(x, 0.0) + jnp.log1p(jnp.exp(-jnp.abs(x)))


def sigmoid(x):
    return 1.0 / (1.0 + jnp.exp(-x))


def rates_of(r_ref, rows, hp_ref, tri):
    back = lax.rem(128 - lax.axis_index("seq") * HL, 128)
    raw = pltpu.roll(r_ref[rows, :].astype(F32), back, 1) + hp_ref[0:1, :]
    dt = softplus(raw)
    lam = nn(tri, dt * hp_ref[1:2, :], HIGH)
    return raw, dt, lam


def spread(mat, h):
    return jnp.broadcast_to(mat[:, h : h + 1], (mat.shape[0], 128))


def scan_fwd_blocks(
    v_ref, s_ref, r_ref, kw_ref, hp_ref, ex_ref, mixed_ref, st_ref, buf, hst, xw_s, er_s, between
):
    blocks = v_ref.shape[0] // Q
    row = lax.broadcasted_iota(jnp.int32, (Q, Q), 0)
    col = lax.broadcasted_iota(jnp.int32, (Q, Q), 1)
    causal = row >= col
    tri = causal.astype(F32)
    low = lax.broadcasted_iota(jnp.int32, (Q, 128), 1) < HW
    low1 = lax.broadcasted_iota(jnp.int32, (1, 128), 1) < HW
    buf[0:8, :] = jnp.zeros((8, CH), F32)
    hst[...] = jnp.zeros_like(hst)

    def block(b, carry):
        rows = pl.ds(pl.multiple_of(b * Q, Q), Q)
        buf[8 : 8 + Q, 0:W] = v_ref[rows, :].astype(F32)
        buf[8 : 8 + Q, W:CH] = s_ref[rows, :].astype(F32)
        k = kw_ref[4:5, :] + buf[5 : 5 + Q, :] * kw_ref[0:1, :]
        for j in range(1, 4):
            k = k + buf[5 + j : 5 + j + Q, :] * kw_ref[j : j + 1, :]
        buf[0:8, :] = buf[Q : Q + 8, :]
        x = k * sigmoid(k)
        bs, cs = x[:, W : W + STATE], x[:, W + STATE :]
        _, dt, lam = rates_of(r_ref, rows, hp_ref, tri)
        lam_t, dt_t = lam.T, dt.T
        last = lam[Q - 1 : Q, :]
        tail = dt * jnp.exp(last - lam)
        aff = nt(cs, bs, HIGH)
        st_ref[b] = hst[...].astype(BF16)
        ch = nn(cs.astype(BF16), st_ref[b])
        for i in range(HL // 2):
            at = slice(128 * i, 128 * i + 128)
            xp = x[:, at]
            xb = xp.astype(BF16)
            y, lc = [], []
            for h in (2 * i, 2 * i + 1):
                lcol = spread(lam, h)
                within = jnp.exp(jnp.where(causal, lcol - lam_t[h : h + 1, :], -1e30))
                y.append(nn((aff * within * dt_t[h : h + 1, :]).astype(BF16), xb))
                lc.append(lcol)
            out = jnp.where(low, y[0], y[1])
            out = out + jnp.exp(jnp.where(low, lc[0], lc[1])) * ch[:, at] + ex_ref[0:1, at] * xp
            mixed_ref[rows, at] = out.astype(BF16)
            xw_s[:, at] = (xp * jnp.where(low, spread(tail, 2 * i), spread(tail, 2 * i + 1))).astype(BF16)
            er_s[0:1, at] = jnp.exp(jnp.where(low1, spread(last, 2 * i), spread(last, 2 * i + 1)))
        hst[...] = hst[...] * er_s[0:1, :] + nn(bs.T.astype(BF16), xw_s[...])
        between(b)
        return carry

    lax.fori_loop(0, blocks, block, 0)


def scan_bwd_blocks(
    v_ref, s_ref, r_ref, dy_ref, st_ref, kw_ref, hp_ref, ex_ref,
    dv_ref, gcw_ref, gch_ref, ghd_ref,
    buf, cbuf, dhst, rowp, xw_s, e_s, er_s, between,
):
    blocks = v_ref.shape[0] // Q
    row = lax.broadcasted_iota(jnp.int32, (Q, Q), 0)
    col = lax.broadcasted_iota(jnp.int32, (Q, Q), 1)
    tri = (row >= col).astype(F32)
    later = col >= row
    suffix = later.astype(F32)
    strict = (col < row).astype(F32)
    lane = lax.broadcasted_iota(jnp.int32, (Q, 128), 1)
    lane1 = lax.broadcasted_iota(jnp.int32, (1, 128), 1)
    low = lane < HW
    low1 = lane1 < HW
    buf[Q : Q + 8, :] = jnp.zeros((8, CH), F32)
    dhst[...] = jnp.zeros_like(dhst)
    rowp[...] = jnp.zeros_like(rowp)
    gcw_ref[...] = jnp.zeros_like(gcw_ref)
    gch_ref[...] = jnp.zeros_like(gch_ref)
    ghd_ref[...] = jnp.zeros_like(ghd_ref)

    def block(i0, carry):
        b = blocks - 1 - i0
        rows = pl.ds(pl.multiple_of(b * Q, Q), Q)
        before = pl.ds(pl.multiple_of(jnp.maximum(b * Q - 16, 0), 16), 16)
        keep = (b > 0).astype(F32)
        cbuf[0:8, 0:W] = v_ref[before, :].astype(F32)[8:16, :] * keep
        cbuf[0:8, W:CH] = s_ref[before, :].astype(F32)[8:16, :] * keep
        cbuf[8 : 8 + Q, 0:W] = v_ref[rows, :].astype(F32)
        cbuf[8 : 8 + Q, W:CH] = s_ref[rows, :].astype(F32)
        k = kw_ref[4:5, :] + cbuf[5 : 5 + Q, :] * kw_ref[0:1, :]
        for j in range(1, 4):
            k = k + cbuf[5 + j : 5 + j + Q, :] * kw_ref[j : j + 1, :]
        sg = sigmoid(k)
        x = k * sg
        ds = sg * (1.0 + k * (1.0 - sg))
        bs, cs = x[:, W : W + STATE], x[:, W + STATE :]
        bb, cb = bs.astype(BF16), cs.astype(BF16)
        raw, dt, lam = rates_of(r_ref, rows, hp_ref, tri)
        lam_t = lam.T
        last = lam[Q - 1 : Q, :]
        aff_t = nt(bs, cs, HIGH)
        hb = st_ref[b]
        dhb = dhst[...].astype(BF16)
        ch = nn(cb, hb)
        bd = nn(bb, dhb)
        daff_t = jnp.zeros((Q, Q), F32)
        col_n = jnp.zeros((Q, 128), F32)
        col_i = jnp.zeros((Q, 128), F32)
        row_i = jnp.zeros((Q, 128), F32)
        through = jnp.zeros((1, 128), F32)
        for i in range(HL // 2):
            at = slice(128 * i, 128 * i + 128)
            xp = x[:, at]
            xb = xp.astype(BF16)
            dyb = dy_ref[rows, at]
            dyf = dyb.astype(F32)
            z, lc, dc = [], [], []
            for h in (2 * i, 2 * i + 1):
                mine = low if h % 2 == 0 else jnp.logical_not(low)
                lcol, dcol = spread(lam, h), spread(dt, h)
                within = jnp.exp(jnp.where(later, lam_t[h : h + 1, :] - lcol, -1e30))
                g = nt(jnp.where(mine, xp, 0.0).astype(BF16), dyb)
                lg = within * g
                lgd = lg * dcol
                daff_t = daff_t + lgd
                col_n = jnp.where(lane == h, jnp.sum(aff_t * lg, axis=1, keepdims=True), col_n)
                rowp[h : h + 1, :] = jnp.sum(aff_t * lgd, axis=0, keepdims=True)
                z.append(nn((aff_t * within).astype(BF16), dyb))
                lc.append(lcol)
                dc.append(dcol)
            lamp = jnp.where(low, lc[0], lc[1])
            dtp = jnp.where(low, dc[0], dc[1])
            lastp = jnp.where(low1, spread(last, 2 * i), spread(last, 2 * i + 1))
            e = dyf * jnp.exp(lamp)
            e_s[:, at] = e.astype(BF16)
            ew = jnp.exp(lastp - lamp)
            bdp = bd[:, at]
            xw_s[:, at] = (xp * (dtp * ew)).astype(BF16)
            er_s[0:1, at] = jnp.exp(lastp)
            re = e * ch[:, at]
            ci = xp * bdp * ew
            th = jnp.sum(dhst[:, at] * hb[:, at].astype(F32), axis=0, keepdims=True) * er_s[0:1, at]
            for h in (2 * i, 2 * i + 1):
                mine = low if h % 2 == 0 else jnp.logical_not(low)
                mine1 = low1 if h % 2 == 0 else jnp.logical_not(low1)
                row_i = jnp.where(lane == h, jnp.sum(jnp.where(mine, re, 0.0), axis=1, keepdims=True), row_i)
                col_i = jnp.where(lane == h, jnp.sum(jnp.where(mine, ci, 0.0), axis=1, keepdims=True), col_i)
                through = jnp.where(
                    lane1 == h, jnp.sum(jnp.where(mine1, th, 0.0), axis=1, keepdims=True), through
                )
            dx = dtp * jnp.where(low, z[0], z[1]) + bdp * (dtp * ew) + ex_ref[0:1, at] * dyf
            gch_ref[0:1, at] += jnp.sum(dyf * xp, axis=0, keepdims=True)
            buf[0:Q, at] = dx * ds[:, at]
        daff_b = daff_t.astype(BF16)
        d_bs = nt(xw_s[...], dhb) + nn(daff_b, cb)
        d_cs = nt(e_s[...], hb) + nn(daff_t.T.astype(BF16), bb)
        buf[0:Q, W : W + STATE] = d_bs * ds[:, W : W + STATE]
        buf[0:Q, W + STATE : CH] = d_cs * ds[:, W + STATE :]
        dhst[...] = dhst[...] * er_s[0:1, :] + nn(cs.T.astype(BF16), e_s[...])
        after = nn(suffix, rowp[...].T - dt * col_n + row_i, HIGH) + nn(strict, dt * col_i, HIGH) + through
        d_rate = (col_n + col_i + hp_ref[1:2, :] * after) * sigmoid(raw)
        ghd_ref[0:1, :] += jnp.sum(d_rate, axis=0, keepdims=True)
        ghd_ref[1:2, :] += jnp.sum(dt * after, axis=0, keepdims=True) * hp_ref[1:2, :]
        dv_ref[rows, CH:VC] = pltpu.roll(d_rate, lax.axis_index("seq") * HL, 1).astype(BF16)
        for at in (slice(0, W), slice(W, CH)):
            raw_v = cbuf[8 : 8 + Q, at]
            dk = buf[0:Q, at]
            dv = dk * kw_ref[3:4, at]
            gcw_ref[4:5, at] += jnp.sum(dk, axis=0, keepdims=True)
            gcw_ref[3:4, at] += jnp.sum(dk * raw_v, axis=0, keepdims=True)
            for j in range(3):
                dk = buf[3 - j : 3 - j + Q, at]
                dv = dv + dk * kw_ref[j : j + 1, at]
                gcw_ref[j : j + 1, at] += jnp.sum(dk * raw_v, axis=0, keepdims=True)
            dv_ref[rows, at] = dv.astype(BF16)
        buf[Q : Q + 8, :] = buf[0:8, :]
        between(i0)
        return carry

    lax.fori_loop(0, blocks, block, 0)


GROUPS = 4


def place(block, at, width):
    start, shift = at // 128 * 128, at % 128
    lanes = -(-(width + shift) // 128) * 128
    have = block.shape[1]
    if lanes > have:
        block = jnp.concatenate([block, jnp.zeros((block.shape[0], lanes - have), block.dtype)], axis=1)
    else:
        block = block[:, :lanes]
    if shift:
        block = pltpu.roll(block, shift, 1)
    return start, lanes, block


def front_kernel(
    nf, tok, cot, win, wst, wout, small,
    x_out, cot_out, nrm_out, wv_out, ws_out, wg_out, wo_out, mix_out, gate_out, mixed_out, st_out, dsh_out,
    kw_s, hp_s, ex_s, pre_s, stat_s,
    x_s, cot_s, nrm_s, wv_s, ws_s, wg_s, wo_s, mix_s, gate_s, mixed_s, st_s, dsh_s,
    small_s, conv_s, post_s, stat_own, stat_got,
    buf, hst, xw_s, er_s,
    xs, xr, zs, zr, ms, mr, es, er, ls, os_,
):
    s = lax.axis_index("seq")
    f = lax.axis_index("fsdp")
    px, py = s ^ 1, s ^ 2
    nl = nf // 2
    p, c = f // 2, f % 2
    partner = p * 2 + 1 - c
    bar = pltpu.get_barrier_semaphore()
    for k in range(1, SEQ):
        signal(bar, {"seq": s ^ k})
    for k in range(1, nf):
        signal(bar, {"fsdp": lax.rem(f + k, nf)})
    pl.semaphore_wait(bar, nf - 1 + SEQ - 1)

    n = win.shape[0]
    rows = tok.shape[0]
    length = rows * SEQ
    ins = (
        win.at[:, pl.ds(pl.multiple_of(INNER + s * W, 128), W)],
        wst,
        win.at[:, pl.ds(pl.multiple_of(s * W, 128), W)],
        wout.at[:, pl.ds(pl.multiple_of(s * W, 128), W)],
    )
    outs = (wv_s, ws_s, wg_s, wo_s)

    def row(g, i):
        return outs[g].at[pl.ds(i * n, n)]

    def hop(g, src, i, way, k, device):
        return rcopy(src, row(g, i), zs.at[g, way, k], zr.at[g, i], {"fsdp": device})

    def own_send(g):
        @pl.when(p < nl - 1)
        def _():
            hop(g, ins[g], f, 0, 0, f + 2).start()

        @pl.when(p > 0)
        def _():
            hop(g, ins[g], f, 1, 0, f - 2).start()

        hop(g, ins[g], f, 2, 0, partner).start()
        pltpu.make_async_copy(ins[g], row(g, f), ls.at[g]).start()

    def step(g, k):
        @pl.when(p - k >= 0)
        def _():
            o = f - 2 * k
            hop(g, row(g, o), o, 0, k, f).wait_recv()

            @pl.when(p < nl - 1)
            def _():
                hop(g, row(g, o), o, 0, k, f + 2).start()

            hop(g, row(g, o), o, 2, k, partner).start()

        @pl.when(p + k < nl)
        def _():
            o = f + 2 * k
            hop(g, row(g, o), o, 1, k, f).wait_recv()

            @pl.when(p > 0)
            def _():
                hop(g, row(g, o), o, 1, k, f - 2).start()

            hop(g, row(g, o), o, 3, k, partner).start()

    def arrive(g):
        pltpu.make_async_copy(ins[g], row(g, f), ls.at[g]).wait()
        for q in range(nl):
            o = q * 2 + 1 - c
            hop(g, row(g, o), o, 2, 0, partner).wait_recv()

    def sent(g):
        hop(g, ins[g], f, 2, 0, partner).wait_send()

        @pl.when(p < nl - 1)
        def _():
            hop(g, ins[g], f, 0, 0, f + 2).wait_send()

        @pl.when(p > 0)
        def _():
            hop(g, ins[g], f, 1, 0, f - 2).wait_send()

        for k in range(1, nl):
            @pl.when(p - k >= 0)
            def _():
                o = f - 2 * k

                @pl.when(p < nl - 1)
                def _():
                    hop(g, row(g, o), o, 0, k, f + 2).wait_send()

                hop(g, row(g, o), o, 2, k, partner).wait_send()

            @pl.when(p + k < nl)
            def _():
                o = f + 2 * k

                @pl.when(p > 0)
                def _():
                    hop(g, row(g, o), o, 1, k, f - 2).wait_send()

                hop(g, row(g, o), o, 3, k, partner).wait_send()

    def small_copy(k):
        return rcopy(small, small_s.at[f], ms.at[k], mr.at[k], {"fsdp": lax.rem(f + k, nf)})

    mine = pl.ds(s * rows, rows)
    own_small = pltpu.make_async_copy(small, small_s.at[f], ls.at[4])
    own_tok = pltpu.make_async_copy(tok, x_s.at[mine], ls.at[5])
    own_cot = pltpu.make_async_copy(cot, cot_s.at[mine], ls.at[6])

    for k in range(1, nf):
        small_copy(k).start()
    own_small.start()
    own_tok.start()
    seq_gather_start((tok,), (x_s,), xs, xr, px, py, s)
    own_send(0)
    own_send(1)
    own_cot.start()
    step(0, 1)
    step(1, 1)
    seq_gather_relay(0, tok, x_s, xs, xr, px, py, s)
    own = cot_s.at[mine]
    rcopy(cot, own, xs.at[1, 0], xr.at[1, 0], {"seq": px}).start()
    rcopy(cot, own, xs.at[1, 1], xr.at[1, 1], {"seq": py}).start()

    own_small.wait()
    for k in range(1, nf):
        small_copy(k).wait()
    conv_s[...] = jnp.zeros_like(conv_s)
    pre_s[...] = jnp.zeros_like(pre_s)
    post_s[...] = jnp.zeros_like(post_s)
    heads = [jnp.zeros((8, 128), F32) for _ in range(3)]
    for i in range(nf):
        block = small_s[i]
        at, lanes, moved = place(block, i * (XBC // nf), XBC // nf)
        conv_s[:, at : at + lanes] += moved
        at, lanes, moved = place(block, i * (D // nf), D // nf)
        pre_s[:, at : at + lanes] += jnp.where(lax.broadcasted_iota(jnp.int32, moved.shape, 0) == 5, moved, 0.0)
        at, lanes, moved = place(block, i * (INNER // nf), INNER // nf)
        post_s[:, at : at + lanes] += jnp.where(lax.broadcasted_iota(jnp.int32, moved.shape, 0) == 6, moved, 0.0)
        for j in range(3):
            piece = block[:, 128 * j : 128 * j + 128]
            at = i * (HEADS // nf)
            heads[j] = heads[j] + (pltpu.roll(piece, at, 1) if at else piece)
    kw_s[:, 0:W] = conv_s[:, pl.ds(pl.multiple_of(s * W, 128), W)]
    kw_s[:, W:CH] = conv_s[:, INNER:XBC]
    lane1 = lax.broadcasted_iota(jnp.int32, (1, 128), 1)
    low1 = lane1 < HW
    back = lax.rem(128 - s * HL, 128)
    step_b, decay, skip = [pltpu.roll(h, back, 1)[7:8, :] for h in heads]
    hp_s[...] = jnp.zeros_like(hp_s)
    hp_s[0:1, :] = jnp.where(lane1 < HL, step_b, 0.0)
    hp_s[1:2, :] = jnp.where(lane1 < HL, -jnp.exp(decay), 0.0)
    ex_s[...] = jnp.zeros_like(ex_s)
    for i in range(HL // 2):
        ex_s[0:1, 128 * i : 128 * i + 128] = jnp.where(low1, spread(skip, 2 * i), spread(skip, 2 * i + 1))
    ex_s[1:2, :] = post_s[6:7, pl.ds(pl.multiple_of(s * W, 128), W)]

    for k in range(2, nl):
        step(0, k)
        step(1, k)
        if k == 2:
            own_send(2)
            own_send(3)
    if nl < 3:
        own_send(2)
        own_send(3)
    own_tok.wait()
    seq_gather_finish(0, tok, x_s, xs, xr, px, py, s)

    def norm(i, carry):
        r = pl.ds(pl.multiple_of(i * 128, 128), 128)
        x = x_s[r, :].astype(F32)
        rho = lax.rsqrt(jnp.sum(x * x, axis=1, keepdims=True) * (1.0 / D) + EPS)
        nrm_s[r, :] = (x * rho * pre_s[5:6, :]).astype(BF16)
        return carry

    lax.fori_loop(0, length // 128, norm, 0)
    arrive(0)
    arrive(1)

    saves = [
        pltpu.make_async_copy(a, b, os_.at[i])
        for i, (a, b) in enumerate(
            (
                (x_s, x_out), (cot_s, cot_out), (nrm_s, nrm_out), (wv_s, wv_out), (ws_s, ws_out), (wg_s, wg_out),
                (wo_s, wo_out), (mix_s, mix_out), (gate_s, gate_out), (mixed_s, mixed_out), (st_s, st_out),
                (dsh_s, dsh_out),
            )
        )
    ]
    for i in (0, 2, 3, 4):
        saves[i].start()

    def project(i, carry):
        r = pl.ds(pl.multiple_of(i * 256, 256), 256)
        a = nrm_s[r, :]
        mix_s[r, 0:W] = nn(a, wv_s[...]).astype(BF16)
        mix_s[r, W:VC] = nn(a, ws_s[...]).astype(BF16)
        return carry

    lax.fori_loop(0, length // 256, project, 0)
    step(2, 1)
    saves[7].start()

    def between(b):
        @pl.when(b == 1)
        def _():
            seq_gather_relay(1, cot, cot_s, xs, xr, px, py, s)

        @pl.when(b == 2)
        def _():
            step(3, 1)

        @pl.when(b == 5)
        def _():
            step(2, 2)

    scan_fwd_blocks(
        mix_s.at[:, 0:W], mix_s.at[:, W:CH], mix_s.at[:, CH:VC], kw_s, hp_s, ex_s, mixed_s, st_s,
        buf, hst, xw_s, er_s, between,
    )
    for i in (9, 10):
        saves[i].start()
    step(3, 2)
    for k in range(3, nl):
        step(2, k)
    arrive(2)
    saves[5].start()

    def project_gate(i, carry):
        r = pl.ds(pl.multiple_of(i * 256, 256), 256)
        gate_s[r, :] = nn(nrm_s[r, :], wg_s[...]).astype(BF16)
        return carry

    lax.fori_loop(0, length // 256, project_gate, 0)
    saves[8].start()
    for k in range(3, nl):
        step(3, k)
    own_cot.wait()
    seq_gather_finish(1, cot, cot_s, xs, xr, px, py, s)
    saves[1].start()
    arrive(3)
    saves[6].start()
    eye = lax.broadcasted_iota(jnp.int32, (128, 128), 0) == lax.broadcasted_iota(jnp.int32, (128, 128), 1)

    def stats(i, carry):
        r = pl.ds(pl.multiple_of(i * 128, 128), 128)
        dsh = nn(cot_s[r, :], wo_s[...])
        dsh_s[r, :] = dsh
        gate = gate_s[r, :].astype(F32)
        gated = mixed_s[r, :].astype(F32) * (gate * sigmoid(gate))
        one = jnp.sum(gated * gated, axis=1, keepdims=True)
        two = jnp.sum(dsh * ex_s[1:2, :] * gated, axis=1, keepdims=True)
        stat_own[pl.ds(i, 1), :] = jnp.sum(jnp.where(eye, one, 0.0), axis=0, keepdims=True)
        stat_own[pl.ds(length // 128 + i, 1), :] = jnp.sum(jnp.where(eye, two, 0.0), axis=0, keepdims=True)
        return carry

    lax.fori_loop(0, length // 128, stats, 0)
    saves[11].start()
    copies = [rcopy(stat_own, stat_got.at[k], es.at[k], er.at[k], {"seq": s ^ k}) for k in range(1, SEQ)]
    for copy in copies:
        copy.start()
    for copy in copies:
        copy.wait()
    stat_s[...] = stat_own[...] + stat_got[1] + (stat_got[2] + stat_got[3])
    for g in range(GROUPS):
        sent(g)
    for save in saves:
        save.wait()


def front(nf, tok, cot, win, wst, wout, small):
    shape = jax.ShapeDtypeStruct
    dma = pltpu.SemaphoreType.DMA
    length = SEQ * tok.shape[0]
    big = [
        shape((length, D), BF16),
        shape((length, D), BF16),
        shape((length, D), BF16),
        shape((D, W), BF16),
        shape((D, VC - W), BF16),
        shape((D, W), BF16),
        shape((D, W), BF16),
        shape((length, VC), BF16),
        shape((length, W), BF16),
        shape((length, W), BF16),
        shape((length // Q, STATE, W), BF16),
        shape((length, W), F32),
    ]
    par = [
        shape((8, CH), F32),
        shape((8, 128), F32),
        shape((8, W), F32),
        shape((8, D), F32),
        shape((2 * length // 128, 128), F32),
    ]
    return pl.pallas_call(
        functools.partial(front_kernel, nf),
        out_shape=big + par,
        in_specs=[ANY] * 5 + [VMEM],
        out_specs=[ANY] * len(big) + [VMEM] * len(par),
        scratch_shapes=[pltpu.VMEM(b.shape, b.dtype) for b in big]
        + [
            pltpu.VMEM((nf, 8, 512), F32),
            pltpu.VMEM((8, XBC), F32),
            pltpu.VMEM((8, INNER), F32),
            pltpu.VMEM((2 * length // 128, 128), F32),
            pltpu.VMEM((SEQ, 2 * length // 128, 128), F32),
            pltpu.VMEM((Q + 8, CH), F32),
            pltpu.VMEM((STATE, W), F32),
            pltpu.VMEM((Q, W), BF16),
            pltpu.VMEM((8, W), F32),
            dma((2, 4)),
            dma((2, 4)),
            dma((GROUPS, 4, nf // 2)),
            dma((GROUPS, nf)),
            dma((nf,)),
            dma((nf,)),
            dma((SEQ,)),
            dma((SEQ,)),
            dma((7,)),
            dma((len(big),)),
        ],
        name="front",
        compiler_params=pltpu.CompilerParams(
            collective_id=1, has_side_effects=True, vmem_limit_bytes=VMEM_LIMIT
        ),
    )(tok, cot, win, wst, wout, small)


TN = (((0,), (0,)), ((), ()))
STRIP = 384


def unplace(block, at, width):
    start, shift = at // 128 * 128, at % 128
    lanes = -(-(width + shift) // 128) * 128
    piece = block[:, start : start + lanes]
    if shift:
        piece = pltpu.roll(piece, lanes - shift, 1)
    if lanes < 512:
        piece = jnp.concatenate([piece, jnp.zeros((piece.shape[0], 512 - lanes), piece.dtype)], axis=1)
    else:
        piece = piece[:, :512]
    return jnp.where(lax.broadcasted_iota(jnp.int32, piece.shape, 1) < width, piece, 0.0)


def back_kernel(
    nf, x_in, cot_in, nrm_in, wv_in, ws_in, wg_in, wo_in, mix_in, gate_in, mixed_in, st_in, dsh_in,
    kw_s, hp_s, ex_s, pre_s, stat_s,
    out_ref, gt_ref, go_ref, gg_ref, gv_ref, gs_ref, small_ref,
    xc_s, nrm_s, wv_s, ws_s, wg_s, wo_s, mix_s, gate_s, mixed_s, st_s, dsh_s,
    dy_s, dv_s, cotrow_s, part_s, ga_s, gb_s, gc_s,
    pb0, pb1, pb2, pb3, lb0, lb1, lb2, lb3, own0, own1, own2, own3,
    ab0, ab1, az0, az1,
    gcw_s, gch_s, ghd_s, gpost_s, gpre_s, conv_s, post_s, snd_s, got_s, sown_s, sgot_s,
    buf, cbuf, dhst, rowp, xw_s, e_s, er_s,
    ls, zs, zr, xs, xr, as_, ar, ms, mr, es, er, os_,
):
    s = lax.axis_index("seq")
    f = lax.axis_index("fsdp")
    px, py = s ^ 1, s ^ 2
    nl = nf // 2
    p, c = f // 2, f % 2
    partner = p * 2 + 1 - c
    bar = pltpu.get_barrier_semaphore()
    for k in range(1, SEQ):
        signal(bar, {"seq": s ^ k})
    for k in range(1, nf):
        signal(bar, {"fsdp": lax.rem(f + k, nf)})

    length = nrm_s.shape[0]
    rows = length // SEQ
    n = D // nf
    mine = pl.ds(s * rows, rows)
    loads = [
        pltpu.make_async_copy(a, b, ls.at[i])
        for i, (a, b) in enumerate(
            (
                (gate_in, gate_s), (mixed_in, mixed_s), (dsh_in, dsh_s), (cot_in, xc_s), (wo_in, wo_s),
                (nrm_in, nrm_s), (mix_in, mix_s), (st_in, st_s), (wg_in, wg_s), (wv_in, wv_s), (ws_in, ws_s),
                (cot_in.at[mine], cotrow_s), (x_in, xc_s),
            )
        )
    ]
    for load in loads[:-1]:
        load.start()
    pl.semaphore_wait(bar, nf - 1 + SEQ - 1)

    half = D // 2
    cols = (slice(0, half), slice(half, D))
    first, second = (px, py), (py, px)
    ab, az = (ab0, ab1), (az0, az1)

    def chunk(i, a):
        return part_s.at[pl.ds(i * rows, rows), cols[a]]

    def seq_one(t, a, m):
        i = (first[a] ^ second[a] ^ s) if m == 0 else first[a]
        return rcopy(chunk(i, a), ab[t].at[a, m], xs.at[t, a, m], xr.at[t, a, m], {"seq": first[a]})

    def seq_two(t, a):
        return rcopy(az[t].at[a, 0], az[t].at[a, 1], xs.at[t, a, 2], xr.at[t, a, 2], {"seq": second[a]})

    def add(*terms):
        total = terms[0].astype(F32)
        for term in terms[1:]:
            total = total + term.astype(F32)
        return total

    def seq_pass(t):
        for a in range(2):
            seq_one(t, a, 0).wait_recv()
            az[t][a, 0] = add(chunk(second[a], a)[...], ab[t][a, 0]).astype(BF16)
            seq_two(t, a).start()

    def seq_last(t, out):
        for a in range(2):
            seq_one(t, a, 1).wait_recv()
            seq_two(t, a).wait_recv()
            out[:, cols[a]] = add(chunk(s, a)[...], ab[t][a, 1], az[t][a, 1])

    def seq_one_sent(t):
        for a in range(2):
            seq_one(t, a, 0).wait_send()
            seq_one(t, a, 1).wait_send()

    parts = (ga_s, gb_s, ga_s, gc_s)
    pbs, lbs, owns = (pb0, pb1, pb2, pb3), (lb0, lb1, lb2, lb3), (own0, own1, own2, own3)
    gouts = (go_ref, gg_ref, gv_ref, gs_ref)

    def piece(g, i):
        return parts[g].at[pl.ds(pl.multiple_of(i * n, 16), n)]

    def swap(g, q):
        return rcopy(piece(g, q * 2 + 1 - c), pbs[g].at[q], zs.at[g, 0, q], zr.at[g, 0, q], {"fsdp": partner})

    def up(g, q):
        return rcopy(pbs[g].at[q], lbs[g].at[q], zs.at[g, 1, q], zr.at[g, 1, q], {"fsdp": f + 2})

    def down(g, q):
        to = jnp.where(q == p - 1, nl, q)
        return rcopy(pbs[g].at[q], lbs[g].at[to], zs.at[g, 2, q], zr.at[g, 2, q], {"fsdp": f - 2})

    def send_up(g, q, terms):
        pbs[g][q] = add(piece(g, q * 2 + c)[...], pbs[g][q], *terms).astype(BF16)
        up(g, q).start()

    def send_down(g, q, terms):
        pbs[g][q] = add(piece(g, q * 2 + c)[...], pbs[g][q], *terms).astype(BF16)
        down(g, q).start()

    def ends(g, shards):
        for k in shards:
            @pl.when(p == 0)
            def _():
                swap(g, nl - 1 - k).wait_recv()
                send_up(g, nl - 1 - k, ())

            @pl.when(p == nl - 1)
            def _():
                swap(g, k).wait_recv()
                send_down(g, k, ())

    def slot(g, t):
        @pl.when(jnp.logical_and(p > 0, p <= t))
        def _():
            q = nl - 1 - t + p
            swap(g, q).wait_recv()
            up(g, q).wait_recv()
            send_up(g, q, (lbs[g][q],))

        @pl.when(jnp.logical_and(p < nl - 1, nl - 1 - p <= t))
        def _():
            q = t - (nl - 1 - p)
            swap(g, q).wait_recv()
            down(g, q).wait_recv()
            send_down(g, q, (lbs[g][q],))

    def close(g):
        swap(g, p).wait_recv()

        @pl.when(p > 0)
        def _():
            up(g, p).wait_recv()

        @pl.when(p < nl - 1)
        def _():
            down(g, p).wait_recv()

        @pl.when(p == 0)
        def _():
            owns[g][...] = add(piece(g, f)[...], pbs[g][p], lbs[g][nl]).astype(BF16)

        @pl.when(p == nl - 1)
        def _():
            owns[g][...] = add(piece(g, f)[...], pbs[g][p], lbs[g][p]).astype(BF16)

        @pl.when(jnp.logical_and(p > 0, p < nl - 1))
        def _():
            owns[g][...] = add(piece(g, f)[...], pbs[g][p], lbs[g][p], lbs[g][nl]).astype(BF16)

        place_ = gouts[g].at[pl.ds(s * n, n)]
        rcopy(owns[g], place_, as_.at[g, 0], ar.at[g, 0], {"seq": px}).start()
        rcopy(owns[g], place_, as_.at[g, 1], ar.at[g, 1], {"seq": py}).start()
        pltpu.make_async_copy(owns[g], place_, os_.at[g]).start()

    def relay(g):
        seq_gather_relay(g, owns[g], gouts[g], as_, ar, px, py, s)

    def swaps_sent(g):
        for q in range(nl):
            swap(g, q).wait_send()

    def line_sent(g):
        for q in range(nl):
            @pl.when(q > p)
            def _():
                up(g, q).wait_send()

            @pl.when(q < p)
            def _():
                down(g, q).wait_send()

    order = []
    for k in range(D // STRIP // 2):
        order += [D // STRIP - 1 - k, k]

    def strip(j, a_ref, b_ref, bcols, g):
        at = slice(j * STRIP, (j + 1) * STRIP)
        parts[g][at, :] = lax.dot_general(a_ref[:, at], b_ref[:, bcols], TN, preferred_element_type=F32).astype(BF16)
        for q in range(nl):
            if j * STRIP <= q * 2 * n < (j + 1) * STRIP:
                swap(g, q).start()

    for i in range(3):
        loads[i].wait()
    eye = lax.broadcasted_iota(jnp.int32, (128, 128), 0) == lax.broadcasted_iota(jnp.int32, (128, 128), 1)
    gpost_s[...] = jnp.zeros_like(gpost_s)

    def gated_norm(i, carry):
        r = pl.ds(pl.multiple_of(i * 128, 128), 128)
        one = jnp.sum(jnp.where(eye, stat_s[pl.ds(i, 1), :], 0.0), axis=1, keepdims=True)
        two = jnp.sum(jnp.where(eye, stat_s[pl.ds(length // 128 + i, 1), :], 0.0), axis=1, keepdims=True)
        rho = lax.rsqrt(one * (1.0 / INNER) + EPS)
        mean = rho * two * (1.0 / INNER)
        gate = gate_s[r, :].astype(F32)
        mixed = mixed_s[r, :].astype(F32)
        dsh = dsh_s[r, :]
        post = ex_s[1:2, :]
        sg = sigmoid(gate)
        sl = gate * sg
        n1 = mixed * sl * rho
        gpost_s[0:1, :] += jnp.sum(dsh * n1, axis=0, keepdims=True)
        d_gated = rho * (dsh * post - n1 * mean)
        mixed_s[r, :] = (n1 * post).astype(BF16)
        dy_s[r, :] = (d_gated * sl).astype(BF16)
        gate_s[r, :] = (d_gated * mixed * (sg * (1.0 + gate * (1.0 - sg)))).astype(BF16)
        return carry

    lax.fori_loop(0, length // 128, gated_norm, 0)

    every = slice(0, W)
    loads[4].wait()

    def out_part(i, carry):
        r = pl.ds(pl.multiple_of((s ^ (SEQ - 1 - i)) * rows, rows), rows)
        part_s[r, :] = nt(mixed_s[r, :], wo_s[...]).astype(BF16)

        @pl.when(i == 0)
        def _():
            for a in range(2):
                seq_one(0, a, 0).start()

        @pl.when(i == 2)
        def _():
            for a in range(2):
                seq_one(0, a, 1).start()

        return carry

    lax.fori_loop(0, SEQ, out_part, 0)
    loads[3].wait()
    for j in order:
        strip(j, xc_s, mixed_s, every, 0)
    loads[-1].start()
    ends(0, range(nl - 1))

    loads[5].wait()
    for j in order:
        strip(j, nrm_s, gate_s, every, 1)
    ends(1, range(nl - 1))
    loads[6].wait()
    loads[7].wait()

    def between(i):
        @pl.when(i == 0)
        def _():
            slot(0, 1)

        @pl.when(i == 1)
        def _():
            seq_pass(0)

        @pl.when(i == 2)
        def _():
            for t in range(2, nl - 1):
                slot(0, t)

        @pl.when(i == 3)
        def _():
            close(0)

        @pl.when(i == 4)
        def _():
            slot(1, 1)

        @pl.when(i == 6)
        def _():
            for t in range(2, nl - 1):
                slot(1, t)
            relay(0)

    scan_bwd_blocks(
        mix_s.at[:, 0:W], mix_s.at[:, W:CH], mix_s.at[:, CH:VC], dy_s, st_s, kw_s, hp_s, ex_s,
        dv_s, gcw_s, gch_s, ghd_s, buf, cbuf, dhst, rowp, xw_s, e_s, er_s, between,
    )

    loads[-1].wait()
    swaps_sent(0)
    seq_one_sent(0)
    for i in range(8, 12):
        loads[i].wait()
    gpre_s[...] = jnp.zeros_like(gpre_s)

    def dn_part(i, carry):
        r = pl.ds(pl.multiple_of((s ^ (SEQ - 1 - i)) * rows, rows), rows)
        dn = nt(gate_s[r, :], wg_s[...]) + nt(dv_s[r, 0:W], wv_s[...]) + nt(dv_s[r, W:VC], ws_s[...])
        part_s[r, :] = dn.astype(BF16)
        x = xc_s[r, :].astype(F32)
        rho = lax.rsqrt(jnp.sum(x * x, axis=1, keepdims=True) * (1.0 / D) + EPS)
        gpre_s[5:6, :] += jnp.sum(dn * (x * rho), axis=0, keepdims=True)

        @pl.when(i == 0)
        def _():
            for a in range(2):
                seq_one(1, a, 0).start()
            for j in order[2:]:
                strip(j, nrm_s, dv_s, every, 2)
            ends(2, range(1, nl - 1))

        @pl.when(i == 2)
        def _():
            for a in range(2):
                seq_one(1, a, 1).start()
            for j in order:
                strip(j, nrm_s, dv_s, slice(W, VC), 3)

        @pl.when(i == 1)
        def _():
            close(1)
            slot(2, 1)

        return carry

    def rows_of(t, a):
        return pl.ds((2 * t + a) * rows, rows)

    def result(t, a):
        out = (out_ref, gt_ref)[t].at[:, cols[a]]
        return pltpu.make_async_copy(dsh_s.at[rows_of(t, a)], out, ls.at[2 * t + a])

    for a in range(2):
        seq_one(0, a, 1).wait_recv()
        seq_two(0, a).wait_recv()
        dsh_s[rows_of(0, a), :] = add(xc_s[mine, cols[a]], chunk(s, a)[...], ab0[a, 1], az0[a, 1])
        result(0, a).start()
    for j in order[:2]:
        strip(j, nrm_s, dv_s, every, 2)
    ends(2, range(1))
    lax.fori_loop(0, SEQ, dn_part, 0)

    conv_s[...] = jnp.zeros_like(conv_s)
    conv_s[:, pl.ds(pl.multiple_of(s * W, 128), W)] = gcw_s[:, 0:W]
    conv_s[:, INNER:XBC] = gcw_s[:, W:CH]
    post_s[...] = jnp.zeros_like(post_s)
    post_s[6:7, pl.ds(pl.multiple_of(s * W, 128), W)] = gpost_s[0:1, :]
    lane8 = lax.broadcasted_iota(jnp.int32, (8, 128), 1)
    row8 = lax.broadcasted_iota(jnp.int32, (8, 128), 0)
    skip = jnp.zeros((1, 128), F32)
    lane1 = lax.broadcasted_iota(jnp.int32, (1, 128), 1)
    for h in range(HL):
        at = slice(128 * (h // 2), 128 * (h // 2) + 128)
        half_of = (lane1 < HW) if h % 2 == 0 else (lane1 >= HW)
        skip = jnp.where(lane1 == h, jnp.sum(jnp.where(half_of, gch_s[0:1, at], 0.0), axis=1, keepdims=True), skip)
    heads = [
        pltpu.roll(jnp.where(row8 == 7, jnp.broadcast_to(v, (8, 128)), 0.0), s * HL, 1)
        for v in (ghd_s[0:1, :], ghd_s[1:2, :], skip)
    ]
    row512 = lax.broadcasted_iota(jnp.int32, (8, 512), 0)
    hn = HEADS // nf
    for i in range(nf):
        conv = unplace(conv_s, i * (XBC // nf), XBC // nf)
        block = jnp.where(row512 < 5, conv, 0.0)
        block = block + unplace(gpre_s, i * (D // nf), D // nf)
        block = block + unplace(post_s, i * (INNER // nf), INNER // nf)
        tiles = []
        for v in heads:
            moved = pltpu.roll(v, (128 - i * hn) % 128, 1) if i else v
            tiles.append(jnp.where(lane8 < hn, moved, 0.0))
        block = block + jnp.concatenate(tiles + [jnp.zeros((8, 128), F32)], axis=1)
        snd_s[i] = block

    def small_send(k):
        to = lax.rem(f + k, nf)
        return rcopy(snd_s.at[to], got_s.at[k], ms.at[k], mr.at[k], {"fsdp": to})

    for k in range(1, nf):
        small_send(k).start()
    ends(3, range(nl - 1))
    for t in range(2, nl - 1):
        slot(2, t)
    seq_pass(1)
    relay(1)
    close(2)
    for t in range(1, nl - 1):
        slot(3, t)

    total = snd_s[f]
    for k in range(1, nf):
        small_send(k).wait_recv()
        total = total + got_s[k]
    sown_s[...] = total

    def small_share(k):
        return rcopy(sown_s, sgot_s.at[s], es.at[k], er.at[k], {"seq": s ^ k})

    for k in range(1, SEQ):
        small_share(k).start()
    close(3)
    relay(2)

    for a in range(2):
        seq_one(1, a, 1).wait_recv()
        seq_two(1, a).wait_recv()
        dsh_s[rows_of(1, a), :] = add(chunk(s, a)[...], ab1[a, 1], az1[a, 1])

    def grad_tokens(i, carry):
        x = xc_s[pl.ds(pl.multiple_of(s * rows + i * 64, 64), 64), :].astype(F32)
        rho = lax.rsqrt(jnp.sum(x * x, axis=1, keepdims=True) * (1.0 / D) + EPS)
        at = [pl.ds(pl.multiple_of((2 + a) * rows + i * 64, 64), 64) for a in range(2)]
        n0 = [x[:, cols[a]] * rho for a in range(2)]
        e0 = [dsh_s[at[a], :] * pre_s[5:6, cols[a]] for a in range(2)]
        dot = sum(jnp.sum(e0[a] * n0[a], axis=1, keepdims=True) for a in range(2))
        mean = dot * (1.0 / D)
        cot = cotrow_s[pl.ds(pl.multiple_of(i * 64, 64), 64), :].astype(F32)
        for a in range(2):
            dsh_s[at[a], :] = cot[:, cols[a]] + rho * (e0[a] - n0[a] * mean)
        return carry

    lax.fori_loop(0, rows // 64, grad_tokens, 0)
    for a in range(2):
        result(1, a).start()
    relay(3)

    for k in range(1, SEQ):
        small_share(k).wait()
    total = jnp.zeros_like(sown_s)
    for k in range(SEQ):
        total = total + jnp.where(s == k, sown_s[...], sgot_s[k])
    small_ref[...] = total
    for t in range(2):
        for a in range(2):
            result(t, a).wait()
    for k in range(1, nf):
        small_send(k).wait_send()
    seq_one_sent(1)
    for t in range(2):
        for a in range(2):
            seq_two(t, a).wait_send()
    for g in range(4):
        seq_gather_finish(g, owns[g], gouts[g], as_, ar, px, py, s)
        pltpu.make_async_copy(owns[g], gouts[g].at[pl.ds(s * n, n)], os_.at[g]).wait()
        line_sent(g)
    for g in range(1, 4):
        swaps_sent(g)


def back(nf, big, par):
    shape = jax.ShapeDtypeStruct
    vm = pltpu.VMEM
    dma = pltpu.SemaphoreType.DMA
    length = big[0].shape[0]
    rows = length // SEQ
    nl = nf // 2
    n = D // nf
    widths = (W, W, W, VC - W)
    boxes = [vm((nl, n, w), BF16) for w in widths] + [vm((nl + 1, n, w), BF16) for w in widths]
    boxes += [vm((n, w), BF16) for w in widths]
    return pl.pallas_call(
        functools.partial(back_kernel, nf),
        out_shape=[shape((rows, D), F32)] * 2 + [shape((SEQ * n, w), BF16) for w in widths] + [shape((8, 512), F32)],
        in_specs=[ANY] * len(big) + [VMEM] * len(par),
        out_specs=[ANY] * 6 + [VMEM],
        scratch_shapes=[
            vm((length, D), BF16),
            vm((length, D), BF16),
            vm((D, W), BF16),
            vm((D, VC - W), BF16),
            vm((D, W), BF16),
            vm((D, W), BF16),
            vm((length, VC), BF16),
            vm((length, W), BF16),
            vm((length, W), BF16),
            vm((length // Q, STATE, W), BF16),
            vm((length, W), F32),
            vm((length, W), BF16),
            vm((length, VC), BF16),
            vm((rows, D), BF16),
            vm((length, D), BF16),
            vm((D, W), BF16),
            vm((D, W), BF16),
            vm((D, VC - W), BF16),
        ]
        + boxes
        + [vm((2, 2, rows, D // 2), BF16)] * 4
        + [
            vm((8, CH), F32),
            vm((8, W), F32),
            vm((8, 128), F32),
            vm((8, W), F32),
            vm((8, D), F32),
            vm((8, XBC), F32),
            vm((8, INNER), F32),
            vm((nf, 8, 512), F32),
            vm((nf, 8, 512), F32),
            vm((8, 512), F32),
            vm((SEQ, 8, 512), F32),
            vm((Q + 8, CH), F32),
            vm((Q + 8, CH), F32),
            vm((STATE, W), F32),
            vm((128, Q), F32),
            vm((Q, W), BF16),
            vm((Q, W), BF16),
            vm((8, W), F32),
            dma((13,)),
            dma((4, 3, nl)),
            dma((4, 3, nl)),
            dma((2, 2, 3)),
            dma((2, 2, 3)),
            dma((4, 4)),
            dma((4, 4)),
            dma((nf,)),
            dma((nf,)),
            dma((SEQ,)),
            dma((SEQ,)),
            dma((4,)),
        ],
        name="back",
        compiler_params=pltpu.CompilerParams(
            collective_id=2, has_side_effects=True, vmem_limit_bytes=67043328
        ),
    )(*big, *par)


def finish_kernel(
    go, gg, gv, gs, out, gt, small, out_o, gt_o, gin_o, gout_o, cw_o, cb_o, pre_o, post_o, step_o, decay_o, skip_o
):
    out_o[...] = out[...]
    gt_o[...] = gt[...]
    for i in range(SEQ):
        gin_o[:, i * W : i * W + W] = gg[i].astype(F32)
        gin_o[:, INNER + i * W : INNER + i * W + W] = gv[i].astype(F32)
    total = gs[0].astype(F32)
    for i in range(1, SEQ):
        total = total + gs[i].astype(F32)
    rest = gin_o.shape[1] - 2 * INNER
    gin_o[:, 2 * INNER :] = total[:, :rest]
    gout_o[...] = go[0].astype(F32)

    @pl.when(pl.program_id(0) == 0)
    def _():
        cw_o[...] = small[0:4, : cw_o.shape[1]]
        cb_o[...] = small[4:5, : cb_o.shape[1]]
        pre_o[...] = small[5:6, : pre_o.shape[1]]
        post_o[...] = small[6:7, : post_o.shape[1]]
        heads = step_o.shape[1]
        step_o[...] = small[7:8, :heads]
        decay_o[...] = small[7:8, 128 : 128 + heads]
        skip_o[...] = small[7:8, 256 : 256 + heads]


def finish(nf, go, gg, gv, gs, out, gt, small):
    shape = jax.ShapeDtypeStruct
    n = D // nf
    step, rows = n // SEQ, out.shape[0] // SEQ
    proj = 2 * INNER + 2 * STATE + HEADS
    go, gg, gv, gs = (g.reshape(SEQ, n, g.shape[1]) for g in (go, gg, gv, gs))

    def whole(*dims):
        return pl.BlockSpec(dims, lambda i: (0,) * len(dims))

    tiny = [(4, XBC // nf), (1, XBC // nf), (1, n), (1, INNER // nf)] + [(1, HEADS // nf)] * 3
    return pl.pallas_call(
        finish_kernel,
        grid=(SEQ,),
        out_shape=[shape(out.shape, F32)] * 2
        + [shape((n, proj), F32), shape((n, INNER), F32)]
        + [shape(dims, F32) for dims in tiny],
        in_specs=[
            pl.BlockSpec((1, n, W), lambda i: (i, 0, 0)),
            pl.BlockSpec((SEQ, step, W), lambda i: (0, i, 0)),
            pl.BlockSpec((SEQ, step, W), lambda i: (0, i, 0)),
            pl.BlockSpec((SEQ, step, VC - W), lambda i: (0, i, 0)),
            pl.BlockSpec((rows, D), lambda i: (i, 0)),
            pl.BlockSpec((rows, D), lambda i: (i, 0)),
            whole(8, 512),
        ],
        out_specs=[
            pl.BlockSpec((rows, D), lambda i: (i, 0)),
            pl.BlockSpec((rows, D), lambda i: (i, 0)),
            pl.BlockSpec((step, proj), lambda i: (i, 0)),
            pl.BlockSpec((n, W), lambda i: (0, i)),
        ]
        + [whole(*dims) for dims in tiny],
        name="finish",
        compiler_params=pltpu.CompilerParams(vmem_limit_bytes=VMEM_LIMIT),
    )(go, gg, gv, gs, out, gt, small)


def body(
    tokens,
    input_projection_weight,
    pre_gain,
    conv_weight,
    conv_bias,
    step_bias,
    decay_log,
    skip_gain,
    post_gain,
    output_projection_weight,
    cotangent,
):
    nf = lax.axis_size("fsdp")
    tok = tokens.reshape(tokens.shape[1:])
    cot = cotangent.reshape(cotangent.shape[1:])
    win = input_projection_weight

    w_state = jnp.pad(win[:, 2 * INNER :], ((0, 0), (0, VC - W - (win.shape[1] - 2 * INNER))))
    w_out = output_projection_weight.T

    flat, at = jnp.zeros((2048,), F32), 0
    for v, size in (
        (conv_bias, 512), (pre_gain, 512), (post_gain, 512), (step_bias, 128), (decay_log, 128), (skip_gain, 256),
    ):
        flat = flat + jnp.pad(v.astype(F32), (at, 2048 - at - v.shape[0]))
        at += size
    taps = jnp.pad(conv_weight.T.astype(F32), ((0, 4), (0, 512 - conv_weight.shape[0])))
    small = taps + jnp.pad(flat.reshape(4, 512), ((4, 0), (0, 0)))
    outs = front(nf, tok, cot, win, w_state, w_out, small)
    out, gt, g_out, g_gate, g_val, g_state, small = back(nf, outs[:12], outs[12:])
    block_out, grad_tokens, grad_in, grad_out, cw, cb, pre, post, step, decay, skip = finish(
        nf, g_out, g_gate, g_val, g_state, out, gt, small
    )
    return (
        block_out[None],
        grad_tokens[None],
        grad_in,
        pre.reshape(-1),
        cw.T,
        cb.reshape(-1),
        step.reshape(-1),
        decay.reshape(-1),
        skip.reshape(-1),
        post.reshape(-1),
        grad_out.T,
    )


def solution(mesh):
    in_specs = (
        P("fsdp", "seq", None),
        P("fsdp", None),
        P("fsdp"),
        P("fsdp", None),
        P("fsdp"),
        P("fsdp"),
        P("fsdp"),
        P("fsdp"),
        P("fsdp"),
        P(None, "fsdp"),
        P("fsdp", "seq", None),
    )
    out_specs = (
        P("fsdp", "seq", None),
        P("fsdp", "seq", None),
        P("fsdp", None),
        P("fsdp"),
        P("fsdp", None),
        P("fsdp"),
        P("fsdp"),
        P("fsdp"),
        P("fsdp"),
        P("fsdp"),
        P(None, "fsdp"),
    )
    return jax.shard_map(body, mesh=mesh, in_specs=in_specs, out_specs=out_specs, check_vma=False)
```

```python
import functools

import jax
import jax.numpy as jnp
from jax import lax
from jax.experimental import pallas as pl
from jax.experimental.pallas import tpu as pltpu
from jax.sharding import PartitionSpec as P

D = 1536
INNER = 3072
STATE = 128
HEADS = 48
XBC = INNER + 2 * STATE
EPS = 1e-05

SEQ = 4
W = INNER // SEQ
HL = HEADS // SEQ
HW = INNER // HEADS
CH = W + 2 * STATE
VC = CH + 128
Q = 128

F32 = jnp.float32
BF16 = jnp.bfloat16
MESH = pl.DeviceIdType.MESH
HIGH = lax.Precision.HIGHEST
VMEM = pl.BlockSpec(memory_space=pltpu.VMEM)
ANY = pl.BlockSpec(memory_space=pl.ANY)
VMEM_LIMIT = 64000 * 1024


def rcopy(src, dst, send_sem, recv_sem, device):
    return pltpu.make_async_remote_copy(
        src_ref=src, dst_ref=dst, send_sem=send_sem, recv_sem=recv_sem, device_id=device, device_id_type=MESH
    )


def signal(sem, device):
    pl.semaphore_signal(sem, inc=1, device_id=device, device_id_type=MESH)


def nn(a, b, precision=None):
    return lax.dot_general(a, b, (((1,), (0,)), ((), ())), precision=precision, preferred_element_type=F32)


def nt(a, b, precision=None):
    return lax.dot_general(a, b, (((1,), (1,)), ((), ())), precision=precision, preferred_element_type=F32)


def seq_gather_start(refs, outs, send, recv, px, py, me):
    for g, (src, out) in enumerate(zip(refs, outs)):
        n = src.shape[0]
        own = out.at[pl.ds(me * n, n)]
        rcopy(src, own, send.at[g, 0], recv.at[g, 0], {"seq": px}).start()
        rcopy(src, own, send.at[g, 1], recv.at[g, 1], {"seq": py}).start()


def seq_gather_relay(g, src, out, send, recv, px, py, me):
    n = src.shape[0]
    h = n // 2
    own = out.at[pl.ds(me * n, n)]
    rcopy(src, own, send.at[g, 0], recv.at[g, 0], {"seq": px}).wait_recv()
    top = out.at[pl.ds(px * n, h)]
    rcopy(top, top, send.at[g, 2], recv.at[g, 2], {"seq": py}).start()
    rcopy(src, own, send.at[g, 1], recv.at[g, 1], {"seq": py}).wait_recv()
    low = out.at[pl.ds(py * n + h, h)]
    rcopy(low, low, send.at[g, 3], recv.at[g, 3], {"seq": px}).start()


def seq_gather_finish(g, src, out, send, recv, px, py, me):
    n = src.shape[0]
    h = n // 2
    own = out.at[pl.ds(me * n, n)]
    half = out.at[pl.ds(me * n, h)]
    rcopy(half, half, send.at[g, 2], recv.at[g, 2], {"seq": py}).wait()
    rcopy(half, half, send.at[g, 3], recv.at[g, 3], {"seq": px}).wait()
    rcopy(src, own, send.at[g, 0], recv.at[g, 0], {"seq": px}).wait_send()
    rcopy(src, own, send.at[g, 1], recv.at[g, 1], {"seq": py}).wait_send()


def softplus(x):
    return jnp.maximum(x, 0.0) + jnp.log1p(jnp.exp(-jnp.abs(x)))


def sigmoid(x):
    return 1.0 / (1.0 + jnp.exp(-x))


def rates_of(r_ref, rows, hp_ref, tri):
    back = lax.rem(128 - lax.axis_index("seq") * HL, 128)
    raw = pltpu.roll(r_ref[rows, :].astype(F32), back, 1) + hp_ref[0:1, :]
    dt = softplus(raw)
    lam = nn(tri, dt * hp_ref[1:2, :], HIGH)
    return raw, dt, lam


def spread(mat, h):
    return jnp.broadcast_to(mat[:, h : h + 1], (mat.shape[0], 128))


def scan_fwd_blocks(
    v_ref, s_ref, r_ref, kw_ref, hp_ref, ex_ref, mixed_ref, st_ref, buf, hst, xw_s, er_s, between
):
    blocks = v_ref.shape[0] // Q
    row = lax.broadcasted_iota(jnp.int32, (Q, Q), 0)
    col = lax.broadcasted_iota(jnp.int32, (Q, Q), 1)
    causal = row >= col
    tri = causal.astype(F32)
    low = lax.broadcasted_iota(jnp.int32, (Q, 128), 1) < HW
    low1 = lax.broadcasted_iota(jnp.int32, (1, 128), 1) < HW
    buf[0:8, :] = jnp.zeros((8, CH), F32)
    hst[...] = jnp.zeros_like(hst)

    def block(b, carry):
        rows = pl.ds(pl.multiple_of(b * Q, Q), Q)
        buf[8 : 8 + Q, 0:W] = v_ref[rows, :].astype(F32)
        buf[8 : 8 + Q, W:CH] = s_ref[rows, :].astype(F32)
        k = kw_ref[4:5, :] + buf[5 : 5 + Q, :] * kw_ref[0:1, :]
        for j in range(1, 4):
            k = k + buf[5 + j : 5 + j + Q, :] * kw_ref[j : j + 1, :]
        buf[0:8, :] = buf[Q : Q + 8, :]
        x = k * sigmoid(k)
        bs, cs = x[:, W : W + STATE], x[:, W + STATE :]
        _, dt, lam = rates_of(r_ref, rows, hp_ref, tri)
        lam_t, dt_t = lam.T, dt.T
        last = lam[Q - 1 : Q, :]
        tail = dt * jnp.exp(last - lam)
        aff = nt(cs, bs, HIGH)
        st_ref[b] = hst[...].astype(BF16)
        ch = nn(cs.astype(BF16), st_ref[b])
        for i in range(HL // 2):
            at = slice(128 * i, 128 * i + 128)
            xp = x[:, at]
            xb = xp.astype(BF16)
            y, lc = [], []
            for h in (2 * i, 2 * i + 1):
                lcol = spread(lam, h)
                within = jnp.exp(jnp.where(causal, lcol - lam_t[h : h + 1, :], -1e30))
                y.append(nn((aff * within * dt_t[h : h + 1, :]).astype(BF16), xb))
                lc.append(lcol)
            out = jnp.where(low, y[0], y[1])
            out = out + jnp.exp(jnp.where(low, lc[0], lc[1])) * ch[:, at] + ex_ref[0:1, at] * xp
            mixed_ref[rows, at] = out.astype(BF16)
            xw_s[:, at] = (xp * jnp.where(low, spread(tail, 2 * i), spread(tail, 2 * i + 1))).astype(BF16)
            er_s[0:1, at] = jnp.exp(jnp.where(low1, spread(last, 2 * i), spread(last, 2 * i + 1)))
        hst[...] = hst[...] * er_s[0:1, :] + nn(bs.T.astype(BF16), xw_s[...])
        between(b)
        return carry

    lax.fori_loop(0, blocks, block, 0)


def scan_bwd_blocks(
    v_ref, s_ref, r_ref, dy_ref, st_ref, kw_ref, hp_ref, ex_ref,
    dv_ref, gcw_ref, gch_ref, ghd_ref,
    buf, cbuf, dhst, rowp, xw_s, e_s, er_s, between,
):
    blocks = v_ref.shape[0] // Q
    row = lax.broadcasted_iota(jnp.int32, (Q, Q), 0)
    col = lax.broadcasted_iota(jnp.int32, (Q, Q), 1)
    tri = (row >= col).astype(F32)
    later = col >= row
    suffix = later.astype(F32)
    strict = (col < row).astype(F32)
    lane = lax.broadcasted_iota(jnp.int32, (Q, 128), 1)
    lane1 = lax.broadcasted_iota(jnp.int32, (1, 128), 1)
    low = lane < HW
    low1 = lane1 < HW
    buf[Q : Q + 8, :] = jnp.zeros((8, CH), F32)
    dhst[...] = jnp.zeros_like(dhst)
    rowp[...] = jnp.zeros_like(rowp)
    gcw_ref[...] = jnp.zeros_like(gcw_ref)
    gch_ref[...] = jnp.zeros_like(gch_ref)
    ghd_ref[...] = jnp.zeros_like(ghd_ref)

    def block(i0, carry):
        b = blocks - 1 - i0
        rows = pl.ds(pl.multiple_of(b * Q, Q), Q)
        before = pl.ds(pl.multiple_of(jnp.maximum(b * Q - 16, 0), 16), 16)
        keep = (b > 0).astype(F32)
        cbuf[0:8, 0:W] = v_ref[before, :].astype(F32)[8:16, :] * keep
        cbuf[0:8, W:CH] = s_ref[before, :].astype(F32)[8:16, :] * keep
        cbuf[8 : 8 + Q, 0:W] = v_ref[rows, :].astype(F32)
        cbuf[8 : 8 + Q, W:CH] = s_ref[rows, :].astype(F32)
        k = kw_ref[4:5, :] + cbuf[5 : 5 + Q, :] * kw_ref[0:1, :]
        for j in range(1, 4):
            k = k + cbuf[5 + j : 5 + j + Q, :] * kw_ref[j : j + 1, :]
        sg = sigmoid(k)
        x = k * sg
        ds = sg * (1.0 + k * (1.0 - sg))
        bs, cs = x[:, W : W + STATE], x[:, W + STATE :]
        bb, cb = bs.astype(BF16), cs.astype(BF16)
        raw, dt, lam = rates_of(r_ref, rows, hp_ref, tri)
        lam_t = lam.T
        last = lam[Q - 1 : Q, :]
        aff_t = nt(bs, cs, HIGH)
        hb = st_ref[b]
        dhb = dhst[...].astype(BF16)
        ch = nn(cb, hb)
        bd = nn(bb, dhb)
        daff_t = jnp.zeros((Q, Q), F32)
        col_n = jnp.zeros((Q, 128), F32)
        col_i = jnp.zeros((Q, 128), F32)
        row_i = jnp.zeros((Q, 128), F32)
        through = jnp.zeros((1, 128), F32)
        for i in range(HL // 2):
            at = slice(128 * i, 128 * i + 128)
            xp = x[:, at]
            xb = xp.astype(BF16)
            dyb = dy_ref[rows, at]
            dyf = dyb.astype(F32)
            z, lc, dc = [], [], []
            for h in (2 * i, 2 * i + 1):
                mine = low if h % 2 == 0 else jnp.logical_not(low)
                lcol, dcol = spread(lam, h), spread(dt, h)
                within = jnp.exp(jnp.where(later, lam_t[h : h + 1, :] - lcol, -1e30))
                g = nt(jnp.where(mine, xp, 0.0).astype(BF16), dyb)
                lg = within * g
                lgd = lg * dcol
                daff_t = daff_t + lgd
                col_n = jnp.where(lane == h, jnp.sum(aff_t * lg, axis=1, keepdims=True), col_n)
                rowp[h : h + 1, :] = jnp.sum(aff_t * lgd, axis=0, keepdims=True)
                z.append(nn((aff_t * within).astype(BF16), dyb))
                lc.append(lcol)
                dc.append(dcol)
            lamp = jnp.where(low, lc[0], lc[1])
            dtp = jnp.where(low, dc[0], dc[1])
            lastp = jnp.where(low1, spread(last, 2 * i), spread(last, 2 * i + 1))
            e = dyf * jnp.exp(lamp)
            e_s[:, at] = e.astype(BF16)
            ew = jnp.exp(lastp - lamp)
            bdp = bd[:, at]
            xw_s[:, at] = (xp * (dtp * ew)).astype(BF16)
            er_s[0:1, at] = jnp.exp(lastp)
            re = e * ch[:, at]
            ci = xp * bdp * ew
            th = jnp.sum(dhst[:, at] * hb[:, at].astype(F32), axis=0, keepdims=True) * er_s[0:1, at]
            for h in (2 * i, 2 * i + 1):
                mine = low if h % 2 == 0 else jnp.logical_not(low)
                mine1 = low1 if h % 2 == 0 else jnp.logical_not(low1)
                row_i = jnp.where(lane == h, jnp.sum(jnp.where(mine, re, 0.0), axis=1, keepdims=True), row_i)
                col_i = jnp.where(lane == h, jnp.sum(jnp.where(mine, ci, 0.0), axis=1, keepdims=True), col_i)
                through = jnp.where(
                    lane1 == h, jnp.sum(jnp.where(mine1, th, 0.0), axis=1, keepdims=True), through
                )
            dx = dtp * jnp.where(low, z[0], z[1]) + bdp * (dtp * ew) + ex_ref[0:1, at] * dyf
            gch_ref[0:1, at] += jnp.sum(dyf * xp, axis=0, keepdims=True)
            buf[0:Q, at] = dx * ds[:, at]
        daff_b = daff_t.astype(BF16)
        d_bs = nt(xw_s[...], dhb) + nn(daff_b, cb)
        d_cs = nt(e_s[...], hb) + nn(daff_t.T.astype(BF16), bb)
        buf[0:Q, W : W + STATE] = d_bs * ds[:, W : W + STATE]
        buf[0:Q, W + STATE : CH] = d_cs * ds[:, W + STATE :]
        dhst[...] = dhst[...] * er_s[0:1, :] + nn(cs.T.astype(BF16), e_s[...])
        after = nn(suffix, rowp[...].T - dt * col_n + row_i, HIGH) + nn(strict, dt * col_i, HIGH) + through
        d_rate = (col_n + col_i + hp_ref[1:2, :] * after) * sigmoid(raw)
        ghd_ref[0:1, :] += jnp.sum(d_rate, axis=0, keepdims=True)
        ghd_ref[1:2, :] += jnp.sum(dt * after, axis=0, keepdims=True) * hp_ref[1:2, :]
        dv_ref[rows, CH:VC] = pltpu.roll(d_rate, lax.axis_index("seq") * HL, 1).astype(BF16)
        for at in (slice(0, W), slice(W, CH)):
            raw_v = cbuf[8 : 8 + Q, at]
            dk = buf[0:Q, at]
            dv = dk * kw_ref[3:4, at]
            gcw_ref[4:5, at] += jnp.sum(dk, axis=0, keepdims=True)
            gcw_ref[3:4, at] += jnp.sum(dk * raw_v, axis=0, keepdims=True)
            for j in range(3):
                dk = buf[3 - j : 3 - j + Q, at]
                dv = dv + dk * kw_ref[j : j + 1, at]
                gcw_ref[j : j + 1, at] += jnp.sum(dk * raw_v, axis=0, keepdims=True)
            dv_ref[rows, at] = dv.astype(BF16)
        buf[Q : Q + 8, :] = buf[0:8, :]
        between(i0)
        return carry

    lax.fori_loop(0, blocks, block, 0)


GROUPS = 4


def place(block, at, width):
    start, shift = at // 128 * 128, at % 128
    lanes = -(-(width + shift) // 128) * 128
    have = block.shape[1]
    if lanes > have:
        block = jnp.concatenate([block, jnp.zeros((block.shape[0], lanes - have), block.dtype)], axis=1)
    else:
        block = block[:, :lanes]
    if shift:
        block = pltpu.roll(block, shift, 1)
    return start, lanes, block


TN = (((0,), (0,)), ((), ()))
STRIP = 384


def unplace(block, at, width):
    start, shift = at // 128 * 128, at % 128
    lanes = -(-(width + shift) // 128) * 128
    piece = block[:, start : start + lanes]
    if shift:
        piece = pltpu.roll(piece, lanes - shift, 1)
    if lanes < 512:
        piece = jnp.concatenate([piece, jnp.zeros((piece.shape[0], 512 - lanes), piece.dtype)], axis=1)
    else:
        piece = piece[:, :512]
    return jnp.where(lax.broadcasted_iota(jnp.int32, piece.shape, 1) < width, piece, 0.0)


def mixer_kernel(
    nf, tok, cot, win, wst, wout, small,
    out_ref, gt_ref, go_ref, gg_ref, gv_ref, gs_ref, small_ref, x_hbm,
    cot_s, nrm_s, wv_s, ws_s, wg_s, wo_s, mix_s, gate_s, mixed_s, st_s, dsh_s,
    dy_s, dv_s, cotrow_s, part_s, ga_s, gb_s, gc_s,
    pb0, pb1, pb2, pb3, pb4, lb0, lb1, lb2, lb3, lb4, own0, own1, own2, own3, own4,
    ab0, ab1, az0, az1,
    kw_s, hp_s, ex_s, pre_s, stat_s, stat_own, stat_got,
    gcw_s, gch_s, ghd_s, gpost_s, gpre_s, conv_s, post_s, snd_s, got_s, sown_s, sgot_s,
    buf, cbuf, dhst, rowp, xw_s, e_s, er_s,
    ls, xs, xr, zs, zr, ms, mr, es, er, bzs, bzr, bxs, bxr, as_, ar, bms, bmr, bes, ber, os_,
):
    x_s, small_s = part_s, snd_s
    s = lax.axis_index("seq")
    f = lax.axis_index("fsdp")
    px, py = s ^ 1, s ^ 2
    nl = nf // 2
    p, c = f // 2, f % 2
    partner = p * 2 + 1 - c
    bar = pltpu.get_barrier_semaphore()
    for k in range(1, SEQ):
        signal(bar, {"seq": s ^ k})
    for k in range(1, nf):
        signal(bar, {"fsdp": lax.rem(f + k, nf)})
    pl.semaphore_wait(bar, nf - 1 + SEQ - 1)

    n = win.shape[0]
    rows = tok.shape[0]
    length = rows * SEQ
    quarter = n // SEQ
    ins = (
        win.at[:, pl.ds(pl.multiple_of(INNER + s * W, 128), W)],
        wst.at[pl.ds(pl.multiple_of(s * quarter, 8), quarter)],
        win.at[:, pl.ds(pl.multiple_of(s * W, 128), W)],
        wout.at[:, pl.ds(pl.multiple_of(s * W, 128), W)],
    )
    outs = (wv_s, ws_s, wg_s, wo_s)

    def row(g, i):
        return ws_s.at[i, s] if g == 1 else outs[g].at[pl.ds(i * n, n)]

    def hop(g, src, i, way, k, device):
        return rcopy(src, row(g, i), zs.at[g, way, k], zr.at[g, i], {"fsdp": device})

    def own_send(g):
        @pl.when(p < nl - 1)
        def _():
            hop(g, ins[g], f, 0, 0, f + 2).start()

        @pl.when(p > 0)
        def _():
            hop(g, ins[g], f, 1, 0, f - 2).start()

        hop(g, ins[g], f, 2, 0, partner).start()
        pltpu.make_async_copy(ins[g], row(g, f), ls.at[g]).start()

    def step(g, k):
        @pl.when(p - k >= 0)
        def _():
            o = f - 2 * k
            hop(g, row(g, o), o, 0, k, f).wait_recv()

            @pl.when(p < nl - 1)
            def _():
                hop(g, row(g, o), o, 0, k, f + 2).start()

            hop(g, row(g, o), o, 2, k, partner).start()

        @pl.when(p + k < nl)
        def _():
            o = f + 2 * k
            hop(g, row(g, o), o, 1, k, f).wait_recv()

            @pl.when(p > 0)
            def _():
                hop(g, row(g, o), o, 1, k, f - 2).start()

            hop(g, row(g, o), o, 3, k, partner).start()

    def arrive(g):
        pltpu.make_async_copy(ins[g], row(g, f), ls.at[g]).wait()
        for q in range(nl):
            o = q * 2 + 1 - c
            hop(g, row(g, o), o, 2, 0, partner).wait_recv()

    def sent(g):
        hop(g, ins[g], f, 2, 0, partner).wait_send()

        @pl.when(p < nl - 1)
        def _():
            hop(g, ins[g], f, 0, 0, f + 2).wait_send()

        @pl.when(p > 0)
        def _():
            hop(g, ins[g], f, 1, 0, f - 2).wait_send()

        for k in range(1, nl):
            @pl.when(p - k >= 0)
            def _():
                o = f - 2 * k

                @pl.when(p < nl - 1)
                def _():
                    hop(g, row(g, o), o, 0, k, f + 2).wait_send()

                hop(g, row(g, o), o, 2, k, partner).wait_send()

            @pl.when(p + k < nl)
            def _():
                o = f + 2 * k

                @pl.when(p > 0)
                def _():
                    hop(g, row(g, o), o, 1, k, f - 2).wait_send()

                hop(g, row(g, o), o, 3, k, partner).wait_send()

    def small_copy(k):
        return rcopy(small, small_s.at[f], ms.at[k], mr.at[k], {"fsdp": lax.rem(f + k, nf)})

    mine = pl.ds(s * rows, rows)
    own_small = pltpu.make_async_copy(small, small_s.at[f], ls.at[4])
    own_tok = pltpu.make_async_copy(tok, x_s.at[mine], ls.at[5])
    own_cot = pltpu.make_async_copy(cot, cot_s.at[mine], ls.at[6])
    own_row = pltpu.make_async_copy(cot, cotrow_s, ls.at[7])

    def st_hop(k, region, device):
        return rcopy(region, region, xs.at[2, k], xr.at[2, k], {"seq": device})

    st_own = ws_s.at[:, s]
    st_top, st_low = ws_s.at[pl.ds(0, nl), px], ws_s.at[pl.ds(nl, nl), py]

    for k in range(1, nf):
        small_copy(k).start()
    own_small.start()
    own_tok.start()
    seq_gather_start((tok,), (x_s,), xs, xr, px, py, s)
    own_send(1)
    own_send(0)
    own_cot.start()
    own_row.start()
    for k in range(1, min(3, nl)):
        step(1, k)
    step(0, 1)
    for k in range(3, nl):
        step(1, k)
    arrive(1)
    st_hop(0, st_own, px).start()
    st_hop(1, st_own, py).start()
    seq_gather_relay(0, tok, x_s, xs, xr, px, py, s)
    for k in range(2, min(3, nl)):
        step(0, k)
    own_send(2)
    own_send(3)

    own_small.wait()
    for k in range(1, nf):
        small_copy(k).wait()
    conv_s[...] = jnp.zeros_like(conv_s)
    pre_s[...] = jnp.zeros_like(pre_s)
    post_s[...] = jnp.zeros_like(post_s)
    heads = [jnp.zeros((8, 128), F32) for _ in range(3)]
    for i in range(nf):
        block = small_s[i]
        at, lanes, moved = place(block, i * (XBC // nf), XBC // nf)
        conv_s[:, at : at + lanes] += moved
        at, lanes, moved = place(block, i * (D // nf), D // nf)
        pre_s[:, at : at + lanes] += jnp.where(lax.broadcasted_iota(jnp.int32, moved.shape, 0) == 5, moved, 0.0)
        at, lanes, moved = place(block, i * (INNER // nf), INNER // nf)
        post_s[:, at : at + lanes] += jnp.where(lax.broadcasted_iota(jnp.int32, moved.shape, 0) == 6, moved, 0.0)
        for j in range(3):
            piece = block[:, 128 * j : 128 * j + 128]
            at = i * (HEADS // nf)
            heads[j] = heads[j] + (pltpu.roll(piece, at, 1) if at else piece)
    kw_s[:, 0:W] = conv_s[:, pl.ds(pl.multiple_of(s * W, 128), W)]
    kw_s[:, W:CH] = conv_s[:, INNER:XBC]
    lane1 = lax.broadcasted_iota(jnp.int32, (1, 128), 1)
    low1 = lane1 < HW
    back = lax.rem(128 - s * HL, 128)
    step_b, decay, skip = [pltpu.roll(h, back, 1)[7:8, :] for h in heads]
    hp_s[...] = jnp.zeros_like(hp_s)
    hp_s[0:1, :] = jnp.where(lane1 < HL, step_b, 0.0)
    hp_s[1:2, :] = jnp.where(lane1 < HL, -jnp.exp(decay), 0.0)
    ex_s[...] = jnp.zeros_like(ex_s)
    for i in range(HL // 2):
        ex_s[0:1, 128 * i : 128 * i + 128] = jnp.where(low1, spread(skip, 2 * i), spread(skip, 2 * i + 1))
    ex_s[1:2, :] = post_s[6:7, pl.ds(pl.multiple_of(s * W, 128), W)]

    st_hop(0, st_own, px).wait_recv()
    st_hop(2, st_top, py).start()
    st_hop(1, st_own, py).wait_recv()
    st_hop(3, st_low, px).start()
    own = cot_s.at[mine]
    rcopy(cot, own, xs.at[1, 0], xr.at[1, 0], {"seq": px}).start()
    rcopy(cot, own, xs.at[1, 1], xr.at[1, 1], {"seq": py}).start()
    for k in range(3, nl):
        step(0, k)
    own_tok.wait()
    seq_gather_finish(0, tok, x_s, xs, xr, px, py, s)

    def norm(i, carry):
        r = pl.ds(pl.multiple_of(i * 128, 128), 128)
        x = x_s[r, :].astype(F32)
        rho = lax.rsqrt(jnp.sum(x * x, axis=1, keepdims=True) * (1.0 / D) + EPS)
        nrm_s[r, :] = (x * rho * pre_s[5:6, :]).astype(BF16)
        return carry

    lax.fori_loop(0, length // 128, norm, 0)
    x_save = pltpu.make_async_copy(x_s, x_hbm, ls.at[8])
    x_save.start()
    arrive(0)

    def project(i, carry):
        r = pl.ds(pl.multiple_of(i * 256, 256), 256)
        mix_s[r, 0:W] = nn(nrm_s[r, :], wv_s[...]).astype(BF16)
        return carry

    def project_state(i, carry):
        r = pl.ds(pl.multiple_of(i * 256, 256), 256)
        mix_s[r, W:VC] = nn(nrm_s[r, :], ws_s[...].reshape(D, VC - W)).astype(BF16)
        return carry

    lax.fori_loop(0, length // 256, project, 0)
    step(2, 1)
    st_hop(2, st_top, py).wait()
    st_hop(3, st_low, px).wait()
    lax.fori_loop(0, length // 256, project_state, 0)

    def between(b):
        @pl.when(b == 1)
        def _():
            step(3, 1)

        @pl.when(b == 4)
        def _():
            step(2, 2)

    scan_fwd_blocks(
        mix_s.at[:, 0:W], mix_s.at[:, W:CH], mix_s.at[:, CH:VC], kw_s, hp_s, ex_s, mixed_s, st_s,
        buf, dhst, xw_s, er_s, between,
    )
    step(3, 2)
    seq_gather_relay(1, cot, cot_s, xs, xr, px, py, s)
    for k in range(3, nl):
        step(2, k)
    arrive(2)

    def project_gate(i, carry):
        r = pl.ds(pl.multiple_of(i * 256, 256), 256)
        gate_s[r, :] = nn(nrm_s[r, :], wg_s[...]).astype(BF16)
        return carry

    lax.fori_loop(0, length // 256, project_gate, 0)
    for k in range(3, nl):
        step(3, k)
    own_cot.wait()
    seq_gather_finish(1, cot, cot_s, xs, xr, px, py, s)
    arrive(3)
    eye = lax.broadcasted_iota(jnp.int32, (128, 128), 0) == lax.broadcasted_iota(jnp.int32, (128, 128), 1)

    def stats(i, carry):
        r = pl.ds(pl.multiple_of(i * 128, 128), 128)
        dsh = nn(cot_s[r, :], wo_s[...])
        dsh_s[r, :] = dsh
        gate = gate_s[r, :].astype(F32)
        gated = mixed_s[r, :].astype(F32) * (gate * sigmoid(gate))
        one = jnp.sum(gated * gated, axis=1, keepdims=True)
        two = jnp.sum(dsh * ex_s[1:2, :] * gated, axis=1, keepdims=True)
        stat_own[pl.ds(i, 1), :] = jnp.sum(jnp.where(eye, one, 0.0), axis=0, keepdims=True)
        stat_own[pl.ds(length // 128 + i, 1), :] = jnp.sum(jnp.where(eye, two, 0.0), axis=0, keepdims=True)
        return carry

    lax.fori_loop(0, length // 128, stats, 0)
    copies = [rcopy(stat_own, stat_got.at[k], es.at[k], er.at[k], {"seq": s ^ k}) for k in range(1, SEQ)]
    for copy in copies:
        copy.start()
    for copy in copies:
        copy.wait()
    stat_s[...] = stat_own[...] + stat_got[1] + (stat_got[2] + stat_got[3])
    for g in range(GROUPS):
        sent(g)
    st_hop(0, st_own, px).wait_send()
    st_hop(1, st_own, py).wait_send()
    own_row.wait()

    half = D // 2
    cols = (slice(0, half), slice(half, D))
    first, second = (px, py), (py, px)
    ab, az = (ab0, ab1), (az0, az1)

    def chunk(i, a):
        return part_s.at[pl.ds(i * rows, rows), cols[a]]

    def seq_one(t, a, m):
        i = (first[a] ^ second[a] ^ s) if m == 0 else first[a]
        return rcopy(chunk(i, a), ab[t].at[a, m], bxs.at[t, a, m], bxr.at[t, a, m], {"seq": first[a]})

    def seq_two(t, a):
        return rcopy(az[t].at[a, 0], az[t].at[a, 1], bxs.at[t, a, 2], bxr.at[t, a, 2], {"seq": second[a]})

    def add(*terms):
        total = terms[0].astype(F32)
        for term in terms[1:]:
            total = total + term.astype(F32)
        return total

    def seq_pass(t):
        for a in range(2):
            seq_one(t, a, 0).wait_recv()
            az[t][a, 0] = add(chunk(second[a], a)[...], ab[t][a, 0]).astype(BF16)
            seq_two(t, a).start()

    def seq_last(t, out):
        for a in range(2):
            seq_one(t, a, 1).wait_recv()
            seq_two(t, a).wait_recv()
            out[:, cols[a]] = add(chunk(s, a)[...], ab[t][a, 1], az[t][a, 1])

    def seq_one_sent(t):
        for a in range(2):
            seq_one(t, a, 0).wait_send()
            seq_one(t, a, 1).wait_send()

    low_half, high_half = slice(0, W // 2), slice(W // 2, W)
    parts = (ga_s, gb_s, ga_s.at[:, low_half], ga_s.at[:, high_half], gc_s)
    pbs, lbs, owns = (pb0, pb1, pb2, pb3, pb4), (lb0, lb1, lb2, lb3, lb4), (own0, own1, own2, own3, own4)
    gouts = (go_ref, gg_ref, gv_ref.at[:, low_half], gv_ref.at[:, high_half], gs_ref)

    def piece(g, i):
        return parts[g].at[pl.ds(pl.multiple_of(i * n, 16), n)]

    def swap(g, q):
        return rcopy(piece(g, q * 2 + 1 - c), pbs[g].at[q], bzs.at[g, 0, q], bzr.at[g, 0, q], {"fsdp": partner})

    def up(g, q):
        return rcopy(pbs[g].at[q], lbs[g].at[q], bzs.at[g, 1, q], bzr.at[g, 1, q], {"fsdp": f + 2})

    def down(g, q):
        to = jnp.where(q == p - 1, nl, q)
        return rcopy(pbs[g].at[q], lbs[g].at[to], bzs.at[g, 2, q], bzr.at[g, 2, q], {"fsdp": f - 2})

    def send_up(g, q, terms):
        pbs[g][q] = add(piece(g, q * 2 + c)[...], pbs[g][q], *terms).astype(BF16)
        up(g, q).start()

    def send_down(g, q, terms):
        pbs[g][q] = add(piece(g, q * 2 + c)[...], pbs[g][q], *terms).astype(BF16)
        down(g, q).start()

    def ends(g, shards):
        for k in shards:
            @pl.when(p == 0)
            def _():
                swap(g, nl - 1 - k).wait_recv()
                send_up(g, nl - 1 - k, ())

            @pl.when(p == nl - 1)
            def _():
                swap(g, k).wait_recv()
                send_down(g, k, ())

    def slot(g, t):
        @pl.when(jnp.logical_and(p > 0, p <= t))
        def _():
            q = nl - 1 - t + p
            swap(g, q).wait_recv()
            up(g, q).wait_recv()
            send_up(g, q, (lbs[g][q],))

        @pl.when(jnp.logical_and(p < nl - 1, nl - 1 - p <= t))
        def _():
            q = t - (nl - 1 - p)
            swap(g, q).wait_recv()
            down(g, q).wait_recv()
            send_down(g, q, (lbs[g][q],))

    def close(g):
        swap(g, p).wait_recv()

        @pl.when(p > 0)
        def _():
            up(g, p).wait_recv()

        @pl.when(p < nl - 1)
        def _():
            down(g, p).wait_recv()

        @pl.when(p == 0)
        def _():
            owns[g][...] = add(piece(g, f)[...], pbs[g][p], lbs[g][nl]).astype(BF16)

        @pl.when(p == nl - 1)
        def _():
            owns[g][...] = add(piece(g, f)[...], pbs[g][p], lbs[g][p]).astype(BF16)

        @pl.when(jnp.logical_and(p > 0, p < nl - 1))
        def _():
            owns[g][...] = add(piece(g, f)[...], pbs[g][p], lbs[g][p], lbs[g][nl]).astype(BF16)

        place_ = gouts[g].at[pl.ds(s * n, n)]
        rcopy(owns[g], place_, as_.at[g, 0], ar.at[g, 0], {"seq": px}).start()
        rcopy(owns[g], place_, as_.at[g, 1], ar.at[g, 1], {"seq": py}).start()
        pltpu.make_async_copy(owns[g], place_, os_.at[g]).start()

    def relay(g):
        seq_gather_relay(g, owns[g], gouts[g], as_, ar, px, py, s)

    def swaps_sent(g):
        for q in range(nl):
            swap(g, q).wait_send()

    def line_sent(g):
        for q in range(nl):
            @pl.when(q > p)
            def _():
                up(g, q).wait_send()

            @pl.when(q < p)
            def _():
                down(g, q).wait_send()

    order = []
    for k in range(D // STRIP // 2):
        order += [D // STRIP - 1 - k, k]

    def strip(j, a_ref, b_ref, bcols, to, groups):
        at = slice(j * STRIP, (j + 1) * STRIP)
        to[at, :] = lax.dot_general(a_ref[:, at], b_ref[:, bcols], TN, preferred_element_type=F32).astype(BF16)
        for q in range(nl):
            if j * STRIP <= q * 2 * n < (j + 1) * STRIP:
                for g in groups:
                    swap(g, q).start()

    gpost_s[...] = jnp.zeros_like(gpost_s)

    def gated_norm(i, carry):
        r = pl.ds(pl.multiple_of(i * 128, 128), 128)
        one = jnp.sum(jnp.where(eye, stat_s[pl.ds(i, 1), :], 0.0), axis=1, keepdims=True)
        two = jnp.sum(jnp.where(eye, stat_s[pl.ds(length // 128 + i, 1), :], 0.0), axis=1, keepdims=True)
        rho = lax.rsqrt(one * (1.0 / INNER) + EPS)
        mean = rho * two * (1.0 / INNER)
        gate = gate_s[r, :].astype(F32)
        mixed = mixed_s[r, :].astype(F32)
        dsh = dsh_s[r, :]
        post = ex_s[1:2, :]
        sg = sigmoid(gate)
        sl = gate * sg
        n1 = mixed * sl * rho
        gpost_s[0:1, :] += jnp.sum(dsh * n1, axis=0, keepdims=True)
        d_gated = rho * (dsh * post - n1 * mean)
        mixed_s[r, :] = (n1 * post).astype(BF16)
        dy_s[r, :] = (d_gated * sl).astype(BF16)
        gate_s[r, :] = (d_gated * mixed * (sg * (1.0 + gate * (1.0 - sg)))).astype(BF16)
        return carry

    lax.fori_loop(0, length // 128, gated_norm, 0)

    every = slice(0, W)
    for j in order:
        strip(j, cot_s, mixed_s, every, ga_s, (0,))
    ends(0, range(nl // 2))
    x_save.wait()
    x_load = pltpu.make_async_copy(x_hbm, cot_s, ls.at[8])
    x_load.start()

    def out_part(i, carry):
        r = pl.ds(pl.multiple_of((s ^ (SEQ - 1 - i)) * rows, rows), rows)
        part_s[r, :] = nt(mixed_s[r, :], wo_s[...]).astype(BF16)

        @pl.when(i == 0)
        def _():
            for a in range(2):
                seq_one(0, a, 0).start()

        @pl.when(i == 2)
        def _():
            for a in range(2):
                seq_one(0, a, 1).start()

        return carry

    lax.fori_loop(0, SEQ, out_part, 0)

    def rows_of(t, a):
        return pl.ds((2 * t + a) * rows, rows)

    def result(t, a):
        out = (out_ref, gt_ref)[t].at[:, cols[a]]
        return pltpu.make_async_copy(dsh_s.at[rows_of(t, a)], out, ls.at[2 * t + a])

    for a in range(2):
        dsh_s[rows_of(0, a), :] = chunk(s, a)[...].astype(F32)

    for j in order:
        strip(j, nrm_s, gate_s, every, gb_s, (1,))
    ends(1, range(nl // 2))
    ends(0, range(nl // 2, nl - 1))
    ends(1, range(nl // 2, nl - 1))
    slot(0, 1)

    gpre_s[...] = jnp.zeros_like(gpre_s)

    def dn_chunk(j):
        r = pl.ds(pl.multiple_of(j * rows, rows), rows)
        dn = nt(gate_s[r, :], wg_s[...]) + nt(dv_s[r, 0:W], wv_s[...])
        dn = dn + nt(dv_s[r, W:VC], ws_s[...].reshape(D, VC - W))
        part_s[r, :] = dn.astype(BF16)
        x = cot_s[r, :].astype(F32)
        rho = lax.rsqrt(jnp.sum(x * x, axis=1, keepdims=True) * (1.0 / D) + EPS)
        gpre_s[5:6, :] += jnp.sum(dn * (x * rho), axis=0, keepdims=True)

        @pl.when((s ^ j) == 3)
        def _():
            seq_one(1, 0, 0).start()
            seq_one(1, 1, 0).start()

        @pl.when((s ^ j) == 1)
        def _():
            seq_one(1, 0, 1).start()

        @pl.when((s ^ j) == 2)
        def _():
            seq_one(1, 1, 1).start()

    def dn_pass(j):
        for a in range(2):
            @pl.when((s ^ j) == 2 - a)
            def _():
                seq_one(1, a, 0).wait_recv()
                az1[a, 0] = add(chunk(second[a], a)[...], ab1[a, 0]).astype(BF16)
                seq_two(1, a).start()

    def between(i):
        @pl.when(i == 1)
        def _():
            seq_pass(0)
            seq_one_sent(0)
            x_load.wait()

        @pl.when(jnp.logical_or(i == 1, i == 3))
        def _():
            dn_chunk(SEQ - 1 - i // 2)

        @pl.when(i == 1)
        def _():
            for t in range(2, nl - 1):
                slot(0, t)

        @pl.when(i == 2)
        def _():
            slot(1, 1)

        @pl.when(i == 4)
        def _():
            for t in range(2, nl - 1):
                slot(1, t)
            close(0)

        @pl.when(i == 5)
        def _():
            dn_pass(3)

        @pl.when(i == 6)
        def _():
            close(1)

    scan_bwd_blocks(
        mix_s.at[:, 0:W], mix_s.at[:, W:CH], mix_s.at[:, CH:VC], dy_s, st_s, kw_s, hp_s, ex_s,
        dv_s, gcw_s, gch_s, ghd_s, buf, cbuf, dhst, rowp, xw_s, e_s, er_s, between,
    )

    swaps_sent(0)
    for j in order[:2]:
        strip(j, nrm_s, dv_s, every, ga_s, (2, 3))
    ends(2, range(1))
    ends(3, range(1))
    dn_chunk(0)
    for j in order[2:]:
        strip(j, nrm_s, dv_s, every, ga_s, (2, 3))
    for k in range(1, nl - 1):
        ends(2, (k,))
        ends(3, (k,))
    slot(2, 1)
    dn_chunk(1)
    slot(3, 1)
    dn_pass(2)
    relay(0)
    for j in order:
        strip(j, nrm_s, dv_s, slice(W, VC), gc_s, (4,))
    for t in range(2, nl - 1):
        slot(2, t)

    conv_s[...] = jnp.zeros_like(conv_s)
    conv_s[:, pl.ds(pl.multiple_of(s * W, 128), W)] = gcw_s[:, 0:W]
    conv_s[:, INNER:XBC] = gcw_s[:, W:CH]
    post_s[...] = jnp.zeros_like(post_s)
    post_s[6:7, pl.ds(pl.multiple_of(s * W, 128), W)] = gpost_s[0:1, :]
    lane8 = lax.broadcasted_iota(jnp.int32, (8, 128), 1)
    row8 = lax.broadcasted_iota(jnp.int32, (8, 128), 0)
    skip = jnp.zeros((1, 128), F32)
    lane1 = lax.broadcasted_iota(jnp.int32, (1, 128), 1)
    for h in range(HL):
        at = slice(128 * (h // 2), 128 * (h // 2) + 128)
        half_of = (lane1 < HW) if h % 2 == 0 else (lane1 >= HW)
        skip = jnp.where(lane1 == h, jnp.sum(jnp.where(half_of, gch_s[0:1, at], 0.0), axis=1, keepdims=True), skip)
    heads = [
        pltpu.roll(jnp.where(row8 == 7, jnp.broadcast_to(v, (8, 128)), 0.0), s * HL, 1)
        for v in (ghd_s[0:1, :], ghd_s[1:2, :], skip)
    ]
    row512 = lax.broadcasted_iota(jnp.int32, (8, 512), 0)
    hn = HEADS // nf
    for i in range(nf):
        conv = unplace(conv_s, i * (XBC // nf), XBC // nf)
        block = jnp.where(row512 < 5, conv, 0.0)
        block = block + unplace(gpre_s, i * (D // nf), D // nf)
        block = block + unplace(post_s, i * (INNER // nf), INNER // nf)
        tiles = []
        for v in heads:
            moved = pltpu.roll(v, (128 - i * hn) % 128, 1) if i else v
            tiles.append(jnp.where(lane8 < hn, moved, 0.0))
        block = block + jnp.concatenate(tiles + [jnp.zeros((8, 128), F32)], axis=1)
        snd_s[i] = block

    def small_send(k):
        to = lax.rem(f + k, nf)
        return rcopy(snd_s.at[to], got_s.at[k], bms.at[k], bmr.at[k], {"fsdp": to})

    for k in range(1, nf):
        small_send(k).start()
    ends(4, range(nl - 1))
    for t in range(2, nl - 1):
        slot(3, t)
    relay(1)
    dn_pass(0)
    close(2)
    dn_pass(1)
    close(3)

    for a in range(2):
        seq_one(0, a, 1).wait_recv()
        seq_two(0, a).wait_recv()
        at = rows_of(0, a)
        dsh_s[at, :] = add(dsh_s[at, :], cot_s[mine, cols[a]], ab0[a, 1], az0[a, 1])
        result(0, a).start()

    for t in range(1, nl - 1):
        slot(4, t)

    total = snd_s[f]
    for k in range(1, nf):
        small_send(k).wait_recv()
        total = total + got_s[k]
    sown_s[...] = total

    def small_share(k):
        return rcopy(sown_s, sgot_s.at[s], bes.at[k], ber.at[k], {"seq": s ^ k})

    for k in range(1, SEQ):
        small_share(k).start()
    relay(2)
    relay(3)
    close(4)

    for a in range(2):
        seq_one(1, a, 1).wait_recv()
        seq_two(1, a).wait_recv()
        dsh_s[rows_of(1, a), :] = add(chunk(s, a)[...], ab1[a, 1], az1[a, 1])

    def grad_tokens(i, carry):
        x = cot_s[pl.ds(pl.multiple_of(s * rows + i * 64, 64), 64), :].astype(F32)
        rho = lax.rsqrt(jnp.sum(x * x, axis=1, keepdims=True) * (1.0 / D) + EPS)
        at = [pl.ds(pl.multiple_of((2 + a) * rows + i * 64, 64), 64) for a in range(2)]
        n0 = [x[:, cols[a]] * rho for a in range(2)]
        e0 = [dsh_s[at[a], :] * pre_s[5:6, cols[a]] for a in range(2)]
        dot = sum(jnp.sum(e0[a] * n0[a], axis=1, keepdims=True) for a in range(2))
        mean = dot * (1.0 / D)
        cot = cotrow_s[pl.ds(pl.multiple_of(i * 64, 64), 64), :].astype(F32)
        for a in range(2):
            dsh_s[at[a], :] = cot[:, cols[a]] + rho * (e0[a] - n0[a] * mean)
        return carry

    lax.fori_loop(0, rows // 64, grad_tokens, 0)
    for a in range(2):
        result(1, a).start()
    relay(4)

    for k in range(1, SEQ):
        small_share(k).wait()
    total = jnp.zeros_like(sown_s)
    for k in range(SEQ):
        total = total + jnp.where(s == k, sown_s[...], sgot_s[k])
    small_ref[...] = total
    for t in range(2):
        for a in range(2):
            result(t, a).wait()
    for k in range(1, nf):
        small_send(k).wait_send()
    seq_one_sent(1)
    for t in range(2):
        for a in range(2):
            seq_two(t, a).wait_send()
    for g in range(5):
        seq_gather_finish(g, owns[g], gouts[g], as_, ar, px, py, s)
        pltpu.make_async_copy(owns[g], gouts[g].at[pl.ds(s * n, n)], os_.at[g]).wait()
        line_sent(g)
    for g in range(1, 5):
        swaps_sent(g)


def mixer(nf, tok, cot, win, wst, wout, small):
    shape = jax.ShapeDtypeStruct
    vm = pltpu.VMEM
    dma = pltpu.SemaphoreType.DMA
    rows = tok.shape[0]
    length = SEQ * rows
    nl = nf // 2
    n = D // nf
    widths = (W, W, W, VC - W)
    groups = (W, W, W // 2, W // 2, VC - W)
    boxes = [vm((nl, n, w), BF16) for w in groups] + [vm((nl + 1, n, w), BF16) for w in groups]
    boxes += [vm((n, w), BF16) for w in groups]
    return pl.pallas_call(
        functools.partial(mixer_kernel, nf),
        out_shape=[shape((rows, D), F32)] * 2
        + [shape((SEQ * n, w), BF16) for w in widths]
        + [shape((8, 512), F32), shape((length, D), BF16)],
        in_specs=[ANY] * 5 + [VMEM],
        out_specs=[ANY] * 6 + [VMEM, ANY],
        scratch_shapes=[
            vm((length, D), BF16),
            vm((length, D), BF16),
            vm((D, W), BF16),
            vm((nf, SEQ, n // SEQ, VC - W), BF16),
            vm((D, W), BF16),
            vm((D, W), BF16),
            vm((length, VC), BF16),
            vm((length, W), BF16),
            vm((length, W), BF16),
            vm((length // Q, STATE, W), BF16),
            vm((length, W), F32),
            vm((length, W), BF16),
            vm((length, VC), BF16),
            vm((rows, D), BF16),
            vm((length, D), BF16),
            vm((D, W), BF16),
            vm((D, W), BF16),
            vm((D, VC - W), BF16),
        ]
        + boxes
        + [vm((2, 2, rows, D // 2), BF16)] * 4
        + [
            vm((8, CH), F32),
            vm((8, 128), F32),
            vm((8, W), F32),
            vm((8, D), F32),
            vm((2 * length // 128, 128), F32),
            vm((2 * length // 128, 128), F32),
            vm((SEQ, 2 * length // 128, 128), F32),
            vm((8, CH), F32),
            vm((8, W), F32),
            vm((8, 128), F32),
            vm((8, W), F32),
            vm((8, D), F32),
            vm((8, XBC), F32),
            vm((8, INNER), F32),
            vm((nf, 8, 512), F32),
            vm((nf, 8, 512), F32),
            vm((8, 512), F32),
            vm((SEQ, 8, 512), F32),
            vm((Q + 8, CH), F32),
            vm((Q + 8, CH), F32),
            vm((STATE, W), F32),
            vm((128, Q), F32),
            vm((Q, W), BF16),
            vm((Q, W), BF16),
            vm((8, W), F32),
            dma((9,)),
            dma((3, 4)),
            dma((3, 4)),
            dma((GROUPS, 4, nl)),
            dma((GROUPS, nf)),
            dma((nf,)),
            dma((nf,)),
            dma((SEQ,)),
            dma((SEQ,)),
            dma((5, 3, nl)),
            dma((5, 3, nl)),
            dma((2, 2, 3)),
            dma((2, 2, 3)),
            dma((5, 4)),
            dma((5, 4)),
            dma((nf,)),
            dma((nf,)),
            dma((SEQ,)),
            dma((SEQ,)),
            dma((5,)),
        ],
        name="mixer",
        compiler_params=pltpu.CompilerParams(
            collective_id=1, has_side_effects=True, vmem_limit_bytes=67043328
        ),
    )(tok, cot, win, wst, wout, small)


def finish_kernel(
    go, gg, gv, gs, out, gt, small, out_o, gt_o, gin_o, gout_o, cw_o, cb_o, pre_o, post_o, step_o, decay_o, skip_o
):
    out_o[...] = out[...]
    gt_o[...] = gt[...]
    for i in range(SEQ):
        gin_o[:, i * W : i * W + W] = gg[i].astype(F32)
        gin_o[:, INNER + i * W : INNER + i * W + W] = gv[i].astype(F32)
    total = gs[0].astype(F32)
    for i in range(1, SEQ):
        total = total + gs[i].astype(F32)
    rest = gin_o.shape[1] - 2 * INNER
    gin_o[:, 2 * INNER :] = total[:, :rest]
    gout_o[...] = go[0].astype(F32)

    @pl.when(pl.program_id(0) == 0)
    def _():
        cw_o[...] = small[0:4, : cw_o.shape[1]]
        cb_o[...] = small[4:5, : cb_o.shape[1]]
        pre_o[...] = small[5:6, : pre_o.shape[1]]
        post_o[...] = small[6:7, : post_o.shape[1]]
        heads = step_o.shape[1]
        step_o[...] = small[7:8, :heads]
        decay_o[...] = small[7:8, 128 : 128 + heads]
        skip_o[...] = small[7:8, 256 : 256 + heads]


def finish(nf, go, gg, gv, gs, out, gt, small):
    shape = jax.ShapeDtypeStruct
    n = D // nf
    step, rows = n // SEQ, out.shape[0] // SEQ
    proj = 2 * INNER + 2 * STATE + HEADS
    go, gg, gv, gs = (g.reshape(SEQ, n, g.shape[1]) for g in (go, gg, gv, gs))

    def whole(*dims):
        return pl.BlockSpec(dims, lambda i: (0,) * len(dims))

    tiny = [(4, XBC // nf), (1, XBC // nf), (1, n), (1, INNER // nf)] + [(1, HEADS // nf)] * 3
    return pl.pallas_call(
        finish_kernel,
        grid=(SEQ,),
        out_shape=[shape(out.shape, F32)] * 2
        + [shape((n, proj), F32), shape((n, INNER), F32)]
        + [shape(dims, F32) for dims in tiny],
        in_specs=[
            pl.BlockSpec((1, n, W), lambda i: (i, 0, 0)),
            pl.BlockSpec((SEQ, step, W), lambda i: (0, i, 0)),
            pl.BlockSpec((SEQ, step, W), lambda i: (0, i, 0)),
            pl.BlockSpec((SEQ, step, VC - W), lambda i: (0, i, 0)),
            pl.BlockSpec((rows, D), lambda i: (i, 0)),
            pl.BlockSpec((rows, D), lambda i: (i, 0)),
            whole(8, 512),
        ],
        out_specs=[
            pl.BlockSpec((rows, D), lambda i: (i, 0)),
            pl.BlockSpec((rows, D), lambda i: (i, 0)),
            pl.BlockSpec((step, proj), lambda i: (i, 0)),
            pl.BlockSpec((n, W), lambda i: (0, i)),
        ]
        + [whole(*dims) for dims in tiny],
        name="finish",
        compiler_params=pltpu.CompilerParams(vmem_limit_bytes=VMEM_LIMIT),
    )(go, gg, gv, gs, out, gt, small)


def body(
    tokens,
    input_projection_weight,
    pre_gain,
    conv_weight,
    conv_bias,
    step_bias,
    decay_log,
    skip_gain,
    post_gain,
    output_projection_weight,
    cotangent,
):
    nf = lax.axis_size("fsdp")
    tok = tokens.reshape(tokens.shape[1:])
    cot = cotangent.reshape(cotangent.shape[1:])
    win = input_projection_weight

    w_state = jnp.pad(win[:, 2 * INNER :], ((0, 0), (0, VC - W - (win.shape[1] - 2 * INNER))))
    w_out = output_projection_weight.T

    flat, at = jnp.zeros((2048,), F32), 0
    for v, size in (
        (conv_bias, 512), (pre_gain, 512), (post_gain, 512), (step_bias, 128), (decay_log, 128), (skip_gain, 256),
    ):
        flat = flat + jnp.pad(v.astype(F32), (at, 2048 - at - v.shape[0]))
        at += size
    taps = jnp.pad(conv_weight.T.astype(F32), ((0, 4), (0, 512 - conv_weight.shape[0])))
    small = taps + jnp.pad(flat.reshape(4, 512), ((4, 0), (0, 0)))
    out, gt, g_out, g_gate, g_val, g_state, small, _ = mixer(nf, tok, cot, win, w_state, w_out, small)
    block_out, grad_tokens, grad_in, grad_out, cw, cb, pre, post, step, decay, skip = finish(
        nf, g_out, g_gate, g_val, g_state, out, gt, small
    )
    return (
        block_out[None],
        grad_tokens[None],
        grad_in,
        pre.reshape(-1),
        cw.T,
        cb.reshape(-1),
        step.reshape(-1),
        decay.reshape(-1),
        skip.reshape(-1),
        post.reshape(-1),
        grad_out.T,
    )


def solution(mesh):
    in_specs = (
        P("fsdp", "seq", None),
        P("fsdp", None),
        P("fsdp"),
        P("fsdp", None),
        P("fsdp"),
        P("fsdp"),
        P("fsdp"),
        P("fsdp"),
        P("fsdp"),
        P(None, "fsdp"),
        P("fsdp", "seq", None),
    )
    out_specs = (
        P("fsdp", "seq", None),
        P("fsdp", "seq", None),
        P("fsdp", None),
        P("fsdp"),
        P("fsdp", None),
        P("fsdp"),
        P("fsdp"),
        P("fsdp"),
        P("fsdp"),
        P("fsdp"),
        P(None, "fsdp"),
    )
    return jax.shard_map(body, mesh=mesh, in_specs=in_specs, out_specs=out_specs, check_vma=False)
```

```python
import functools

import jax
import jax.numpy as jnp
from jax import lax
from jax.experimental import pallas as pl
from jax.experimental.pallas import tpu as pltpu
from jax.sharding import PartitionSpec as P

D = 1536
INNER = 3072
STATE = 128
HEADS = 48
XBC = INNER + 2 * STATE
EPS = 1e-05

SEQ = 4
W = INNER // SEQ
HL = HEADS // SEQ
HW = INNER // HEADS
CH = W + 2 * STATE
VC = CH + 128
Q = 128

F32 = jnp.float32
BF16 = jnp.bfloat16
MESH = pl.DeviceIdType.MESH
HIGH = lax.Precision.HIGHEST
VMEM = pl.BlockSpec(memory_space=pltpu.VMEM)
ANY = pl.BlockSpec(memory_space=pl.ANY)
VMEM_LIMIT = 64000 * 1024


def rcopy(src, dst, send_sem, recv_sem, device):
    return pltpu.make_async_remote_copy(
        src_ref=src, dst_ref=dst, send_sem=send_sem, recv_sem=recv_sem, device_id=device, device_id_type=MESH
    )


def signal(sem, device):
    pl.semaphore_signal(sem, inc=1, device_id=device, device_id_type=MESH)


def nn(a, b, precision=None):
    return lax.dot_general(a, b, (((1,), (0,)), ((), ())), precision=precision, preferred_element_type=F32)


def nt(a, b, precision=None):
    return lax.dot_general(a, b, (((1,), (1,)), ((), ())), precision=precision, preferred_element_type=F32)


def seq_gather_start(refs, outs, send, recv, px, py, me):
    for g, (src, out) in enumerate(zip(refs, outs)):
        n = src.shape[0]
        own = out.at[pl.ds(me * n, n)]
        rcopy(src, own, send.at[g, 0], recv.at[g, 0], {"seq": px}).start()
        rcopy(src, own, send.at[g, 1], recv.at[g, 1], {"seq": py}).start()


def seq_gather_relay(g, src, out, send, recv, px, py, me):
    n = src.shape[0]
    h = n // 2
    own = out.at[pl.ds(me * n, n)]
    rcopy(src, own, send.at[g, 0], recv.at[g, 0], {"seq": px}).wait_recv()
    top = out.at[pl.ds(px * n, h)]
    rcopy(top, top, send.at[g, 2], recv.at[g, 2], {"seq": py}).start()
    rcopy(src, own, send.at[g, 1], recv.at[g, 1], {"seq": py}).wait_recv()
    low = out.at[pl.ds(py * n + h, h)]
    rcopy(low, low, send.at[g, 3], recv.at[g, 3], {"seq": px}).start()


def seq_gather_finish(g, src, out, send, recv, px, py, me):
    n = src.shape[0]
    h = n // 2
    own = out.at[pl.ds(me * n, n)]
    half = out.at[pl.ds(me * n, h)]
    rcopy(half, half, send.at[g, 2], recv.at[g, 2], {"seq": py}).wait()
    rcopy(half, half, send.at[g, 3], recv.at[g, 3], {"seq": px}).wait()
    rcopy(src, own, send.at[g, 0], recv.at[g, 0], {"seq": px}).wait_send()
    rcopy(src, own, send.at[g, 1], recv.at[g, 1], {"seq": py}).wait_send()


def softplus(x):
    return jnp.maximum(x, 0.0) + jnp.log1p(jnp.exp(-jnp.abs(x)))


def sigmoid(x):
    return 0.5 + 0.5 * jnp.tanh(0.5 * x)


def rates_of(r_ref, rows, hp_ref, tri):
    back = lax.rem(128 - lax.axis_index("seq") * HL, 128)
    raw = pltpu.roll(r_ref[rows, :].astype(F32), back, 1) + hp_ref[0:1, :]
    dt = softplus(raw)
    lam = nn(tri, dt * hp_ref[1:2, :], HIGH)
    return raw, dt, lam


def fold(x):
    return jnp.sum(x.reshape(x.shape[0] // 8, 8, x.shape[1]), axis=0)


def spread(mat, h):
    return jnp.broadcast_to(mat[:, h : h + 1], (mat.shape[0], 128))


def scan_fwd_blocks(
    v_ref, s_ref, r_ref, kw_ref, hp_ref, ex_ref, mixed_ref, st_ref, buf, hst, xw_s, er_s, between
):
    blocks = v_ref.shape[0] // Q
    row = lax.broadcasted_iota(jnp.int32, (Q, Q), 0)
    col = lax.broadcasted_iota(jnp.int32, (Q, Q), 1)
    causal = row >= col
    tri = causal.astype(F32)
    low = lax.broadcasted_iota(jnp.int32, (Q, 128), 1) < HW
    low1 = lax.broadcasted_iota(jnp.int32, (1, 128), 1) < HW
    buf[0:8, :] = jnp.zeros((8, CH), F32)
    hst[...] = jnp.zeros_like(hst)

    def block(b, carry):
        rows = pl.ds(pl.multiple_of(b * Q, Q), Q)
        buf[8 : 8 + Q, 0:W] = v_ref[rows, :].astype(F32)
        buf[8 : 8 + Q, W:CH] = s_ref[rows, :].astype(F32)
        k = kw_ref[4:5, :] + buf[5 : 5 + Q, :] * kw_ref[0:1, :]
        for j in range(1, 4):
            k = k + buf[5 + j : 5 + j + Q, :] * kw_ref[j : j + 1, :]
        buf[0:8, :] = buf[Q : Q + 8, :]
        x = k * sigmoid(k)
        bs, cs = x[:, W : W + STATE], x[:, W + STATE :]
        _, dt, lam = rates_of(r_ref, rows, hp_ref, tri)
        lam_t, dt_t = lam.T, dt.T
        last = lam[Q - 1 : Q, :]
        tail = dt * jnp.exp(last - lam)
        aff = nt(cs, bs, HIGH)
        st_ref[b] = hst[...].astype(BF16)
        ch = nn(cs.astype(BF16), st_ref[b])
        for i in range(HL // 2):
            at = slice(128 * i, 128 * i + 128)
            xp = x[:, at]
            xb = xp.astype(BF16)
            y, lc = [], []
            for h in (2 * i, 2 * i + 1):
                lcol = spread(lam, h)
                within = jnp.exp(jnp.where(causal, lcol - lam_t[h : h + 1, :], -1e30))
                y.append(nn((aff * within * dt_t[h : h + 1, :]).astype(BF16), xb))
                lc.append(lcol)
            out = jnp.where(low, y[0], y[1])
            out = out + jnp.exp(jnp.where(low, lc[0], lc[1])) * ch[:, at] + ex_ref[0:1, at] * xp
            mixed_ref[rows, at] = out.astype(BF16)
            xw_s[:, at] = (xp * jnp.where(low, spread(tail, 2 * i), spread(tail, 2 * i + 1))).astype(BF16)
            er_s[0:1, at] = jnp.exp(jnp.where(low1, spread(last, 2 * i), spread(last, 2 * i + 1)))
        hst[...] = hst[...] * er_s[0:1, :] + nn(bs.T.astype(BF16), xw_s[...])
        between(b)
        return carry

    lax.fori_loop(0, blocks, block, 0)


def scan_bwd_blocks(
    v_ref, s_ref, r_ref, dy_ref, st_ref, kw_ref, hp_ref, ex_ref,
    dv_ref, gcw_ref, gch_ref, ghd_ref,
    buf, cbuf, dhst, rowp, xw_s, e_s, er_s, between,
):
    blocks = v_ref.shape[0] // Q
    row = lax.broadcasted_iota(jnp.int32, (Q, Q), 0)
    col = lax.broadcasted_iota(jnp.int32, (Q, Q), 1)
    tri = (row >= col).astype(F32)
    later = col >= row
    suffix = later.astype(F32)
    strict = (col < row).astype(F32)
    lane = lax.broadcasted_iota(jnp.int32, (Q, 128), 1)
    lane1 = lax.broadcasted_iota(jnp.int32, (1, 128), 1)
    low = lane < HW
    low1 = lane1 < HW
    buf[Q : Q + 8, :] = jnp.zeros((8, CH), F32)
    dhst[...] = jnp.zeros_like(dhst)
    rowp[...] = jnp.zeros_like(rowp)
    gcw_ref[...] = jnp.zeros_like(gcw_ref)
    gch_ref[...] = jnp.zeros_like(gch_ref)
    ghd_ref[...] = jnp.zeros_like(ghd_ref)

    def block(i0, carry):
        b = blocks - 1 - i0
        rows = pl.ds(pl.multiple_of(b * Q, Q), Q)
        before = pl.ds(pl.multiple_of(jnp.maximum(b * Q - 16, 0), 16), 16)
        keep = (b > 0).astype(F32)
        cbuf[0:8, 0:W] = v_ref[before, :].astype(F32)[8:16, :] * keep
        cbuf[0:8, W:CH] = s_ref[before, :].astype(F32)[8:16, :] * keep
        cbuf[8 : 8 + Q, 0:W] = v_ref[rows, :].astype(F32)
        cbuf[8 : 8 + Q, W:CH] = s_ref[rows, :].astype(F32)
        k = kw_ref[4:5, :] + cbuf[5 : 5 + Q, :] * kw_ref[0:1, :]
        for j in range(1, 4):
            k = k + cbuf[5 + j : 5 + j + Q, :] * kw_ref[j : j + 1, :]
        sg = sigmoid(k)
        x = k * sg
        ds = sg * (1.0 + k * (1.0 - sg))
        bs, cs = x[:, W : W + STATE], x[:, W + STATE :]
        bb, cb = bs.astype(BF16), cs.astype(BF16)
        raw, dt, lam = rates_of(r_ref, rows, hp_ref, tri)
        lam_t = lam.T
        last = lam[Q - 1 : Q, :]
        aff_t = nt(bs, cs, HIGH)
        hb = st_ref[b]
        dhb = dhst[...].astype(BF16)
        ch = nn(cb, hb)
        bd = nn(bb, dhb)
        daff_t = jnp.zeros((Q, Q), F32)
        col_n = jnp.zeros((Q, 128), F32)
        col_i = jnp.zeros((Q, 128), F32)
        row_i = jnp.zeros((Q, 128), F32)
        through = jnp.zeros((1, 128), F32)
        for i in range(HL // 2):
            at = slice(128 * i, 128 * i + 128)
            xp = x[:, at]
            xb = xp.astype(BF16)
            dyb = dy_ref[rows, at]
            dyf = dyb.astype(F32)
            z, lc, dc = [], [], []
            for h in (2 * i, 2 * i + 1):
                mine = low if h % 2 == 0 else jnp.logical_not(low)
                lcol, dcol = spread(lam, h), spread(dt, h)
                within = jnp.exp(jnp.where(later, lam_t[h : h + 1, :] - lcol, -1e30))
                g = nt(jnp.where(mine, xp, 0.0).astype(BF16), dyb)
                lg = within * g
                lgd = lg * dcol
                daff_t = daff_t + lgd
                pair = (aff_t * lg).astype(BF16)
                col_n = col_n + nn(pair, jnp.where(lane == h, 1.0, 0.0).astype(BF16))
                rowp[h : h + 1, :] = jnp.sum(pair.astype(F32) * dcol, axis=0, keepdims=True)
                z.append(nn((aff_t * within).astype(BF16), dyb))
                lc.append(lcol)
                dc.append(dcol)
            lamp = jnp.where(low, lc[0], lc[1])
            dtp = jnp.where(low, dc[0], dc[1])
            lastp = jnp.where(low1, spread(last, 2 * i), spread(last, 2 * i + 1))
            e = dyf * jnp.exp(lamp)
            e_s[:, at] = e.astype(BF16)
            ew = jnp.exp(lastp - lamp)
            bdp = bd[:, at]
            xw_s[:, at] = (xp * (dtp * ew)).astype(BF16)
            er_s[0:1, at] = jnp.exp(lastp)
            re = e * ch[:, at]
            ci = xp * bdp * ew
            th = jnp.sum(dhst[:, at] * hb[:, at].astype(F32), axis=0, keepdims=True) * er_s[0:1, at]
            heads = jnp.where(lane == 2 * i + jnp.where(row < HW, 0, 1), 1.0, 0.0).astype(BF16)
            row_i = row_i + nn(re.astype(BF16), heads)
            col_i = col_i + nn(ci.astype(BF16), heads)
            for h in (2 * i, 2 * i + 1):
                mine1 = low1 if h % 2 == 0 else jnp.logical_not(low1)
                through = jnp.where(
                    lane1 == h, jnp.sum(jnp.where(mine1, th, 0.0), axis=1, keepdims=True), through
                )
            dx = dtp * jnp.where(low, z[0], z[1]) + bdp * (dtp * ew) + ex_ref[0:1, at] * dyf
            gch_ref[:, at] += fold(dyf * xp)
            buf[0:Q, at] = dx * ds[:, at]
        daff_b = daff_t.astype(BF16)
        d_bs = nt(xw_s[...], dhb) + nn(daff_b, cb)
        d_cs = nt(e_s[...], hb) + nn(daff_t.T.astype(BF16), bb)
        buf[0:Q, W : W + STATE] = d_bs * ds[:, W : W + STATE]
        buf[0:Q, W + STATE : CH] = d_cs * ds[:, W + STATE :]
        dhst[...] = dhst[...] * er_s[0:1, :] + nn(cs.T.astype(BF16), e_s[...])
        after = nn(suffix, rowp[...].T - dt * col_n + row_i, HIGH) + nn(strict, dt * col_i, HIGH) + through
        d_rate = (col_n + col_i + hp_ref[1:2, :] * after) * sigmoid(raw)
        ghd_ref[0:1, :] += jnp.sum(d_rate, axis=0, keepdims=True)
        ghd_ref[1:2, :] += jnp.sum(dt * after, axis=0, keepdims=True) * hp_ref[1:2, :]
        dv_ref[rows, CH:VC] = pltpu.roll(d_rate, lax.axis_index("seq") * HL, 1).astype(BF16)
        for at in (slice(0, W), slice(W, CH)):
            raw_v = cbuf[8 : 8 + Q, at]
            dk = buf[0:Q, at]
            dv = dk * kw_ref[3:4, at]
            gcw_ref[4, :, at] += fold(dk)
            gcw_ref[3, :, at] += fold(dk * raw_v)
            for j in range(3):
                dk = buf[3 - j : 3 - j + Q, at]
                dv = dv + dk * kw_ref[j : j + 1, at]
                gcw_ref[j, :, at] += fold(dk * raw_v)
            dv_ref[rows, at] = dv.astype(BF16)
        buf[Q : Q + 8, :] = buf[0:8, :]
        between(i0)
        return carry

    lax.fori_loop(0, blocks, block, 0)


GROUPS = 4


def place(block, at, width):
    start, shift = at // 128 * 128, at % 128
    lanes = -(-(width + shift) // 128) * 128
    have = block.shape[1]
    if lanes > have:
        block = jnp.concatenate([block, jnp.zeros((block.shape[0], lanes - have), block.dtype)], axis=1)
    else:
        block = block[:, :lanes]
    if shift:
        block = pltpu.roll(block, shift, 1)
    return start, lanes, block


TN = (((0,), (0,)), ((), ()))
STRIP = 384


def unplace(block, at, width):
    start, shift = at // 128 * 128, at % 128
    lanes = -(-(width + shift) // 128) * 128
    piece = block[:, start : start + lanes]
    if shift:
        piece = pltpu.roll(piece, lanes - shift, 1)
    if lanes < 512:
        piece = jnp.concatenate([piece, jnp.zeros((piece.shape[0], 512 - lanes), piece.dtype)], axis=1)
    else:
        piece = piece[:, :512]
    return jnp.where(lax.broadcasted_iota(jnp.int32, piece.shape, 1) < width, piece, 0.0)


def mixer_kernel(
    nf, tok, cot, win, wst, wout, small,
    out_ref, gt_ref, go_ref, gg_ref, gv_ref, gs_ref, small_ref, x_hbm,
    cot_s, nrm_s, wv_s, ws_s, wg_s, wo_s, mix_s, gate_s, mixed_s, st_s, dsh_s,
    dy_s, dv_s, cotrow_s, part_s, gb_s, gc_s,
    pb0, pb1, pb2, pb3, pb4, lb0, lb1, lb2, lb3, lb4, own0, own1, own2, own3, own4,
    ab0, ab1, az0, az1,
    kw_s, hp_s, ex_s, pre_s, stat_s, stat_own, stat_got,
    gcw_s, gch_s, ghd_s, gpost_s, gpre_s, conv_s, post_s, snd_s, got_s, sown_s, sgot_s,
    buf, cbuf, dhst, rowp, xw_s, e_s, er_s,
    ls, xs, xr, zs, zr, ms, mr, es, er, bzs, bzr, bxs, bxr, as_, ar, bms, bmr, bes, ber, os_,
):
    x_s, small_s, ga_s = part_s, snd_s, wo_s
    s = lax.axis_index("seq")
    f = lax.axis_index("fsdp")
    px, py = s ^ 1, s ^ 2
    nl = nf // 2
    p, c = f // 2, f % 2
    partner = p * 2 + 1 - c
    bar = pltpu.get_barrier_semaphore()
    for k in range(1, SEQ):
        signal(bar, {"seq": s ^ k})
    for k in range(1, nf):
        signal(bar, {"fsdp": lax.rem(f + k, nf)})
    pl.semaphore_wait(bar, nf - 1 + SEQ - 1)

    n = win.shape[0]
    rows = tok.shape[0]
    length = rows * SEQ
    quarter = n // SEQ
    ins = (
        win.at[:, pl.ds(pl.multiple_of(INNER + s * W, 128), W)],
        wst.at[pl.ds(pl.multiple_of(s * quarter, 8), quarter)],
        win.at[:, pl.ds(pl.multiple_of(s * W, 128), W)],
        wout.at[:, pl.ds(pl.multiple_of(s * W, 128), W)],
    )
    outs = (wv_s, ws_s, wg_s, wo_s)

    def row(g, i):
        return ws_s.at[i, s] if g == 1 else outs[g].at[pl.ds(i * n, n)]

    def hop(g, src, i, way, k, device):
        return rcopy(src, row(g, i), zs.at[g, way, k], zr.at[g, i], {"fsdp": device})

    def own_send(g):
        @pl.when(p < nl - 1)
        def _():
            hop(g, ins[g], f, 0, 0, f + 2).start()

        @pl.when(p > 0)
        def _():
            hop(g, ins[g], f, 1, 0, f - 2).start()

        hop(g, ins[g], f, 2, 0, partner).start()
        pltpu.make_async_copy(ins[g], row(g, f), ls.at[g]).start()

    def step(g, k):
        @pl.when(p - k >= 0)
        def _():
            o = f - 2 * k
            hop(g, row(g, o), o, 0, k, f).wait_recv()

            @pl.when(p < nl - 1)
            def _():
                hop(g, row(g, o), o, 0, k, f + 2).start()

            hop(g, row(g, o), o, 2, k, partner).start()

        @pl.when(p + k < nl)
        def _():
            o = f + 2 * k
            hop(g, row(g, o), o, 1, k, f).wait_recv()

            @pl.when(p > 0)
            def _():
                hop(g, row(g, o), o, 1, k, f - 2).start()

            hop(g, row(g, o), o, 3, k, partner).start()

    def arrive(g):
        pltpu.make_async_copy(ins[g], row(g, f), ls.at[g]).wait()
        for q in range(nl):
            o = q * 2 + 1 - c
            hop(g, row(g, o), o, 2, 0, partner).wait_recv()

    def sent(g):
        hop(g, ins[g], f, 2, 0, partner).wait_send()

        @pl.when(p < nl - 1)
        def _():
            hop(g, ins[g], f, 0, 0, f + 2).wait_send()

        @pl.when(p > 0)
        def _():
            hop(g, ins[g], f, 1, 0, f - 2).wait_send()

        for k in range(1, nl):
            @pl.when(p - k >= 0)
            def _():
                o = f - 2 * k

                @pl.when(p < nl - 1)
                def _():
                    hop(g, row(g, o), o, 0, k, f + 2).wait_send()

                hop(g, row(g, o), o, 2, k, partner).wait_send()

            @pl.when(p + k < nl)
            def _():
                o = f + 2 * k

                @pl.when(p > 0)
                def _():
                    hop(g, row(g, o), o, 1, k, f - 2).wait_send()

                hop(g, row(g, o), o, 3, k, partner).wait_send()

    def small_copy(k):
        return rcopy(small, small_s.at[f], ms.at[k], mr.at[k], {"fsdp": lax.rem(f + k, nf)})

    mine = pl.ds(s * rows, rows)
    own_small = pltpu.make_async_copy(small, small_s.at[f], ls.at[4])
    own_tok = pltpu.make_async_copy(tok, x_s.at[mine], ls.at[5])
    own_cot = pltpu.make_async_copy(cot, cot_s.at[mine], ls.at[6])
    own_row = pltpu.make_async_copy(cot, cotrow_s, ls.at[7])

    def st_hop(k, region, device):
        return rcopy(region, region, xs.at[2, k], xr.at[2, k], {"seq": device})

    st_own = ws_s.at[:, s]
    st_top, st_low = ws_s.at[pl.ds(0, nl), px], ws_s.at[pl.ds(nl, nl), py]

    for k in range(1, nf):
        small_copy(k).start()
    own_small.start()
    own_tok.start()
    seq_gather_start((tok,), (x_s,), xs, xr, px, py, s)
    own_send(1)
    own_send(0)
    own_cot.start()
    own_row.start()
    for k in range(1, min(3, nl)):
        step(1, k)
    step(0, 1)
    for k in range(3, nl):
        step(1, k)
    arrive(1)
    st_hop(0, st_own, px).start()
    st_hop(1, st_own, py).start()
    seq_gather_relay(0, tok, x_s, xs, xr, px, py, s)
    for k in range(2, min(3, nl)):
        step(0, k)
    own_send(2)
    own_send(3)

    own_small.wait()
    for k in range(1, nf):
        small_copy(k).wait()
    conv_s[...] = jnp.zeros_like(conv_s)
    pre_s[...] = jnp.zeros_like(pre_s)
    post_s[...] = jnp.zeros_like(post_s)
    heads = [jnp.zeros((8, 128), F32) for _ in range(3)]
    for i in range(nf):
        block = small_s[i]
        at, lanes, moved = place(block, i * (XBC // nf), XBC // nf)
        conv_s[:, at : at + lanes] += moved
        at, lanes, moved = place(block, i * (D // nf), D // nf)
        pre_s[:, at : at + lanes] += jnp.where(lax.broadcasted_iota(jnp.int32, moved.shape, 0) == 5, moved, 0.0)
        at, lanes, moved = place(block, i * (INNER // nf), INNER // nf)
        post_s[:, at : at + lanes] += jnp.where(lax.broadcasted_iota(jnp.int32, moved.shape, 0) == 6, moved, 0.0)
        for j in range(3):
            piece = block[:, 128 * j : 128 * j + 128]
            at = i * (HEADS // nf)
            heads[j] = heads[j] + (pltpu.roll(piece, at, 1) if at else piece)
    kw_s[:, 0:W] = conv_s[:, pl.ds(pl.multiple_of(s * W, 128), W)]
    kw_s[:, W:CH] = conv_s[:, INNER:XBC]
    lane1 = lax.broadcasted_iota(jnp.int32, (1, 128), 1)
    low1 = lane1 < HW
    back = lax.rem(128 - s * HL, 128)
    step_b, decay, skip = [pltpu.roll(h, back, 1)[7:8, :] for h in heads]
    hp_s[...] = jnp.zeros_like(hp_s)
    hp_s[0:1, :] = jnp.where(lane1 < HL, step_b, 0.0)
    hp_s[1:2, :] = jnp.where(lane1 < HL, -jnp.exp(decay), 0.0)
    ex_s[...] = jnp.zeros_like(ex_s)
    for i in range(HL // 2):
        ex_s[0:1, 128 * i : 128 * i + 128] = jnp.where(low1, spread(skip, 2 * i), spread(skip, 2 * i + 1))
    ex_s[1:2, :] = post_s[6:7, pl.ds(pl.multiple_of(s * W, 128), W)]

    st_hop(0, st_own, px).wait_recv()
    st_hop(2, st_top, py).start()
    st_hop(1, st_own, py).wait_recv()
    st_hop(3, st_low, px).start()
    own = cot_s.at[mine]
    rcopy(cot, own, xs.at[1, 0], xr.at[1, 0], {"seq": px}).start()
    rcopy(cot, own, xs.at[1, 1], xr.at[1, 1], {"seq": py}).start()
    for k in range(3, nl):
        step(0, k)
    own_tok.wait()
    seq_gather_finish(0, tok, x_s, xs, xr, px, py, s)

    def norm(i, carry):
        r = pl.ds(pl.multiple_of(i * 128, 128), 128)
        x = x_s[r, :].astype(F32)
        rho = lax.rsqrt(jnp.sum(x * x, axis=1, keepdims=True) * (1.0 / D) + EPS)
        nrm_s[r, :] = (x * rho * pre_s[5:6, :]).astype(BF16)
        return carry

    lax.fori_loop(0, length // 128, norm, 0)
    x_save = pltpu.make_async_copy(x_s, x_hbm, ls.at[8])
    x_save.start()
    arrive(0)

    def project(i, carry):
        r = pl.ds(pl.multiple_of(i * 256, 256), 256)
        mix_s[r, 0:W] = nn(nrm_s[r, :], wv_s[...]).astype(BF16)
        return carry

    def project_state(i, carry):
        r = pl.ds(pl.multiple_of(i * 256, 256), 256)
        mix_s[r, W:VC] = nn(nrm_s[r, :], ws_s[...].reshape(D, VC - W)).astype(BF16)
        return carry

    lax.fori_loop(0, length // 256, project, 0)
    step(2, 1)
    st_hop(2, st_top, py).wait()
    st_hop(3, st_low, px).wait()
    lax.fori_loop(0, length // 256, project_state, 0)

    def between(b):
        @pl.when(b == 1)
        def _():
            step(3, 1)

        @pl.when(b == 4)
        def _():
            step(2, 2)

    scan_fwd_blocks(
        mix_s.at[:, 0:W], mix_s.at[:, W:CH], mix_s.at[:, CH:VC], kw_s, hp_s, ex_s, mixed_s, st_s,
        buf, dhst, xw_s, er_s, between,
    )
    step(3, 2)
    seq_gather_relay(1, cot, cot_s, xs, xr, px, py, s)
    for k in range(3, nl):
        step(2, k)
    arrive(2)

    def project_gate(i, carry):
        r = pl.ds(pl.multiple_of(i * 256, 256), 256)
        gate_s[r, :] = nn(nrm_s[r, :], wg_s[...]).astype(BF16)
        return carry

    lax.fori_loop(0, length // 256, project_gate, 0)
    for k in range(3, nl):
        step(3, k)
    own_cot.wait()
    seq_gather_finish(1, cot, cot_s, xs, xr, px, py, s)
    arrive(3)
    eye = lax.broadcasted_iota(jnp.int32, (128, 128), 0) == lax.broadcasted_iota(jnp.int32, (128, 128), 1)

    def stats(i, carry):
        r = pl.ds(pl.multiple_of(i * 128, 128), 128)
        dsh = nn(cot_s[r, :], wo_s[...])
        dsh_s[r, :] = dsh
        gate = gate_s[r, :].astype(F32)
        gated = mixed_s[r, :].astype(F32) * (gate * sigmoid(gate))
        one = jnp.sum(gated * gated, axis=1, keepdims=True)
        gained = gated * ex_s[1:2, :]
        dy_s[r, :] = gained.astype(BF16)
        two = jnp.sum(dsh * gained, axis=1, keepdims=True)
        stat_own[pl.ds(i, 1), :] = jnp.sum(jnp.where(eye, one, 0.0), axis=0, keepdims=True)
        stat_own[pl.ds(length // 128 + i, 1), :] = jnp.sum(jnp.where(eye, two, 0.0), axis=0, keepdims=True)
        return carry

    lax.fori_loop(0, length // 128, stats, 0)
    copies = [rcopy(stat_own, stat_got.at[k], es.at[k], er.at[k], {"seq": s ^ k}) for k in range(1, SEQ)]
    for copy in copies:
        copy.start()

    half = D // 2
    cols = (slice(0, half), slice(half, D))
    first, second = (px, py), (py, px)
    ab, az = (ab0, ab1), (az0, az1)

    def chunk(i, a):
        return part_s.at[pl.ds(i * rows, rows), cols[a]]

    def seq_one(t, a, m):
        i = (first[a] ^ second[a] ^ s) if m == 0 else first[a]
        return rcopy(chunk(i, a), ab[t].at[a, m], bxs.at[t, a, m], bxr.at[t, a, m], {"seq": first[a]})

    def seq_two(t, a):
        return rcopy(az[t].at[a, 0], az[t].at[a, 1], bxs.at[t, a, 2], bxr.at[t, a, 2], {"seq": second[a]})

    def add(*terms):
        total = terms[0].astype(F32)
        for term in terms[1:]:
            total = total + term.astype(F32)
        return total

    def seq_pass(t):
        for a in range(2):
            seq_one(t, a, 0).wait_recv()
            az[t][a, 0] = add(chunk(second[a], a)[...], ab[t][a, 0]).astype(BF16)
            seq_two(t, a).start()

    def seq_last(t, out):
        for a in range(2):
            seq_one(t, a, 1).wait_recv()
            seq_two(t, a).wait_recv()
            out[:, cols[a]] = add(chunk(s, a)[...], ab[t][a, 1], az[t][a, 1])

    def seq_one_sent(t):
        for a in range(2):
            seq_one(t, a, 0).wait_send()
            seq_one(t, a, 1).wait_send()

    x_save.wait()

    def out_part(i, carry):
        r = pl.ds(pl.multiple_of((s ^ (SEQ - 1 - i)) * rows, rows), rows)
        part_s[r, :] = nt(dy_s[r, :], wo_s[...]).astype(BF16)

        @pl.when(i == 0)
        def _():
            for a in range(2):
                seq_one(0, a, 0).start()

        @pl.when(i == 2)
        def _():
            for a in range(2):
                seq_one(0, a, 1).start()

        return carry

    lax.fori_loop(0, SEQ, out_part, 0)

    for copy in copies:
        copy.wait()
    stat_s[...] = stat_own[...] + stat_got[1] + (stat_got[2] + stat_got[3])
    for g in range(GROUPS):
        sent(g)
    st_hop(0, st_own, px).wait_send()
    st_hop(1, st_own, py).wait_send()
    own_row.wait()

    low_half, high_half = slice(0, W // 2), slice(W // 2, W)
    parts = (ga_s, gb_s, ga_s.at[:, low_half], ga_s.at[:, high_half], gc_s)
    pbs, lbs, owns = (pb0, pb1, pb2, pb3, pb4), (lb0, lb1, lb2, lb3, lb4), (own0, own1, own2, own3, own4)
    gouts = (go_ref, gg_ref, gv_ref.at[:, low_half], gv_ref.at[:, high_half], gs_ref)

    def piece(g, i):
        return parts[g].at[pl.ds(pl.multiple_of(i * n, 16), n)]

    def swap(g, q):
        return rcopy(piece(g, q * 2 + 1 - c), pbs[g].at[q], bzs.at[g, 0, q], bzr.at[g, 0, q], {"fsdp": partner})

    def up(g, q):
        return rcopy(pbs[g].at[q], lbs[g].at[q], bzs.at[g, 1, q], bzr.at[g, 1, q], {"fsdp": f + 2})

    def down(g, q):
        to = jnp.where(q == p - 1, nl, q)
        return rcopy(pbs[g].at[q], lbs[g].at[to], bzs.at[g, 2, q], bzr.at[g, 2, q], {"fsdp": f - 2})

    def send_up(g, q, terms):
        pbs[g][q] = add(piece(g, q * 2 + c)[...], pbs[g][q], *terms).astype(BF16)
        up(g, q).start()

    def send_down(g, q, terms):
        pbs[g][q] = add(piece(g, q * 2 + c)[...], pbs[g][q], *terms).astype(BF16)
        down(g, q).start()

    def ends(g, shards):
        for k in shards:
            @pl.when(p == 0)
            def _():
                swap(g, nl - 1 - k).wait_recv()
                send_up(g, nl - 1 - k, ())

            @pl.when(p == nl - 1)
            def _():
                swap(g, k).wait_recv()
                send_down(g, k, ())

    def slot(g, t):
        @pl.when(jnp.logical_and(p > 0, p <= t))
        def _():
            q = nl - 1 - t + p
            swap(g, q).wait_recv()
            up(g, q).wait_recv()
            send_up(g, q, (lbs[g][q],))

        @pl.when(jnp.logical_and(p < nl - 1, nl - 1 - p <= t))
        def _():
            q = t - (nl - 1 - p)
            swap(g, q).wait_recv()
            down(g, q).wait_recv()
            send_down(g, q, (lbs[g][q],))

    def close(g):
        swap(g, p).wait_recv()

        @pl.when(p > 0)
        def _():
            up(g, p).wait_recv()

        @pl.when(p < nl - 1)
        def _():
            down(g, p).wait_recv()

        @pl.when(p == 0)
        def _():
            owns[g][...] = add(piece(g, f)[...], pbs[g][p], lbs[g][nl]).astype(BF16)

        @pl.when(p == nl - 1)
        def _():
            owns[g][...] = add(piece(g, f)[...], pbs[g][p], lbs[g][p]).astype(BF16)

        @pl.when(jnp.logical_and(p > 0, p < nl - 1))
        def _():
            owns[g][...] = add(piece(g, f)[...], pbs[g][p], lbs[g][p], lbs[g][nl]).astype(BF16)

        place_ = gouts[g].at[pl.ds(s * n, n)]
        rcopy(owns[g], place_, as_.at[g, 0], ar.at[g, 0], {"seq": px}).start()
        rcopy(owns[g], place_, as_.at[g, 1], ar.at[g, 1], {"seq": py}).start()
        pltpu.make_async_copy(owns[g], place_, os_.at[g]).start()

    def relay(g):
        seq_gather_relay(g, owns[g], gouts[g], as_, ar, px, py, s)

    def swaps_sent(g):
        for q in range(nl):
            swap(g, q).wait_send()

    def line_sent(g):
        for q in range(nl):
            @pl.when(q > p)
            def _():
                up(g, q).wait_send()

            @pl.when(q < p)
            def _():
                down(g, q).wait_send()

    order = []
    for k in range(D // STRIP // 2):
        order += [D // STRIP - 1 - k, k]

    def strip(j, a_ref, b_ref, bcols, to, groups):
        at = slice(j * STRIP, (j + 1) * STRIP)
        to[at, :] = lax.dot_general(a_ref[:, at], b_ref[:, bcols], TN, preferred_element_type=F32).astype(BF16)
        for q in range(nl):
            if j * STRIP <= q * 2 * n < (j + 1) * STRIP:
                for g in groups:
                    swap(g, q).start()

    gpost_s[...] = jnp.zeros_like(gpost_s)

    def gated_norm(i, carry):
        r = pl.ds(pl.multiple_of(i * 128, 128), 128)
        one = jnp.sum(jnp.where(eye, stat_s[pl.ds(i, 1), :], 0.0), axis=1, keepdims=True)
        two = jnp.sum(jnp.where(eye, stat_s[pl.ds(length // 128 + i, 1), :], 0.0), axis=1, keepdims=True)
        rho = lax.rsqrt(one * (1.0 / INNER) + EPS)
        mean = rho * two * (1.0 / INNER)
        gate = gate_s[r, :].astype(F32)
        mixed = mixed_s[r, :].astype(F32)
        dsh = dsh_s[r, :]
        post = ex_s[1:2, :]
        sg = sigmoid(gate)
        sl = gate * sg
        n1 = mixed * sl * rho
        gpost_s[...] += fold(dsh * n1)
        d_gated = rho * (dsh * post - n1 * mean)
        mixed_s[r, :] = (n1 * post).astype(BF16)
        dy_s[r, :] = (d_gated * sl).astype(BF16)
        gate_s[r, :] = (d_gated * mixed * (sg * (1.0 + gate * (1.0 - sg)))).astype(BF16)
        return carry

    lax.fori_loop(0, length // 128, gated_norm, 0)

    every = slice(0, W)
    for j in order[:2]:
        strip(j, cot_s, mixed_s, every, ga_s, (0,))
    ends(0, range(1))
    for j in order[2:]:
        strip(j, cot_s, mixed_s, every, ga_s, (0,))
    ends(0, range(1, nl // 2))
    x_load = pltpu.make_async_copy(x_hbm, cot_s, ls.at[8])
    x_load.start()

    def rows_of(t, a):
        return pl.ds((2 * t + a) * rows, rows)

    def result(t, a):
        out = (out_ref, gt_ref)[t].at[:, cols[a]]
        return pltpu.make_async_copy(dsh_s.at[rows_of(t, a)], out, ls.at[2 * t + a])

    for a in range(2):
        dsh_s[rows_of(0, a), :] = chunk(s, a)[...].astype(F32)

    for j in order:
        strip(j, nrm_s, gate_s, every, gb_s, (1,))
    ends(1, range(nl // 2))
    ends(0, range(nl // 2, nl - 1))
    ends(1, range(nl // 2, nl - 1))
    slot(0, 1)

    gpre_s[...] = jnp.zeros_like(gpre_s)

    def dn_chunk(j):
        r = pl.ds(pl.multiple_of(j * rows, rows), rows)
        dn = nt(gate_s[r, :], wg_s[...]) + nt(dv_s[r, 0:W], wv_s[...])
        dn = dn + nt(dv_s[r, W:VC], ws_s[...].reshape(D, VC - W))
        part_s[r, :] = dn.astype(BF16)
        x = cot_s[r, :].astype(F32)
        rho = lax.rsqrt(jnp.sum(x * x, axis=1, keepdims=True) * (1.0 / D) + EPS)
        gpre_s[...] += fold(dn * (x * rho))

        @pl.when((s ^ j) == 3)
        def _():
            seq_one(1, 0, 0).start()
            seq_one(1, 1, 0).start()

        @pl.when((s ^ j) == 1)
        def _():
            seq_one(1, 0, 1).start()

        @pl.when((s ^ j) == 2)
        def _():
            seq_one(1, 1, 1).start()

    def dn_pass(j):
        for a in range(2):
            @pl.when((s ^ j) == 2 - a)
            def _():
                seq_one(1, a, 0).wait_recv()
                az1[a, 0] = add(chunk(second[a], a)[...], ab1[a, 0]).astype(BF16)
                seq_two(1, a).start()

    def between(i):
        @pl.when(i == 1)
        def _():
            seq_pass(0)
            seq_one_sent(0)
            x_load.wait()

        @pl.when(jnp.logical_and(lax.rem(i, 2) == 1, i < 2 * SEQ - 1))
        def _():
            dn_chunk(SEQ - 1 - i // 2)

        @pl.when(i == 1)
        def _():
            for t in range(2, nl - 1):
                slot(0, t)

        @pl.when(i == 2)
        def _():
            slot(1, 1)

        @pl.when(i == 4)
        def _():
            for t in range(2, nl - 1):
                slot(1, t)

        @pl.when(i == 5)
        def _():
            close(0)

        @pl.when(i == 6)
        def _():
            dn_pass(3)

    scan_bwd_blocks(
        mix_s.at[:, 0:W], mix_s.at[:, W:CH], mix_s.at[:, CH:VC], dy_s, st_s, kw_s, hp_s, ex_s,
        dv_s, gcw_s, gch_s, ghd_s, buf, cbuf, dhst, rowp, xw_s, e_s, er_s, between,
    )

    swaps_sent(0)
    for j in order[:2]:
        strip(j, nrm_s, dv_s, every, ga_s, (2, 3))
    ends(2, range(1))
    ends(3, range(1))
    dn_chunk(0)
    close(1)
    for j in order[2:]:
        strip(j, nrm_s, dv_s, every, ga_s, (2, 3))
    for k in range(1, nl - 1):
        ends(2, (k,))
        ends(3, (k,))
    slot(2, 1)
    slot(3, 1)
    dn_pass(2)
    for j in order:
        strip(j, nrm_s, dv_s, slice(W, VC), gc_s, (4,))
    for t in range(2, nl - 1):
        slot(2, t)
    relay(0)

    conv_s[...] = jnp.zeros_like(conv_s)
    for j in range(5):
        tap = jnp.sum(gcw_s[j], axis=0, keepdims=True)
        conv_s[j : j + 1, pl.ds(pl.multiple_of(s * W, 128), W)] = tap[:, 0:W]
        conv_s[j : j + 1, INNER:XBC] = tap[:, W:CH]
    gpre_s[5:6, :] = jnp.sum(gpre_s[...], axis=0, keepdims=True)
    post_s[...] = jnp.zeros_like(post_s)
    post_s[6:7, pl.ds(pl.multiple_of(s * W, 128), W)] = jnp.sum(gpost_s[...], axis=0, keepdims=True)
    channels = jnp.sum(gch_s[...], axis=0, keepdims=True)
    lane8 = lax.broadcasted_iota(jnp.int32, (8, 128), 1)
    row8 = lax.broadcasted_iota(jnp.int32, (8, 128), 0)
    skip = jnp.zeros((1, 128), F32)
    lane1 = lax.broadcasted_iota(jnp.int32, (1, 128), 1)
    for h in range(HL):
        at = slice(128 * (h // 2), 128 * (h // 2) + 128)
        half_of = (lane1 < HW) if h % 2 == 0 else (lane1 >= HW)
        skip = jnp.where(lane1 == h, jnp.sum(jnp.where(half_of, channels[:, at], 0.0), axis=1, keepdims=True), skip)
    heads = [
        pltpu.roll(jnp.where(row8 == 7, jnp.broadcast_to(v, (8, 128)), 0.0), s * HL, 1)
        for v in (ghd_s[0:1, :], ghd_s[1:2, :], skip)
    ]
    row512 = lax.broadcasted_iota(jnp.int32, (8, 512), 0)
    hn = HEADS // nf
    for i in range(nf):
        conv = unplace(conv_s, i * (XBC // nf), XBC // nf)
        block = jnp.where(row512 < 5, conv, 0.0)
        block = block + jnp.where(row512 == 5, unplace(gpre_s, i * (D // nf), D // nf), 0.0)
        block = block + unplace(post_s, i * (INNER // nf), INNER // nf)
        tiles = []
        for v in heads:
            moved = pltpu.roll(v, (128 - i * hn) % 128, 1) if i else v
            tiles.append(jnp.where(lane8 < hn, moved, 0.0))
        block = block + jnp.concatenate(tiles + [jnp.zeros((8, 128), F32)], axis=1)
        snd_s[i] = block

    def small_send(k):
        to = lax.rem(f + k, nf)
        return rcopy(snd_s.at[to], got_s.at[k], bms.at[k], bmr.at[k], {"fsdp": to})

    for k in range(1, nf):
        small_send(k).start()
    ends(4, range(nl - 1))
    for t in range(2, nl - 1):
        slot(3, t)
    dn_pass(1)
    dn_pass(0)
    close(2)
    close(3)
    for t in range(1, nl - 1):
        slot(4, t)
    relay(1)

    for a in range(2):
        seq_one(0, a, 1).wait_recv()
        seq_two(0, a).wait_recv()
        for k in range(rows // 128):
            one = stat_s[pl.ds(s * (rows // 128) + k, 1), :]
            rho = lax.rsqrt(jnp.sum(jnp.where(eye, one, 0.0), axis=1, keepdims=True) * (1.0 / INNER) + EPS)
            part = slice(128 * k, 128 * k + 128)
            at = pl.ds(a * rows + 128 * k, 128)
            x = cot_s[pl.ds(pl.multiple_of(s * rows + 128 * k, 128), 128), cols[a]].astype(F32)
            dsh_s[at, :] = x + rho * add(dsh_s[at, :], ab0[a, 1, part], az0[a, 1, part])
        result(0, a).start()

    total = snd_s[f]
    for k in range(1, nf):
        small_send(k).wait_recv()
        total = total + got_s[k]
    sown_s[...] = total

    def small_share(k):
        return rcopy(sown_s, sgot_s.at[s], bes.at[k], ber.at[k], {"seq": s ^ k})

    for k in range(1, SEQ):
        small_share(k).start()
    close(4)
    relay(2)
    relay(3)

    for a in range(2):
        seq_one(1, a, 1).wait_recv()
        seq_two(1, a).wait_recv()
        dsh_s[rows_of(1, a), :] = add(chunk(s, a)[...], ab1[a, 1], az1[a, 1])

    def grad_tokens(i, carry):
        x = cot_s[pl.ds(pl.multiple_of(s * rows + i * 64, 64), 64), :].astype(F32)
        rho = lax.rsqrt(jnp.sum(x * x, axis=1, keepdims=True) * (1.0 / D) + EPS)
        at = [pl.ds(pl.multiple_of((2 + a) * rows + i * 64, 64), 64) for a in range(2)]
        n0 = [x[:, cols[a]] * rho for a in range(2)]
        e0 = [dsh_s[at[a], :] * pre_s[5:6, cols[a]] for a in range(2)]
        dot = sum(jnp.sum(e0[a] * n0[a], axis=1, keepdims=True) for a in range(2))
        mean = dot * (1.0 / D)
        cot = cotrow_s[pl.ds(pl.multiple_of(i * 64, 64), 64), :].astype(F32)
        for a in range(2):
            dsh_s[at[a], :] = cot[:, cols[a]] + rho * (e0[a] - n0[a] * mean)
        return carry

    lax.fori_loop(0, rows // 64, grad_tokens, 0)
    for a in range(2):
        result(1, a).start()
    relay(4)

    for k in range(1, SEQ):
        small_share(k).wait()
    total = jnp.zeros_like(sown_s)
    for k in range(SEQ):
        total = total + jnp.where(s == k, sown_s[...], sgot_s[k])
    small_ref[...] = total
    for t in range(2):
        for a in range(2):
            result(t, a).wait()
    for k in range(1, nf):
        small_send(k).wait_send()
    seq_one_sent(1)
    for t in range(2):
        for a in range(2):
            seq_two(t, a).wait_send()
    for g in range(5):
        seq_gather_finish(g, owns[g], gouts[g], as_, ar, px, py, s)
        pltpu.make_async_copy(owns[g], gouts[g].at[pl.ds(s * n, n)], os_.at[g]).wait()
        line_sent(g)
    for g in range(1, 5):
        swaps_sent(g)


def mixer(nf, tok, cot, win, wst, wout, small):
    shape = jax.ShapeDtypeStruct
    vm = pltpu.VMEM
    dma = pltpu.SemaphoreType.DMA
    rows = tok.shape[0]
    length = SEQ * rows
    nl = nf // 2
    n = D // nf
    widths = (W, W, W, VC - W)
    groups = (W, W, W // 2, W // 2, VC - W)
    boxes = [vm((nl, n, w), BF16) for w in groups] + [vm((nl + 1, n, w), BF16) for w in groups]
    boxes += [vm((n, w), BF16) for w in groups]
    return pl.pallas_call(
        functools.partial(mixer_kernel, nf),
        out_shape=[shape((rows, D), F32)] * 2
        + [shape((SEQ * n, w), BF16) for w in widths]
        + [shape((8, 512), F32), shape((length, D), BF16)],
        in_specs=[ANY] * 5 + [VMEM],
        out_specs=[ANY] * 6 + [VMEM, ANY],
        scratch_shapes=[
            vm((length, D), BF16),
            vm((length, D), BF16),
            vm((D, W), BF16),
            vm((nf, SEQ, n // SEQ, VC - W), BF16),
            vm((D, W), BF16),
            vm((D, W), BF16),
            vm((length, VC), BF16),
            vm((length, W), BF16),
            vm((length, W), BF16),
            vm((length // Q, STATE, W), BF16),
            vm((length, W), F32),
            vm((length, W), BF16),
            vm((length, VC), BF16),
            vm((rows, D), BF16),
            vm((length, D), BF16),
            vm((D, W), BF16),
            vm((D, VC - W), BF16),
        ]
        + boxes
        + [vm((2, 2, rows, D // 2), BF16)] * 4
        + [
            vm((8, CH), F32),
            vm((8, 128), F32),
            vm((8, W), F32),
            vm((8, D), F32),
            vm((2 * length // 128, 128), F32),
            vm((2 * length // 128, 128), F32),
            vm((SEQ, 2 * length // 128, 128), F32),
            vm((5, 8, CH), F32),
            vm((8, W), F32),
            vm((8, 128), F32),
            vm((8, W), F32),
            vm((8, D), F32),
            vm((8, XBC), F32),
            vm((8, INNER), F32),
            vm((nf, 8, 512), F32),
            vm((nf, 8, 512), F32),
            vm((8, 512), F32),
            vm((SEQ, 8, 512), F32),
            vm((Q + 8, CH), F32),
            vm((Q + 8, CH), F32),
            vm((STATE, W), F32),
            vm((128, Q), F32),
            vm((Q, W), BF16),
            vm((Q, W), BF16),
            vm((8, W), F32),
            dma((9,)),
            dma((3, 4)),
            dma((3, 4)),
            dma((GROUPS, 4, nl)),
            dma((GROUPS, nf)),
            dma((nf,)),
            dma((nf,)),
            dma((SEQ,)),
            dma((SEQ,)),
            dma((5, 3, nl)),
            dma((5, 3, nl)),
            dma((2, 2, 3)),
            dma((2, 2, 3)),
            dma((5, 4)),
            dma((5, 4)),
            dma((nf,)),
            dma((nf,)),
            dma((SEQ,)),
            dma((SEQ,)),
            dma((5,)),
        ],
        name="mixer",
        compiler_params=pltpu.CompilerParams(
            collective_id=1, has_side_effects=True, vmem_limit_bytes=67043328
        ),
    )(tok, cot, win, wst, wout, small)


def finish_kernel(
    go, gg, gv, gs, out, gt, small, out_o, gt_o, gin_o, gout_o, cw_o, cb_o, pre_o, post_o, step_o, decay_o, skip_o
):
    out_o[...] = out[...]
    gt_o[...] = gt[...]
    for i in range(SEQ):
        gin_o[:, i * W : i * W + W] = gg[i].astype(F32)
        gin_o[:, INNER + i * W : INNER + i * W + W] = gv[i].astype(F32)
    total = gs[0].astype(F32)
    for i in range(1, SEQ):
        total = total + gs[i].astype(F32)
    rest = gin_o.shape[1] - 2 * INNER
    gin_o[:, 2 * INNER :] = total[:, :rest]
    gout_o[...] = go[0].astype(F32)

    @pl.when(pl.program_id(0) == 0)
    def _():
        cw_o[...] = small[0:4, : cw_o.shape[1]]
        cb_o[...] = small[4:5, : cb_o.shape[1]]
        pre_o[...] = small[5:6, : pre_o.shape[1]]
        post_o[...] = small[6:7, : post_o.shape[1]]
        heads = step_o.shape[1]
        step_o[...] = small[7:8, :heads]
        decay_o[...] = small[7:8, 128 : 128 + heads]
        skip_o[...] = small[7:8, 256 : 256 + heads]


def finish(nf, go, gg, gv, gs, out, gt, small):
    shape = jax.ShapeDtypeStruct
    n = D // nf
    step, rows = n // SEQ, out.shape[0] // SEQ
    proj = 2 * INNER + 2 * STATE + HEADS
    go, gg, gv, gs = (g.reshape(SEQ, n, g.shape[1]) for g in (go, gg, gv, gs))

    def whole(*dims):
        return pl.BlockSpec(dims, lambda i: (0,) * len(dims))

    tiny = [(4, XBC // nf), (1, XBC // nf), (1, n), (1, INNER // nf)] + [(1, HEADS // nf)] * 3
    return pl.pallas_call(
        finish_kernel,
        grid=(SEQ,),
        out_shape=[shape(out.shape, F32)] * 2
        + [shape((n, proj), F32), shape((n, INNER), F32)]
        + [shape(dims, F32) for dims in tiny],
        in_specs=[
            pl.BlockSpec((1, n, W), lambda i: (i, 0, 0)),
            pl.BlockSpec((SEQ, step, W), lambda i: (0, i, 0)),
            pl.BlockSpec((SEQ, step, W), lambda i: (0, i, 0)),
            pl.BlockSpec((SEQ, step, VC - W), lambda i: (0, i, 0)),
            pl.BlockSpec((rows, D), lambda i: (i, 0)),
            pl.BlockSpec((rows, D), lambda i: (i, 0)),
            whole(8, 512),
        ],
        out_specs=[
            pl.BlockSpec((rows, D), lambda i: (i, 0)),
            pl.BlockSpec((rows, D), lambda i: (i, 0)),
            pl.BlockSpec((step, proj), lambda i: (i, 0)),
            pl.BlockSpec((n, W), lambda i: (0, i)),
        ]
        + [whole(*dims) for dims in tiny],
        name="finish",
        compiler_params=pltpu.CompilerParams(vmem_limit_bytes=VMEM_LIMIT),
    )(go, gg, gv, gs, out, gt, small)


def body(
    tokens,
    input_projection_weight,
    pre_gain,
    conv_weight,
    conv_bias,
    step_bias,
    decay_log,
    skip_gain,
    post_gain,
    output_projection_weight,
    cotangent,
):
    nf = lax.axis_size("fsdp")
    tok = tokens.reshape(tokens.shape[1:])
    cot = cotangent.reshape(cotangent.shape[1:])
    win = input_projection_weight

    w_state = jnp.pad(win[:, 2 * INNER :], ((0, 0), (0, VC - W - (win.shape[1] - 2 * INNER))))
    w_out = output_projection_weight.T

    flat, at = jnp.zeros((2048,), F32), 0
    for v, size in (
        (conv_bias, 512), (pre_gain, 512), (post_gain, 512), (step_bias, 128), (decay_log, 128), (skip_gain, 256),
    ):
        flat = flat + jnp.pad(v.astype(F32), (at, 2048 - at - v.shape[0]))
        at += size
    taps = jnp.pad(conv_weight.T.astype(F32), ((0, 4), (0, 512 - conv_weight.shape[0])))
    small = taps + jnp.pad(flat.reshape(4, 512), ((4, 0), (0, 0)))
    out, gt, g_out, g_gate, g_val, g_state, small, _ = mixer(nf, tok, cot, win, w_state, w_out, small)
    block_out, grad_tokens, grad_in, grad_out, cw, cb, pre, post, step, decay, skip = finish(
        nf, g_out, g_gate, g_val, g_state, out, gt, small
    )
    return (
        block_out[None],
        grad_tokens[None],
        grad_in,
        pre.reshape(-1),
        cw.T,
        cb.reshape(-1),
        step.reshape(-1),
        decay.reshape(-1),
        skip.reshape(-1),
        post.reshape(-1),
        grad_out.T,
    )


def solution(mesh):
    in_specs = (
        P("fsdp", "seq", None),
        P("fsdp", None),
        P("fsdp"),
        P("fsdp", None),
        P("fsdp"),
        P("fsdp"),
        P("fsdp"),
        P("fsdp"),
        P("fsdp"),
        P(None, "fsdp"),
        P("fsdp", "seq", None),
    )
    out_specs = (
        P("fsdp", "seq", None),
        P("fsdp", "seq", None),
        P("fsdp", None),
        P("fsdp"),
        P("fsdp", None),
        P("fsdp"),
        P("fsdp"),
        P("fsdp"),
        P("fsdp"),
        P("fsdp"),
        P(None, "fsdp"),
    )
    return jax.shard_map(body, mesh=mesh, in_specs=in_specs, out_specs=out_specs, check_vma=False)
```

```python
import functools

import jax
import jax.numpy as jnp
from jax import lax
from jax.experimental import pallas as pl
from jax.experimental.pallas import tpu as pltpu
from jax.sharding import PartitionSpec as P

D = 1536
INNER = 3072
STATE = 128
HEADS = 48
XBC = INNER + 2 * STATE
EPS = 1e-05

SEQ = 4
W = INNER // SEQ
HL = HEADS // SEQ
HW = INNER // HEADS
CH = W + 2 * STATE
VC = CH + 128
REST = 2 * STATE + HEADS
Q = 128

F32 = jnp.float32
BF16 = jnp.bfloat16
MESH = pl.DeviceIdType.MESH
HIGH = lax.Precision.HIGHEST
VMEM = pl.BlockSpec(memory_space=pltpu.VMEM)
ANY = pl.BlockSpec(memory_space=pl.ANY)
VMEM_LIMIT = 64000 * 1024


def rcopy(src, dst, send_sem, recv_sem, device):
    return pltpu.make_async_remote_copy(
        src_ref=src, dst_ref=dst, send_sem=send_sem, recv_sem=recv_sem, device_id=device, device_id_type=MESH
    )


def signal(sem, device):
    pl.semaphore_signal(sem, inc=1, device_id=device, device_id_type=MESH)


def nn(a, b, precision=None):
    return lax.dot_general(a, b, (((1,), (0,)), ((), ())), precision=precision, preferred_element_type=F32)


def nt(a, b, precision=None):
    return lax.dot_general(a, b, (((1,), (1,)), ((), ())), precision=precision, preferred_element_type=F32)


def seq_gather_start(refs, outs, send, recv, px, py, me):
    for g, (src, out) in enumerate(zip(refs, outs)):
        n = src.shape[0]
        own = out.at[pl.ds(me * n, n)]
        rcopy(src, own, send.at[g, 0], recv.at[g, 0], {"seq": px}).start()
        rcopy(src, own, send.at[g, 1], recv.at[g, 1], {"seq": py}).start()


def seq_gather_relay(g, src, out, send, recv, px, py, me):
    n = src.shape[0]
    h = n // 2
    own = out.at[pl.ds(me * n, n)]
    rcopy(src, own, send.at[g, 0], recv.at[g, 0], {"seq": px}).wait_recv()
    top = out.at[pl.ds(px * n, h)]
    rcopy(top, top, send.at[g, 2], recv.at[g, 2], {"seq": py}).start()
    rcopy(src, own, send.at[g, 1], recv.at[g, 1], {"seq": py}).wait_recv()
    low = out.at[pl.ds(py * n + h, h)]
    rcopy(low, low, send.at[g, 3], recv.at[g, 3], {"seq": px}).start()


def seq_gather_finish(g, src, out, send, recv, px, py, me):
    n = src.shape[0]
    h = n // 2
    own = out.at[pl.ds(me * n, n)]
    half = out.at[pl.ds(me * n, h)]
    rcopy(half, half, send.at[g, 2], recv.at[g, 2], {"seq": py}).wait()
    rcopy(half, half, send.at[g, 3], recv.at[g, 3], {"seq": px}).wait()
    rcopy(src, own, send.at[g, 0], recv.at[g, 0], {"seq": px}).wait_send()
    rcopy(src, own, send.at[g, 1], recv.at[g, 1], {"seq": py}).wait_send()


def softplus(x):
    return jnp.maximum(x, 0.0) + jnp.log1p(jnp.exp(-jnp.abs(x)))


def sigmoid(x):
    return 0.5 + 0.5 * jnp.tanh(0.5 * x)


def rates_of(r_ref, rows, hp_ref, tri):
    back = lax.rem(128 - lax.axis_index("seq") * HL, 128)
    raw = pltpu.roll(r_ref[rows, :].astype(F32), back, 1) + hp_ref[0:1, :]
    dt = softplus(raw)
    lam = nn(tri, dt * hp_ref[1:2, :], HIGH)
    return raw, dt, lam


def fold(x):
    return jnp.sum(x.reshape(x.shape[0] // 8, 8, x.shape[1]), axis=0)


def spread(mat, h):
    return jnp.broadcast_to(mat[:, h : h + 1], (mat.shape[0], 128))


def scan_fwd_blocks(
    v_ref, s_ref, r_ref, kw_ref, hp_ref, ex_ref, mixed_ref, st_ref, buf, hst, xw_s, er_s, between
):
    blocks = v_ref.shape[0] // Q
    row = lax.broadcasted_iota(jnp.int32, (Q, Q), 0)
    col = lax.broadcasted_iota(jnp.int32, (Q, Q), 1)
    causal = row >= col
    tri = causal.astype(F32)
    low = lax.broadcasted_iota(jnp.int32, (Q, 128), 1) < HW
    low1 = lax.broadcasted_iota(jnp.int32, (1, 128), 1) < HW
    buf[0:8, :] = jnp.zeros((8, CH), F32)
    hst[...] = jnp.zeros_like(hst)

    def block(b, carry):
        rows = pl.ds(pl.multiple_of(b * Q, Q), Q)
        buf[8 : 8 + Q, 0:W] = v_ref[rows, :].astype(F32)
        buf[8 : 8 + Q, W:CH] = s_ref[rows, :].astype(F32)
        k = kw_ref[4:5, :] + buf[5 : 5 + Q, :] * kw_ref[0:1, :]
        for j in range(1, 4):
            k = k + buf[5 + j : 5 + j + Q, :] * kw_ref[j : j + 1, :]
        buf[0:8, :] = buf[Q : Q + 8, :]
        x = k * sigmoid(k)
        bs, cs = x[:, W : W + STATE], x[:, W + STATE :]
        _, dt, lam = rates_of(r_ref, rows, hp_ref, tri)
        lam_t, dt_t = lam.T, dt.T
        last = lam[Q - 1 : Q, :]
        tail = dt * jnp.exp(last - lam)
        aff = nt(cs, bs, HIGH)
        st_ref[b] = hst[...].astype(BF16)
        ch = nn(cs.astype(BF16), st_ref[b])
        for i in range(HL // 2):
            at = slice(128 * i, 128 * i + 128)
            xp = x[:, at]
            xb = xp.astype(BF16)
            y, lc = [], []
            for h in (2 * i, 2 * i + 1):
                lcol = spread(lam, h)
                within = jnp.exp(jnp.where(causal, lcol - lam_t[h : h + 1, :], -1e30))
                y.append(nn((aff * within * dt_t[h : h + 1, :]).astype(BF16), xb))
                lc.append(lcol)
            out = jnp.where(low, y[0], y[1])
            out = out + jnp.exp(jnp.where(low, lc[0], lc[1])) * ch[:, at] + ex_ref[0:1, at] * xp
            mixed_ref[rows, at] = out.astype(BF16)
            xw_s[:, at] = (xp * jnp.where(low, spread(tail, 2 * i), spread(tail, 2 * i + 1))).astype(BF16)
            er_s[0:1, at] = jnp.exp(jnp.where(low1, spread(last, 2 * i), spread(last, 2 * i + 1)))
        hst[...] = hst[...] * er_s[0:1, :] + nn(bs.T.astype(BF16), xw_s[...])
        between(b)
        return carry

    lax.fori_loop(0, blocks, block, 0)


def scan_bwd_blocks(
    v_ref, s_ref, r_ref, dy_ref, st_ref, kw_ref, hp_ref, ex_ref,
    dv_ref, gcw_ref, gch_ref, ghd_ref,
    buf, cbuf, dhst, rowp, xw_s, e_s, er_s, between,
):
    blocks = v_ref.shape[0] // Q
    row = lax.broadcasted_iota(jnp.int32, (Q, Q), 0)
    col = lax.broadcasted_iota(jnp.int32, (Q, Q), 1)
    tri = (row >= col).astype(F32)
    later = col >= row
    suffix = later.astype(F32)
    strict = (col < row).astype(F32)
    lane = lax.broadcasted_iota(jnp.int32, (Q, 128), 1)
    lane1 = lax.broadcasted_iota(jnp.int32, (1, 128), 1)
    low = lane < HW
    low1 = lane1 < HW
    buf[Q : Q + 8, :] = jnp.zeros((8, CH), F32)
    dhst[...] = jnp.zeros_like(dhst)
    rowp[...] = jnp.zeros_like(rowp)
    gcw_ref[...] = jnp.zeros_like(gcw_ref)
    gch_ref[...] = jnp.zeros_like(gch_ref)
    ghd_ref[...] = jnp.zeros_like(ghd_ref)

    def block(i0, carry):
        b = blocks - 1 - i0
        rows = pl.ds(pl.multiple_of(b * Q, Q), Q)
        before = pl.ds(pl.multiple_of(jnp.maximum(b * Q - 16, 0), 16), 16)
        keep = (b > 0).astype(F32)
        cbuf[0:8, 0:W] = v_ref[before, :].astype(F32)[8:16, :] * keep
        cbuf[0:8, W:CH] = s_ref[before, :].astype(F32)[8:16, :] * keep
        cbuf[8 : 8 + Q, 0:W] = v_ref[rows, :].astype(F32)
        cbuf[8 : 8 + Q, W:CH] = s_ref[rows, :].astype(F32)
        k = kw_ref[4:5, :] + cbuf[5 : 5 + Q, :] * kw_ref[0:1, :]
        for j in range(1, 4):
            k = k + cbuf[5 + j : 5 + j + Q, :] * kw_ref[j : j + 1, :]
        sg = sigmoid(k)
        x = k * sg
        ds = sg * (1.0 + k * (1.0 - sg))
        bs, cs = x[:, W : W + STATE], x[:, W + STATE :]
        bb, cb = bs.astype(BF16), cs.astype(BF16)
        raw, dt, lam = rates_of(r_ref, rows, hp_ref, tri)
        lam_t = lam.T
        last = lam[Q - 1 : Q, :]
        aff_t = nt(bs, cs, HIGH)
        hb = st_ref[b]
        dhb = dhst[...].astype(BF16)
        ch = nn(cb, hb)
        bd = nn(bb, dhb)
        daff_t = jnp.zeros((Q, Q), F32)
        col_n = jnp.zeros((Q, 128), F32)
        col_i = jnp.zeros((Q, 128), F32)
        row_i = jnp.zeros((Q, 128), F32)
        through = jnp.zeros((1, 128), F32)
        for i in range(HL // 2):
            at = slice(128 * i, 128 * i + 128)
            xp = x[:, at]
            xb = xp.astype(BF16)
            dyb = dy_ref[rows, at]
            dyf = dyb.astype(F32)
            z, lc, dc = [], [], []
            for h in (2 * i, 2 * i + 1):
                mine = low if h % 2 == 0 else jnp.logical_not(low)
                lcol, dcol = spread(lam, h), spread(dt, h)
                within = jnp.exp(jnp.where(later, lam_t[h : h + 1, :] - lcol, -1e30))
                g = nt(jnp.where(mine, xp, 0.0).astype(BF16), dyb)
                lg = within * g
                lgd = lg * dcol
                daff_t = daff_t + lgd
                pair = (aff_t * lg).astype(BF16)
                col_n = col_n + nn(pair, jnp.where(lane == h, 1.0, 0.0).astype(BF16))
                rowp[h : h + 1, :] = jnp.sum(pair.astype(F32) * dcol, axis=0, keepdims=True)
                z.append(nn((aff_t * within).astype(BF16), dyb))
                lc.append(lcol)
                dc.append(dcol)
            lamp = jnp.where(low, lc[0], lc[1])
            dtp = jnp.where(low, dc[0], dc[1])
            lastp = jnp.where(low1, spread(last, 2 * i), spread(last, 2 * i + 1))
            e = dyf * jnp.exp(lamp)
            e_s[:, at] = e.astype(BF16)
            ew = jnp.exp(lastp - lamp)
            bdp = bd[:, at]
            xw_s[:, at] = (xp * (dtp * ew)).astype(BF16)
            er_s[0:1, at] = jnp.exp(lastp)
            re = e * ch[:, at]
            ci = xp * bdp * ew
            th = jnp.sum(dhst[:, at] * hb[:, at].astype(F32), axis=0, keepdims=True) * er_s[0:1, at]
            heads = jnp.where(lane == 2 * i + jnp.where(row < HW, 0, 1), 1.0, 0.0).astype(BF16)
            row_i = row_i + nn(re.astype(BF16), heads)
            col_i = col_i + nn(ci.astype(BF16), heads)
            for h in (2 * i, 2 * i + 1):
                mine1 = low1 if h % 2 == 0 else jnp.logical_not(low1)
                through = jnp.where(
                    lane1 == h, jnp.sum(jnp.where(mine1, th, 0.0), axis=1, keepdims=True), through
                )
            dx = dtp * jnp.where(low, z[0], z[1]) + bdp * (dtp * ew) + ex_ref[0:1, at] * dyf
            gch_ref[:, at] += fold(dyf * xp)
            buf[0:Q, at] = dx * ds[:, at]
        daff_b = daff_t.astype(BF16)
        d_bs = nt(xw_s[...], dhb) + nn(daff_b, cb)
        d_cs = nt(e_s[...], hb) + nn(daff_t.T.astype(BF16), bb)
        buf[0:Q, W : W + STATE] = d_bs * ds[:, W : W + STATE]
        buf[0:Q, W + STATE : CH] = d_cs * ds[:, W + STATE :]
        dhst[...] = dhst[...] * er_s[0:1, :] + nn(cs.T.astype(BF16), e_s[...])
        after = nn(suffix, rowp[...].T - dt * col_n + row_i, HIGH) + nn(strict, dt * col_i, HIGH) + through
        d_rate = (col_n + col_i + hp_ref[1:2, :] * after) * sigmoid(raw)
        ghd_ref[0:1, :] += jnp.sum(d_rate, axis=0, keepdims=True)
        ghd_ref[1:2, :] += jnp.sum(dt * after, axis=0, keepdims=True) * hp_ref[1:2, :]
        dv_ref[rows, CH:VC] = pltpu.roll(d_rate, lax.axis_index("seq") * HL, 1).astype(BF16)
        for at in (slice(0, W), slice(W, CH)):
            raw_v = cbuf[8 : 8 + Q, at]
            dk = buf[0:Q, at]
            dv = dk * kw_ref[3:4, at]
            gcw_ref[4, :, at] += fold(dk)
            gcw_ref[3, :, at] += fold(dk * raw_v)
            for j in range(3):
                dk = buf[3 - j : 3 - j + Q, at]
                dv = dv + dk * kw_ref[j : j + 1, at]
                gcw_ref[j, :, at] += fold(dk * raw_v)
            dv_ref[rows, at] = dv.astype(BF16)
        buf[Q : Q + 8, :] = buf[0:8, :]
        between(i0)
        return carry

    lax.fori_loop(0, blocks, block, 0)


GROUPS = 4


def place(block, at, width):
    start, shift = at // 128 * 128, at % 128
    lanes = -(-(width + shift) // 128) * 128
    have = block.shape[1]
    if lanes > have:
        block = jnp.concatenate([block, jnp.zeros((block.shape[0], lanes - have), block.dtype)], axis=1)
    else:
        block = block[:, :lanes]
    if shift:
        block = pltpu.roll(block, shift, 1)
    return start, lanes, block


TN = (((0,), (0,)), ((), ()))
STRIP = 384


def unplace(block, at, width):
    start, shift = at // 128 * 128, at % 128
    lanes = -(-(width + shift) // 128) * 128
    piece = block[:, start : start + lanes]
    if shift:
        piece = pltpu.roll(piece, lanes - shift, 1)
    if lanes < 512:
        piece = jnp.concatenate([piece, jnp.zeros((piece.shape[0], 512 - lanes), piece.dtype)], axis=1)
    else:
        piece = piece[:, :512]
    return jnp.where(lax.broadcasted_iota(jnp.int32, piece.shape, 1) < width, piece, 0.0)


def mixer_kernel(
    nf, tok, cot, win, wout, small,
    out_ref, gt_ref, go_ref, gg_ref, gv_ref, gs_ref, small_ref, x_hbm,
    cot_s, nrm_s, wv_s, ws_s, wg_s, wo_s, mix_s, gate_s, mixed_s, st_s, dsh_s,
    dy_s, dv_s, cotrow_s, part_s, gb_s, gc_s,
    pb0, pb1, pb2, pb3, pb4, lb0, lb1, lb2, lb3, lb4, own0, own1, own2, own3, own4,
    ab0, ab1, az0, az1,
    kw_s, hp_s, ex_s, pre_s, stat_s, stat_own, stat_got,
    gcw_s, gch_s, ghd_s, gpost_s, gpre_s, conv_s, post_s, snd_s, got_s, sown_s, sgot_s,
    buf, cbuf, dhst, rowp, xw_s, e_s, er_s,
    ls, xs, xr, zs, zr, ms, mr, es, er, bzs, bzr, bxs, bxr, as_, ar, bms, bmr, bes, ber, os_,
):
    x_s, small_s, ga_s = part_s, snd_s, wo_s
    s = lax.axis_index("seq")
    f = lax.axis_index("fsdp")
    px, py = s ^ 1, s ^ 2
    nl = nf // 2
    p, c = f // 2, f % 2
    partner = p * 2 + 1 - c
    bar = pltpu.get_barrier_semaphore()
    for k in range(1, SEQ):
        signal(bar, {"seq": s ^ k})
    for k in range(1, nf):
        signal(bar, {"fsdp": lax.rem(f + k, nf)})
    pl.semaphore_wait(bar, nf - 1 + SEQ - 1)

    n = win.shape[0]
    rows = tok.shape[0]
    length = rows * SEQ
    quarter = n // SEQ
    ins = (
        win.at[:, pl.ds(pl.multiple_of(INNER + s * W, 128), W)],
        win.at[pl.ds(pl.multiple_of(s * quarter, 8), quarter), pl.ds(2 * INNER, REST)],
        win.at[:, pl.ds(pl.multiple_of(s * W, 128), W)],
        wout.at[:, pl.ds(pl.multiple_of(s * W, 128), W)],
    )
    outs = (wv_s, ws_s, wg_s, wo_s)

    def row(g, i):
        return ws_s.at[i, s] if g == 1 else outs[g].at[pl.ds(i * n, n)]

    def hop(g, src, i, way, k, device):
        return rcopy(src, row(g, i), zs.at[g, way, k], zr.at[g, i], {"fsdp": device})

    def own_send(g):
        @pl.when(p < nl - 1)
        def _():
            hop(g, ins[g], f, 0, 0, f + 2).start()

        @pl.when(p > 0)
        def _():
            hop(g, ins[g], f, 1, 0, f - 2).start()

        hop(g, ins[g], f, 2, 0, partner).start()
        pltpu.make_async_copy(ins[g], row(g, f), ls.at[g]).start()

    def step(g, k):
        @pl.when(p - k >= 0)
        def _():
            o = f - 2 * k
            hop(g, row(g, o), o, 0, k, f).wait_recv()

            @pl.when(p < nl - 1)
            def _():
                hop(g, row(g, o), o, 0, k, f + 2).start()

            hop(g, row(g, o), o, 2, k, partner).start()

        @pl.when(p + k < nl)
        def _():
            o = f + 2 * k
            hop(g, row(g, o), o, 1, k, f).wait_recv()

            @pl.when(p > 0)
            def _():
                hop(g, row(g, o), o, 1, k, f - 2).start()

            hop(g, row(g, o), o, 3, k, partner).start()

    def arrive(g):
        pltpu.make_async_copy(ins[g], row(g, f), ls.at[g]).wait()
        for q in range(nl):
            o = q * 2 + 1 - c
            hop(g, row(g, o), o, 2, 0, partner).wait_recv()

    def sent(g):
        hop(g, ins[g], f, 2, 0, partner).wait_send()

        @pl.when(p < nl - 1)
        def _():
            hop(g, ins[g], f, 0, 0, f + 2).wait_send()

        @pl.when(p > 0)
        def _():
            hop(g, ins[g], f, 1, 0, f - 2).wait_send()

        for k in range(1, nl):
            @pl.when(p - k >= 0)
            def _():
                o = f - 2 * k

                @pl.when(p < nl - 1)
                def _():
                    hop(g, row(g, o), o, 0, k, f + 2).wait_send()

                hop(g, row(g, o), o, 2, k, partner).wait_send()

            @pl.when(p + k < nl)
            def _():
                o = f + 2 * k

                @pl.when(p > 0)
                def _():
                    hop(g, row(g, o), o, 1, k, f - 2).wait_send()

                hop(g, row(g, o), o, 3, k, partner).wait_send()

    def small_copy(k):
        return rcopy(small, small_s.at[f], ms.at[k], mr.at[k], {"fsdp": lax.rem(f + k, nf)})

    mine = pl.ds(s * rows, rows)
    own_small = pltpu.make_async_copy(small, small_s.at[f], ls.at[4])
    own_tok = pltpu.make_async_copy(tok, x_s.at[mine], ls.at[5])
    own_cot = pltpu.make_async_copy(cot, cot_s.at[mine], ls.at[6])
    own_row = pltpu.make_async_copy(cot, cotrow_s, ls.at[7])

    def st_hop(k, region, device):
        return rcopy(region, region, xs.at[2, k], xr.at[2, k], {"seq": device})

    st_own = ws_s.at[:, s]
    st_top, st_low = ws_s.at[pl.ds(0, nl), px], ws_s.at[pl.ds(nl, nl), py]

    for k in range(1, nf):
        small_copy(k).start()
    own_small.start()
    own_tok.start()
    seq_gather_start((tok,), (x_s,), xs, xr, px, py, s)
    own_send(1)
    own_send(0)
    own_cot.start()
    own_row.start()
    for k in range(1, min(3, nl)):
        step(1, k)
    step(0, 1)
    for k in range(3, nl):
        step(1, k)
    arrive(1)
    st_hop(0, st_own, px).start()
    st_hop(1, st_own, py).start()
    seq_gather_relay(0, tok, x_s, xs, xr, px, py, s)
    for k in range(2, min(3, nl)):
        step(0, k)
    own_send(2)
    own_send(3)

    mix_s[:, CH:VC] = jnp.zeros((length, VC - CH), BF16)

    own_small.wait()
    for k in range(1, nf):
        small_copy(k).wait()
    conv_s[...] = jnp.zeros_like(conv_s)
    pre_s[...] = jnp.zeros_like(pre_s)
    post_s[...] = jnp.zeros_like(post_s)
    heads = [jnp.zeros((8, 128), F32) for _ in range(3)]
    for i in range(nf):
        block = small_s[i]
        at, lanes, moved = place(block, i * (XBC // nf), XBC // nf)
        conv_s[:, at : at + lanes] += moved
        at, lanes, moved = place(block, i * (D // nf), D // nf)
        pre_s[:, at : at + lanes] += jnp.where(lax.broadcasted_iota(jnp.int32, moved.shape, 0) == 5, moved, 0.0)
        at, lanes, moved = place(block, i * (INNER // nf), INNER // nf)
        post_s[:, at : at + lanes] += jnp.where(lax.broadcasted_iota(jnp.int32, moved.shape, 0) == 6, moved, 0.0)
        for j in range(3):
            piece = block[:, 128 * j : 128 * j + 128]
            at = i * (HEADS // nf)
            heads[j] = heads[j] + (pltpu.roll(piece, at, 1) if at else piece)
    kw_s[:, 0:W] = conv_s[:, pl.ds(pl.multiple_of(s * W, 128), W)]
    kw_s[:, W:CH] = conv_s[:, INNER:XBC]
    lane1 = lax.broadcasted_iota(jnp.int32, (1, 128), 1)
    low1 = lane1 < HW
    back = lax.rem(128 - s * HL, 128)
    step_b, decay, skip = [pltpu.roll(h, back, 1)[7:8, :] for h in heads]
    hp_s[...] = jnp.zeros_like(hp_s)
    hp_s[0:1, :] = jnp.where(lane1 < HL, step_b, 0.0)
    hp_s[1:2, :] = jnp.where(lane1 < HL, -jnp.exp(decay), 0.0)
    ex_s[...] = jnp.zeros_like(ex_s)
    for i in range(HL // 2):
        ex_s[0:1, 128 * i : 128 * i + 128] = jnp.where(low1, spread(skip, 2 * i), spread(skip, 2 * i + 1))
    ex_s[1:2, :] = post_s[6:7, pl.ds(pl.multiple_of(s * W, 128), W)]

    st_hop(0, st_own, px).wait_recv()
    st_hop(2, st_top, py).start()
    st_hop(1, st_own, py).wait_recv()
    st_hop(3, st_low, px).start()
    own = cot_s.at[mine]
    rcopy(cot, own, xs.at[1, 0], xr.at[1, 0], {"seq": px}).start()
    rcopy(cot, own, xs.at[1, 1], xr.at[1, 1], {"seq": py}).start()
    for k in range(3, nl):
        step(0, k)
    own_tok.wait()
    seq_gather_finish(0, tok, x_s, xs, xr, px, py, s)

    def norm(i, carry):
        r = pl.ds(pl.multiple_of(i * 128, 128), 128)
        x = x_s[r, :].astype(F32)
        rho = lax.rsqrt(jnp.sum(x * x, axis=1, keepdims=True) * (1.0 / D) + EPS)
        nrm_s[r, :] = (x * rho * pre_s[5:6, :]).astype(BF16)
        return carry

    lax.fori_loop(0, length // 128, norm, 0)
    x_save = pltpu.make_async_copy(x_s, x_hbm, ls.at[8])
    x_save.start()
    arrive(0)

    def project(i, carry):
        r = pl.ds(pl.multiple_of(i * 256, 256), 256)
        mix_s[r, 0:W] = nn(nrm_s[r, :], wv_s[...]).astype(BF16)
        return carry

    def project_state(i, carry):
        r = pl.ds(pl.multiple_of(i * 256, 256), 256)
        mix_s[r, W : W + REST] = nn(nrm_s[r, :], ws_s[...].reshape(D, REST)).astype(BF16)
        return carry

    lax.fori_loop(0, length // 256, project, 0)
    step(2, 1)
    st_hop(2, st_top, py).wait()
    st_hop(3, st_low, px).wait()
    lax.fori_loop(0, length // 256, project_state, 0)

    def between(b):
        @pl.when(b == 1)
        def _():
            step(3, 1)

        @pl.when(b == 4)
        def _():
            step(2, 2)

    scan_fwd_blocks(
        mix_s.at[:, 0:W], mix_s.at[:, W:CH], mix_s.at[:, CH:VC], kw_s, hp_s, ex_s, mixed_s, st_s,
        buf, dhst, xw_s, er_s, between,
    )
    step(3, 2)
    seq_gather_relay(1, cot, cot_s, xs, xr, px, py, s)
    for k in range(3, nl):
        step(2, k)
    arrive(2)

    def project_gate(i, carry):
        r = pl.ds(pl.multiple_of(i * 256, 256), 256)
        gate_s[r, :] = nn(nrm_s[r, :], wg_s[...]).astype(BF16)
        return carry

    lax.fori_loop(0, length // 256, project_gate, 0)
    for k in range(3, nl):
        step(3, k)
    own_cot.wait()
    seq_gather_finish(1, cot, cot_s, xs, xr, px, py, s)
    arrive(3)
    eye = lax.broadcasted_iota(jnp.int32, (128, 128), 0) == lax.broadcasted_iota(jnp.int32, (128, 128), 1)

    def stats(i, carry):
        r = pl.ds(pl.multiple_of(i * 128, 128), 128)
        dsh = nn(cot_s[r, :], wo_s[...])
        dsh_s[r, :] = dsh
        gate = gate_s[r, :].astype(F32)
        gated = mixed_s[r, :].astype(F32) * (gate * sigmoid(gate))
        one = jnp.sum(gated * gated, axis=1, keepdims=True)
        gained = gated * ex_s[1:2, :]
        dy_s[r, :] = gained.astype(BF16)
        two = jnp.sum(dsh * gained, axis=1, keepdims=True)
        stat_own[pl.ds(i, 1), :] = jnp.sum(jnp.where(eye, one, 0.0), axis=0, keepdims=True)
        stat_own[pl.ds(length // 128 + i, 1), :] = jnp.sum(jnp.where(eye, two, 0.0), axis=0, keepdims=True)
        return carry

    lax.fori_loop(0, length // 128, stats, 0)
    copies = [rcopy(stat_own, stat_got.at[k], es.at[k], er.at[k], {"seq": s ^ k}) for k in range(1, SEQ)]
    for copy in copies:
        copy.start()

    half = D // 2
    cols = (slice(0, half), slice(half, D))
    first, second = (px, py), (py, px)
    ab, az = (ab0, ab1), (az0, az1)

    def chunk(i, a):
        return part_s.at[pl.ds(i * rows, rows), cols[a]]

    def seq_one(t, a, m):
        i = (first[a] ^ second[a] ^ s) if m == 0 else first[a]
        return rcopy(chunk(i, a), ab[t].at[a, m], bxs.at[t, a, m], bxr.at[t, a, m], {"seq": first[a]})

    def seq_two(t, a):
        return rcopy(az[t].at[a, 0], az[t].at[a, 1], bxs.at[t, a, 2], bxr.at[t, a, 2], {"seq": second[a]})

    def add(*terms):
        total = terms[0].astype(F32)
        for term in terms[1:]:
            total = total + term.astype(F32)
        return total

    def seq_pass(t):
        for a in range(2):
            seq_one(t, a, 0).wait_recv()
            az[t][a, 0] = add(chunk(second[a], a)[...], ab[t][a, 0]).astype(BF16)
            seq_two(t, a).start()

    def seq_last(t, out):
        for a in range(2):
            seq_one(t, a, 1).wait_recv()
            seq_two(t, a).wait_recv()
            out[:, cols[a]] = add(chunk(s, a)[...], ab[t][a, 1], az[t][a, 1])

    def seq_one_sent(t):
        for a in range(2):
            seq_one(t, a, 0).wait_send()
            seq_one(t, a, 1).wait_send()

    x_save.wait()

    def out_part(i, carry):
        r = pl.ds(pl.multiple_of((s ^ (SEQ - 1 - i)) * rows, rows), rows)
        part_s[r, :] = nt(dy_s[r, :], wo_s[...]).astype(BF16)

        @pl.when(i == 0)
        def _():
            for a in range(2):
                seq_one(0, a, 0).start()

        @pl.when(i == 2)
        def _():
            for a in range(2):
                seq_one(0, a, 1).start()

        return carry

    lax.fori_loop(0, SEQ, out_part, 0)

    for copy in copies:
        copy.wait()
    stat_s[...] = stat_own[...] + stat_got[1] + (stat_got[2] + stat_got[3])
    for g in range(GROUPS):
        sent(g)
    st_hop(0, st_own, px).wait_send()
    st_hop(1, st_own, py).wait_send()
    own_row.wait()

    low_half, high_half = slice(0, W // 2), slice(W // 2, W)
    parts = (ga_s, gb_s, ga_s.at[:, low_half], ga_s.at[:, high_half], gc_s)
    pbs, lbs, owns = (pb0, pb1, pb2, pb3, pb4), (lb0, lb1, lb2, lb3, lb4), (own0, own1, own2, own3, own4)
    gouts = (go_ref, gg_ref, gv_ref.at[:, low_half], gv_ref.at[:, high_half], gs_ref)

    def piece(g, i):
        return parts[g].at[pl.ds(pl.multiple_of(i * n, 16), n)]

    def swap(g, q):
        return rcopy(piece(g, q * 2 + 1 - c), pbs[g].at[q], bzs.at[g, 0, q], bzr.at[g, 0, q], {"fsdp": partner})

    def up(g, q):
        return rcopy(pbs[g].at[q], lbs[g].at[q], bzs.at[g, 1, q], bzr.at[g, 1, q], {"fsdp": f + 2})

    def down(g, q):
        to = jnp.where(q == p - 1, nl, q)
        return rcopy(pbs[g].at[q], lbs[g].at[to], bzs.at[g, 2, q], bzr.at[g, 2, q], {"fsdp": f - 2})

    def send_up(g, q, terms):
        pbs[g][q] = add(piece(g, q * 2 + c)[...], pbs[g][q], *terms).astype(BF16)
        up(g, q).start()

    def send_down(g, q, terms):
        pbs[g][q] = add(piece(g, q * 2 + c)[...], pbs[g][q], *terms).astype(BF16)
        down(g, q).start()

    def ends(g, shards):
        for k in shards:
            @pl.when(p == 0)
            def _():
                swap(g, nl - 1 - k).wait_recv()
                send_up(g, nl - 1 - k, ())

            @pl.when(p == nl - 1)
            def _():
                swap(g, k).wait_recv()
                send_down(g, k, ())

    def slot(g, t):
        @pl.when(jnp.logical_and(p > 0, p <= t))
        def _():
            q = nl - 1 - t + p
            swap(g, q).wait_recv()
            up(g, q).wait_recv()
            send_up(g, q, (lbs[g][q],))

        @pl.when(jnp.logical_and(p < nl - 1, nl - 1 - p <= t))
        def _():
            q = t - (nl - 1 - p)
            swap(g, q).wait_recv()
            down(g, q).wait_recv()
            send_down(g, q, (lbs[g][q],))

    def close(g):
        swap(g, p).wait_recv()

        @pl.when(p > 0)
        def _():
            up(g, p).wait_recv()

        @pl.when(p < nl - 1)
        def _():
            down(g, p).wait_recv()

        @pl.when(p == 0)
        def _():
            owns[g][...] = add(piece(g, f)[...], pbs[g][p], lbs[g][nl]).astype(BF16)

        @pl.when(p == nl - 1)
        def _():
            owns[g][...] = add(piece(g, f)[...], pbs[g][p], lbs[g][p]).astype(BF16)

        @pl.when(jnp.logical_and(p > 0, p < nl - 1))
        def _():
            owns[g][...] = add(piece(g, f)[...], pbs[g][p], lbs[g][p], lbs[g][nl]).astype(BF16)

        place_ = gouts[g].at[pl.ds(s * n, n)]
        rcopy(owns[g], place_, as_.at[g, 0], ar.at[g, 0], {"seq": px}).start()
        rcopy(owns[g], place_, as_.at[g, 1], ar.at[g, 1], {"seq": py}).start()
        pltpu.make_async_copy(owns[g], place_, os_.at[g]).start()

    def relay(g):
        seq_gather_relay(g, owns[g], gouts[g], as_, ar, px, py, s)

    def swaps_sent(g):
        for q in range(nl):
            swap(g, q).wait_send()

    def line_sent(g):
        for q in range(nl):
            @pl.when(q > p)
            def _():
                up(g, q).wait_send()

            @pl.when(q < p)
            def _():
                down(g, q).wait_send()

    order = []
    for k in range(D // STRIP // 2):
        order += [D // STRIP - 1 - k, k]

    def strip(j, a_ref, b_ref, bcols, to, groups):
        at = slice(j * STRIP, (j + 1) * STRIP)
        to[at, :] = lax.dot_general(a_ref[:, at], b_ref[:, bcols], TN, preferred_element_type=F32).astype(BF16)
        for q in range(nl):
            if j * STRIP <= q * 2 * n < (j + 1) * STRIP:
                for g in groups:
                    swap(g, q).start()

    gpost_s[...] = jnp.zeros_like(gpost_s)

    def gated_norm(i, carry):
        r = pl.ds(pl.multiple_of(i * 128, 128), 128)
        one = jnp.sum(jnp.where(eye, stat_s[pl.ds(i, 1), :], 0.0), axis=1, keepdims=True)
        two = jnp.sum(jnp.where(eye, stat_s[pl.ds(length // 128 + i, 1), :], 0.0), axis=1, keepdims=True)
        rho = lax.rsqrt(one * (1.0 / INNER) + EPS)
        mean = rho * two * (1.0 / INNER)
        gate = gate_s[r, :].astype(F32)
        mixed = mixed_s[r, :].astype(F32)
        dsh = dsh_s[r, :]
        post = ex_s[1:2, :]
        sg = sigmoid(gate)
        sl = gate * sg
        n1 = mixed * sl * rho
        gpost_s[...] += fold(dsh * n1)
        d_gated = rho * (dsh * post - n1 * mean)
        mixed_s[r, :] = (n1 * post).astype(BF16)
        dy_s[r, :] = (d_gated * sl).astype(BF16)
        gate_s[r, :] = (d_gated * mixed * (sg * (1.0 + gate * (1.0 - sg)))).astype(BF16)
        return carry

    lax.fori_loop(0, length // 128, gated_norm, 0)

    every = slice(0, W)
    for j in order[:2]:
        strip(j, cot_s, mixed_s, every, ga_s, (0,))
    ends(0, range(1))
    for j in order[2:]:
        strip(j, cot_s, mixed_s, every, ga_s, (0,))
    ends(0, range(1, nl // 2))
    x_load = pltpu.make_async_copy(x_hbm, cot_s, ls.at[8])
    x_load.start()

    def rows_of(t, a):
        return pl.ds((2 * t + a) * rows, rows)

    def result(t, a):
        out = (out_ref, gt_ref)[t].at[:, cols[a]]
        return pltpu.make_async_copy(dsh_s.at[rows_of(t, a)], out, ls.at[2 * t + a])

    for a in range(2):
        dsh_s[rows_of(0, a), :] = chunk(s, a)[...].astype(F32)

    for j in order:
        strip(j, nrm_s, gate_s, every, gb_s, (1,))
    ends(1, range(nl // 2))
    ends(0, range(nl // 2, nl - 1))
    ends(1, range(nl // 2, nl - 1))
    slot(0, 1)

    gpre_s[...] = jnp.zeros_like(gpre_s)

    def dn_chunk(j):
        r = pl.ds(pl.multiple_of(j * rows, rows), rows)
        dn = nt(gate_s[r, :], wg_s[...]) + nt(dv_s[r, 0:W], wv_s[...])
        dn = dn + nt(dv_s[r, W : W + REST], ws_s[...].reshape(D, REST))
        part_s[r, :] = dn.astype(BF16)
        x = cot_s[r, :].astype(F32)
        rho = lax.rsqrt(jnp.sum(x * x, axis=1, keepdims=True) * (1.0 / D) + EPS)
        gpre_s[...] += fold(dn * (x * rho))

        @pl.when((s ^ j) == 3)
        def _():
            seq_one(1, 0, 0).start()
            seq_one(1, 1, 0).start()

        @pl.when((s ^ j) == 1)
        def _():
            seq_one(1, 0, 1).start()

        @pl.when((s ^ j) == 2)
        def _():
            seq_one(1, 1, 1).start()

    def dn_pass(j):
        for a in range(2):
            @pl.when((s ^ j) == 2 - a)
            def _():
                seq_one(1, a, 0).wait_recv()
                az1[a, 0] = add(chunk(second[a], a)[...], ab1[a, 0]).astype(BF16)
                seq_two(1, a).start()

    def between(i):
        @pl.when(i == 1)
        def _():
            seq_pass(0)
            seq_one_sent(0)
            x_load.wait()

        @pl.when(jnp.logical_and(lax.rem(i, 2) == 1, i < 2 * SEQ - 1))
        def _():
            dn_chunk(SEQ - 1 - i // 2)

        @pl.when(i == 1)
        def _():
            for t in range(2, nl - 1):
                slot(0, t)

        @pl.when(i == 2)
        def _():
            slot(1, 1)

        @pl.when(i == 4)
        def _():
            for t in range(2, nl - 1):
                slot(1, t)

        @pl.when(i == 5)
        def _():
            close(0)

        @pl.when(i == 6)
        def _():
            dn_pass(3)

    scan_bwd_blocks(
        mix_s.at[:, 0:W], mix_s.at[:, W:CH], mix_s.at[:, CH:VC], dy_s, st_s, kw_s, hp_s, ex_s,
        dv_s, gcw_s, gch_s, ghd_s, buf, cbuf, dhst, rowp, xw_s, e_s, er_s, between,
    )

    swaps_sent(0)
    for j in order[:2]:
        strip(j, nrm_s, dv_s, every, ga_s, (2, 3))
    ends(2, range(1))
    ends(3, range(1))
    dn_chunk(0)
    close(1)
    for j in order[2:]:
        strip(j, nrm_s, dv_s, every, ga_s, (2, 3))
    for k in range(1, nl - 1):
        ends(2, (k,))
        ends(3, (k,))
    slot(2, 1)
    slot(3, 1)
    dn_pass(2)
    for j in order:
        strip(j, nrm_s, dv_s, slice(W, VC), gc_s, (4,))
    for t in range(2, nl - 1):
        slot(2, t)
    relay(0)

    conv_s[...] = jnp.zeros_like(conv_s)
    for j in range(5):
        tap = jnp.sum(gcw_s[j], axis=0, keepdims=True)
        conv_s[j : j + 1, pl.ds(pl.multiple_of(s * W, 128), W)] = tap[:, 0:W]
        conv_s[j : j + 1, INNER:XBC] = tap[:, W:CH]
    gpre_s[5:6, :] = jnp.sum(gpre_s[...], axis=0, keepdims=True)
    post_s[...] = jnp.zeros_like(post_s)
    post_s[6:7, pl.ds(pl.multiple_of(s * W, 128), W)] = jnp.sum(gpost_s[...], axis=0, keepdims=True)
    channels = jnp.sum(gch_s[...], axis=0, keepdims=True)
    lane8 = lax.broadcasted_iota(jnp.int32, (8, 128), 1)
    row8 = lax.broadcasted_iota(jnp.int32, (8, 128), 0)
    skip = jnp.zeros((1, 128), F32)
    lane1 = lax.broadcasted_iota(jnp.int32, (1, 128), 1)
    for h in range(HL):
        at = slice(128 * (h // 2), 128 * (h // 2) + 128)
        half_of = (lane1 < HW) if h % 2 == 0 else (lane1 >= HW)
        skip = jnp.where(lane1 == h, jnp.sum(jnp.where(half_of, channels[:, at], 0.0), axis=1, keepdims=True), skip)
    heads = [
        pltpu.roll(jnp.where(row8 == 7, jnp.broadcast_to(v, (8, 128)), 0.0), s * HL, 1)
        for v in (ghd_s[0:1, :], ghd_s[1:2, :], skip)
    ]
    row512 = lax.broadcasted_iota(jnp.int32, (8, 512), 0)
    hn = HEADS // nf
    for i in range(nf):
        conv = unplace(conv_s, i * (XBC // nf), XBC // nf)
        block = jnp.where(row512 < 5, conv, 0.0)
        block = block + jnp.where(row512 == 5, unplace(gpre_s, i * (D // nf), D // nf), 0.0)
        block = block + unplace(post_s, i * (INNER // nf), INNER // nf)
        tiles = []
        for v in heads:
            moved = pltpu.roll(v, (128 - i * hn) % 128, 1) if i else v
            tiles.append(jnp.where(lane8 < hn, moved, 0.0))
        block = block + jnp.concatenate(tiles + [jnp.zeros((8, 128), F32)], axis=1)
        snd_s[i] = block

    def small_send(k):
        to = lax.rem(f + k, nf)
        return rcopy(snd_s.at[to], got_s.at[k], bms.at[k], bmr.at[k], {"fsdp": to})

    for k in range(1, nf):
        small_send(k).start()
    ends(4, range(nl - 1))
    for t in range(2, nl - 1):
        slot(3, t)
    dn_pass(1)
    dn_pass(0)
    close(2)
    close(3)
    for t in range(1, nl - 1):
        slot(4, t)
    relay(1)

    for a in range(2):
        seq_one(0, a, 1).wait_recv()
        seq_two(0, a).wait_recv()
        for k in range(rows // 128):
            one = stat_s[pl.ds(s * (rows // 128) + k, 1), :]
            rho = lax.rsqrt(jnp.sum(jnp.where(eye, one, 0.0), axis=1, keepdims=True) * (1.0 / INNER) + EPS)
            part = slice(128 * k, 128 * k + 128)
            at = pl.ds(a * rows + 128 * k, 128)
            x = cot_s[pl.ds(pl.multiple_of(s * rows + 128 * k, 128), 128), cols[a]].astype(F32)
            dsh_s[at, :] = x + rho * add(dsh_s[at, :], ab0[a, 1, part], az0[a, 1, part])
        result(0, a).start()

    total = snd_s[f]
    for k in range(1, nf):
        small_send(k).wait_recv()
        total = total + got_s[k]
    sown_s[...] = total

    def small_share(k):
        return rcopy(sown_s, sgot_s.at[s], bes.at[k], ber.at[k], {"seq": s ^ k})

    for k in range(1, SEQ):
        small_share(k).start()
    close(4)
    relay(2)
    relay(3)

    for a in range(2):
        seq_one(1, a, 1).wait_recv()
        seq_two(1, a).wait_recv()
        dsh_s[rows_of(1, a), :] = add(chunk(s, a)[...], ab1[a, 1], az1[a, 1])

    def grad_tokens(i, carry):
        x = cot_s[pl.ds(pl.multiple_of(s * rows + i * 64, 64), 64), :].astype(F32)
        rho = lax.rsqrt(jnp.sum(x * x, axis=1, keepdims=True) * (1.0 / D) + EPS)
        at = [pl.ds(pl.multiple_of((2 + a) * rows + i * 64, 64), 64) for a in range(2)]
        n0 = [x[:, cols[a]] * rho for a in range(2)]
        e0 = [dsh_s[at[a], :] * pre_s[5:6, cols[a]] for a in range(2)]
        dot = sum(jnp.sum(e0[a] * n0[a], axis=1, keepdims=True) for a in range(2))
        mean = dot * (1.0 / D)
        cot = cotrow_s[pl.ds(pl.multiple_of(i * 64, 64), 64), :].astype(F32)
        for a in range(2):
            dsh_s[at[a], :] = cot[:, cols[a]] + rho * (e0[a] - n0[a] * mean)
        return carry

    lax.fori_loop(0, rows // 64, grad_tokens, 0)
    for a in range(2):
        result(1, a).start()
    relay(4)

    for k in range(1, SEQ):
        small_share(k).wait()
    total = jnp.zeros_like(sown_s)
    for k in range(SEQ):
        total = total + jnp.where(s == k, sown_s[...], sgot_s[k])
    small_ref[...] = total
    for t in range(2):
        for a in range(2):
            result(t, a).wait()
    for k in range(1, nf):
        small_send(k).wait_send()
    seq_one_sent(1)
    for t in range(2):
        for a in range(2):
            seq_two(t, a).wait_send()
    for g in range(5):
        seq_gather_finish(g, owns[g], gouts[g], as_, ar, px, py, s)
        pltpu.make_async_copy(owns[g], gouts[g].at[pl.ds(s * n, n)], os_.at[g]).wait()
        line_sent(g)
    for g in range(1, 5):
        swaps_sent(g)


def mixer(nf, tok, cot, win, wout, small):
    shape = jax.ShapeDtypeStruct
    vm = pltpu.VMEM
    dma = pltpu.SemaphoreType.DMA
    rows = tok.shape[0]
    length = SEQ * rows
    nl = nf // 2
    n = D // nf
    widths = (W, W, W, VC - W)
    groups = (W, W, W // 2, W // 2, VC - W)
    boxes = [vm((nl, n, w), BF16) for w in groups] + [vm((nl + 1, n, w), BF16) for w in groups]
    boxes += [vm((n, w), BF16) for w in groups]
    return pl.pallas_call(
        functools.partial(mixer_kernel, nf),
        out_shape=[shape((rows, D), F32)] * 2
        + [shape((SEQ * n, w), BF16) for w in widths]
        + [shape((8, 512), F32), shape((length, D), BF16)],
        in_specs=[ANY] * 4 + [VMEM],
        out_specs=[ANY] * 6 + [VMEM, ANY],
        scratch_shapes=[
            vm((length, D), BF16),
            vm((length, D), BF16),
            vm((D, W), BF16),
            vm((nf, SEQ, n // SEQ, REST), BF16),
            vm((D, W), BF16),
            vm((D, W), BF16),
            vm((length, VC), BF16),
            vm((length, W), BF16),
            vm((length, W), BF16),
            vm((length // Q, STATE, W), BF16),
            vm((length, W), F32),
            vm((length, W), BF16),
            vm((length, VC), BF16),
            vm((rows, D), BF16),
            vm((length, D), BF16),
            vm((D, W), BF16),
            vm((D, VC - W), BF16),
        ]
        + boxes
        + [vm((2, 2, rows, D // 2), BF16)] * 4
        + [
            vm((8, CH), F32),
            vm((8, 128), F32),
            vm((8, W), F32),
            vm((8, D), F32),
            vm((2 * length // 128, 128), F32),
            vm((2 * length // 128, 128), F32),
            vm((SEQ, 2 * length // 128, 128), F32),
            vm((5, 8, CH), F32),
            vm((8, W), F32),
            vm((8, 128), F32),
            vm((8, W), F32),
            vm((8, D), F32),
            vm((8, XBC), F32),
            vm((8, INNER), F32),
            vm((nf, 8, 512), F32),
            vm((nf, 8, 512), F32),
            vm((8, 512), F32),
            vm((SEQ, 8, 512), F32),
            vm((Q + 8, CH), F32),
            vm((Q + 8, CH), F32),
            vm((STATE, W), F32),
            vm((128, Q), F32),
            vm((Q, W), BF16),
            vm((Q, W), BF16),
            vm((8, W), F32),
            dma((9,)),
            dma((3, 4)),
            dma((3, 4)),
            dma((GROUPS, 4, nl)),
            dma((GROUPS, nf)),
            dma((nf,)),
            dma((nf,)),
            dma((SEQ,)),
            dma((SEQ,)),
            dma((5, 3, nl)),
            dma((5, 3, nl)),
            dma((2, 2, 3)),
            dma((2, 2, 3)),
            dma((5, 4)),
            dma((5, 4)),
            dma((nf,)),
            dma((nf,)),
            dma((SEQ,)),
            dma((SEQ,)),
            dma((5,)),
        ],
        name="mixer",
        compiler_params=pltpu.CompilerParams(
            collective_id=1, has_side_effects=True, vmem_limit_bytes=67043328
        ),
    )(tok, cot, win, wout, small)


def finish_kernel(
    go, gg, gv, gs, out, gt, small, out_o, gt_o, gin_o, gout_o, cw_o, cb_o, pre_o, post_o, step_o, decay_o, skip_o
):
    out_o[...] = out[...]
    gt_o[...] = gt[...]
    for i in range(SEQ):
        gin_o[:, i * W : i * W + W] = gg[i].astype(F32)
        gin_o[:, INNER + i * W : INNER + i * W + W] = gv[i].astype(F32)
    total = gs[0].astype(F32)
    for i in range(1, SEQ):
        total = total + gs[i].astype(F32)
    rest = gin_o.shape[1] - 2 * INNER
    gin_o[:, 2 * INNER :] = total[:, :rest]
    gout_o[...] = go[0].astype(F32)

    @pl.when(pl.program_id(0) == 0)
    def _():
        cw_o[...] = small[0:4, : cw_o.shape[1]]
        cb_o[...] = small[4:5, : cb_o.shape[1]]
        pre_o[...] = small[5:6, : pre_o.shape[1]]
        for k in range(post_o.shape[0]):
            post_o[k : k + 1, :] = small[6:7, 128 * k : 128 * k + post_o.shape[1]]
        heads = step_o.shape[1]
        step_o[...] = small[7:8, :heads]
        decay_o[...] = small[7:8, 128 : 128 + heads]
        skip_o[...] = small[7:8, 256 : 256 + heads]


def finish(nf, go, gg, gv, gs, out, gt, small):
    shape = jax.ShapeDtypeStruct
    n = D // nf
    step, rows = n // SEQ, out.shape[0] // SEQ
    proj = 2 * INNER + 2 * STATE + HEADS
    go, gg, gv, gs = (g.reshape(SEQ, n, g.shape[1]) for g in (go, gg, gv, gs))

    def whole(*dims):
        return pl.BlockSpec(dims, lambda i: (0,) * len(dims))

    np_ = INNER // nf
    post = (np_ // 128, 128) if np_ % 128 == 0 else (1, np_)
    tiny = [(4, XBC // nf), (1, XBC // nf), (1, n), post] + [(1, HEADS // nf)] * 3
    return pl.pallas_call(
        finish_kernel,
        grid=(SEQ,),
        out_shape=[shape(out.shape, F32)] * 2
        + [shape((n, proj), F32), shape((n, INNER), F32)]
        + [shape(dims, F32) for dims in tiny],
        in_specs=[
            pl.BlockSpec((1, n, W), lambda i: (i, 0, 0)),
            pl.BlockSpec((SEQ, step, W), lambda i: (0, i, 0)),
            pl.BlockSpec((SEQ, step, W), lambda i: (0, i, 0)),
            pl.BlockSpec((SEQ, step, VC - W), lambda i: (0, i, 0)),
            pl.BlockSpec((rows, D), lambda i: (i, 0)),
            pl.BlockSpec((rows, D), lambda i: (i, 0)),
            whole(8, 512),
        ],
        out_specs=[
            pl.BlockSpec((rows, D), lambda i: (i, 0)),
            pl.BlockSpec((rows, D), lambda i: (i, 0)),
            pl.BlockSpec((step, proj), lambda i: (i, 0)),
            pl.BlockSpec((n, W), lambda i: (0, i)),
        ]
        + [whole(*dims) for dims in tiny],
        name="finish",
        compiler_params=pltpu.CompilerParams(vmem_limit_bytes=VMEM_LIMIT),
    )(go, gg, gv, gs, out, gt, small)


def body(
    tokens,
    input_projection_weight,
    pre_gain,
    conv_weight,
    conv_bias,
    step_bias,
    decay_log,
    skip_gain,
    post_gain,
    output_projection_weight,
    cotangent,
):
    nf = lax.axis_size("fsdp")
    tok = tokens.reshape(tokens.shape[1:])
    cot = cotangent.reshape(cotangent.shape[1:])
    win = input_projection_weight

    w_out = output_projection_weight.T

    flat, at = jnp.zeros((2048,), F32), 0
    for v, size in (
        (conv_bias, 512), (pre_gain, 512), (post_gain, 512), (step_bias, 128), (decay_log, 128), (skip_gain, 256),
    ):
        flat = flat + jnp.pad(v.astype(F32), (at, 2048 - at - v.shape[0]))
        at += size
    taps = jnp.pad(conv_weight.T.astype(F32), ((0, 4), (0, 512 - conv_weight.shape[0])))
    small = taps + jnp.pad(flat.reshape(4, 512), ((4, 0), (0, 0)))
    out, gt, g_out, g_gate, g_val, g_state, small, _ = mixer(nf, tok, cot, win, w_out, small)
    block_out, grad_tokens, grad_in, grad_out, cw, cb, pre, post, step, decay, skip = finish(
        nf, g_out, g_gate, g_val, g_state, out, gt, small
    )
    return (
        block_out[None],
        grad_tokens[None],
        grad_in,
        pre.reshape(-1),
        cw.T,
        cb.reshape(-1),
        step.reshape(-1),
        decay.reshape(-1),
        skip.reshape(-1),
        post.reshape(-1),
        grad_out.T,
    )


def solution(mesh):
    in_specs = (
        P("fsdp", "seq", None),
        P("fsdp", None),
        P("fsdp"),
        P("fsdp", None),
        P("fsdp"),
        P("fsdp"),
        P("fsdp"),
        P("fsdp"),
        P("fsdp"),
        P(None, "fsdp"),
        P("fsdp", "seq", None),
    )
    out_specs = (
        P("fsdp", "seq", None),
        P("fsdp", "seq", None),
        P("fsdp", None),
        P("fsdp"),
        P("fsdp", None),
        P("fsdp"),
        P("fsdp"),
        P("fsdp"),
        P("fsdp"),
        P("fsdp"),
        P(None, "fsdp"),
    )
    return jax.shard_map(body, mesh=mesh, in_specs=in_specs, out_specs=out_specs, check_vma=False)
```

```python
import functools

import jax
import jax.numpy as jnp
from jax import lax
from jax.experimental import pallas as pl
from jax.experimental.pallas import tpu as pltpu
from jax.sharding import PartitionSpec as P

D = 1536
INNER = 3072
STATE = 128
HEADS = 48
XBC = INNER + 2 * STATE
EPS = 1e-05

SEQ = 4
W = INNER // SEQ
HL = HEADS // SEQ
HW = INNER // HEADS
CH = W + 2 * STATE
VC = CH + 128
REST = 2 * STATE + HEADS
Q = 128

F32 = jnp.float32
BF16 = jnp.bfloat16
MESH = pl.DeviceIdType.MESH
HIGH = lax.Precision.HIGHEST
VMEM = pl.BlockSpec(memory_space=pltpu.VMEM)
ANY = pl.BlockSpec(memory_space=pl.ANY)
VMEM_LIMIT = 64000 * 1024


def rcopy(src, dst, send_sem, recv_sem, device):
    return pltpu.make_async_remote_copy(
        src_ref=src, dst_ref=dst, send_sem=send_sem, recv_sem=recv_sem, device_id=device, device_id_type=MESH
    )


def signal(sem, device):
    pl.semaphore_signal(sem, inc=1, device_id=device, device_id_type=MESH)


def nn(a, b, precision=None):
    return lax.dot_general(a, b, (((1,), (0,)), ((), ())), precision=precision, preferred_element_type=F32)


def nt(a, b, precision=None):
    return lax.dot_general(a, b, (((1,), (1,)), ((), ())), precision=precision, preferred_element_type=F32)


def seq_gather_start(refs, outs, send, recv, px, py, me):
    for g, (src, out) in enumerate(zip(refs, outs)):
        n = src.shape[0]
        own = out.at[pl.ds(me * n, n)]
        rcopy(src, own, send.at[g, 0], recv.at[g, 0], {"seq": px}).start()
        rcopy(src, own, send.at[g, 1], recv.at[g, 1], {"seq": py}).start()


def seq_gather_relay(g, src, out, send, recv, px, py, me):
    n = src.shape[0]
    h = n // 2
    own = out.at[pl.ds(me * n, n)]
    rcopy(src, own, send.at[g, 0], recv.at[g, 0], {"seq": px}).wait_recv()
    top = out.at[pl.ds(px * n, h)]
    rcopy(top, top, send.at[g, 2], recv.at[g, 2], {"seq": py}).start()
    rcopy(src, own, send.at[g, 1], recv.at[g, 1], {"seq": py}).wait_recv()
    low = out.at[pl.ds(py * n + h, h)]
    rcopy(low, low, send.at[g, 3], recv.at[g, 3], {"seq": px}).start()


def seq_gather_finish(g, src, out, send, recv, px, py, me):
    n = src.shape[0]
    h = n // 2
    own = out.at[pl.ds(me * n, n)]
    half = out.at[pl.ds(me * n, h)]
    rcopy(half, half, send.at[g, 2], recv.at[g, 2], {"seq": py}).wait()
    rcopy(half, half, send.at[g, 3], recv.at[g, 3], {"seq": px}).wait()
    rcopy(src, own, send.at[g, 0], recv.at[g, 0], {"seq": px}).wait_send()
    rcopy(src, own, send.at[g, 1], recv.at[g, 1], {"seq": py}).wait_send()


def softplus(x):
    return jnp.maximum(x, 0.0) + jnp.log1p(jnp.exp(-jnp.abs(x)))


def sigmoid(x):
    return 0.5 + 0.5 * jnp.tanh(0.5 * x)


def rates_of(r_ref, rows, hp_ref, tri):
    back = lax.rem(128 - lax.axis_index("seq") * HL, 128)
    raw = pltpu.roll(r_ref[rows, :].astype(F32), back, 1) + hp_ref[0:1, :]
    dt = softplus(raw)
    lam = nn(tri, dt * hp_ref[1:2, :], HIGH)
    return raw, dt, lam


def fold(x):
    return jnp.sum(x.reshape(x.shape[0] // 8, 8, x.shape[1]), axis=0)


def spread(mat, h):
    return jnp.broadcast_to(mat[:, h : h + 1], (mat.shape[0], 128))


def scan_fwd_blocks(
    v_ref, s_ref, r_ref, kw_ref, hp_ref, ex_ref, mixed_ref, st_ref, buf, hst, xw_s, er_s, between
):
    blocks = v_ref.shape[0] // Q
    row = lax.broadcasted_iota(jnp.int32, (Q, Q), 0)
    col = lax.broadcasted_iota(jnp.int32, (Q, Q), 1)
    causal = row >= col
    tri = causal.astype(F32)
    low = lax.broadcasted_iota(jnp.int32, (Q, 128), 1) < HW
    low1 = lax.broadcasted_iota(jnp.int32, (1, 128), 1) < HW
    buf[0:8, :] = jnp.zeros((8, CH), F32)
    hst[...] = jnp.zeros_like(hst)

    def block(b, carry):
        rows = pl.ds(pl.multiple_of(b * Q, Q), Q)
        buf[8 : 8 + Q, 0:W] = v_ref[rows, :].astype(F32)
        buf[8 : 8 + Q, W:CH] = s_ref[rows, :].astype(F32)
        k = kw_ref[4:5, :] + buf[5 : 5 + Q, :] * kw_ref[0:1, :]
        for j in range(1, 4):
            k = k + buf[5 + j : 5 + j + Q, :] * kw_ref[j : j + 1, :]
        buf[0:8, :] = buf[Q : Q + 8, :]
        x = k * sigmoid(k)
        bs, cs = x[:, W : W + STATE], x[:, W + STATE :]
        _, dt, lam = rates_of(r_ref, rows, hp_ref, tri)
        lam_t, dt_t = lam.T, dt.T
        last = lam[Q - 1 : Q, :]
        tail = dt * jnp.exp(last - lam)
        aff = nt(cs, bs, HIGH)
        st_ref[b] = hst[...].astype(BF16)
        ch = nn(cs.astype(BF16), st_ref[b])
        for i in range(HL // 2):
            at = slice(128 * i, 128 * i + 128)
            xp = x[:, at]
            xb = xp.astype(BF16)
            y, lc = [], []
            for h in (2 * i, 2 * i + 1):
                lcol = spread(lam, h)
                within = jnp.exp(jnp.where(causal, lcol - lam_t[h : h + 1, :], -1e30))
                y.append(nn((aff * within * dt_t[h : h + 1, :]).astype(BF16), xb))
                lc.append(lcol)
            out = jnp.where(low, y[0], y[1])
            out = out + jnp.exp(jnp.where(low, lc[0], lc[1])) * ch[:, at] + ex_ref[0:1, at] * xp
            mixed_ref[rows, at] = out.astype(BF16)
            xw_s[:, at] = (xp * jnp.where(low, spread(tail, 2 * i), spread(tail, 2 * i + 1))).astype(BF16)
            er_s[0:1, at] = jnp.exp(jnp.where(low1, spread(last, 2 * i), spread(last, 2 * i + 1)))
        hst[...] = hst[...] * er_s[0:1, :] + nn(bs.T.astype(BF16), xw_s[...])
        between(b)
        return carry

    lax.fori_loop(0, blocks, block, 0)


def scan_bwd_blocks(
    v_ref, s_ref, r_ref, dy_ref, st_ref, kw_ref, hp_ref, ex_ref,
    dv_ref, gcw_ref, gch_ref, ghd_ref,
    buf, cbuf, dhst, rowp, xw_s, e_s, er_s, between,
):
    blocks = v_ref.shape[0] // Q
    row = lax.broadcasted_iota(jnp.int32, (Q, Q), 0)
    col = lax.broadcasted_iota(jnp.int32, (Q, Q), 1)
    tri = (row >= col).astype(F32)
    later = col >= row
    suffix = later.astype(F32)
    strict = (col < row).astype(F32)
    lane = lax.broadcasted_iota(jnp.int32, (Q, 128), 1)
    lane1 = lax.broadcasted_iota(jnp.int32, (1, 128), 1)
    low = lane < HW
    low1 = lane1 < HW
    buf[Q : Q + 8, :] = jnp.zeros((8, CH), F32)
    dhst[...] = jnp.zeros_like(dhst)
    rowp[...] = jnp.zeros_like(rowp)
    gcw_ref[...] = jnp.zeros_like(gcw_ref)
    gch_ref[...] = jnp.zeros_like(gch_ref)
    ghd_ref[...] = jnp.zeros_like(ghd_ref)

    def block(i0, carry):
        b = blocks - 1 - i0
        rows = pl.ds(pl.multiple_of(b * Q, Q), Q)
        before = pl.ds(pl.multiple_of(jnp.maximum(b * Q - 16, 0), 16), 16)
        keep = (b > 0).astype(F32)
        cbuf[0:8, 0:W] = v_ref[before, :].astype(F32)[8:16, :] * keep
        cbuf[0:8, W:CH] = s_ref[before, :].astype(F32)[8:16, :] * keep
        cbuf[8 : 8 + Q, 0:W] = v_ref[rows, :].astype(F32)
        cbuf[8 : 8 + Q, W:CH] = s_ref[rows, :].astype(F32)
        k = kw_ref[4:5, :] + cbuf[5 : 5 + Q, :] * kw_ref[0:1, :]
        for j in range(1, 4):
            k = k + cbuf[5 + j : 5 + j + Q, :] * kw_ref[j : j + 1, :]
        sg = sigmoid(k)
        x = k * sg
        ds = sg * (1.0 + k * (1.0 - sg))
        bs, cs = x[:, W : W + STATE], x[:, W + STATE :]
        bb, cb = bs.astype(BF16), cs.astype(BF16)
        raw, dt, lam = rates_of(r_ref, rows, hp_ref, tri)
        lam_t = lam.T
        last = lam[Q - 1 : Q, :]
        aff_t = nt(bs, cs, HIGH)
        hb = st_ref[b]
        dhb = dhst[...].astype(BF16)
        ch = nn(cb, hb)
        bd = nn(bb, dhb)
        daff_t = jnp.zeros((Q, Q), F32)
        col_n = jnp.zeros((Q, 128), F32)
        col_i = jnp.zeros((Q, 128), F32)
        row_i = jnp.zeros((Q, 128), F32)
        through = jnp.zeros((1, 128), F32)
        for i in range(HL // 2):
            at = slice(128 * i, 128 * i + 128)
            xp = x[:, at]
            xb = xp.astype(BF16)
            dyb = dy_ref[rows, at]
            dyf = dyb.astype(F32)
            z, lc, dc = [], [], []
            for h in (2 * i, 2 * i + 1):
                mine = low if h % 2 == 0 else jnp.logical_not(low)
                lcol, dcol = spread(lam, h), spread(dt, h)
                within = jnp.exp(jnp.where(later, lam_t[h : h + 1, :] - lcol, -1e30))
                g = nt(jnp.where(mine, xp, 0.0).astype(BF16), dyb)
                lg = within * g
                lgd = lg * dcol
                daff_t = daff_t + lgd
                pair = (aff_t * lg).astype(BF16)
                col_n = col_n + nn(pair, jnp.where(lane == h, 1.0, 0.0).astype(BF16))
                rowp[h : h + 1, :] = jnp.sum(pair.astype(F32) * dcol, axis=0, keepdims=True)
                z.append(nn((aff_t * within).astype(BF16), dyb))
                lc.append(lcol)
                dc.append(dcol)
            lamp = jnp.where(low, lc[0], lc[1])
            dtp = jnp.where(low, dc[0], dc[1])
            lastp = jnp.where(low1, spread(last, 2 * i), spread(last, 2 * i + 1))
            e = dyf * jnp.exp(lamp)
            e_s[:, at] = e.astype(BF16)
            ew = jnp.exp(lastp - lamp)
            bdp = bd[:, at]
            xw_s[:, at] = (xp * (dtp * ew)).astype(BF16)
            er_s[0:1, at] = jnp.exp(lastp)
            re = e * ch[:, at]
            ci = xp * bdp * ew
            th = jnp.sum(dhst[:, at] * hb[:, at].astype(F32), axis=0, keepdims=True) * er_s[0:1, at]
            heads = jnp.where(lane == 2 * i + jnp.where(row < HW, 0, 1), 1.0, 0.0).astype(BF16)
            row_i = row_i + nn(re.astype(BF16), heads)
            col_i = col_i + nn(ci.astype(BF16), heads)
            for h in (2 * i, 2 * i + 1):
                mine1 = low1 if h % 2 == 0 else jnp.logical_not(low1)
                through = jnp.where(
                    lane1 == h, jnp.sum(jnp.where(mine1, th, 0.0), axis=1, keepdims=True), through
                )
            dx = dtp * jnp.where(low, z[0], z[1]) + bdp * (dtp * ew) + ex_ref[0:1, at] * dyf
            gch_ref[:, at] += fold(dyf * xp)
            buf[0:Q, at] = dx * ds[:, at]
        daff_b = daff_t.astype(BF16)
        d_bs = nt(xw_s[...], dhb) + nn(daff_b, cb)
        d_cs = nt(e_s[...], hb) + nn(daff_t.T.astype(BF16), bb)
        buf[0:Q, W : W + STATE] = d_bs * ds[:, W : W + STATE]
        buf[0:Q, W + STATE : CH] = d_cs * ds[:, W + STATE :]
        dhst[...] = dhst[...] * er_s[0:1, :] + nn(cs.T.astype(BF16), e_s[...])
        after = nn(suffix, rowp[...].T - dt * col_n + row_i, HIGH) + nn(strict, dt * col_i, HIGH) + through
        d_rate = (col_n + col_i + hp_ref[1:2, :] * after) * sigmoid(raw)
        ghd_ref[0:1, :] += jnp.sum(d_rate, axis=0, keepdims=True)
        ghd_ref[1:2, :] += jnp.sum(dt * after, axis=0, keepdims=True) * hp_ref[1:2, :]
        dv_ref[rows, CH:VC] = pltpu.roll(d_rate, lax.axis_index("seq") * HL, 1).astype(BF16)
        for at in (slice(0, W), slice(W, CH)):
            raw_v = cbuf[8 : 8 + Q, at]
            dk = buf[0:Q, at]
            dv = dk * kw_ref[3:4, at]
            gcw_ref[4, :, at] += fold(dk)
            gcw_ref[3, :, at] += fold(dk * raw_v)
            for j in range(3):
                dk = buf[3 - j : 3 - j + Q, at]
                dv = dv + dk * kw_ref[j : j + 1, at]
                gcw_ref[j, :, at] += fold(dk * raw_v)
            dv_ref[rows, at] = dv.astype(BF16)
        buf[Q : Q + 8, :] = buf[0:8, :]
        between(i0)
        return carry

    lax.fori_loop(0, blocks, block, 0)


GROUPS = 4


def place(block, at, width):
    start, shift = at // 128 * 128, at % 128
    lanes = -(-(width + shift) // 128) * 128
    have = block.shape[1]
    if lanes > have:
        block = jnp.concatenate([block, jnp.zeros((block.shape[0], lanes - have), block.dtype)], axis=1)
    else:
        block = block[:, :lanes]
    if shift:
        block = pltpu.roll(block, shift, 1)
    return start, lanes, block


TN = (((0,), (0,)), ((), ()))
STRIP = 384


def unplace(block, at, width):
    start, shift = at // 128 * 128, at % 128
    lanes = -(-(width + shift) // 128) * 128
    piece = block[:, start : start + lanes]
    if shift:
        piece = pltpu.roll(piece, lanes - shift, 1)
    if lanes < 512:
        piece = jnp.concatenate([piece, jnp.zeros((piece.shape[0], 512 - lanes), piece.dtype)], axis=1)
    else:
        piece = piece[:, :512]
    return jnp.where(lax.broadcasted_iota(jnp.int32, piece.shape, 1) < width, piece, 0.0)


def mixer_kernel(
    nf, tok, cot, win, wout, small,
    out_ref, gt_ref, go_ref, gg_ref, gv_ref, gs_ref, small_ref, x_hbm,
    cot_s, nrm_s, wv_s, ws_s, wg_s, wo_s, mix_s, gate_s, mixed_s, st_s, dsh_s,
    dy_s, dv_s, cotrow_s, part_s, gb_s, gc_s,
    pb0, pb1, pb2, pb3, pb4, lb0, lb1, lb2, lb3, lb4, own0, own1, own2, own3, own4,
    ab0, ab1, az0, az1,
    kw_s, hp_s, ex_s, pre_s, stat_s, stat_own, stat_got,
    gcw_s, gch_s, ghd_s, gpost_s, gpre_s, conv_s, post_s, snd_s, got_s, sown_s, sgot_s,
    buf, cbuf, dhst, rowp, xw_s, e_s, er_s,
    ls, xs, xr, zs, zr, ms, mr, es, er, bzs, bzr, bxs, bxr, as_, ar, bms, bmr, bes, ber, os_,
):
    x_s, small_s, ga_s = part_s, snd_s, wo_s
    s = lax.axis_index("seq")
    f = lax.axis_index("fsdp")
    px, py = s ^ 1, s ^ 2
    nl = nf // 2
    p, c = f // 2, f % 2
    partner = p * 2 + 1 - c
    bar = pltpu.get_barrier_semaphore()
    for k in range(1, SEQ):
        signal(bar, {"seq": s ^ k})
    for k in range(1, nf):
        signal(bar, {"fsdp": lax.rem(f + k, nf)})
    pl.semaphore_wait(bar, nf - 1 + SEQ - 1)

    n = win.shape[0]
    rows = tok.shape[0]
    length = rows * SEQ
    quarter = n // SEQ
    ins = (
        win.at[:, pl.ds(pl.multiple_of(INNER + s * W, 128), W)],
        win.at[pl.ds(pl.multiple_of(s * quarter, 8), quarter), pl.ds(2 * INNER, REST)],
        win.at[:, pl.ds(pl.multiple_of(s * W, 128), W)],
        wout.at[:, pl.ds(pl.multiple_of(s * W, 128), W)],
    )
    outs = (wv_s, ws_s, wg_s, wo_s)

    def row(g, i):
        return ws_s.at[i, s] if g == 1 else outs[g].at[pl.ds(i * n, n)]

    def hop(g, src, i, way, k, device):
        return rcopy(src, row(g, i), zs.at[g, way, k], zr.at[g, i], {"fsdp": device})

    def own_send(g):
        @pl.when(p < nl - 1)
        def _():
            hop(g, ins[g], f, 0, 0, f + 2).start()

        @pl.when(p > 0)
        def _():
            hop(g, ins[g], f, 1, 0, f - 2).start()

        hop(g, ins[g], f, 2, 0, partner).start()
        pltpu.make_async_copy(ins[g], row(g, f), ls.at[g]).start()

    def step(g, k):
        @pl.when(p - k >= 0)
        def _():
            o = f - 2 * k
            hop(g, row(g, o), o, 0, k, f).wait_recv()

            @pl.when(p < nl - 1)
            def _():
                hop(g, row(g, o), o, 0, k, f + 2).start()

            hop(g, row(g, o), o, 2, k, partner).start()

        @pl.when(p + k < nl)
        def _():
            o = f + 2 * k
            hop(g, row(g, o), o, 1, k, f).wait_recv()

            @pl.when(p > 0)
            def _():
                hop(g, row(g, o), o, 1, k, f - 2).start()

            hop(g, row(g, o), o, 3, k, partner).start()

    def arrive(g):
        pltpu.make_async_copy(ins[g], row(g, f), ls.at[g]).wait()
        for q in range(nl):
            o = q * 2 + 1 - c
            hop(g, row(g, o), o, 2, 0, partner).wait_recv()

    def sent(g):
        hop(g, ins[g], f, 2, 0, partner).wait_send()

        @pl.when(p < nl - 1)
        def _():
            hop(g, ins[g], f, 0, 0, f + 2).wait_send()

        @pl.when(p > 0)
        def _():
            hop(g, ins[g], f, 1, 0, f - 2).wait_send()

        for k in range(1, nl):
            @pl.when(p - k >= 0)
            def _():
                o = f - 2 * k

                @pl.when(p < nl - 1)
                def _():
                    hop(g, row(g, o), o, 0, k, f + 2).wait_send()

                hop(g, row(g, o), o, 2, k, partner).wait_send()

            @pl.when(p + k < nl)
            def _():
                o = f + 2 * k

                @pl.when(p > 0)
                def _():
                    hop(g, row(g, o), o, 1, k, f - 2).wait_send()

                hop(g, row(g, o), o, 3, k, partner).wait_send()

    def small_copy(k):
        return rcopy(small, small_s.at[f], ms.at[k], mr.at[k], {"fsdp": lax.rem(f + k, nf)})

    mine = pl.ds(s * rows, rows)
    own_small = pltpu.make_async_copy(small, small_s.at[f], ls.at[4])
    own_tok = pltpu.make_async_copy(tok, x_s.at[mine], ls.at[5])
    own_cot = pltpu.make_async_copy(cot, cot_s.at[mine], ls.at[6])
    own_row = pltpu.make_async_copy(cot, cotrow_s, ls.at[7])

    def st_hop(k, region, device):
        return rcopy(region, region, xs.at[2, k], xr.at[2, k], {"seq": device})

    st_own = ws_s.at[:, s]
    st_top, st_low = ws_s.at[pl.ds(0, nl), px], ws_s.at[pl.ds(nl, nl), py]

    for k in range(1, nf):
        small_copy(k).start()
    own_small.start()
    own_tok.start()
    seq_gather_start((tok,), (x_s,), xs, xr, px, py, s)
    own_send(1)
    own_send(0)
    own_cot.start()
    own_row.start()
    for k in range(1, min(3, nl)):
        step(1, k)
    step(0, 1)
    for k in range(3, nl):
        step(1, k)
    arrive(1)
    st_hop(0, st_own, px).start()
    st_hop(1, st_own, py).start()
    seq_gather_relay(0, tok, x_s, xs, xr, px, py, s)
    for k in range(2, min(3, nl)):
        step(0, k)
    own_send(2)
    own_send(3)

    mix_s[:, CH:VC] = jnp.zeros((length, VC - CH), BF16)

    own_small.wait()
    for k in range(1, nf):
        small_copy(k).wait()
    conv_s[...] = jnp.zeros_like(conv_s)
    pre_s[...] = jnp.zeros_like(pre_s)
    post_s[...] = jnp.zeros_like(post_s)
    heads = [jnp.zeros((8, 128), F32) for _ in range(3)]
    for i in range(nf):
        block = small_s[i]
        at, lanes, moved = place(block, i * (XBC // nf), XBC // nf)
        conv_s[:, at : at + lanes] += moved
        at, lanes, moved = place(block, i * (D // nf), D // nf)
        pre_s[:, at : at + lanes] += jnp.where(lax.broadcasted_iota(jnp.int32, moved.shape, 0) == 5, moved, 0.0)
        at, lanes, moved = place(block, i * (INNER // nf), INNER // nf)
        post_s[:, at : at + lanes] += jnp.where(lax.broadcasted_iota(jnp.int32, moved.shape, 0) == 6, moved, 0.0)
        for j in range(3):
            piece = block[:, 128 * j : 128 * j + 128]
            at = i * (HEADS // nf)
            heads[j] = heads[j] + (pltpu.roll(piece, at, 1) if at else piece)
    kw_s[:, 0:W] = conv_s[:, pl.ds(pl.multiple_of(s * W, 128), W)]
    kw_s[:, W:CH] = conv_s[:, INNER:XBC]
    lane1 = lax.broadcasted_iota(jnp.int32, (1, 128), 1)
    low1 = lane1 < HW
    back = lax.rem(128 - s * HL, 128)
    step_b, decay, skip = [pltpu.roll(h, back, 1)[7:8, :] for h in heads]
    hp_s[...] = jnp.zeros_like(hp_s)
    hp_s[0:1, :] = jnp.where(lane1 < HL, step_b, 0.0)
    hp_s[1:2, :] = jnp.where(lane1 < HL, -jnp.exp(decay), 0.0)
    ex_s[...] = jnp.zeros_like(ex_s)
    for i in range(HL // 2):
        ex_s[0:1, 128 * i : 128 * i + 128] = jnp.where(low1, spread(skip, 2 * i), spread(skip, 2 * i + 1))
    ex_s[1:2, :] = post_s[6:7, pl.ds(pl.multiple_of(s * W, 128), W)]

    st_hop(0, st_own, px).wait_recv()
    st_hop(2, st_top, py).start()
    st_hop(1, st_own, py).wait_recv()
    st_hop(3, st_low, px).start()
    own = cot_s.at[mine]
    rcopy(cot, own, xs.at[1, 0], xr.at[1, 0], {"seq": px}).start()
    rcopy(cot, own, xs.at[1, 1], xr.at[1, 1], {"seq": py}).start()
    for k in range(3, nl):
        step(0, k)
    own_tok.wait()
    seq_gather_finish(0, tok, x_s, xs, xr, px, py, s)

    def norm(i, carry):
        r = pl.ds(pl.multiple_of(i * 128, 128), 128)
        x = x_s[r, :].astype(F32)
        rho = lax.rsqrt(jnp.sum(x * x, axis=1, keepdims=True) * (1.0 / D) + EPS)
        nrm_s[r, :] = (x * rho * pre_s[5:6, :]).astype(BF16)
        return carry

    lax.fori_loop(0, length // 128, norm, 0)
    x_save = pltpu.make_async_copy(x_s, x_hbm, ls.at[8])
    x_save.start()
    arrive(0)

    def project(i, carry):
        r = pl.ds(pl.multiple_of(i * 256, 256), 256)
        mix_s[r, 0:W] = nn(nrm_s[r, :], wv_s[...]).astype(BF16)
        return carry

    def project_state(i, carry):
        r = pl.ds(pl.multiple_of(i * 256, 256), 256)
        mix_s[r, W : W + REST] = nn(nrm_s[r, :], ws_s[...].reshape(D, REST)).astype(BF16)
        return carry

    lax.fori_loop(0, length // 256, project, 0)
    step(2, 1)
    st_hop(2, st_top, py).wait()
    st_hop(3, st_low, px).wait()
    lax.fori_loop(0, length // 256, project_state, 0)

    def between(b):
        @pl.when(b == 1)
        def _():
            step(3, 1)

        @pl.when(b == 4)
        def _():
            step(2, 2)

    scan_fwd_blocks(
        mix_s.at[:, 0:W], mix_s.at[:, W:CH], mix_s.at[:, CH:VC], kw_s, hp_s, ex_s, mixed_s, st_s,
        buf, dhst, xw_s, er_s, between,
    )
    step(3, 2)
    seq_gather_relay(1, cot, cot_s, xs, xr, px, py, s)
    for k in range(3, nl):
        step(2, k)
    arrive(2)

    def project_gate(i, carry):
        r = pl.ds(pl.multiple_of(i * 256, 256), 256)
        gate_s[r, :] = nn(nrm_s[r, :], wg_s[...]).astype(BF16)
        return carry

    lax.fori_loop(0, length // 256, project_gate, 0)
    for k in range(3, nl):
        step(3, k)
    own_cot.wait()
    seq_gather_finish(1, cot, cot_s, xs, xr, px, py, s)
    arrive(3)
    eye = lax.broadcasted_iota(jnp.int32, (128, 128), 0) == lax.broadcasted_iota(jnp.int32, (128, 128), 1)

    def stats(i, carry):
        r = pl.ds(pl.multiple_of(i * 128, 128), 128)
        dsh = nn(cot_s[r, :], wo_s[...])
        dsh_s[r, :] = dsh
        gate = gate_s[r, :].astype(F32)
        gated = mixed_s[r, :].astype(F32) * (gate * sigmoid(gate))
        one = jnp.sum(gated * gated, axis=1, keepdims=True)
        gained = gated * ex_s[1:2, :]
        dy_s[r, :] = gained.astype(BF16)
        two = jnp.sum(dsh * gained, axis=1, keepdims=True)
        stat_own[pl.ds(i, 1), :] = jnp.sum(jnp.where(eye, one, 0.0), axis=0, keepdims=True)
        stat_own[pl.ds(length // 128 + i, 1), :] = jnp.sum(jnp.where(eye, two, 0.0), axis=0, keepdims=True)
        return carry

    lax.fori_loop(0, length // 128, stats, 0)
    copies = [rcopy(stat_own, stat_got.at[k], es.at[k], er.at[k], {"seq": s ^ k}) for k in range(1, SEQ)]
    for copy in copies:
        copy.start()

    half = D // 2
    cols = (slice(0, half), slice(half, D))
    first, second = (px, py), (py, px)
    ab, az = (ab0, ab1), (az0, az1)

    def chunk(i, a):
        return part_s.at[pl.ds(i * rows, rows), cols[a]]

    def seq_one(t, a, m):
        i = (first[a] ^ second[a] ^ s) if m == 0 else first[a]
        return rcopy(chunk(i, a), ab[t].at[a, m], bxs.at[t, a, m], bxr.at[t, a, m], {"seq": first[a]})

    def seq_two(t, a):
        return rcopy(az[t].at[a, 0], az[t].at[a, 1], bxs.at[t, a, 2], bxr.at[t, a, 2], {"seq": second[a]})

    def add(*terms):
        total = terms[0].astype(F32)
        for term in terms[1:]:
            total = total + term.astype(F32)
        return total

    def seq_pass(t):
        for a in range(2):
            seq_one(t, a, 0).wait_recv()
            az[t][a, 0] = add(chunk(second[a], a)[...], ab[t][a, 0]).astype(BF16)
            seq_two(t, a).start()

    def seq_last(t, out):
        for a in range(2):
            seq_one(t, a, 1).wait_recv()
            seq_two(t, a).wait_recv()
            out[:, cols[a]] = add(chunk(s, a)[...], ab[t][a, 1], az[t][a, 1])

    def seq_one_sent(t):
        for a in range(2):
            seq_one(t, a, 0).wait_send()
            seq_one(t, a, 1).wait_send()

    x_save.wait()

    def out_part(i, carry):
        r = pl.ds(pl.multiple_of((s ^ (SEQ - 1 - i)) * rows, rows), rows)
        part_s[r, :] = nt(dy_s[r, :], wo_s[...]).astype(BF16)

        @pl.when(i == 0)
        def _():
            for a in range(2):
                seq_one(0, a, 0).start()

        @pl.when(i == 2)
        def _():
            for a in range(2):
                seq_one(0, a, 1).start()

        return carry

    lax.fori_loop(0, SEQ, out_part, 0)

    for copy in copies:
        copy.wait()
    stat_s[...] = stat_own[...] + stat_got[1] + (stat_got[2] + stat_got[3])
    for g in range(GROUPS):
        sent(g)
    st_hop(0, st_own, px).wait_send()
    st_hop(1, st_own, py).wait_send()
    own_row.wait()

    low_half, high_half = slice(0, W // 2), slice(W // 2, W)
    parts = (ga_s, gb_s, ga_s.at[:, low_half], ga_s.at[:, high_half], gc_s)
    pbs, lbs, owns = (pb0, pb1, pb2, pb3, pb4), (lb0, lb1, lb2, lb3, lb4), (own0, own1, own2, own3, own4)
    gouts = (go_ref, gg_ref, gv_ref.at[:, low_half], gv_ref.at[:, high_half], gs_ref)

    def piece(g, i):
        return parts[g].at[pl.ds(pl.multiple_of(i * n, 16), n)]

    def swap(g, q):
        return rcopy(piece(g, q * 2 + 1 - c), pbs[g].at[q], bzs.at[g, 0, q], bzr.at[g, 0, q], {"fsdp": partner})

    def up(g, q):
        return rcopy(pbs[g].at[q], lbs[g].at[q], bzs.at[g, 1, q], bzr.at[g, 1, q], {"fsdp": f + 2})

    def down(g, q):
        to = jnp.where(q == p - 1, nl, q)
        return rcopy(pbs[g].at[q], lbs[g].at[to], bzs.at[g, 2, q], bzr.at[g, 2, q], {"fsdp": f - 2})

    def send_up(g, q, terms):
        pbs[g][q] = add(piece(g, q * 2 + c)[...], pbs[g][q], *terms).astype(BF16)
        up(g, q).start()

    def send_down(g, q, terms):
        pbs[g][q] = add(piece(g, q * 2 + c)[...], pbs[g][q], *terms).astype(BF16)
        down(g, q).start()

    def ends(g, shards):
        for k in shards:
            @pl.when(p == 0)
            def _():
                swap(g, nl - 1 - k).wait_recv()
                send_up(g, nl - 1 - k, ())

            @pl.when(p == nl - 1)
            def _():
                swap(g, k).wait_recv()
                send_down(g, k, ())

    def slot(g, t):
        @pl.when(jnp.logical_and(p > 0, p <= t))
        def _():
            q = nl - 1 - t + p
            swap(g, q).wait_recv()
            up(g, q).wait_recv()
            send_up(g, q, (lbs[g][q],))

        @pl.when(jnp.logical_and(p < nl - 1, nl - 1 - p <= t))
        def _():
            q = t - (nl - 1 - p)
            swap(g, q).wait_recv()
            down(g, q).wait_recv()
            send_down(g, q, (lbs[g][q],))

    def close(g):
        swap(g, p).wait_recv()

        @pl.when(p > 0)
        def _():
            up(g, p).wait_recv()

        @pl.when(p < nl - 1)
        def _():
            down(g, p).wait_recv()

        @pl.when(p == 0)
        def _():
            owns[g][...] = add(piece(g, f)[...], pbs[g][p], lbs[g][nl]).astype(BF16)

        @pl.when(p == nl - 1)
        def _():
            owns[g][...] = add(piece(g, f)[...], pbs[g][p], lbs[g][p]).astype(BF16)

        @pl.when(jnp.logical_and(p > 0, p < nl - 1))
        def _():
            owns[g][...] = add(piece(g, f)[...], pbs[g][p], lbs[g][p], lbs[g][nl]).astype(BF16)

        place_ = gouts[g].at[pl.ds(s * n, n)]
        rcopy(owns[g], place_, as_.at[g, 0], ar.at[g, 0], {"seq": px}).start()
        rcopy(owns[g], place_, as_.at[g, 1], ar.at[g, 1], {"seq": py}).start()
        pltpu.make_async_copy(owns[g], place_, os_.at[g]).start()

    def relay(g):
        seq_gather_relay(g, owns[g], gouts[g], as_, ar, px, py, s)

    def swaps_sent(g):
        for q in range(nl):
            swap(g, q).wait_send()

    def line_sent(g):
        for q in range(nl):
            @pl.when(q > p)
            def _():
                up(g, q).wait_send()

            @pl.when(q < p)
            def _():
                down(g, q).wait_send()

    order = []
    for k in range(D // STRIP // 2):
        order += [D // STRIP - 1 - k, k]

    def strip(j, a_ref, b_ref, bcols, to, groups):
        at = slice(j * STRIP, (j + 1) * STRIP)
        to[at, :] = lax.dot_general(a_ref[:, at], b_ref[:, bcols], TN, preferred_element_type=F32).astype(BF16)
        for q in range(nl):
            if j * STRIP <= q * 2 * n < (j + 1) * STRIP:
                for g in groups:
                    swap(g, q).start()

    gpost_s[...] = jnp.zeros_like(gpost_s)

    def gated_norm(i, carry):
        r = pl.ds(pl.multiple_of(i * 128, 128), 128)
        one = jnp.sum(jnp.where(eye, stat_s[pl.ds(i, 1), :], 0.0), axis=1, keepdims=True)
        two = jnp.sum(jnp.where(eye, stat_s[pl.ds(length // 128 + i, 1), :], 0.0), axis=1, keepdims=True)
        rho = lax.rsqrt(one * (1.0 / INNER) + EPS)
        mean = rho * two * (1.0 / INNER)
        gate = gate_s[r, :].astype(F32)
        mixed = mixed_s[r, :].astype(F32)
        dsh = dsh_s[r, :]
        post = ex_s[1:2, :]
        sg = sigmoid(gate)
        sl = gate * sg
        n1 = mixed * sl * rho
        gpost_s[...] += fold(dsh * n1)
        d_gated = rho * (dsh * post - n1 * mean)
        mixed_s[r, :] = (n1 * post).astype(BF16)
        dy_s[r, :] = (d_gated * sl).astype(BF16)
        gate_s[r, :] = (d_gated * mixed * (sg * (1.0 + gate * (1.0 - sg)))).astype(BF16)
        return carry

    lax.fori_loop(0, length // 128, gated_norm, 0)

    every = slice(0, W)
    for j in order[:2]:
        strip(j, cot_s, mixed_s, every, ga_s, (0,))
    ends(0, range(1))
    for j in order[2:]:
        strip(j, cot_s, mixed_s, every, ga_s, (0,))
    ends(0, range(1, nl - 1))
    x_load = pltpu.make_async_copy(x_hbm, cot_s, ls.at[8])
    x_load.start()

    def rows_of(t, a):
        return pl.ds((2 * t + a) * rows, rows)

    def result(t, a):
        out = (out_ref, gt_ref)[t].at[:, cols[a]]
        return pltpu.make_async_copy(dsh_s.at[rows_of(t, a)], out, ls.at[2 * t + a])

    for a in range(2):
        dsh_s[rows_of(0, a), :] = chunk(s, a)[...].astype(F32)

    for j in order:
        strip(j, nrm_s, gate_s, every, gb_s, (1,))
    ends(1, range(nl - 1))
    slot(0, 1)

    gpre_s[...] = jnp.zeros_like(gpre_s)

    def dn_chunk(j):
        r = pl.ds(pl.multiple_of(j * rows, rows), rows)
        dn = nt(gate_s[r, :], wg_s[...]) + nt(dv_s[r, 0:W], wv_s[...])
        dn = dn + nt(dv_s[r, W : W + REST], ws_s[...].reshape(D, REST))
        part_s[r, :] = dn.astype(BF16)
        x = cot_s[r, :].astype(F32)
        rho = lax.rsqrt(jnp.sum(x * x, axis=1, keepdims=True) * (1.0 / D) + EPS)
        gpre_s[...] += fold(dn * (x * rho))

        @pl.when((s ^ j) == 3)
        def _():
            seq_one(1, 0, 0).start()
            seq_one(1, 1, 0).start()

        @pl.when((s ^ j) == 1)
        def _():
            seq_one(1, 0, 1).start()

        @pl.when((s ^ j) == 2)
        def _():
            seq_one(1, 1, 1).start()

    def dn_pass(j):
        for a in range(2):
            @pl.when((s ^ j) == 2 - a)
            def _():
                seq_one(1, a, 0).wait_recv()
                az1[a, 0] = add(chunk(second[a], a)[...], ab1[a, 0]).astype(BF16)
                seq_two(1, a).start()

    def between(i):
        @pl.when(i == 1)
        def _():
            seq_pass(0)
            seq_one_sent(0)
            x_load.wait()

        @pl.when(jnp.logical_and(lax.rem(i, 2) == 1, i < 2 * SEQ - 1))
        def _():
            dn_chunk(SEQ - 1 - i // 2)

        @pl.when(i == 1)
        def _():
            for t in range(2, nl - 1):
                slot(0, t)

        @pl.when(i == 3)
        def _():
            close(0)

        @pl.when(i == 4)
        def _():
            slot(1, 1)

        @pl.when(i == 6)
        def _():
            for t in range(2, nl - 1):
                slot(1, t)
            dn_pass(3)

    scan_bwd_blocks(
        mix_s.at[:, 0:W], mix_s.at[:, W:CH], mix_s.at[:, CH:VC], dy_s, st_s, kw_s, hp_s, ex_s,
        dv_s, gcw_s, gch_s, ghd_s, buf, cbuf, dhst, rowp, xw_s, e_s, er_s, between,
    )

    swaps_sent(0)
    for j in order[:2]:
        strip(j, nrm_s, dv_s, every, ga_s, (2, 3))
    ends(2, range(1))
    ends(3, range(1))
    dn_chunk(0)
    close(1)
    for j in order[2:]:
        strip(j, nrm_s, dv_s, every, ga_s, (2, 3))
    for k in range(1, nl - 1):
        ends(2, (k,))
        ends(3, (k,))
    slot(2, 1)
    slot(3, 1)
    dn_pass(2)
    relay(0)
    for j in order:
        strip(j, nrm_s, dv_s, slice(W, VC), gc_s, (4,))
    for t in range(2, nl - 1):
        slot(2, t)

    conv_s[...] = jnp.zeros_like(conv_s)
    for j in range(5):
        tap = jnp.sum(gcw_s[j], axis=0, keepdims=True)
        conv_s[j : j + 1, pl.ds(pl.multiple_of(s * W, 128), W)] = tap[:, 0:W]
        conv_s[j : j + 1, INNER:XBC] = tap[:, W:CH]
    gpre_s[5:6, :] = jnp.sum(gpre_s[...], axis=0, keepdims=True)
    post_s[...] = jnp.zeros_like(post_s)
    post_s[6:7, pl.ds(pl.multiple_of(s * W, 128), W)] = jnp.sum(gpost_s[...], axis=0, keepdims=True)
    channels = jnp.sum(gch_s[...], axis=0, keepdims=True)
    lane8 = lax.broadcasted_iota(jnp.int32, (8, 128), 1)
    row8 = lax.broadcasted_iota(jnp.int32, (8, 128), 0)
    skip = jnp.zeros((1, 128), F32)
    lane1 = lax.broadcasted_iota(jnp.int32, (1, 128), 1)
    for h in range(HL):
        at = slice(128 * (h // 2), 128 * (h // 2) + 128)
        half_of = (lane1 < HW) if h % 2 == 0 else (lane1 >= HW)
        skip = jnp.where(lane1 == h, jnp.sum(jnp.where(half_of, channels[:, at], 0.0), axis=1, keepdims=True), skip)
    heads = [
        pltpu.roll(jnp.where(row8 == 7, jnp.broadcast_to(v, (8, 128)), 0.0), s * HL, 1)
        for v in (ghd_s[0:1, :], ghd_s[1:2, :], skip)
    ]
    row512 = lax.broadcasted_iota(jnp.int32, (8, 512), 0)
    hn = HEADS // nf
    for i in range(nf):
        conv = unplace(conv_s, i * (XBC // nf), XBC // nf)
        block = jnp.where(row512 < 5, conv, 0.0)
        block = block + jnp.where(row512 == 5, unplace(gpre_s, i * (D // nf), D // nf), 0.0)
        block = block + unplace(post_s, i * (INNER // nf), INNER // nf)
        tiles = []
        for v in heads:
            moved = pltpu.roll(v, (128 - i * hn) % 128, 1) if i else v
            tiles.append(jnp.where(lane8 < hn, moved, 0.0))
        block = block + jnp.concatenate(tiles + [jnp.zeros((8, 128), F32)], axis=1)
        snd_s[i] = block

    def small_send(k):
        to = lax.rem(f + k, nf)
        return rcopy(snd_s.at[to], got_s.at[k], bms.at[k], bmr.at[k], {"fsdp": to})

    for k in range(1, nf):
        small_send(k).start()
    ends(4, range(nl - 1))
    for t in range(2, nl - 1):
        slot(3, t)
    dn_pass(1)
    dn_pass(0)
    close(2)
    close(3)
    for t in range(1, nl - 1):
        slot(4, t)
    relay(1)

    for a in range(2):
        seq_one(0, a, 1).wait_recv()
        seq_two(0, a).wait_recv()
        for k in range(rows // 128):
            one = stat_s[pl.ds(s * (rows // 128) + k, 1), :]
            rho = lax.rsqrt(jnp.sum(jnp.where(eye, one, 0.0), axis=1, keepdims=True) * (1.0 / INNER) + EPS)
            part = slice(128 * k, 128 * k + 128)
            at = pl.ds(a * rows + 128 * k, 128)
            x = cot_s[pl.ds(pl.multiple_of(s * rows + 128 * k, 128), 128), cols[a]].astype(F32)
            dsh_s[at, :] = x + rho * add(dsh_s[at, :], ab0[a, 1, part], az0[a, 1, part])
        result(0, a).start()

    total = snd_s[f]
    for k in range(1, nf):
        small_send(k).wait_recv()
        total = total + got_s[k]
    sown_s[...] = total

    def small_share(k):
        return rcopy(sown_s, sgot_s.at[s], bes.at[k], ber.at[k], {"seq": s ^ k})

    for k in range(1, SEQ):
        small_share(k).start()
    close(4)
    relay(2)
    relay(3)

    for a in range(2):
        seq_one(1, a, 1).wait_recv()
        seq_two(1, a).wait_recv()
        dsh_s[rows_of(1, a), :] = add(chunk(s, a)[...], ab1[a, 1], az1[a, 1])

    def grad_tokens(i, carry):
        x = cot_s[pl.ds(pl.multiple_of(s * rows + i * 64, 64), 64), :].astype(F32)
        rho = lax.rsqrt(jnp.sum(x * x, axis=1, keepdims=True) * (1.0 / D) + EPS)
        at = [pl.ds(pl.multiple_of((2 + a) * rows + i * 64, 64), 64) for a in range(2)]
        n0 = [x[:, cols[a]] * rho for a in range(2)]
        e0 = [dsh_s[at[a], :] * pre_s[5:6, cols[a]] for a in range(2)]
        dot = sum(jnp.sum(e0[a] * n0[a], axis=1, keepdims=True) for a in range(2))
        mean = dot * (1.0 / D)
        cot = cotrow_s[pl.ds(pl.multiple_of(i * 64, 64), 64), :].astype(F32)
        for a in range(2):
            dsh_s[at[a], :] = cot[:, cols[a]] + rho * (e0[a] - n0[a] * mean)
        return carry

    lax.fori_loop(0, rows // 64, grad_tokens, 0)
    for a in range(2):
        result(1, a).start()
    relay(4)

    for k in range(1, SEQ):
        small_share(k).wait()
    total = jnp.zeros_like(sown_s)
    for k in range(SEQ):
        total = total + jnp.where(s == k, sown_s[...], sgot_s[k])
    small_ref[...] = total
    for t in range(2):
        for a in range(2):
            result(t, a).wait()
    for k in range(1, nf):
        small_send(k).wait_send()
    seq_one_sent(1)
    for t in range(2):
        for a in range(2):
            seq_two(t, a).wait_send()
    for g in range(5):
        seq_gather_finish(g, owns[g], gouts[g], as_, ar, px, py, s)
        pltpu.make_async_copy(owns[g], gouts[g].at[pl.ds(s * n, n)], os_.at[g]).wait()
        line_sent(g)
    for g in range(1, 5):
        swaps_sent(g)


def mixer(nf, tok, cot, win, wout, small):
    shape = jax.ShapeDtypeStruct
    vm = pltpu.VMEM
    dma = pltpu.SemaphoreType.DMA
    rows = tok.shape[0]
    length = SEQ * rows
    nl = nf // 2
    n = D // nf
    widths = (W, W, W, VC - W)
    groups = (W, W, W // 2, W // 2, VC - W)
    boxes = [vm((nl, n, w), BF16) for w in groups] + [vm((nl + 1, n, w), BF16) for w in groups]
    boxes += [vm((n, w), BF16) for w in groups]
    return pl.pallas_call(
        functools.partial(mixer_kernel, nf),
        out_shape=[shape((rows, D), F32)] * 2
        + [shape((SEQ * n, w), BF16) for w in widths]
        + [shape((8, 512), F32), shape((length, D), BF16)],
        in_specs=[ANY] * 4 + [VMEM],
        out_specs=[ANY] * 6 + [VMEM, ANY],
        scratch_shapes=[
            vm((length, D), BF16),
            vm((length, D), BF16),
            vm((D, W), BF16),
            vm((nf, SEQ, n // SEQ, REST), BF16),
            vm((D, W), BF16),
            vm((D, W), BF16),
            vm((length, VC), BF16),
            vm((length, W), BF16),
            vm((length, W), BF16),
            vm((length // Q, STATE, W), BF16),
            vm((length, W), F32),
            vm((length, W), BF16),
            vm((length, VC), BF16),
            vm((rows, D), BF16),
            vm((length, D), BF16),
            vm((D, W), BF16),
            vm((D, VC - W), BF16),
        ]
        + boxes
        + [vm((2, 2, rows, D // 2), BF16)] * 4
        + [
            vm((8, CH), F32),
            vm((8, 128), F32),
            vm((8, W), F32),
            vm((8, D), F32),
            vm((2 * length // 128, 128), F32),
            vm((2 * length // 128, 128), F32),
            vm((SEQ, 2 * length // 128, 128), F32),
            vm((5, 8, CH), F32),
            vm((8, W), F32),
            vm((8, 128), F32),
            vm((8, W), F32),
            vm((8, D), F32),
            vm((8, XBC), F32),
            vm((8, INNER), F32),
            vm((nf, 8, 512), F32),
            vm((nf, 8, 512), F32),
            vm((8, 512), F32),
            vm((SEQ, 8, 512), F32),
            vm((Q + 8, CH), F32),
            vm((Q + 8, CH), F32),
            vm((STATE, W), F32),
            vm((128, Q), F32),
            vm((Q, W), BF16),
            vm((Q, W), BF16),
            vm((8, W), F32),
            dma((9,)),
            dma((3, 4)),
            dma((3, 4)),
            dma((GROUPS, 4, nl)),
            dma((GROUPS, nf)),
            dma((nf,)),
            dma((nf,)),
            dma((SEQ,)),
            dma((SEQ,)),
            dma((5, 3, nl)),
            dma((5, 3, nl)),
            dma((2, 2, 3)),
            dma((2, 2, 3)),
            dma((5, 4)),
            dma((5, 4)),
            dma((nf,)),
            dma((nf,)),
            dma((SEQ,)),
            dma((SEQ,)),
            dma((5,)),
        ],
        name="mixer",
        compiler_params=pltpu.CompilerParams(
            collective_id=1, has_side_effects=True, vmem_limit_bytes=67043328
        ),
    )(tok, cot, win, wout, small)


def finish_kernel(
    go, gg, gv, gs, out, gt, small, out_o, gt_o, gin_o, gout_o, cw_o, cb_o, pre_o, post_o, step_o, decay_o, skip_o
):
    out_o[...] = out[...]
    gt_o[...] = gt[...]
    for i in range(SEQ):
        gin_o[:, i * W : i * W + W] = gg[i].astype(F32)
        gin_o[:, INNER + i * W : INNER + i * W + W] = gv[i].astype(F32)
    total = gs[0].astype(F32)
    for i in range(1, SEQ):
        total = total + gs[i].astype(F32)
    rest = gin_o.shape[1] - 2 * INNER
    gin_o[:, 2 * INNER :] = total[:, :rest]
    gout_o[...] = go[0].astype(F32)

    @pl.when(pl.program_id(0) == 0)
    def _():
        cw_o[...] = small[0:4, : cw_o.shape[1]]
        cb_o[...] = small[4:5, : cb_o.shape[1]]
        pre_o[...] = small[5:6, : pre_o.shape[1]]
        for k in range(post_o.shape[0]):
            post_o[k : k + 1, :] = small[6:7, 128 * k : 128 * k + post_o.shape[1]]
        heads = step_o.shape[1]
        step_o[...] = small[7:8, :heads]
        decay_o[...] = small[7:8, 128 : 128 + heads]
        skip_o[...] = small[7:8, 256 : 256 + heads]


def finish(nf, go, gg, gv, gs, out, gt, small):
    shape = jax.ShapeDtypeStruct
    n = D // nf
    step, rows = n // SEQ, out.shape[0] // SEQ
    proj = 2 * INNER + 2 * STATE + HEADS
    go, gg, gv, gs = (g.reshape(SEQ, n, g.shape[1]) for g in (go, gg, gv, gs))

    def whole(*dims):
        return pl.BlockSpec(dims, lambda i: (0,) * len(dims))

    np_ = INNER // nf
    post = (np_ // 128, 128) if np_ % 128 == 0 else (1, np_)
    tiny = [(4, XBC // nf), (1, XBC // nf), (1, n), post] + [(1, HEADS // nf)] * 3
    return pl.pallas_call(
        finish_kernel,
        grid=(SEQ,),
        out_shape=[shape(out.shape, F32)] * 2
        + [shape((n, proj), F32), shape((n, INNER), F32)]
        + [shape(dims, F32) for dims in tiny],
        in_specs=[
            pl.BlockSpec((1, n, W), lambda i: (i, 0, 0)),
            pl.BlockSpec((SEQ, step, W), lambda i: (0, i, 0)),
            pl.BlockSpec((SEQ, step, W), lambda i: (0, i, 0)),
            pl.BlockSpec((SEQ, step, VC - W), lambda i: (0, i, 0)),
            pl.BlockSpec((rows, D), lambda i: (i, 0)),
            pl.BlockSpec((rows, D), lambda i: (i, 0)),
            whole(8, 512),
        ],
        out_specs=[
            pl.BlockSpec((rows, D), lambda i: (i, 0)),
            pl.BlockSpec((rows, D), lambda i: (i, 0)),
            pl.BlockSpec((step, proj), lambda i: (i, 0)),
            pl.BlockSpec((n, W), lambda i: (0, i)),
        ]
        + [whole(*dims) for dims in tiny],
        name="finish",
        compiler_params=pltpu.CompilerParams(vmem_limit_bytes=VMEM_LIMIT),
    )(go, gg, gv, gs, out, gt, small)


def body(
    tokens,
    input_projection_weight,
    pre_gain,
    conv_weight,
    conv_bias,
    step_bias,
    decay_log,
    skip_gain,
    post_gain,
    output_projection_weight,
    cotangent,
):
    nf = lax.axis_size("fsdp")
    tok = tokens.reshape(tokens.shape[1:])
    cot = cotangent.reshape(cotangent.shape[1:])
    win = input_projection_weight

    w_out = output_projection_weight.T

    flat, at = jnp.zeros((2048,), F32), 0
    for v, size in (
        (conv_bias, 512), (pre_gain, 512), (post_gain, 512), (step_bias, 128), (decay_log, 128), (skip_gain, 256),
    ):
        flat = flat + jnp.pad(v.astype(F32), (at, 2048 - at - v.shape[0]))
        at += size
    taps = jnp.pad(conv_weight.T.astype(F32), ((0, 4), (0, 512 - conv_weight.shape[0])))
    small = taps + jnp.pad(flat.reshape(4, 512), ((4, 0), (0, 0)))
    out, gt, g_out, g_gate, g_val, g_state, small, _ = mixer(nf, tok, cot, win, w_out, small)
    block_out, grad_tokens, grad_in, grad_out, cw, cb, pre, post, step, decay, skip = finish(
        nf, g_out, g_gate, g_val, g_state, out, gt, small
    )
    return (
        block_out[None],
        grad_tokens[None],
        grad_in,
        pre.reshape(-1),
        cw.T,
        cb.reshape(-1),
        step.reshape(-1),
        decay.reshape(-1),
        skip.reshape(-1),
        post.reshape(-1),
        grad_out.T,
    )


def solution(mesh):
    in_specs = (
        P("fsdp", "seq", None),
        P("fsdp", None),
        P("fsdp"),
        P("fsdp", None),
        P("fsdp"),
        P("fsdp"),
        P("fsdp"),
        P("fsdp"),
        P("fsdp"),
        P(None, "fsdp"),
        P("fsdp", "seq", None),
    )
    out_specs = (
        P("fsdp", "seq", None),
        P("fsdp", "seq", None),
        P("fsdp", None),
        P("fsdp"),
        P("fsdp", None),
        P("fsdp"),
        P("fsdp"),
        P("fsdp"),
        P("fsdp"),
        P("fsdp"),
        P(None, "fsdp"),
    )
    return jax.shard_map(body, mesh=mesh, in_specs=in_specs, out_specs=out_specs, check_vma=False)
```

```python
import functools

import jax
import jax.numpy as jnp
from jax import lax
from jax.experimental import pallas as pl
from jax.experimental.pallas import tpu as pltpu
from jax.sharding import PartitionSpec as P

D = 1536
INNER = 3072
STATE = 128
HEADS = 48
XBC = INNER + 2 * STATE
EPS = 1e-05

SEQ = 4
W = INNER // SEQ
HL = HEADS // SEQ
HW = INNER // HEADS
CH = W + 2 * STATE
VC = CH + 128
REST = 2 * STATE + HEADS
Q = 128

F32 = jnp.float32
BF16 = jnp.bfloat16
MESH = pl.DeviceIdType.MESH
HIGH = lax.Precision.HIGHEST
VMEM = pl.BlockSpec(memory_space=pltpu.VMEM)
ANY = pl.BlockSpec(memory_space=pl.ANY)
VMEM_LIMIT = 64000 * 1024


def rcopy(src, dst, send_sem, recv_sem, device):
    return pltpu.make_async_remote_copy(
        src_ref=src, dst_ref=dst, send_sem=send_sem, recv_sem=recv_sem, device_id=device, device_id_type=MESH
    )


def signal(sem, device):
    pl.semaphore_signal(sem, inc=1, device_id=device, device_id_type=MESH)


def nn(a, b, precision=None):
    return lax.dot_general(a, b, (((1,), (0,)), ((), ())), precision=precision, preferred_element_type=F32)


def nt(a, b, precision=None):
    return lax.dot_general(a, b, (((1,), (1,)), ((), ())), precision=precision, preferred_element_type=F32)


def seq_gather_start(refs, outs, send, recv, px, py, me):
    for g, (src, out) in enumerate(zip(refs, outs)):
        n = src.shape[0]
        own = out.at[pl.ds(me * n, n)]
        rcopy(src, own, send.at[g, 0], recv.at[g, 0], {"seq": px}).start()
        rcopy(src, own, send.at[g, 1], recv.at[g, 1], {"seq": py}).start()


def seq_gather_relay(g, src, out, send, recv, px, py, me):
    n = src.shape[0]
    h = n // 2
    own = out.at[pl.ds(me * n, n)]
    rcopy(src, own, send.at[g, 0], recv.at[g, 0], {"seq": px}).wait_recv()
    top = out.at[pl.ds(px * n, h)]
    rcopy(top, top, send.at[g, 2], recv.at[g, 2], {"seq": py}).start()
    rcopy(src, own, send.at[g, 1], recv.at[g, 1], {"seq": py}).wait_recv()
    low = out.at[pl.ds(py * n + h, h)]
    rcopy(low, low, send.at[g, 3], recv.at[g, 3], {"seq": px}).start()


def seq_gather_finish(g, src, out, send, recv, px, py, me):
    n = src.shape[0]
    h = n // 2
    own = out.at[pl.ds(me * n, n)]
    half = out.at[pl.ds(me * n, h)]
    rcopy(half, half, send.at[g, 2], recv.at[g, 2], {"seq": py}).wait()
    rcopy(half, half, send.at[g, 3], recv.at[g, 3], {"seq": px}).wait()
    rcopy(src, own, send.at[g, 0], recv.at[g, 0], {"seq": px}).wait_send()
    rcopy(src, own, send.at[g, 1], recv.at[g, 1], {"seq": py}).wait_send()


def softplus(x):
    return jnp.maximum(x, 0.0) + jnp.log1p(jnp.exp(-jnp.abs(x)))


def sigmoid(x):
    return 0.5 + 0.5 * jnp.tanh(0.5 * x)


def rates_of(r_ref, rows, hp_ref, tri):
    back = lax.rem(128 - lax.axis_index("seq") * HL, 128)
    raw = pltpu.roll(r_ref[rows, :].astype(F32), back, 1) + hp_ref[0:1, :]
    dt = softplus(raw)
    lam = nn(tri, dt * hp_ref[1:2, :], HIGH)
    return raw, dt, lam


def fold(x):
    return jnp.sum(x.reshape(x.shape[0] // 8, 8, x.shape[1]), axis=0)


def spread(mat, h):
    return jnp.broadcast_to(mat[:, h : h + 1], (mat.shape[0], 128))


def scan_fwd_blocks(
    v_ref, s_ref, r_ref, kw_ref, hp_ref, ex_ref, mixed_ref, st_ref, buf, hst, xw_s, er_s, between
):
    blocks = v_ref.shape[0] // Q
    row = lax.broadcasted_iota(jnp.int32, (Q, Q), 0)
    col = lax.broadcasted_iota(jnp.int32, (Q, Q), 1)
    causal = row >= col
    tri = causal.astype(F32)
    low = lax.broadcasted_iota(jnp.int32, (Q, 128), 1) < HW
    low1 = lax.broadcasted_iota(jnp.int32, (1, 128), 1) < HW
    buf[0:8, :] = jnp.zeros((8, CH), F32)
    hst[...] = jnp.zeros_like(hst)

    def block(b, carry):
        rows = pl.ds(pl.multiple_of(b * Q, Q), Q)
        buf[8 : 8 + Q, 0:W] = v_ref[rows, :].astype(F32)
        buf[8 : 8 + Q, W:CH] = s_ref[rows, :].astype(F32)
        k = kw_ref[4:5, :] + buf[5 : 5 + Q, :] * kw_ref[0:1, :]
        for j in range(1, 4):
            k = k + buf[5 + j : 5 + j + Q, :] * kw_ref[j : j + 1, :]
        buf[0:8, :] = buf[Q : Q + 8, :]
        x = k * sigmoid(k)
        bs, cs = x[:, W : W + STATE], x[:, W + STATE :]
        _, dt, lam = rates_of(r_ref, rows, hp_ref, tri)
        lam_t, dt_t = lam.T, dt.T
        last = lam[Q - 1 : Q, :]
        tail = dt * jnp.exp(last - lam)
        aff = nt(cs, bs, HIGH)
        st_ref[b] = hst[...].astype(BF16)
        ch = nn(cs.astype(BF16), st_ref[b])
        for i in range(HL // 2):
            at = slice(128 * i, 128 * i + 128)
            xp = x[:, at]
            xb = xp.astype(BF16)
            y, lc = [], []
            for h in (2 * i, 2 * i + 1):
                lcol = spread(lam, h)
                within = jnp.exp(jnp.where(causal, lcol - lam_t[h : h + 1, :], -1e30))
                y.append(nn((aff * within * dt_t[h : h + 1, :]).astype(BF16), xb))
                lc.append(lcol)
            out = jnp.where(low, y[0], y[1])
            out = out + jnp.exp(jnp.where(low, lc[0], lc[1])) * ch[:, at] + ex_ref[0:1, at] * xp
            mixed_ref[rows, at] = out.astype(BF16)
            xw_s[:, at] = (xp * jnp.where(low, spread(tail, 2 * i), spread(tail, 2 * i + 1))).astype(BF16)
            er_s[0:1, at] = jnp.exp(jnp.where(low1, spread(last, 2 * i), spread(last, 2 * i + 1)))
        hst[...] = hst[...] * er_s[0:1, :] + nn(bs.T.astype(BF16), xw_s[...])
        between(b)
        return carry

    lax.fori_loop(0, blocks, block, 0)


def scan_bwd_blocks(
    v_ref, s_ref, r_ref, dy_ref, st_ref, kw_ref, hp_ref, ex_ref,
    dv_ref, gcw_ref, gch_ref, ghd_ref,
    buf, cbuf, dhst, rowp, xw_s, e_s, er_s, between,
):
    blocks = v_ref.shape[0] // Q
    row = lax.broadcasted_iota(jnp.int32, (Q, Q), 0)
    col = lax.broadcasted_iota(jnp.int32, (Q, Q), 1)
    tri = (row >= col).astype(F32)
    later = col >= row
    suffix = later.astype(F32)
    strict = (col < row).astype(F32)
    lane = lax.broadcasted_iota(jnp.int32, (Q, 128), 1)
    lane1 = lax.broadcasted_iota(jnp.int32, (1, 128), 1)
    low = lane < HW
    low1 = lane1 < HW
    buf[Q : Q + 8, :] = jnp.zeros((8, CH), F32)
    dhst[...] = jnp.zeros_like(dhst)
    rowp[...] = jnp.zeros_like(rowp)
    gcw_ref[...] = jnp.zeros_like(gcw_ref)
    gch_ref[...] = jnp.zeros_like(gch_ref)
    ghd_ref[...] = jnp.zeros_like(ghd_ref)

    def block(i0, carry):
        b = blocks - 1 - i0
        rows = pl.ds(pl.multiple_of(b * Q, Q), Q)
        before = pl.ds(pl.multiple_of(jnp.maximum(b * Q - 16, 0), 16), 16)
        keep = (b > 0).astype(F32)
        cbuf[0:8, 0:W] = v_ref[before, :].astype(F32)[8:16, :] * keep
        cbuf[0:8, W:CH] = s_ref[before, :].astype(F32)[8:16, :] * keep
        cbuf[8 : 8 + Q, 0:W] = v_ref[rows, :].astype(F32)
        cbuf[8 : 8 + Q, W:CH] = s_ref[rows, :].astype(F32)
        k = kw_ref[4:5, :] + cbuf[5 : 5 + Q, :] * kw_ref[0:1, :]
        for j in range(1, 4):
            k = k + cbuf[5 + j : 5 + j + Q, :] * kw_ref[j : j + 1, :]
        sg = sigmoid(k)
        x = k * sg
        ds = sg * (1.0 + k * (1.0 - sg))
        bs, cs = x[:, W : W + STATE], x[:, W + STATE :]
        bb, cb = bs.astype(BF16), cs.astype(BF16)
        raw, dt, lam = rates_of(r_ref, rows, hp_ref, tri)
        lam_t = lam.T
        last = lam[Q - 1 : Q, :]
        aff_t = nt(bs, cs, HIGH)
        hb = st_ref[b]
        dhb = dhst[...].astype(BF16)
        ch = nn(cb, hb)
        bd = nn(bb, dhb)
        daff_t = jnp.zeros((Q, Q), F32)
        col_n = jnp.zeros((Q, 128), F32)
        col_i = jnp.zeros((Q, 128), F32)
        row_i = jnp.zeros((Q, 128), F32)
        through = jnp.zeros((1, 128), F32)
        for i in range(HL // 2):
            at = slice(128 * i, 128 * i + 128)
            xp = x[:, at]
            xb = xp.astype(BF16)
            dyb = dy_ref[rows, at]
            dyf = dyb.astype(F32)
            z, lc, dc = [], [], []
            for h in (2 * i, 2 * i + 1):
                mine = low if h % 2 == 0 else jnp.logical_not(low)
                lcol, dcol = spread(lam, h), spread(dt, h)
                within = jnp.exp(jnp.where(later, lam_t[h : h + 1, :] - lcol, -1e30))
                g = nt(jnp.where(mine, xp, 0.0).astype(BF16), dyb)
                lg = within * g
                lgd = lg * dcol
                daff_t = daff_t + lgd
                pair = (aff_t * lg).astype(BF16)
                col_n = col_n + nn(pair, jnp.where(lane == h, 1.0, 0.0).astype(BF16))
                rowp[h : h + 1, :] = jnp.sum(pair.astype(F32) * dcol, axis=0, keepdims=True)
                z.append(nn((aff_t * within).astype(BF16), dyb))
                lc.append(lcol)
                dc.append(dcol)
            lamp = jnp.where(low, lc[0], lc[1])
            dtp = jnp.where(low, dc[0], dc[1])
            lastp = jnp.where(low1, spread(last, 2 * i), spread(last, 2 * i + 1))
            e = dyf * jnp.exp(lamp)
            e_s[:, at] = e.astype(BF16)
            ew = jnp.exp(lastp - lamp)
            bdp = bd[:, at]
            xw_s[:, at] = (xp * (dtp * ew)).astype(BF16)
            er_s[0:1, at] = jnp.exp(lastp)
            re = e * ch[:, at]
            ci = xp * bdp * ew
            th = jnp.sum(dhst[:, at] * hb[:, at].astype(F32), axis=0, keepdims=True) * er_s[0:1, at]
            heads = jnp.where(lane == 2 * i + jnp.where(row < HW, 0, 1), 1.0, 0.0).astype(BF16)
            row_i = row_i + nn(re.astype(BF16), heads)
            col_i = col_i + nn(ci.astype(BF16), heads)
            for h in (2 * i, 2 * i + 1):
                mine1 = low1 if h % 2 == 0 else jnp.logical_not(low1)
                through = jnp.where(
                    lane1 == h, jnp.sum(jnp.where(mine1, th, 0.0), axis=1, keepdims=True), through
                )
            dx = dtp * jnp.where(low, z[0], z[1]) + bdp * (dtp * ew) + ex_ref[0:1, at] * dyf
            gch_ref[:, at] += fold(dyf * xp)
            buf[0:Q, at] = dx * ds[:, at]
        daff_b = daff_t.astype(BF16)
        d_bs = nt(xw_s[...], dhb) + nn(daff_b, cb)
        d_cs = nt(e_s[...], hb) + nn(daff_t.T.astype(BF16), bb)
        buf[0:Q, W : W + STATE] = d_bs * ds[:, W : W + STATE]
        buf[0:Q, W + STATE : CH] = d_cs * ds[:, W + STATE :]
        dhst[...] = dhst[...] * er_s[0:1, :] + nn(cs.T.astype(BF16), e_s[...])
        after = nn(suffix, rowp[...].T - dt * col_n + row_i, HIGH) + nn(strict, dt * col_i, HIGH) + through
        d_rate = (col_n + col_i + hp_ref[1:2, :] * after) * sigmoid(raw)
        ghd_ref[0:1, :] += jnp.sum(d_rate, axis=0, keepdims=True)
        ghd_ref[1:2, :] += jnp.sum(dt * after, axis=0, keepdims=True) * hp_ref[1:2, :]
        dv_ref[rows, CH:VC] = pltpu.roll(d_rate, lax.axis_index("seq") * HL, 1).astype(BF16)
        for at in (slice(0, W), slice(W, CH)):
            raw_v = cbuf[8 : 8 + Q, at]
            dk = buf[0:Q, at]
            dv = dk * kw_ref[3:4, at]
            gcw_ref[4, :, at] += fold(dk)
            gcw_ref[3, :, at] += fold(dk * raw_v)
            for j in range(3):
                dk = buf[3 - j : 3 - j + Q, at]
                dv = dv + dk * kw_ref[j : j + 1, at]
                gcw_ref[j, :, at] += fold(dk * raw_v)
            dv_ref[rows, at] = dv.astype(BF16)
        buf[Q : Q + 8, :] = buf[0:8, :]
        between(i0)
        return carry

    lax.fori_loop(0, blocks, block, 0)


GROUPS = 4


def place(block, at, width):
    start, shift = at // 128 * 128, at % 128
    lanes = -(-(width + shift) // 128) * 128
    have = block.shape[1]
    if lanes > have:
        block = jnp.concatenate([block, jnp.zeros((block.shape[0], lanes - have), block.dtype)], axis=1)
    else:
        block = block[:, :lanes]
    if shift:
        block = pltpu.roll(block, shift, 1)
    return start, lanes, block


TN = (((0,), (0,)), ((), ()))
STRIP = 384


def unplace(block, at, width):
    start, shift = at // 128 * 128, at % 128
    lanes = -(-(width + shift) // 128) * 128
    piece = block[:, start : start + lanes]
    if shift:
        piece = pltpu.roll(piece, lanes - shift, 1)
    if lanes < 512:
        piece = jnp.concatenate([piece, jnp.zeros((piece.shape[0], 512 - lanes), piece.dtype)], axis=1)
    else:
        piece = piece[:, :512]
    return jnp.where(lax.broadcasted_iota(jnp.int32, piece.shape, 1) < width, piece, 0.0)


def mixer_kernel(
    nf, tok, cot, win, wout, small,
    out_ref, gt_ref, go_ref, gg_ref, gv_ref, gs_ref, small_ref, x_hbm,
    cot_s, nrm_s, wv_s, ws_s, wg_s, wo_s, mix_s, gate_s, mixed_s, st_s, dsh_s,
    dy_s, dv_s, cotrow_s, part_s, gb_s, gc_s,
    pb0, pb1, pb2, pb3, pb4, lb0, lb1, lb2, lb3, lb4, own0, own1, own2, own3, own4,
    ab0, ab1, az0, az1,
    kw_s, hp_s, ex_s, pre_s, stat_s, stat_own, stat_got,
    gcw_s, gch_s, ghd_s, gpost_s, gpre_s, conv_s, post_s, snd_s, got_s, sown_s, sgot_s,
    buf, cbuf, dhst, rowp, xw_s, e_s, er_s,
    ls, xs, xr, zs, zr, ms, mr, es, er, bzs, bzr, bxs, bxr, as_, ar, bms, bmr, bes, ber, os_,
):
    x_s, small_s, ga_s = part_s, snd_s, wo_s
    s = lax.axis_index("seq")
    f = lax.axis_index("fsdp")
    px, py = s ^ 1, s ^ 2
    nl = nf // 2
    p, c = f // 2, f % 2
    partner = p * 2 + 1 - c
    bar = pltpu.get_barrier_semaphore()
    for k in range(1, SEQ):
        signal(bar, {"seq": s ^ k})
    for k in range(1, nf):
        signal(bar, {"fsdp": lax.rem(f + k, nf)})
    pl.semaphore_wait(bar, nf - 1 + SEQ - 1)

    n = win.shape[0]
    rows = tok.shape[0]
    length = rows * SEQ
    quarter = n // SEQ
    ins = (
        win.at[:, pl.ds(pl.multiple_of(INNER + s * W, 128), W)],
        win.at[pl.ds(pl.multiple_of(s * quarter, 8), quarter), pl.ds(2 * INNER, REST)],
        win.at[:, pl.ds(pl.multiple_of(s * W, 128), W)],
        wout.at[:, pl.ds(pl.multiple_of(s * W, 128), W)],
    )
    outs = (wv_s, ws_s, wg_s, wo_s)

    def row(g, i):
        return ws_s.at[i, s] if g == 1 else outs[g].at[pl.ds(i * n, n)]

    def hop(g, src, i, way, k, device):
        return rcopy(src, row(g, i), zs.at[g, way, k], zr.at[g, i], {"fsdp": device})

    def own_send(g):
        @pl.when(p < nl - 1)
        def _():
            hop(g, ins[g], f, 0, 0, f + 2).start()

        @pl.when(p > 0)
        def _():
            hop(g, ins[g], f, 1, 0, f - 2).start()

        hop(g, ins[g], f, 2, 0, partner).start()
        pltpu.make_async_copy(ins[g], row(g, f), ls.at[g]).start()

    def step(g, k):
        @pl.when(p - k >= 0)
        def _():
            o = f - 2 * k
            hop(g, row(g, o), o, 0, k, f).wait_recv()

            @pl.when(p < nl - 1)
            def _():
                hop(g, row(g, o), o, 0, k, f + 2).start()

            hop(g, row(g, o), o, 2, k, partner).start()

        @pl.when(p + k < nl)
        def _():
            o = f + 2 * k
            hop(g, row(g, o), o, 1, k, f).wait_recv()

            @pl.when(p > 0)
            def _():
                hop(g, row(g, o), o, 1, k, f - 2).start()

            hop(g, row(g, o), o, 3, k, partner).start()

    def arrive(g):
        pltpu.make_async_copy(ins[g], row(g, f), ls.at[g]).wait()
        for q in range(nl):
            o = q * 2 + 1 - c
            hop(g, row(g, o), o, 2, 0, partner).wait_recv()

    def sent(g):
        hop(g, ins[g], f, 2, 0, partner).wait_send()

        @pl.when(p < nl - 1)
        def _():
            hop(g, ins[g], f, 0, 0, f + 2).wait_send()

        @pl.when(p > 0)
        def _():
            hop(g, ins[g], f, 1, 0, f - 2).wait_send()

        for k in range(1, nl):
            @pl.when(p - k >= 0)
            def _():
                o = f - 2 * k

                @pl.when(p < nl - 1)
                def _():
                    hop(g, row(g, o), o, 0, k, f + 2).wait_send()

                hop(g, row(g, o), o, 2, k, partner).wait_send()

            @pl.when(p + k < nl)
            def _():
                o = f + 2 * k

                @pl.when(p > 0)
                def _():
                    hop(g, row(g, o), o, 1, k, f - 2).wait_send()

                hop(g, row(g, o), o, 3, k, partner).wait_send()

    def small_copy(k):
        return rcopy(small, small_s.at[f], ms.at[k], mr.at[k], {"fsdp": lax.rem(f + k, nf)})

    mine = pl.ds(s * rows, rows)
    own_small = pltpu.make_async_copy(small, small_s.at[f], ls.at[4])
    own_tok = pltpu.make_async_copy(tok, x_s.at[mine], ls.at[5])
    own_cot = pltpu.make_async_copy(cot, cot_s.at[mine], ls.at[6])
    own_row = pltpu.make_async_copy(cot, cotrow_s, ls.at[7])

    def st_hop(k, region, device):
        return rcopy(region, region, xs.at[2, k], xr.at[2, k], {"seq": device})

    st_own = ws_s.at[:, s]
    st_top, st_low = ws_s.at[pl.ds(0, nl), px], ws_s.at[pl.ds(nl, nl), py]

    for k in range(1, nf):
        small_copy(k).start()
    own_small.start()
    own_tok.start()
    seq_gather_start((tok,), (x_s,), xs, xr, px, py, s)
    own_send(1)
    own_send(0)
    own_cot.start()
    own_row.start()
    for k in range(1, min(3, nl)):
        step(1, k)
    step(0, 1)
    for k in range(3, nl):
        step(1, k)
    arrive(1)
    st_hop(0, st_own, px).start()
    st_hop(1, st_own, py).start()
    seq_gather_relay(0, tok, x_s, xs, xr, px, py, s)
    for k in range(2, min(3, nl)):
        step(0, k)
    own_send(2)
    own_send(3)

    mix_s[:, CH:VC] = jnp.zeros((length, VC - CH), BF16)

    own_small.wait()
    for k in range(1, nf):
        small_copy(k).wait()
    conv_s[...] = jnp.zeros_like(conv_s)
    pre_s[...] = jnp.zeros_like(pre_s)
    post_s[...] = jnp.zeros_like(post_s)
    heads = [jnp.zeros((8, 128), F32) for _ in range(3)]
    for i in range(nf):
        block = small_s[i]
        at, lanes, moved = place(block, i * (XBC // nf), XBC // nf)
        conv_s[:, at : at + lanes] += moved
        at, lanes, moved = place(block, i * (D // nf), D // nf)
        pre_s[:, at : at + lanes] += jnp.where(lax.broadcasted_iota(jnp.int32, moved.shape, 0) == 5, moved, 0.0)
        at, lanes, moved = place(block, i * (INNER // nf), INNER // nf)
        post_s[:, at : at + lanes] += jnp.where(lax.broadcasted_iota(jnp.int32, moved.shape, 0) == 6, moved, 0.0)
        for j in range(3):
            piece = block[:, 128 * j : 128 * j + 128]
            at = i * (HEADS // nf)
            heads[j] = heads[j] + (pltpu.roll(piece, at, 1) if at else piece)
    kw_s[:, 0:W] = conv_s[:, pl.ds(pl.multiple_of(s * W, 128), W)]
    kw_s[:, W:CH] = conv_s[:, INNER:XBC]
    lane1 = lax.broadcasted_iota(jnp.int32, (1, 128), 1)
    low1 = lane1 < HW
    back = lax.rem(128 - s * HL, 128)
    step_b, decay, skip = [pltpu.roll(h, back, 1)[7:8, :] for h in heads]
    hp_s[...] = jnp.zeros_like(hp_s)
    hp_s[0:1, :] = jnp.where(lane1 < HL, step_b, 0.0)
    hp_s[1:2, :] = jnp.where(lane1 < HL, -jnp.exp(decay), 0.0)
    ex_s[...] = jnp.zeros_like(ex_s)
    for i in range(HL // 2):
        ex_s[0:1, 128 * i : 128 * i + 128] = jnp.where(low1, spread(skip, 2 * i), spread(skip, 2 * i + 1))
    ex_s[1:2, :] = post_s[6:7, pl.ds(pl.multiple_of(s * W, 128), W)]

    st_hop(0, st_own, px).wait_recv()
    st_hop(2, st_top, py).start()
    st_hop(1, st_own, py).wait_recv()
    st_hop(3, st_low, px).start()
    own = cot_s.at[mine]
    rcopy(cot, own, xs.at[1, 0], xr.at[1, 0], {"seq": px}).start()
    rcopy(cot, own, xs.at[1, 1], xr.at[1, 1], {"seq": py}).start()
    for k in range(3, nl):
        step(0, k)
    own_tok.wait()
    seq_gather_finish(0, tok, x_s, xs, xr, px, py, s)

    def norm(i, carry):
        r = pl.ds(pl.multiple_of(i * 128, 128), 128)
        x = x_s[r, :].astype(F32)
        rho = lax.rsqrt(jnp.sum(x * x, axis=1, keepdims=True) * (1.0 / D) + EPS)
        nrm_s[r, :] = (x * rho * pre_s[5:6, :]).astype(BF16)
        return carry

    lax.fori_loop(0, length // 128, norm, 0)
    x_save = pltpu.make_async_copy(x_s, x_hbm, ls.at[8])
    x_save.start()
    arrive(0)

    def project(i, carry):
        r = pl.ds(pl.multiple_of(i * 256, 256), 256)
        mix_s[r, 0:W] = nn(nrm_s[r, :], wv_s[...]).astype(BF16)
        return carry

    def project_state(i, carry):
        r = pl.ds(pl.multiple_of(i * 256, 256), 256)
        mix_s[r, W : W + REST] = nn(nrm_s[r, :], ws_s[...].reshape(D, REST)).astype(BF16)
        return carry

    lax.fori_loop(0, length // 256, project, 0)
    step(2, 1)
    st_hop(2, st_top, py).wait()
    st_hop(3, st_low, px).wait()
    lax.fori_loop(0, length // 256, project_state, 0)

    def between(b):
        @pl.when(b == 1)
        def _():
            step(3, 1)

        @pl.when(b == 4)
        def _():
            step(2, 2)

    scan_fwd_blocks(
        mix_s.at[:, 0:W], mix_s.at[:, W:CH], mix_s.at[:, CH:VC], kw_s, hp_s, ex_s, mixed_s, st_s,
        buf, dhst, xw_s, er_s, between,
    )
    step(3, 2)
    seq_gather_relay(1, cot, cot_s, xs, xr, px, py, s)
    for k in range(3, nl):
        step(2, k)
    arrive(2)

    def project_gate(i, carry):
        r = pl.ds(pl.multiple_of(i * 256, 256), 256)
        gate_s[r, :] = nn(nrm_s[r, :], wg_s[...]).astype(BF16)
        return carry

    lax.fori_loop(0, length // 256, project_gate, 0)
    for k in range(3, nl):
        step(3, k)
    own_cot.wait()
    seq_gather_finish(1, cot, cot_s, xs, xr, px, py, s)
    arrive(3)
    eye = lax.broadcasted_iota(jnp.int32, (128, 128), 0) == lax.broadcasted_iota(jnp.int32, (128, 128), 1)

    def stats(i, carry):
        r = pl.ds(pl.multiple_of(i * 128, 128), 128)
        dsh = nn(cot_s[r, :], wo_s[...])
        dsh_s[r, :] = dsh
        gate = gate_s[r, :].astype(F32)
        gated = mixed_s[r, :].astype(F32) * (gate * sigmoid(gate))
        one = jnp.sum(gated * gated, axis=1, keepdims=True)
        gained = gated * ex_s[1:2, :]
        dy_s[r, :] = gained.astype(BF16)
        two = jnp.sum(dsh * gained, axis=1, keepdims=True)
        stat_own[pl.ds(i, 1), :] = jnp.sum(jnp.where(eye, one, 0.0), axis=0, keepdims=True)
        stat_own[pl.ds(length // 128 + i, 1), :] = jnp.sum(jnp.where(eye, two, 0.0), axis=0, keepdims=True)
        return carry

    lax.fori_loop(0, length // 128, stats, 0)
    copies = [rcopy(stat_own, stat_got.at[k], es.at[k], er.at[k], {"seq": s ^ k}) for k in range(1, SEQ)]
    for copy in copies:
        copy.start()

    half = D // 2
    cols = (slice(0, half), slice(half, D))
    first, second = (px, py), (py, px)
    ab, az = (ab0, ab1), (az0, az1)

    def chunk(i, a):
        return part_s.at[pl.ds(i * rows, rows), cols[a]]

    def seq_one(t, a, m):
        i = (first[a] ^ second[a] ^ s) if m == 0 else first[a]
        return rcopy(chunk(i, a), ab[t].at[a, m], bxs.at[t, a, m], bxr.at[t, a, m], {"seq": first[a]})

    def seq_two(t, a):
        return rcopy(az[t].at[a, 0], az[t].at[a, 1], bxs.at[t, a, 2], bxr.at[t, a, 2], {"seq": second[a]})

    def add(*terms):
        total = terms[0].astype(F32)
        for term in terms[1:]:
            total = total + term.astype(F32)
        return total

    def seq_pass(t):
        for a in range(2):
            seq_one(t, a, 0).wait_recv()
            az[t][a, 0] = add(chunk(second[a], a)[...], ab[t][a, 0]).astype(BF16)
            seq_two(t, a).start()

    def seq_last(t, out):
        for a in range(2):
            seq_one(t, a, 1).wait_recv()
            seq_two(t, a).wait_recv()
            out[:, cols[a]] = add(chunk(s, a)[...], ab[t][a, 1], az[t][a, 1])

    def seq_one_sent(t):
        for a in range(2):
            seq_one(t, a, 0).wait_send()
            seq_one(t, a, 1).wait_send()

    x_save.wait()

    def out_part(i, carry):
        r = pl.ds(pl.multiple_of((s ^ (SEQ - 1 - i)) * rows, rows), rows)
        part_s[r, :] = nt(dy_s[r, :], wo_s[...]).astype(BF16)

        @pl.when(i == 0)
        def _():
            for a in range(2):
                seq_one(0, a, 0).start()

        @pl.when(i == 2)
        def _():
            for a in range(2):
                seq_one(0, a, 1).start()

        return carry

    lax.fori_loop(0, SEQ, out_part, 0)

    for copy in copies:
        copy.wait()
    stat_s[...] = stat_own[...] + stat_got[1] + (stat_got[2] + stat_got[3])
    for g in range(GROUPS):
        sent(g)
    st_hop(0, st_own, px).wait_send()
    st_hop(1, st_own, py).wait_send()
    own_row.wait()

    low_half, high_half = slice(0, W // 2), slice(W // 2, W)
    parts = (ga_s, gb_s, ga_s.at[:, low_half], ga_s.at[:, high_half], gc_s)
    pbs, lbs, owns = (pb0, pb1, pb2, pb3, pb4), (lb0, lb1, lb2, lb3, lb4), (own0, own1, own2, own3, own4)
    gouts = (go_ref, gg_ref, gv_ref.at[:, low_half], gv_ref.at[:, high_half], gs_ref)

    def piece(g, i):
        return parts[g].at[pl.ds(pl.multiple_of(i * n, 16), n)]

    def swap(g, q):
        return rcopy(piece(g, q * 2 + 1 - c), pbs[g].at[q], bzs.at[g, 0, q], bzr.at[g, 0, q], {"fsdp": partner})

    def up(g, q):
        return rcopy(pbs[g].at[q], lbs[g].at[q], bzs.at[g, 1, q], bzr.at[g, 1, q], {"fsdp": f + 2})

    def down(g, q):
        to = jnp.where(q == p - 1, nl, q)
        return rcopy(pbs[g].at[q], lbs[g].at[to], bzs.at[g, 2, q], bzr.at[g, 2, q], {"fsdp": f - 2})

    def send_up(g, q, terms):
        pbs[g][q] = add(piece(g, q * 2 + c)[...], pbs[g][q], *terms).astype(BF16)
        up(g, q).start()

    def send_down(g, q, terms):
        pbs[g][q] = add(piece(g, q * 2 + c)[...], pbs[g][q], *terms).astype(BF16)
        down(g, q).start()

    def ends(g, shards):
        for k in shards:
            @pl.when(p == 0)
            def _():
                swap(g, nl - 1 - k).wait_recv()
                send_up(g, nl - 1 - k, ())

            @pl.when(p == nl - 1)
            def _():
                swap(g, k).wait_recv()
                send_down(g, k, ())

    def slot(g, t):
        @pl.when(jnp.logical_and(p > 0, p <= t))
        def _():
            q = nl - 1 - t + p
            swap(g, q).wait_recv()
            up(g, q).wait_recv()
            send_up(g, q, (lbs[g][q],))

        @pl.when(jnp.logical_and(p < nl - 1, nl - 1 - p <= t))
        def _():
            q = t - (nl - 1 - p)
            swap(g, q).wait_recv()
            down(g, q).wait_recv()
            send_down(g, q, (lbs[g][q],))

    def close(g):
        swap(g, p).wait_recv()

        @pl.when(p > 0)
        def _():
            up(g, p).wait_recv()

        @pl.when(p < nl - 1)
        def _():
            down(g, p).wait_recv()

        @pl.when(p == 0)
        def _():
            owns[g][...] = add(piece(g, f)[...], pbs[g][p], lbs[g][nl]).astype(BF16)

        @pl.when(p == nl - 1)
        def _():
            owns[g][...] = add(piece(g, f)[...], pbs[g][p], lbs[g][p]).astype(BF16)

        @pl.when(jnp.logical_and(p > 0, p < nl - 1))
        def _():
            owns[g][...] = add(piece(g, f)[...], pbs[g][p], lbs[g][p], lbs[g][nl]).astype(BF16)

        place_ = gouts[g].at[pl.ds(s * n, n)]
        rcopy(owns[g], place_, as_.at[g, 0], ar.at[g, 0], {"seq": px}).start()
        rcopy(owns[g], place_, as_.at[g, 1], ar.at[g, 1], {"seq": py}).start()
        pltpu.make_async_copy(owns[g], place_, os_.at[g]).start()

    def relay(g):
        seq_gather_relay(g, owns[g], gouts[g], as_, ar, px, py, s)

    def swaps_sent(g):
        for q in range(nl):
            swap(g, q).wait_send()

    def line_sent(g):
        for q in range(nl):
            @pl.when(q > p)
            def _():
                up(g, q).wait_send()

            @pl.when(q < p)
            def _():
                down(g, q).wait_send()

    order = []
    for k in range(D // STRIP // 2):
        order += [D // STRIP - 1 - k, k]

    def strip(j, a_ref, b_ref, bcols, to, groups):
        at = slice(j * STRIP, (j + 1) * STRIP)
        to[at, :] = lax.dot_general(a_ref[:, at], b_ref[:, bcols], TN, preferred_element_type=F32).astype(BF16)
        for q in range(nl):
            if j * STRIP <= q * 2 * n < (j + 1) * STRIP:
                for g in groups:
                    swap(g, q).start()

    gpost_s[...] = jnp.zeros_like(gpost_s)

    def gated_norm(i, carry):
        r = pl.ds(pl.multiple_of(i * 128, 128), 128)
        one = jnp.sum(jnp.where(eye, stat_s[pl.ds(i, 1), :], 0.0), axis=1, keepdims=True)
        two = jnp.sum(jnp.where(eye, stat_s[pl.ds(length // 128 + i, 1), :], 0.0), axis=1, keepdims=True)
        rho = lax.rsqrt(one * (1.0 / INNER) + EPS)
        mean = rho * two * (1.0 / INNER)
        gate = gate_s[r, :].astype(F32)
        mixed = mixed_s[r, :].astype(F32)
        dsh = dsh_s[r, :]
        post = ex_s[1:2, :]
        sg = sigmoid(gate)
        sl = gate * sg
        n1 = mixed * sl * rho
        gpost_s[...] += fold(dsh * n1)
        d_gated = rho * (dsh * post - n1 * mean)
        mixed_s[r, :] = (n1 * post).astype(BF16)
        dy_s[r, :] = (d_gated * sl).astype(BF16)
        gate_s[r, :] = (d_gated * mixed * (sg * (1.0 + gate * (1.0 - sg)))).astype(BF16)
        return carry

    lax.fori_loop(0, length // 128, gated_norm, 0)

    every = slice(0, W)
    for j in order[:2]:
        strip(j, cot_s, mixed_s, every, ga_s, (0,))
    ends(0, range(1))
    for j in order[2:]:
        strip(j, cot_s, mixed_s, every, ga_s, (0,))
    ends(0, range(1, nl - 1))
    x_load = pltpu.make_async_copy(x_hbm, cot_s, ls.at[8])
    x_load.start()

    def rows_of(t, a):
        return pl.ds((2 * t + a) * rows, rows)

    def result(t, a):
        out = (out_ref, gt_ref)[t].at[:, cols[a]]
        return pltpu.make_async_copy(dsh_s.at[rows_of(t, a)], out, ls.at[2 * t + a])

    for a in range(2):
        dsh_s[rows_of(0, a), :] = chunk(s, a)[...].astype(F32)

    for j in order:
        strip(j, nrm_s, gate_s, every, gb_s, (1,))
    ends(1, range(nl - 1))
    slot(0, 1)

    gpre_s[...] = jnp.zeros_like(gpre_s)

    def dn_chunk(j):
        r = pl.ds(pl.multiple_of(j * rows, rows), rows)
        dn = nt(gate_s[r, :], wg_s[...]) + nt(dv_s[r, 0:W], wv_s[...])
        dn = dn + nt(dv_s[r, W : W + REST], ws_s[...].reshape(D, REST))
        part_s[r, :] = dn.astype(BF16)
        x = cot_s[r, :].astype(F32)
        rho = lax.rsqrt(jnp.sum(x * x, axis=1, keepdims=True) * (1.0 / D) + EPS)
        gpre_s[...] += fold(dn * (x * rho))

        @pl.when((s ^ j) == 3)
        def _():
            seq_one(1, 0, 0).start()
            seq_one(1, 1, 0).start()

        @pl.when((s ^ j) == 1)
        def _():
            seq_one(1, 0, 1).start()

        @pl.when((s ^ j) == 2)
        def _():
            seq_one(1, 1, 1).start()

    def dn_pass(j):
        for a in range(2):
            @pl.when((s ^ j) == 2 - a)
            def _():
                seq_one(1, a, 0).wait_recv()
                az1[a, 0] = add(chunk(second[a], a)[...], ab1[a, 0]).astype(BF16)
                seq_two(1, a).start()

    def between(i):
        @pl.when(i == 1)
        def _():
            seq_pass(0)
            seq_one_sent(0)
            x_load.wait()

        @pl.when(jnp.logical_and(lax.rem(i, 2) == 1, i < 2 * SEQ - 1))
        def _():
            dn_chunk(SEQ - 1 - i // 2)

        @pl.when(i == 1)
        def _():
            for t in range(2, nl - 1):
                slot(0, t)

        @pl.when(i == 3)
        def _():
            close(0)

        @pl.when(i == 4)
        def _():
            slot(1, 1)

        @pl.when(i == 6)
        def _():
            for t in range(2, nl - 1):
                slot(1, t)
            dn_pass(3)

    scan_bwd_blocks(
        mix_s.at[:, 0:W], mix_s.at[:, W:CH], mix_s.at[:, CH:VC], dy_s, st_s, kw_s, hp_s, ex_s,
        dv_s, gcw_s, gch_s, ghd_s, buf, cbuf, dhst, rowp, xw_s, e_s, er_s, between,
    )

    swaps_sent(0)
    for j in order[:2]:
        strip(j, nrm_s, dv_s, every, ga_s, (2, 3))
    ends(2, range(1))
    ends(3, range(1))
    dn_chunk(0)
    close(1)
    for j in order[2:]:
        strip(j, nrm_s, dv_s, every, ga_s, (2, 3))
    for k in range(1, nl - 1):
        ends(2, (k,))
        ends(3, (k,))
    slot(2, 1)
    slot(3, 1)
    dn_pass(2)
    relay(0)
    for j in order:
        strip(j, nrm_s, dv_s, slice(W, VC), gc_s, (4,))
    for t in range(2, nl - 1):
        slot(2, t)

    conv_s[...] = jnp.zeros_like(conv_s)
    for j in range(5):
        tap = jnp.sum(gcw_s[j], axis=0, keepdims=True)
        conv_s[j : j + 1, pl.ds(pl.multiple_of(s * W, 128), W)] = tap[:, 0:W]
        conv_s[j : j + 1, INNER:XBC] = tap[:, W:CH]
    gpre_s[5:6, :] = jnp.sum(gpre_s[...], axis=0, keepdims=True)
    post_s[...] = jnp.zeros_like(post_s)
    post_s[6:7, pl.ds(pl.multiple_of(s * W, 128), W)] = jnp.sum(gpost_s[...], axis=0, keepdims=True)
    channels = jnp.sum(gch_s[...], axis=0, keepdims=True)
    lane8 = lax.broadcasted_iota(jnp.int32, (8, 128), 1)
    row8 = lax.broadcasted_iota(jnp.int32, (8, 128), 0)
    skip = jnp.zeros((1, 128), F32)
    lane1 = lax.broadcasted_iota(jnp.int32, (1, 128), 1)
    for h in range(HL):
        at = slice(128 * (h // 2), 128 * (h // 2) + 128)
        half_of = (lane1 < HW) if h % 2 == 0 else (lane1 >= HW)
        skip = jnp.where(lane1 == h, jnp.sum(jnp.where(half_of, channels[:, at], 0.0), axis=1, keepdims=True), skip)
    heads = [
        pltpu.roll(jnp.where(row8 == 7, jnp.broadcast_to(v, (8, 128)), 0.0), s * HL, 1)
        for v in (ghd_s[0:1, :], ghd_s[1:2, :], skip)
    ]
    row512 = lax.broadcasted_iota(jnp.int32, (8, 512), 0)
    hn = HEADS // nf
    for i in range(nf):
        conv = unplace(conv_s, i * (XBC // nf), XBC // nf)
        block = jnp.where(row512 < 5, conv, 0.0)
        block = block + jnp.where(row512 == 5, unplace(gpre_s, i * (D // nf), D // nf), 0.0)
        block = block + unplace(post_s, i * (INNER // nf), INNER // nf)
        tiles = []
        for v in heads:
            moved = pltpu.roll(v, (128 - i * hn) % 128, 1) if i else v
            tiles.append(jnp.where(lane8 < hn, moved, 0.0))
        block = block + jnp.concatenate(tiles + [jnp.zeros((8, 128), F32)], axis=1)
        snd_s[i] = block

    def small_send(k):
        to = lax.rem(f + k, nf)
        return rcopy(snd_s.at[to], got_s.at[k], bms.at[k], bmr.at[k], {"fsdp": to})

    for k in range(1, nf):
        small_send(k).start()
    ends(4, range(nl - 1))
    for t in range(2, nl - 1):
        slot(3, t)
    dn_pass(1)
    dn_pass(0)
    close(2)
    close(3)
    for t in range(1, nl - 1):
        slot(4, t)
    relay(1)

    for a in range(2):
        seq_one(0, a, 1).wait_recv()
        seq_two(0, a).wait_recv()
        for k in range(rows // 128):
            one = stat_s[pl.ds(s * (rows // 128) + k, 1), :]
            rho = lax.rsqrt(jnp.sum(jnp.where(eye, one, 0.0), axis=1, keepdims=True) * (1.0 / INNER) + EPS)
            part = slice(128 * k, 128 * k + 128)
            at = pl.ds(a * rows + 128 * k, 128)
            x = cot_s[pl.ds(pl.multiple_of(s * rows + 128 * k, 128), 128), cols[a]].astype(F32)
            dsh_s[at, :] = x + rho * add(dsh_s[at, :], ab0[a, 1, part], az0[a, 1, part])
        result(0, a).start()

    total = snd_s[f]
    for k in range(1, nf):
        small_send(k).wait_recv()
        total = total + got_s[k]
    sown_s[...] = total

    def small_share(k):
        return rcopy(sown_s, sgot_s.at[s], bes.at[k], ber.at[k], {"seq": s ^ k})

    for k in range(1, SEQ):
        small_share(k).start()
    close(4)
    relay(2)
    relay(3)

    for a in range(2):
        seq_one(1, a, 1).wait_recv()
        seq_two(1, a).wait_recv()
        dsh_s[rows_of(1, a), :] = add(chunk(s, a)[...], ab1[a, 1], az1[a, 1])

    def grad_tokens(i, carry):
        x = cot_s[pl.ds(pl.multiple_of(s * rows + i * 64, 64), 64), :].astype(F32)
        rho = lax.rsqrt(jnp.sum(x * x, axis=1, keepdims=True) * (1.0 / D) + EPS)
        at = [pl.ds(pl.multiple_of((2 + a) * rows + i * 64, 64), 64) for a in range(2)]
        n0 = [x[:, cols[a]] * rho for a in range(2)]
        e0 = [dsh_s[at[a], :] * pre_s[5:6, cols[a]] for a in range(2)]
        dot = sum(jnp.sum(e0[a] * n0[a], axis=1, keepdims=True) for a in range(2))
        mean = dot * (1.0 / D)
        cot = cotrow_s[pl.ds(pl.multiple_of(i * 64, 64), 64), :].astype(F32)
        for a in range(2):
            dsh_s[at[a], :] = cot[:, cols[a]] + rho * (e0[a] - n0[a] * mean)
        return carry

    lax.fori_loop(0, rows // 64, grad_tokens, 0)
    for a in range(2):
        result(1, a).start()
    relay(4)

    for k in range(1, SEQ):
        small_share(k).wait()
    total = jnp.zeros_like(sown_s)
    for k in range(SEQ):
        total = total + jnp.where(s == k, sown_s[...], sgot_s[k])
    small_ref[...] = total
    for t in range(2):
        for a in range(2):
            result(t, a).wait()
    for k in range(1, nf):
        small_send(k).wait_send()
    seq_one_sent(1)
    for t in range(2):
        for a in range(2):
            seq_two(t, a).wait_send()
    for g in range(5):
        seq_gather_finish(g, owns[g], gouts[g], as_, ar, px, py, s)
        pltpu.make_async_copy(owns[g], gouts[g].at[pl.ds(s * n, n)], os_.at[g]).wait()
        line_sent(g)
    for g in range(1, 5):
        swaps_sent(g)


def mixer(nf, tok, cot, win, wout, small):
    shape = jax.ShapeDtypeStruct
    vm = pltpu.VMEM
    dma = pltpu.SemaphoreType.DMA
    rows = tok.shape[0]
    length = SEQ * rows
    nl = nf // 2
    n = D // nf
    widths = (W, W, W, VC - W)
    groups = (W, W, W // 2, W // 2, VC - W)
    boxes = [vm((nl, n, w), BF16) for w in groups] + [vm((nl + 1, n, w), BF16) for w in groups]
    boxes += [vm((n, w), BF16) for w in groups]
    return pl.pallas_call(
        functools.partial(mixer_kernel, nf),
        out_shape=[shape((rows, D), F32)] * 2
        + [shape((SEQ * n, w), BF16) for w in widths]
        + [shape((8, 512), F32), shape((length, D), BF16)],
        in_specs=[ANY] * 4 + [VMEM],
        out_specs=[ANY] * 6 + [VMEM, ANY],
        scratch_shapes=[
            vm((length, D), BF16),
            vm((length, D), BF16),
            vm((D, W), BF16),
            vm((nf, SEQ, n // SEQ, REST), BF16),
            vm((D, W), BF16),
            vm((D, W), BF16),
            vm((length, VC), BF16),
            vm((length, W), BF16),
            vm((length, W), BF16),
            vm((length // Q, STATE, W), BF16),
            vm((length, W), F32),
            vm((length, W), BF16),
            vm((length, VC), BF16),
            vm((rows, D), BF16),
            vm((length, D), BF16),
            vm((D, W), BF16),
            vm((D, VC - W), BF16),
        ]
        + boxes
        + [vm((2, 2, rows, D // 2), BF16)] * 4
        + [
            vm((8, CH), F32),
            vm((8, 128), F32),
            vm((8, W), F32),
            vm((8, D), F32),
            vm((2 * length // 128, 128), F32),
            vm((2 * length // 128, 128), F32),
            vm((SEQ, 2 * length // 128, 128), F32),
            vm((5, 8, CH), F32),
            vm((8, W), F32),
            vm((8, 128), F32),
            vm((8, W), F32),
            vm((8, D), F32),
            vm((8, XBC), F32),
            vm((8, INNER), F32),
            vm((nf, 8, 512), F32),
            vm((nf, 8, 512), F32),
            vm((8, 512), F32),
            vm((SEQ, 8, 512), F32),
            vm((Q + 8, CH), F32),
            vm((Q + 8, CH), F32),
            vm((STATE, W), F32),
            vm((128, Q), F32),
            vm((Q, W), BF16),
            vm((Q, W), BF16),
            vm((8, W), F32),
            dma((9,)),
            dma((3, 4)),
            dma((3, 4)),
            dma((GROUPS, 4, nl)),
            dma((GROUPS, nf)),
            dma((nf,)),
            dma((nf,)),
            dma((SEQ,)),
            dma((SEQ,)),
            dma((5, 3, nl)),
            dma((5, 3, nl)),
            dma((2, 2, 3)),
            dma((2, 2, 3)),
            dma((5, 4)),
            dma((5, 4)),
            dma((nf,)),
            dma((nf,)),
            dma((SEQ,)),
            dma((SEQ,)),
            dma((5,)),
        ],
        name="mixer",
        compiler_params=pltpu.CompilerParams(
            collective_id=1, has_side_effects=True, vmem_limit_bytes=67043328
        ),
    )(tok, cot, win, wout, small)


def finish_kernel(
    go, gg, gv, gs, out, gt, small, out_o, gt_o, gin_o, gout_o, cw_o, cb_o, pre_o, post_o, step_o, decay_o, skip_o
):
    out_o[...] = out[...]
    gt_o[...] = gt[...]
    for i in range(SEQ):
        gin_o[:, i * W : i * W + W] = gg[i].astype(F32)
        gin_o[:, INNER + i * W : INNER + i * W + W] = gv[i].astype(F32)
    total = gs[0].astype(F32)
    for i in range(1, SEQ):
        total = total + gs[i].astype(F32)
    rest = gin_o.shape[1] - 2 * INNER
    gin_o[:, 2 * INNER :] = total[:, :rest]
    for i in range(2):
        gout_o[:, i * W : i * W + W] = go[i].astype(F32)

    @pl.when(pl.program_id(0) == 0)
    def _():
        cw_o[...] = small[0:4, : cw_o.shape[1]]
        cb_o[...] = small[4:5, : cb_o.shape[1]]
        pre_o[...] = small[5:6, : pre_o.shape[1]]
        for k in range(post_o.shape[0]):
            post_o[k : k + 1, :] = small[6:7, 128 * k : 128 * k + post_o.shape[1]]
        heads = step_o.shape[1]
        step_o[...] = small[7:8, :heads]
        decay_o[...] = small[7:8, 128 : 128 + heads]
        skip_o[...] = small[7:8, 256 : 256 + heads]


def finish(nf, go, gg, gv, gs, out, gt, small):
    shape = jax.ShapeDtypeStruct
    n = D // nf
    steps = SEQ // 2
    step, rows = n // steps, out.shape[0] // steps
    proj = 2 * INNER + 2 * STATE + HEADS
    go, gg, gv, gs = (g.reshape(SEQ, n, g.shape[1]) for g in (go, gg, gv, gs))

    def whole(*dims):
        return pl.BlockSpec(dims, lambda i: (0,) * len(dims))

    np_ = INNER // nf
    post = (np_ // 128, 128) if np_ % 128 == 0 else (1, np_)
    tiny = [(4, XBC // nf), (1, XBC // nf), (1, n), post] + [(1, HEADS // nf)] * 3
    return pl.pallas_call(
        finish_kernel,
        grid=(steps,),
        out_shape=[shape(out.shape, F32)] * 2
        + [shape((n, proj), F32), shape((n, INNER), F32)]
        + [shape(dims, F32) for dims in tiny],
        in_specs=[
            pl.BlockSpec((2, n, W), lambda i: (i, 0, 0)),
            pl.BlockSpec((SEQ, step, W), lambda i: (0, i, 0)),
            pl.BlockSpec((SEQ, step, W), lambda i: (0, i, 0)),
            pl.BlockSpec((SEQ, step, VC - W), lambda i: (0, i, 0)),
            pl.BlockSpec((rows, D), lambda i: (i, 0)),
            pl.BlockSpec((rows, D), lambda i: (i, 0)),
            whole(8, 512),
        ],
        out_specs=[
            pl.BlockSpec((rows, D), lambda i: (i, 0)),
            pl.BlockSpec((rows, D), lambda i: (i, 0)),
            pl.BlockSpec((step, proj), lambda i: (i, 0)),
            pl.BlockSpec((n, 2 * W), lambda i: (0, i)),
        ]
        + [whole(*dims) for dims in tiny],
        name="finish",
        compiler_params=pltpu.CompilerParams(vmem_limit_bytes=VMEM_LIMIT),
    )(go, gg, gv, gs, out, gt, small)


def body(
    tokens,
    input_projection_weight,
    pre_gain,
    conv_weight,
    conv_bias,
    step_bias,
    decay_log,
    skip_gain,
    post_gain,
    output_projection_weight,
    cotangent,
):
    nf = lax.axis_size("fsdp")
    tok = tokens.reshape(tokens.shape[1:])
    cot = cotangent.reshape(cotangent.shape[1:])
    win = input_projection_weight

    w_out = output_projection_weight.T

    flat, at = jnp.zeros((2048,), F32), 0
    for v, size in (
        (conv_bias, 512), (pre_gain, 512), (post_gain, 512), (step_bias, 128), (decay_log, 128), (skip_gain, 256),
    ):
        flat = flat + jnp.pad(v.astype(F32), (at, 2048 - at - v.shape[0]))
        at += size
    taps = jnp.pad(conv_weight.T.astype(F32), ((0, 4), (0, 512 - conv_weight.shape[0])))
    small = taps + jnp.pad(flat.reshape(4, 512), ((4, 0), (0, 0)))
    out, gt, g_out, g_gate, g_val, g_state, small, _ = mixer(nf, tok, cot, win, w_out, small)
    block_out, grad_tokens, grad_in, grad_out, cw, cb, pre, post, step, decay, skip = finish(
        nf, g_out, g_gate, g_val, g_state, out, gt, small
    )
    return (
        block_out[None],
        grad_tokens[None],
        grad_in,
        pre.reshape(-1),
        cw.T,
        cb.reshape(-1),
        step.reshape(-1),
        decay.reshape(-1),
        skip.reshape(-1),
        post.reshape(-1),
        grad_out.T,
    )


def solution(mesh):
    in_specs = (
        P("fsdp", "seq", None),
        P("fsdp", None),
        P("fsdp"),
        P("fsdp", None),
        P("fsdp"),
        P("fsdp"),
        P("fsdp"),
        P("fsdp"),
        P("fsdp"),
        P(None, "fsdp"),
        P("fsdp", "seq", None),
    )
    out_specs = (
        P("fsdp", "seq", None),
        P("fsdp", "seq", None),
        P("fsdp", None),
        P("fsdp"),
        P("fsdp", None),
        P("fsdp"),
        P("fsdp"),
        P("fsdp"),
        P("fsdp"),
        P("fsdp"),
        P(None, "fsdp"),
    )
    return jax.shard_map(body, mesh=mesh, in_specs=in_specs, out_specs=out_specs, check_vma=False)
```
